32 devices in a mesh: rep: 4 (over z), seq: 8 (over y, x, core).
Axes of the slice: x: 2, y: 2, z: 4, core: 2. Of those that a mesh axis runs over, the one named last changes fastest.
Arguments:
- frames_in: bfloat16 [4, 8, 4, 128, 1152], P('rep', 'seq'), may hold values from -6 to 6
- conditioning: float32 [4, 1152], P('rep'), may hold values from -6 to 6
- mod_first: bfloat16 [1152, 6912], P('seq'), may hold values from -0.1875 to 0.1875
- qkv_first: bfloat16 [1152, 3456], P('seq'), may hold values from -0.1875 to 0.1875
- out_first: bfloat16 [1152, 1152], P('seq'), may hold values from -0.75 to 0.75
- up_first: bfloat16 [1152, 4608], P('seq'), may hold values from -0.1875 to 0.1875
- down_first: bfloat16 [4608, 1152], P('seq'), may hold values from -0.09375 to 0.09375
- mod_second: bfloat16 [1152, 6912], P('seq'), may hold values from -0.1875 to 0.1875
- qkv_second: bfloat16 [1152, 3456], P('seq'), may hold values from -0.1875 to 0.1875
- out_second: bfloat16 [1152, 1152], P('seq'), may hold values from -0.375 to 0.375
- up_second: bfloat16 [1152, 4608], P('seq'), may hold values from -0.1875 to 0.1875
- down_second: bfloat16 [4608, 1152], P('seq'), may hold values from -0.09375 to 0.09375
- cotangent: float32 [4, 8, 4, 128, 1152], P('rep', 'seq'), may hold values from -6 to 6
Outputs:
- block_out: float32 [4, 8, 4, 128, 1152], P('rep', 'seq')
- input_grad: float32 [4, 8, 4, 128, 1152], P('rep', 'seq')
- conditioning_grad: float32 [4, 1152], P('rep', 'seq')
- mod_first_grad: float32 [1152, 6912], P('seq')
- qkv_first_grad: float32 [1152, 3456], P('seq')
- out_first_grad: float32 [1152, 1152], P('seq')
- up_first_grad: float32 [1152, 4608], P('seq')
- first_down_gradient: float32 [4608, 1152], P('seq')
- mod_second_grad: float32 [1152, 6912], P('seq')
- qkv_second_grad: float32 [1152, 3456], P('seq')
- out_second_grad: float32 [1152, 1152], P('seq')
- up_second_grad: float32 [1152, 4608], P('seq')
- down_second_grad: float32 [4608, 1152], P('seq')
The draws below stay inside these ranges and needn't reach their ends.
All inputs are finite; a program needn't handle non-finite values.
Results may differ from the reference program's by a relative error of at most 0.02175.
Values may be sent and summed in bfloat16 or wider, within the bound.
A program may use at most 384 MiB of HBM per device.

```python
import jax
import jax.numpy as jnp
from jax import lax

D = 1152
HEADS = 16
HEAD_WIDTH = 72
FF = 4608
CLIPS = 4
PIECES = 8
FRAME_DEV = 4
HALF = 128


def block_scale(rng, extent, cuts, low, high):
    gain, own = 1.0, jax.random.fold_in(rng, 6)
    for axis_at, blocks in cuts:
        steps = jnp.exp(jax.random.uniform(jax.random.fold_in(own, axis_at), (blocks,), jnp.float32, low / len(cuts), high / len(cuts)))
        gain = gain * jnp.repeat(steps, extent[axis_at] // blocks).reshape([-1 if axis == axis_at else 1 for axis in range(len(extent))])
    return gain


def bell_draw(rng, dims, deviation, most, cuts=(), dtype=jnp.bfloat16):
    loudness = block_scale(rng, dims, cuts, -0.22, 0.18) if cuts else 1.0
    entries = jax.random.normal(rng, dims, jnp.float32) * deviation * loudness
    return jnp.minimum(jnp.maximum(entries, -most), most).astype(dtype)


def setup_inputs(seed: int = 0) -> dict:
    streams_of = jax.random.split(jax.random.key(seed), 14)
    return {
        "frames_in": bell_draw(streams_of[0], (CLIPS, PIECES, FRAME_DEV, HALF, D), 1.0, 6.0, ((0, 4), (1, 8))),
        "conditioning": bell_draw(streams_of[1], (CLIPS, D), 1.0, 6.0, ((0, 4),), jnp.float32),
        "mod_first": bell_draw(streams_of[2], (D, 6 * D), D ** -0.5, 0.1875, ((0, 8),)),
        "qkv_first": bell_draw(streams_of[3], (D, 3 * D), D ** -0.5, 0.1875, ((0, 8),)),
        "out_first": bell_draw(streams_of[4], (D, D), (D // 16) ** -0.5, 0.75, ((0, 8),)),
        "up_first": bell_draw(streams_of[5], (D, FF), D ** -0.5, 0.1875, ((0, 8),)),
        "down_first": bell_draw(streams_of[6], (FF, D), FF ** -0.5, 0.09375, ((0, 8),)),
        "mod_second": bell_draw(streams_of[7], (D, 6 * D), D ** -0.5, 0.1875, ((0, 8),)),
        "qkv_second": bell_draw(streams_of[8], (D, 3 * D), D ** -0.5, 0.1875, ((0, 8),)),
        "out_second": bell_draw(streams_of[9], (D, D), (D // 4) ** -0.5, 0.375, ((0, 8),)),
        "up_second": bell_draw(streams_of[10], (D, FF), D ** -0.5, 0.1875, ((0, 8),)),
        "down_second": bell_draw(streams_of[11], (FF, D), FF ** -0.5, 0.09375, ((0, 8),)),
        "cotangent": bell_draw(streams_of[12], (CLIPS, PIECES, FRAME_DEV, HALF, D), 1.0, 6.0, ((0, 4), (1, 8)), jnp.float32),
    }


@jax.custom_vjp
def low(v):
    return lax.optimization_barrier(v.astype(jnp.bfloat16)).astype(jnp.float32)

@jax.custom_vjp
def low_back(v):
    return v

def low_keep(v):
    return (low(v), None)

def low_pass(kept, grad):
    return (grad,)

def back_keep(v):
    return (v, None)

def back_low(kept, grad):
    return (low(grad),)
low.defvjp(low_keep, low_pass)
low_back.defvjp(back_keep, back_low)
norm_epsilon = 1e-06
highest_precision = lax.Precision.HIGHEST

def layer_mod(stream, shift_part, scale_part):
    row_mean = lax.optimization_barrier(jnp.mean(stream, axis=-1, keepdims=True))
    centred = stream - row_mean
    row_var = lax.optimization_barrier(jnp.mean(centred * centred, axis=-1, keepdims=True))
    return centred * lax.rsqrt(row_var + norm_epsilon) * (1.0 + scale_part) + shift_part

def project(left_operand, right_operand):
    return jnp.einsum('xhp,pb->xhb', left_operand, right_operand, precision=highest_precision)

def residual_block(stream, modulation, qkv_w, out_w, up_w, down_w):
    seq_count, seq_len, features = stream.shape
    shift_attn, scale_attn, gate_attn, shift_mlp, scale_mlp, gate_mlp = jnp.split(modulation, 6)
    normed = low(layer_mod(stream, shift_attn, scale_attn))
    projected = low(low_back(project(normed, qkv_w)))
    queries, keys_all, values_all = [component.reshape(seq_count, seq_len, HEADS, HEAD_WIDTH) for component in jnp.split(projected, 3, axis=-1)]
    scores = low_back(jnp.einsum('slhe,smhe->shlm', queries, keys_all, precision=highest_precision) * HEAD_WIDTH ** (-0.5))
    attention = low(jax.nn.softmax(scores, axis=-1))
    attended = low(low_back(jnp.einsum('shlm,smhe->slhe', attention, values_all, precision=highest_precision)))
    branch = low_back(project(attended.reshape(seq_count, seq_len, features), out_w))
    middle = stream + gate_attn * branch
    normed_mid = low(layer_mod(middle, shift_mlp, scale_mlp))
    hidden_pre = low_back(project(normed_mid, up_w))
    hidden = low(jax.nn.gelu(hidden_pre, approximate=True))
    return middle + gate_mlp * low_back(project(hidden, down_w))

def clip_forward(stream, condition, params):
    mod_one, qkv_one, out_one, up_one, down_one, mod_two, qkv_two, out_two, up_two, down_two = params
    silu_low = low(jax.nn.silu(condition))
    modulation_one = low_back(jnp.dot(silu_low, mod_one, precision=highest_precision))
    modulation_two = low_back(jnp.dot(silu_low, mod_two, precision=highest_precision))
    spatial = residual_block(stream, modulation_one, qkv_one, out_one, up_one, down_one)
    temporal = residual_block(jnp.transpose(spatial, (1, 0, 2)), modulation_two, qkv_two, out_two, up_two, down_two)
    return jnp.transpose(temporal, (1, 0, 2))

def to_natural(blocks):
    clip_count, pieces, frame_dev, half_places, features = blocks.shape
    arranged = blocks.reshape(clip_count, pieces // 2, 2, frame_dev, half_places, features)
    arranged = jnp.transpose(arranged, (0, 1, 3, 2, 4, 5))
    return arranged.reshape(clip_count, pieces // 2 * frame_dev, 2 * half_places, features)

def from_natural(natural, pieces, frame_dev):
    clip_count, frame_total, place_total, features = natural.shape
    arranged = natural.reshape(clip_count, pieces // 2, frame_dev, 2, place_total // 2, features)
    arranged = jnp.transpose(arranged, (0, 1, 3, 2, 4, 5))
    return arranged.reshape(clip_count, pieces, frame_dev, place_total // 2, features)

def reference(frames_in, conditioning, mod_first, qkv_first, out_first, up_first, down_first, mod_second, qkv_second, out_second, up_second, down_second, cotangent):
    params = tuple((weight.astype(jnp.float32) for weight in (mod_first, qkv_first, out_first, up_first, down_first, mod_second, qkv_second, out_second, up_second, down_second)))
    natural_in = to_natural(frames_in.astype(jnp.float32))
    natural_cot = to_natural(cotangent)

    def one_clip(totals, clip_item):
        stream, condition, cot_clip = clip_item
        result, pullback = jax.vjp(clip_forward, stream, condition, params)
        stream_grad, condition_grad, param_grads = pullback(cot_clip)
        return (jax.tree.map(jnp.add, totals, param_grads), (result, stream_grad, condition_grad))
    zero_grads = tuple((jnp.zeros_like(weight) for weight in params))
    totals, (results, stream_grads, condition_grads) = lax.scan(one_clip, zero_grads, (natural_in, conditioning, natural_cot))
    pieces = frames_in.shape[1]
    frame_dev = frames_in.shape[2]
    return (from_natural(results, pieces, frame_dev), from_natural(stream_grads, pieces, frame_dev), condition_grads, totals[0], totals[1], totals[2], totals[3], totals[4], totals[5], totals[6], totals[7], totals[8], totals[9])
```

```python
import jax
import jax.numpy as jnp
from jax import lax
from jax.sharding import PartitionSpec as P

HEADS = 16
HEAD_WIDTH = 72


norm_epsilon = 1e-06


def from_partner(block, axis, apart):
    count = lax.axis_size(axis)
    route = []
    for low in range(count):
        high = low | 1 << apart
        if high != low and high < count:
            route += [(low, high), (high, low)]
    return lax.ppermute(block, axis, route)


def shortened(x):
    return jax.tree.map(lambda a: a.astype(jnp.bfloat16) if a.dtype == jnp.float32 else a, x)


def layer_mod(stream, shift_part, scale_part):
    row_mean = jnp.mean(stream, axis=-1, keepdims=True)
    centred = stream - row_mean
    row_var = jnp.mean(centred * centred, axis=-1, keepdims=True)
    return centred * lax.rsqrt(row_var + norm_epsilon) * (1.0 + scale_part) + shift_part


def gelu_tanh(pre_value):
    return jax.nn.gelu(pre_value, approximate=True)


def project(left_operand, right_operand):
    return jnp.einsum(
        "csld,de->csle", left_operand, right_operand, preferred_element_type=jnp.float32
    )


def project_back(incoming, right_operand):
    return jnp.einsum("csle,de->csld", incoming, right_operand, preferred_element_type=jnp.float32)


def mod_parts(modulation):
    return [segment[:, None, None, :] for segment in jnp.split(modulation, 6, axis=-1)]


def modulations(conditioning, mod_one, mod_two):
    row_count = mod_one.shape[0]
    row_start = lax.axis_index("seq") * row_count
    silu_local = lax.dynamic_slice_in_dim(
        jax.nn.silu(conditioning), row_start, row_count, 1
    ).astype(jnp.bfloat16)
    part_one = jnp.dot(silu_local, mod_one, preferred_element_type=jnp.float32)
    part_two = jnp.dot(silu_local, mod_two, preferred_element_type=jnp.float32)
    summed = lax.psum((part_one, part_two), "seq")
    return (summed[0], summed[1], silu_local, row_start)


def gather_layer(qkv_w, out_w, up_w, down_w):
    return (
        lax.all_gather(qkv_w, "seq", axis=0, tiled=True),
        lax.all_gather(out_w, "seq", axis=0, tiled=True),
        lax.all_gather(up_w, "seq", axis=0, tiled=True),
        lax.all_gather(down_w, "seq", axis=0, tiled=True),
    )


def gather_layer_again(qkv_w, out_w, up_w, down_w):
    return (
        lax.all_gather(qkv_w, "seq", axis=0, tiled=True),
        lax.all_gather(out_w, "seq", axis=0, tiled=True),
        lax.all_gather(up_w, "seq", axis=0, tiled=True),
        lax.all_gather(down_w, "seq", axis=0, tiled=True),
    )


def partner_values(stacked):
    return from_partner(stacked, "seq", 0)


def partner_grads(stacked):
    return from_partner(stacked.astype(jnp.bfloat16), "seq", 0).astype(stacked.dtype)


def to_places(stream):
    clip_count, frame_dev, half_places, features = stream.shape
    devices = lax.axis_size("seq")
    place_part = half_places // devices
    exchanged = lax.all_to_all(
        stream.reshape(1, clip_count, frame_dev, devices, place_part, features).astype(
            jnp.bfloat16
        ),
        "seq",
        split_axis=3,
        concat_axis=0,
        tiled=True,
    ).astype(jnp.float32)
    exchanged = exchanged.reshape(devices // 2, 2, clip_count, frame_dev, place_part, features)
    exchanged = jnp.transpose(exchanged, (2, 1, 4, 0, 3, 5))
    return exchanged.reshape(clip_count, 2 * place_part, devices // 2 * frame_dev, features)


def to_frames(stream, frame_dev):
    clip_count, place_count, frame_total, features = stream.shape
    devices = lax.axis_size("seq")
    place_part = place_count // 2
    arranged = stream.reshape(clip_count, 2, place_part, devices // 2, frame_dev, features)
    arranged = jnp.transpose(arranged, (3, 1, 0, 4, 2, 5)).reshape(
        devices, clip_count, frame_dev, 1, place_part, features
    )
    exchanged = lax.all_to_all(
        shortened(arranged), "seq", split_axis=0, concat_axis=3, tiled=True
    ).astype(arranged.dtype)
    return exchanged.reshape(clip_count, frame_dev, devices * place_part, features)


def forward_layer(stream, modulation, weights, spatial):
    qkv_w, out_w, up_w, down_w = weights
    shift_attn, scale_attn, gate_attn, shift_mlp, scale_mlp, gate_mlp = mod_parts(modulation)
    clip_count, seq_count, seq_len, features = stream.shape
    normed = layer_mod(stream, shift_attn, scale_attn).astype(jnp.bfloat16)
    projected = project(normed, qkv_w).astype(jnp.bfloat16)
    queries, keys_all, values_all = jnp.split(projected, 3, axis=-1)
    if spatial:
        remote = partner_values(jnp.stack([keys_all, values_all]))
        keys_all = jnp.concatenate([keys_all, remote[0]], axis=2)
        values_all = jnp.concatenate([values_all, remote[1]], axis=2)
    key_len = keys_all.shape[2]
    queries = queries.reshape(clip_count, seq_count, seq_len, HEADS, HEAD_WIDTH)
    keys_all = keys_all.reshape(clip_count, seq_count, key_len, HEADS, HEAD_WIDTH)
    values_all = values_all.reshape(clip_count, seq_count, key_len, HEADS, HEAD_WIDTH)
    scores = jnp.einsum(
        "cslhe,csmhe->cshlm", queries, keys_all, preferred_element_type=jnp.float32
    ) * HEAD_WIDTH ** (-0.5)
    peak_score = jnp.max(scores, axis=-1, keepdims=True)
    scaled_exp = jnp.exp(scores - peak_score)
    attention = scaled_exp / jnp.sum(scaled_exp, axis=-1, keepdims=True)
    attention_low = attention.astype(jnp.bfloat16)
    attended = jnp.einsum(
        "cshlm,csmhe->cslhe", attention_low, values_all, preferred_element_type=jnp.float32
    )
    attended = attended.astype(jnp.bfloat16).reshape(clip_count, seq_count, seq_len, features)
    branch = project(attended, out_w)
    middle = stream + gate_attn * branch
    normed_mid = layer_mod(middle, shift_mlp, scale_mlp).astype(jnp.bfloat16)
    hidden_pre = project(normed_mid, up_w)
    hidden = gelu_tanh(hidden_pre).astype(jnp.bfloat16)
    mlp_out = project(hidden, down_w)
    result = middle + gate_mlp * mlp_out
    kept_state = (
        normed,
        queries,
        keys_all,
        values_all,
        attention,
        attention_low,
        attended,
        branch,
        middle,
        normed_mid,
        hidden_pre,
        hidden,
        mlp_out,
    )
    return (result, kept_state)


def backward_layer(result_grad, stream, modulation, weights, kept_state, spatial):
    qkv_w, out_w, up_w, down_w = weights
    (
        normed,
        queries,
        keys_all,
        values_all,
        attention,
        attention_low,
        attended,
        branch,
        middle,
        normed_mid,
        hidden_pre,
        hidden,
        mlp_out,
    ) = kept_state
    shift_attn, scale_attn, gate_attn, shift_mlp, scale_mlp, gate_mlp = mod_parts(modulation)
    clip_count, seq_count, seq_len, features = stream.shape
    gate_mlp_grad = jnp.sum(result_grad * mlp_out, axis=(1, 2))
    mlp_grad = (gate_mlp * result_grad).astype(jnp.bfloat16)
    hidden_grad = project_back(mlp_grad, down_w)
    pre_grad = jax.vjp(gelu_tanh, hidden_pre)[1](hidden_grad)[0].astype(jnp.bfloat16)
    normed_mid_grad = project_back(pre_grad, up_w)
    middle_ln_grad, shift_mlp_grad, scale_mlp_grad = jax.vjp(
        layer_mod, middle, shift_mlp, scale_mlp
    )[1](normed_mid_grad)
    middle_grad = result_grad + middle_ln_grad
    gate_attn_grad = jnp.sum(middle_grad * branch, axis=(1, 2))
    branch_grad = (gate_attn * middle_grad).astype(jnp.bfloat16)
    attended_grad = project_back(branch_grad, out_w).astype(jnp.bfloat16)
    attended_grad = attended_grad.reshape(clip_count, seq_count, seq_len, HEADS, HEAD_WIDTH)
    attention_grad = jnp.einsum(
        "cslhe,csmhe->cshlm", attended_grad, values_all, preferred_element_type=jnp.float32
    )
    scores_grad = attention * (
        attention_grad - jnp.sum(attention_grad * attention, axis=-1, keepdims=True)
    )
    scores_grad = scores_grad.astype(jnp.bfloat16)
    inv_root = HEAD_WIDTH ** (-0.5)
    queries_grad = (
        jnp.einsum("cshlm,csmhe->cslhe", scores_grad, keys_all, preferred_element_type=jnp.float32)
        * inv_root
    )
    keys_grad = (
        jnp.einsum("cshlm,cslhe->csmhe", scores_grad, queries, preferred_element_type=jnp.float32)
        * inv_root
    )
    values_grad = jnp.einsum(
        "cshlm,cslhe->csmhe", attention_low, attended_grad, preferred_element_type=jnp.float32
    )
    if spatial:
        returned = partner_grads(
            jnp.stack([keys_grad[:, :, seq_len:], values_grad[:, :, seq_len:]])
        )
        keys_grad = keys_grad[:, :, :seq_len] + returned[0]
        values_grad = values_grad[:, :, :seq_len] + returned[1]
    qkv_grad = jnp.concatenate(
        [
            component.reshape(clip_count, seq_count, seq_len, features)
            for component in (queries_grad, keys_grad, values_grad)
        ],
        axis=-1,
    )
    qkv_grad = qkv_grad.astype(jnp.bfloat16)
    normed_grad = project_back(qkv_grad, qkv_w)
    stream_ln_grad, attention_shift_gradient, scale_attn_grad = jax.vjp(
        layer_mod, stream, shift_attn, scale_attn
    )[1](normed_grad)
    stream_grad = middle_grad + stream_ln_grad
    mod_grad = jnp.concatenate(
        [
            attention_shift_gradient.reshape(clip_count, features),
            scale_attn_grad.reshape(clip_count, features),
            gate_attn_grad,
            shift_mlp_grad.reshape(clip_count, features),
            scale_mlp_grad.reshape(clip_count, features),
            gate_mlp_grad,
        ],
        axis=-1,
    )
    grad_pairs = (
        (normed, qkv_grad),
        (attended, branch_grad),
        (normed_mid, pre_grad),
        (hidden, mlp_grad),
    )
    return (stream_grad, mod_grad, grad_pairs)


def bit_count(axis):
    return lax.axis_size(axis).bit_length() - 1


def swap(block, axis, bit):
    count = lax.axis_size(axis)
    return lax.ppermute(block, axis, [(at, at ^ (1 << bit)) for at in range(count)])


def bit_of(axis, bit):
    return (lax.axis_index(axis) >> bit) & 1


def pick(block, which, axis):
    return lax.dynamic_index_in_dim(block, which, axis, keepdims=False)


def spread_rows_out(left_turned, right_operand, flipped):
    bits = bit_count("seq")
    total_rows, tokens = left_turned.shape
    rows = total_rows >> bits
    halves = left_turned.reshape(1 << (bits - 1), 2, rows, tokens)
    core = bit_of("seq", 0)

    def product(which):
        left = pick(halves, which, 1).reshape(-1, tokens)
        return jnp.dot(left, right_operand, preferred_element_type=jnp.float32).astype(
            jnp.bfloat16
        )

    arrived = swap(product(1 - core), "seq", 0)
    held = product(core)
    left_bits = list(range(bits - 1, 0, -1))
    shape = [2] * (bits - 1) + [rows, right_operand.shape[1]]
    held = held.reshape(shape)
    arrived = arrived.reshape(shape)
    order = list(left_bits) if flipped else left_bits[::-1]
    for bit in order:
        at = left_bits.index(bit)
        mine = bit_of("seq", bit)
        away = pick(held, 1 - mine, at).astype(jnp.float32) + pick(arrived, 1 - mine, at)
        kept = pick(held, mine, at).astype(jnp.float32) + pick(arrived, mine, at)
        arrived = swap(away.astype(jnp.bfloat16), "seq", bit)
        held = kept.astype(jnp.bfloat16)
        left_bits.remove(bit)
    return held.astype(jnp.float32) + arrived


def rep_sum(block, axis):
    bits = bit_count("rep")
    held = block.astype(jnp.bfloat16)
    for bit in range(bits):
        mine = bit_of("rep", bit)
        low, high = jnp.split(held, 2, axis)
        away = jnp.where(mine == 0, high, low)
        kept = jnp.where(mine == 0, low, high)
        held = (kept.astype(jnp.float32) + swap(away, "rep", bit)).astype(jnp.bfloat16)
    for bit in reversed(range(bits)):
        mine = bit_of("rep", bit)
        other = swap(held, "rep", bit)
        low = jnp.where(mine == 0, held, other)
        high = jnp.where(mine == 0, other, held)
        held = jnp.concatenate([low, high], axis)
    return held.astype(jnp.float32)


def turned(operand):
    return operand.reshape(-1, operand.shape[-1]).T


def flat(operand):
    return operand.reshape(-1, operand.shape[-1])


def cut(width, parts, of):
    return width * parts // of // 128 * 128


def down_grad(pair):
    left, right = turned(pair[0]), flat(pair[1])
    edge = cut(right.shape[1], 5, 9)
    return jnp.concatenate(
        [
            rep_sum(spread_rows_out(left, right[:, :edge], False), 0),
            rep_sum(spread_rows_out(left, right[:, edge:], True), 0),
        ],
        1,
    )


def up_grad(pair):
    left, right = turned(pair[0]), flat(pair[1])
    edge = cut(right.shape[1], 4, 9)
    return jnp.concatenate(
        [
            rep_sum(spread_rows_out(left, right[:, :edge], False), 1),
            rep_sum(spread_rows_out(left, right[:, edge:], True), 1),
        ],
        1,
    )


def attention_grads(qkv_pair, out_pair):
    left, right = turned(qkv_pair[0]), flat(qkv_pair[1])
    width = right.shape[1]
    edge = cut(width, 16, 27)
    first = rep_sum(spread_rows_out(left, right[:, :edge], False), 1)
    second = spread_rows_out(left, right[:, edge:], True)
    third = spread_rows_out(turned(out_pair[0]), flat(out_pair[1]), True)
    joined = rep_sum(jnp.concatenate([second, third], 1), 1)
    return (
        jnp.concatenate([first, joined[:, : width - edge]], 1),
        joined[:, width - edge :],
    )


def layer_grads(grad_pairs):
    qkv_pair, out_pair, up_pair, down_pair = grad_pairs
    down = down_grad(down_pair)
    up = up_grad(up_pair)
    qkv, out = attention_grads(qkv_pair, out_pair)
    return (qkv, out, up, down)


def seq_sum(block):
    for bit in range(bit_count("seq")):
        block = block + swap(block, "seq", bit)
    return block


def per_device(
    frames_in,
    conditioning,
    mod_first,
    qkv_first,
    out_first,
    up_first,
    down_first,
    mod_second,
    qkv_second,
    out_second,
    up_second,
    down_second,
    cotangent,
):
    clip_count = frames_in.shape[0]
    frame_dev = frames_in.shape[2]
    half_places = frames_in.shape[3]
    features = frames_in.shape[4]
    start_stream = frames_in.reshape(clip_count, frame_dev, half_places, features).astype(
        jnp.float32
    )
    mod_one, mod_two, silu_local, row_start = modulations(conditioning, mod_first, mod_second)
    weights_one = gather_layer(qkv_first, out_first, up_first, down_first)
    spatial_out, unused_one = forward_layer(start_stream, mod_one, weights_one, True)
    weights_two = gather_layer(qkv_second, out_second, up_second, down_second)
    temporal_out, unused_two = forward_layer(to_places(spatial_out), mod_two, weights_two, False)
    block_out = to_frames(temporal_out, frame_dev)
    mod_one, mod_two, silu_local, row_start = modulations(conditioning, mod_first, mod_second)
    again_one = gather_layer_again(qkv_first, out_first, up_first, down_first)
    spatial_again, state_one = forward_layer(start_stream, mod_one, again_one, True)
    again_two = gather_layer_again(qkv_second, out_second, up_second, down_second)
    placed_again = to_places(spatial_again)
    unused_three, state_two = forward_layer(placed_again, mod_two, again_two, False)
    cotangent_sites = to_places(cotangent.reshape(clip_count, frame_dev, half_places, features))
    placed_grad, mod_grad_two, pairs_two = backward_layer(
        cotangent_sites, placed_again, mod_two, again_two, state_two, False
    )
    row_attn = qkv_first.shape[0]
    grads_two = layer_grads(pairs_two)
    spatial_grad = to_frames(placed_grad, frame_dev)
    stream_grad, mod_grad_one, pairs_one = backward_layer(
        spatial_grad, start_stream, mod_one, again_one, state_one, True
    )
    grads_one = layer_grads(pairs_one)
    mod_total = lax.psum(
        jnp.concatenate([mod_grad_one, mod_grad_two], 1).astype(jnp.bfloat16), "seq"
    ).astype(jnp.bfloat16)
    mod_width = mod_grad_one.shape[1]
    low_one, low_two = mod_total[:, :mod_width], mod_total[:, mod_width:]
    every_mod = lax.all_gather(mod_total, "rep", axis=0, tiled=True)
    every_silu = lax.all_gather(silu_local, "rep", axis=0, tiled=True)
    mod_weights = jnp.einsum(
        "cd,ce->de", every_silu, every_mod, preferred_element_type=jnp.float32
    )
    silu_grad = jnp.einsum("ce,de->cd", low_one, mod_first, preferred_element_type=jnp.float32)
    silu_grad = silu_grad + jnp.einsum(
        "ce,de->cd", low_two, mod_second, preferred_element_type=jnp.float32
    )
    condition_local = lax.dynamic_slice_in_dim(conditioning, row_start, row_attn, 1)
    condition_grad = jax.vjp(jax.nn.silu, condition_local)[1](silu_grad)[0]
    summed = (
        (mod_weights[:, :mod_width],)
        + tuple(grads_one)
        + (mod_weights[:, mod_width:],)
        + tuple(grads_two)
    )
    out_shape = (clip_count, 1, frame_dev, half_places, features)
    return (
        block_out.reshape(out_shape),
        stream_grad.reshape(out_shape),
        condition_grad,
        summed[0],
        summed[1],
        summed[2],
        summed[3],
        summed[4],
        summed[5],
        summed[6],
        summed[7],
        summed[8],
        summed[9],
    )


def solution(mesh):
    return jax.shard_map(
        per_device,
        mesh=mesh,
        in_specs=(
            P("rep", "seq", None, None, None),
            P("rep", None),
            P("seq", None),
            P("seq", None),
            P("seq", None),
            P("seq", None),
            P("seq", None),
            P("seq", None),
            P("seq", None),
            P("seq", None),
            P("seq", None),
            P("seq", None),
            P("rep", "seq", None, None, None),
        ),
        out_specs=(
            P("rep", "seq", None, None, None),
            P("rep", "seq", None, None, None),
            P("rep", "seq"),
            P("seq", None),
            P("seq", None),
            P("seq", None),
            P("seq", None),
            P("seq", None),
            P("seq", None),
            P("seq", None),
            P("seq", None),
            P("seq", None),
            P("seq", None),
        ),
        check_vma=False,
    )
```

```python
import functools

import jax
import jax.numpy as jnp
from jax import lax
from jax.experimental import pallas as pl
from jax.experimental.pallas import tpu as pltpu
from jax.sharding import PartitionSpec as P

HEADS = 16
HEAD_WIDTH = 72


norm_epsilon = 1e-06


def from_partner(block, axis, apart):
    count = lax.axis_size(axis)
    route = []
    for low in range(count):
        high = low | 1 << apart
        if high != low and high < count:
            route += [(low, high), (high, low)]
    return lax.ppermute(block, axis, route)


def shortened(x):
    return jax.tree.map(lambda a: a.astype(jnp.bfloat16) if a.dtype == jnp.float32 else a, x)


def layer_mod(stream, shift_part, scale_part):
    row_mean = jnp.mean(stream, axis=-1, keepdims=True)
    centred = stream - row_mean
    row_var = jnp.mean(centred * centred, axis=-1, keepdims=True)
    return centred * lax.rsqrt(row_var + norm_epsilon) * (1.0 + scale_part) + shift_part


def gelu_tanh(pre_value):
    return jax.nn.gelu(pre_value, approximate=True)


def project(left_operand, right_operand):
    return jnp.einsum(
        "csld,de->csle", left_operand, right_operand, preferred_element_type=jnp.float32
    )


def project_back(incoming, right_operand):
    return jnp.einsum("csle,de->csld", incoming, right_operand, preferred_element_type=jnp.float32)


def mod_parts(modulation):
    return [segment[:, None, None, :] for segment in jnp.split(modulation, 6, axis=-1)]


def partner_values(stacked):
    return from_partner(stacked, "seq", 0)


def partner_grads(stacked):
    return from_partner(stacked.astype(jnp.bfloat16), "seq", 0).astype(stacked.dtype)


def to_places(stream):
    clip_count, frame_dev, half_places, features = stream.shape
    devices = lax.axis_size("seq")
    place_part = half_places // devices
    exchanged = lax.all_to_all(
        stream.reshape(1, clip_count, frame_dev, devices, place_part, features).astype(
            jnp.bfloat16
        ),
        "seq",
        split_axis=3,
        concat_axis=0,
        tiled=True,
    ).astype(jnp.float32)
    exchanged = exchanged.reshape(devices // 2, 2, clip_count, frame_dev, place_part, features)
    exchanged = jnp.transpose(exchanged, (2, 1, 4, 0, 3, 5))
    return exchanged.reshape(clip_count, 2 * place_part, devices // 2 * frame_dev, features)


def to_frames(stream, frame_dev):
    clip_count, place_count, frame_total, features = stream.shape
    devices = lax.axis_size("seq")
    place_part = place_count // 2
    arranged = stream.reshape(clip_count, 2, place_part, devices // 2, frame_dev, features)
    arranged = jnp.transpose(arranged, (3, 1, 0, 4, 2, 5)).reshape(
        devices, clip_count, frame_dev, 1, place_part, features
    )
    exchanged = lax.all_to_all(
        shortened(arranged), "seq", split_axis=0, concat_axis=3, tiled=True
    ).astype(arranged.dtype)
    return exchanged.reshape(clip_count, frame_dev, devices * place_part, features)


def forward_layer(stream, modulation, weights, spatial):
    qkv_w, out_w, up_w, down_w = weights
    shift_attn, scale_attn, gate_attn, shift_mlp, scale_mlp, gate_mlp = mod_parts(modulation)
    clip_count, seq_count, seq_len, features = stream.shape
    normed = layer_mod(stream, shift_attn, scale_attn).astype(jnp.bfloat16)
    projected = project(normed, qkv_w).astype(jnp.bfloat16)
    queries, keys_all, values_all = jnp.split(projected, 3, axis=-1)
    if spatial:
        remote = partner_values(jnp.stack([keys_all, values_all]))
        keys_all = jnp.concatenate([keys_all, remote[0]], axis=2)
        values_all = jnp.concatenate([values_all, remote[1]], axis=2)
    key_len = keys_all.shape[2]
    queries = queries.reshape(clip_count, seq_count, seq_len, HEADS, HEAD_WIDTH)
    keys_all = keys_all.reshape(clip_count, seq_count, key_len, HEADS, HEAD_WIDTH)
    values_all = values_all.reshape(clip_count, seq_count, key_len, HEADS, HEAD_WIDTH)
    scores = jnp.einsum(
        "cslhe,csmhe->cshlm", queries, keys_all, preferred_element_type=jnp.float32
    ) * HEAD_WIDTH ** (-0.5)
    peak_score = jnp.max(scores, axis=-1, keepdims=True)
    scaled_exp = jnp.exp(scores - peak_score)
    attention = scaled_exp / jnp.sum(scaled_exp, axis=-1, keepdims=True)
    attention_low = attention.astype(jnp.bfloat16)
    attended = jnp.einsum(
        "cshlm,csmhe->cslhe", attention_low, values_all, preferred_element_type=jnp.float32
    )
    attended = attended.astype(jnp.bfloat16).reshape(clip_count, seq_count, seq_len, features)
    branch = project(attended, out_w)
    middle = stream + gate_attn * branch
    normed_mid = layer_mod(middle, shift_mlp, scale_mlp).astype(jnp.bfloat16)
    hidden_pre = project(normed_mid, up_w)
    hidden = gelu_tanh(hidden_pre).astype(jnp.bfloat16)
    mlp_out = project(hidden, down_w)
    result = middle + gate_mlp * mlp_out
    kept_state = (
        normed,
        queries,
        keys_all,
        values_all,
        attention,
        attention_low,
        attended,
        branch,
        middle,
        normed_mid,
        hidden_pre,
        hidden,
        mlp_out,
    )
    return (result, kept_state)


def backward_layer(result_grad, stream, modulation, weights, kept_state, spatial):
    qkv_w, out_w, up_w, down_w = weights
    (
        normed,
        queries,
        keys_all,
        values_all,
        attention,
        attention_low,
        attended,
        branch,
        middle,
        normed_mid,
        hidden_pre,
        hidden,
        mlp_out,
    ) = kept_state
    shift_attn, scale_attn, gate_attn, shift_mlp, scale_mlp, gate_mlp = mod_parts(modulation)
    clip_count, seq_count, seq_len, features = stream.shape
    gate_mlp_grad = jnp.sum(result_grad * mlp_out, axis=(1, 2))
    mlp_grad = (gate_mlp * result_grad).astype(jnp.bfloat16)
    hidden_grad = project_back(mlp_grad, down_w)
    pre_grad = jax.vjp(gelu_tanh, hidden_pre)[1](hidden_grad)[0].astype(jnp.bfloat16)
    normed_mid_grad = project_back(pre_grad, up_w)
    middle_ln_grad, shift_mlp_grad, scale_mlp_grad = jax.vjp(
        layer_mod, middle, shift_mlp, scale_mlp
    )[1](normed_mid_grad)
    middle_grad = result_grad + middle_ln_grad
    gate_attn_grad = jnp.sum(middle_grad * branch, axis=(1, 2))
    branch_grad = (gate_attn * middle_grad).astype(jnp.bfloat16)
    attended_grad = project_back(branch_grad, out_w).astype(jnp.bfloat16)
    attended_grad = attended_grad.reshape(clip_count, seq_count, seq_len, HEADS, HEAD_WIDTH)
    attention_grad = jnp.einsum(
        "cslhe,csmhe->cshlm", attended_grad, values_all, preferred_element_type=jnp.float32
    )
    scores_grad = attention * (
        attention_grad - jnp.sum(attention_grad * attention, axis=-1, keepdims=True)
    )
    scores_grad = scores_grad.astype(jnp.bfloat16)
    inv_root = HEAD_WIDTH ** (-0.5)
    queries_grad = (
        jnp.einsum("cshlm,csmhe->cslhe", scores_grad, keys_all, preferred_element_type=jnp.float32)
        * inv_root
    )
    keys_grad = (
        jnp.einsum("cshlm,cslhe->csmhe", scores_grad, queries, preferred_element_type=jnp.float32)
        * inv_root
    )
    values_grad = jnp.einsum(
        "cshlm,cslhe->csmhe", attention_low, attended_grad, preferred_element_type=jnp.float32
    )
    if spatial:
        returned = partner_grads(
            jnp.stack([keys_grad[:, :, seq_len:], values_grad[:, :, seq_len:]])
        )
        keys_grad = keys_grad[:, :, :seq_len] + returned[0]
        values_grad = values_grad[:, :, :seq_len] + returned[1]
    qkv_grad = jnp.concatenate(
        [
            component.reshape(clip_count, seq_count, seq_len, features)
            for component in (queries_grad, keys_grad, values_grad)
        ],
        axis=-1,
    )
    qkv_grad = qkv_grad.astype(jnp.bfloat16)
    normed_grad = project_back(qkv_grad, qkv_w)
    stream_ln_grad, attention_shift_gradient, scale_attn_grad = jax.vjp(
        layer_mod, stream, shift_attn, scale_attn
    )[1](normed_grad)
    stream_grad = middle_grad + stream_ln_grad
    mod_grad = jnp.concatenate(
        [
            attention_shift_gradient.reshape(clip_count, features),
            scale_attn_grad.reshape(clip_count, features),
            gate_attn_grad,
            shift_mlp_grad.reshape(clip_count, features),
            scale_mlp_grad.reshape(clip_count, features),
            gate_mlp_grad,
        ],
        axis=-1,
    )
    grad_pairs = (
        (normed, qkv_grad),
        (attended, branch_grad),
        (normed_mid, pre_grad),
        (hidden, mlp_grad),
    )
    return (stream_grad, mod_grad, grad_pairs)


def bit_count(axis):
    return lax.axis_size(axis).bit_length() - 1


def swap(block, axis, bit):
    count = lax.axis_size(axis)
    return lax.ppermute(block, axis, [(at, at ^ (1 << bit)) for at in range(count)])


def bit_of(axis, bit):
    return (lax.axis_index(axis) >> bit) & 1


def pick(block, which, axis):
    return lax.dynamic_index_in_dim(block, which, axis, keepdims=False)


def spread_rows_out(left_turned, right_operand, flipped):
    bits = bit_count("seq")
    total_rows, tokens = left_turned.shape
    rows = total_rows >> bits
    halves = left_turned.reshape(1 << (bits - 1), 2, rows, tokens)
    core = bit_of("seq", 0)

    def product(which):
        left = pick(halves, which, 1).reshape(-1, tokens)
        return jnp.dot(left, right_operand, preferred_element_type=jnp.float32).astype(
            jnp.bfloat16
        )

    arrived = swap(product(1 - core), "seq", 0)
    held = product(core)
    left_bits = list(range(bits - 1, 0, -1))
    shape = [2] * (bits - 1) + [rows, right_operand.shape[1]]
    held = held.reshape(shape)
    arrived = arrived.reshape(shape)
    order = list(left_bits) if flipped else left_bits[::-1]
    for bit in order:
        at = left_bits.index(bit)
        mine = bit_of("seq", bit)
        away = pick(held, 1 - mine, at).astype(jnp.float32) + pick(arrived, 1 - mine, at)
        kept = pick(held, mine, at).astype(jnp.float32) + pick(arrived, mine, at)
        arrived = swap(away.astype(jnp.bfloat16), "seq", bit)
        held = kept.astype(jnp.bfloat16)
        left_bits.remove(bit)
    return held.astype(jnp.float32) + arrived


def rep_sum(block, axis):
    bits = bit_count("rep")
    held = block.astype(jnp.bfloat16)
    for bit in range(bits):
        mine = bit_of("rep", bit)
        low, high = jnp.split(held, 2, axis)
        away = jnp.where(mine == 0, high, low)
        kept = jnp.where(mine == 0, low, high)
        held = (kept.astype(jnp.float32) + swap(away, "rep", bit)).astype(jnp.bfloat16)
    for bit in reversed(range(bits)):
        mine = bit_of("rep", bit)
        other = swap(held, "rep", bit)
        low = jnp.where(mine == 0, held, other)
        high = jnp.where(mine == 0, other, held)
        held = jnp.concatenate([low, high], axis)
    return held.astype(jnp.float32)


def turned(operand):
    return operand.reshape(-1, operand.shape[-1]).T


def flat(operand):
    return operand.reshape(-1, operand.shape[-1])


def cut(width, parts, of):
    return width * parts // of // 128 * 128


def down_grad(pair):
    left, right = turned(pair[0]), flat(pair[1])
    edge = cut(right.shape[1], 5, 9)
    return jnp.concatenate(
        [
            rep_sum(spread_rows_out(left, right[:, :edge], False), 0),
            rep_sum(spread_rows_out(left, right[:, edge:], True), 0),
        ],
        1,
    )


def up_grad(pair):
    left, right = turned(pair[0]), flat(pair[1])
    edge = cut(right.shape[1], 4, 9)
    return jnp.concatenate(
        [
            rep_sum(spread_rows_out(left, right[:, :edge], False), 1),
            rep_sum(spread_rows_out(left, right[:, edge:], True), 1),
        ],
        1,
    )


def attention_grads(qkv_pair, out_pair):
    left, right = turned(qkv_pair[0]), flat(qkv_pair[1])
    width = right.shape[1]
    edge = cut(width, 16, 27)
    first = rep_sum(spread_rows_out(left, right[:, :edge], False), 1)
    second = spread_rows_out(left, right[:, edge:], True)
    third = spread_rows_out(turned(out_pair[0]), flat(out_pair[1]), True)
    joined = rep_sum(jnp.concatenate([second, third], 1), 1)
    return (
        jnp.concatenate([first, joined[:, : width - edge]], 1),
        joined[:, width - edge :],
    )


def layer_grads(grad_pairs):
    qkv_pair, out_pair, up_pair, down_pair = grad_pairs
    down = down_grad(down_pair)
    up = up_grad(up_pair)
    qkv, out = attention_grads(qkv_pair, out_pair)
    return (qkv, out, up, down)


AHEAD = 2


def gather_pieces(shapes):
    pieces = []
    for at, (rows, columns) in enumerate(shapes):
        last = at == len(shapes) - 1
        if rows > columns // 3:
            parts = 4 if last else 2
            tall = rows // parts
            pieces += [(at, j * tall, tall, 0, columns) for j in range(parts)]
        elif columns % 256 == 0 and columns > 2048:
            wide = columns // 2
            pieces += [(at, 0, rows, j * wide, wide) for j in range(2)]
        else:
            pieces.append((at, 0, rows, 0, columns))
    return pieces


def gather_kernel(pieces, count, *refs):
    shards, partial, condition = refs[:count], refs[count], refs[count + 1]
    fulls = refs[count + 2 : 2 * count + 2]
    partials, conditions = refs[2 * count + 2 : 2 * count + 4]
    held = refs[2 * count + 4 : 3 * count + 4]
    first_sem, second_sem, rep_sem, pair_sem, local_sem, small_sem = refs[3 * count + 4 :]
    me, z = lax.axis_index("seq"), lax.axis_index("rep")
    odd = z & 1
    first, second = 2 + 2 * odd, 4 - 2 * odd

    barrier = pltpu.get_barrier_semaphore()
    for mask in range(1, 8):
        pl.semaphore_signal(barrier, inc=1, device_id={"seq": me ^ mask})
    for mask in range(1, 4):
        pl.semaphore_signal(barrier, inc=1, device_id={"rep": z ^ mask})
    pl.semaphore_wait(barrier, 10)

    small = []
    for mask in range(1, 8):
        small.append(pltpu.make_async_remote_copy(
            partial, partials.at[me], small_sem.at[0, mask], small_sem.at[1, mask],
            device_id={"seq": me ^ mask}))
    for mask in range(1, 4):
        small.append(pltpu.make_async_remote_copy(
            condition, conditions.at[z], small_sem.at[0, 7 + mask], small_sem.at[1, 7 + mask],
            device_id={"rep": z ^ mask}))
    small.append(pltpu.make_async_copy(partial, partials.at[me], small_sem.at[0, 0]))
    small.append(pltpu.make_async_copy(condition, conditions.at[z], small_sem.at[1, 0]))
    for copy in small:
        copy.start()

    def place(owner, piece):
        at, row, rows, column, columns = piece
        return fulls[at].at[owner, pl.ds(row, rows), pl.ds(column, columns)]

    def own(piece):
        at, row, rows, column, columns = piece
        return shards[at].at[pl.ds(row, rows), pl.ds(column, columns)]

    def send(source, owner, piece, sems, at, target):
        return pltpu.make_async_remote_copy(
            source, place(owner, piece), sems.at[0, at], sems.at[1, at], device_id=target)

    firsts, pairs, others, stores = [], [], [], []
    fetches = [
        pltpu.make_async_copy(shard, hold, local_sem.at[0, at])
        for at, (shard, hold) in enumerate(zip(shards, held))
    ]
    for copy in fetches:
        copy.start()

    def begin(at):
        piece = pieces[at]
        copy = send(own(piece), me, piece, first_sem, at, {"seq": me ^ first})
        copy.start()
        firsts.append(copy)
        copy = send(own(piece), me, piece, pair_sem.at[0], at, {"seq": me ^ 1})
        copy.start()
        pairs.append(copy)

    for at in range(AHEAD):
        begin(at)
    for at, copy in enumerate(fetches):
        copy.wait()
        stores.append(pltpu.make_async_copy(held[at], fulls[at].at[me], local_sem.at[1, at]))
        stores[-1].start()

    def forward(at):
        others[at][0].wait_recv()
        others[at][1].wait_recv()
        piece = pieces[at]
        for which, mask in ((2, first ^ second), (3, second)):
            owner = me ^ mask
            copy = send(place(owner, piece), owner, piece, pair_sem.at[which], at, {"seq": me ^ 1})
            copy.start()
            pairs.append(copy)

    for at, piece in enumerate(pieces):
        firsts[at].wait_recv()
        if at + AHEAD < len(pieces):
            begin(at + AHEAD)
        owner = me ^ first
        two = [
            send(place(owner, piece), owner, piece, second_sem, at, {"seq": me ^ second}),
            send(place(owner, piece), owner, piece, rep_sem, at, {"rep": z ^ 1}),
        ]
        copy = send(place(owner, piece), owner, piece, pair_sem.at[1], at, {"seq": me ^ 1})
        for each in two + [copy]:
            each.start()
        others.append(two)
        pairs.append(copy)
        if at:
            forward(at - 1)
    forward(len(pieces) - 1)
    for copy in firsts:
        copy.wait_send()
    for two in others:
        for copy in two:
            copy.wait_send()
    for copy in pairs + stores + small:
        copy.wait()


def gather_weights(shards, partial, condition, cid):
    shapes = [shard.shape for shard in shards]
    pieces = gather_pieces(shapes)
    count = len(shards)
    dma = pltpu.SemaphoreType.DMA
    size = len(pieces)
    outs = [jax.ShapeDtypeStruct((8,) + shape, jnp.bfloat16) for shape in shapes]
    outs.append(jax.ShapeDtypeStruct((8,) + partial.shape, partial.dtype))
    outs.append(jax.ShapeDtypeStruct((4,) + condition.shape, condition.dtype))
    got = pl.pallas_call(
        functools.partial(gather_kernel, pieces, count),
        out_shape=outs,
        in_specs=[pl.BlockSpec(memory_space=pl.ANY)] * (count + 2),
        out_specs=[pl.BlockSpec(memory_space=pl.ANY)] * len(outs),
        scratch_shapes=[pltpu.VMEM(shape, jnp.bfloat16) for shape in shapes]
        + [
            dma((2, size)), dma((2, size)), dma((2, size)), dma((4, 2, size)), dma((2, count)), dma((2, 11)),
        ],
        compiler_params=pltpu.CompilerParams(
            collective_id=cid, has_side_effects=True,
        ),
        name="gather_weights",
    )(*shards, partial, condition)
    fulls = [full.reshape(-1, full.shape[2]) for full in got[:count]]
    return fulls, got[count], got[count + 1]


SLOTS = 3
BACK = 4


def reduce_kernel(layers, rows, width, edge, *refs):
    ins, mods = refs[: 8 * layers], refs[8 * layers]
    outs, every_mod = refs[8 * layers + 1 : 12 * layers + 1], refs[12 * layers + 1]
    (
        left, right, away, pair_in, part,
        first_in_a, first_in_b, mid_a, mid_b, second_in_a, second_in_b,
        clip, rep_in, joined, inner_in, final, back_in, wide,
        mod_in, load_sem, pair_sem, link_sem, rep_sem, back_sem, store_sem, mod_sem,
    ) = refs[12 * layers + 2 :]
    me, z = lax.axis_index("seq"), lax.axis_index("rep")
    core, x, y = me & 1, (me >> 1) & 1, (me >> 2) & 1
    inner = (z == 1) | (z == 2)
    outer = (z == 0) | (z == 3)

    barrier = pltpu.get_barrier_semaphore()
    for mask in range(1, 8):
        pl.semaphore_signal(barrier, inc=1, device_id={"seq": me ^ mask})
    for mask in range(1, 4):
        pl.semaphore_signal(barrier, inc=1, device_id={"rep": z ^ mask})
    pl.semaphore_wait(barrier, 10)

    mod_copies = [
        pltpu.make_async_remote_copy(
            mods, mod_in.at[me], mod_sem.at[0, mask], mod_sem.at[1, mask],
            device_id={"seq": me ^ mask},
        )
        for mask in range(1, 8)
    ]
    clip_copies = [
        pltpu.make_async_remote_copy(
            every_mod.at[z], every_mod.at[z], mod_sem.at[0, 7 + mask], mod_sem.at[1, 7 + mask],
            device_id={"rep": z ^ mask},
        )
        for mask in range(1, 4)
    ]
    for copy in mod_copies:
        copy.start()
    mod_in[me] = mods[...]

    spans, start = [], 0
    for layer in range(layers):
        for kind in range(4):
            shape = outs[4 * layer + kind].shape
            count = shape[0] // rows * (shape[1] // width)
            spans.append((layer, kind, start, count))
            start += count
    total = start

    def loads(block, slot):
        for layer, kind, first, count in spans:
            @pl.when((block >= first) & (block < first + count))
            def _():
                source = ins[8 * layer + kind]
                if kind == 3:
                    source = source.at[:, :, block - first]
                pltpu.make_async_copy(source, left.at[slot], load_sem.at[0, slot]).start()
                source = ins[8 * layer + 4 + kind]
                if kind in (0, 2):
                    column = pl.multiple_of((block - first) * width, width)
                    source = source.at[:, pl.ds(column, width)]
                pltpu.make_async_copy(source, right.at[slot], load_sem.at[1, slot]).start()

    def wait_loads(slot):
        pltpu.make_async_copy(ins[0], left.at[slot], load_sem.at[0, slot]).wait()
        pltpu.make_async_copy(ins[5], right.at[slot], load_sem.at[1, slot]).wait()

    def store(block, slot):
        for layer, kind, first, count in spans:
            @pl.when((block >= first) & (block < first + count))
            def _():
                target = outs[4 * layer + kind]
                if kind == 3:
                    row = pl.multiple_of((block - first) * rows, rows)
                    target = target.at[pl.ds(row, rows)]
                elif kind in (0, 2):
                    column = pl.multiple_of((block - first) * width, width)
                    target = target.at[:, pl.ds(column, width)]
                pltpu.make_async_copy(wide.at[slot], target, store_sem.at[slot]).start()

    def to_seq(source, target, which, slot, mask):
        return pltpu.make_async_remote_copy(
            source, target, link_sem.at[0, which, slot], link_sem.at[1, which, slot],
            device_id={"seq": me ^ mask},
        )

    def pair_copy(t):
        slot = lax.rem(t, 2)
        return pltpu.make_async_remote_copy(
            away, pair_in.at[slot], pair_sem.at[0, slot], pair_sem.at[1, slot],
            device_id={"seq": me ^ 1},
        )

    def first_copies(t):
        slot, block = lax.rem(t, SLOTS), lax.rem(t - 1, SLOTS)
        return (
            to_seq(part.at[block, :, 1 - x, :, pl.ds(0, edge)], first_in_a.at[slot], 0, slot, 2),
            to_seq(
                part.at[block, 1 - y, :, :, pl.ds(edge, width - edge)],
                first_in_b.at[slot], 1, slot, 4,
            ),
        )

    def second_copies(t):
        slot, block = lax.rem(t, SLOTS), lax.rem(t, 2)
        return (
            to_seq(mid_a.at[block, 1 - y], second_in_a.at[slot], 2, slot, 4),
            to_seq(mid_b.at[block, 1 - x], second_in_b.at[slot], 3, slot, 2),
        )

    def rep_copy(t):
        slot = lax.rem(t, SLOTS)
        return pltpu.make_async_remote_copy(
            clip.at[lax.rem(t, 2)], rep_in.at[slot], rep_sem.at[0, 0, slot], rep_sem.at[1, 0, slot],
            device_id={"rep": z ^ 1},
        )

    def inner_copy(t):
        slot = lax.rem(t, SLOTS)
        return pltpu.make_async_remote_copy(
            joined.at[lax.rem(t, 2)], inner_in.at[slot],
            rep_sem.at[0, 1, slot], rep_sem.at[1, 1, slot],
            device_id={"rep": z ^ 3},
        )

    def back_copy(t):
        slot = lax.rem(t, BACK)
        return pltpu.make_async_remote_copy(
            final.at[lax.rem(t, 2)], back_in.at[slot], back_sem.at[0, slot], back_sem.at[1, slot],
            device_id={"rep": z ^ 1},
        )

    loads(0, 0)

    def turn(t, carry):
        def stage(back):
            return (t >= back) & (t < total + back)

        now2, was2 = lax.rem(t, 2), lax.rem(t + 1, 2)
        was3 = lax.rem(t + 2, SLOTS)

        @pl.when(t + 1 < total)
        def _():
            loads(t + 1, was2)

        @pl.when(stage(1))
        def _():
            for copy in first_copies(t):
                copy.start()

        @pl.when(stage(2))
        def _():
            block = lax.rem(t + 1, SLOTS)
            for at in range(2):
                mid_a[now2, at] = part[block, at, x, :, :edge] + first_in_a[was3, at]
                mid_b[now2, at] = part[block, y, at, :, edge:] + first_in_b[was3, at]
            for copy in second_copies(t):
                copy.start()

        @pl.when(stage(3))
        def _():
            clip[now2, :, :edge] = mid_a[was2, y] + second_in_a[was3]
            clip[now2, :, edge:] = mid_b[was2, x] + second_in_b[was3]

            @pl.when(outer)
            def _():
                rep_copy(t).start()

        @pl.when(stage(4) & inner)
        def _():
            joined[now2] = clip[was2] + rep_in[was3]
            inner_copy(t).start()

        @pl.when(stage(5) & inner)
        def _():
            final[now2] = joined[was2] + inner_in[was3]
            back_copy(t).start()

        @pl.when(stage(6))
        def _():
            @pl.when(inner)
            def _():
                wide[now2] = final[was2].astype(jnp.float32)

            @pl.when(outer)
            def _():
                wide[now2] = back_in[lax.rem(t + 3, BACK)].astype(jnp.float32)

            store(t - 6, now2)

        @pl.when(t < total)
        def _():
            wait_loads(now2)
            slot3 = lax.rem(t, SLOTS)

            def product(which):
                def columns(j, carry):
                    at = pl.ds(pl.multiple_of(j * (width // 3), width // 3), width // 3)
                    block = left[now2, :, which]
                    four, _, depth = block.shape
                    got = jnp.dot(
                        block.reshape(four * rows, depth), right[now2, :, at],
                        preferred_element_type=jnp.float32,
                    ).astype(jnp.bfloat16)
                    return at, got.reshape(four, rows, width // 3)
                return columns

            def away_columns(j, carry):
                at, got = product(1 - core)(j, carry)
                away[:, :, at] = got
                return carry

            lax.fori_loop(0, 3, away_columns, 0)
            pair_copy(t).start()

            def kept_columns(j, carry):
                at, got = product(core)(j, carry)
                part[slot3, 0, :, :, at] = got[:2]
                part[slot3, 1, :, :, at] = got[2:]
                return carry

            lax.fori_loop(0, 3, kept_columns, 0)
            pair_copy(t).wait()

            def add(j, carry):
                part[slot3, j // 2, j % 2] = part[slot3, j // 2, j % 2] + pair_in[now2, j]
                return carry

            lax.fori_loop(0, 4, add, 0)

        @pl.when(stage(1))
        def _():
            for copy in first_copies(t):
                copy.wait()

        @pl.when(stage(2))
        def _():
            for copy in second_copies(t):
                copy.wait()

        @pl.when(stage(3))
        def _():
            @pl.when(outer)
            def _():
                rep_copy(t).wait_send()

            @pl.when(inner)
            def _():
                rep_copy(t).wait_recv()

        @pl.when(stage(4) & inner)
        def _():
            inner_copy(t).wait()

        @pl.when(stage(5))
        def _():
            @pl.when(inner)
            def _():
                back_copy(t).wait_send()

            @pl.when(outer)
            def _():
                back_copy(t).wait_recv()

        @pl.when(stage(6))
        def _():
            pltpu.make_async_copy(wide.at[now2], outs[1], store_sem.at[now2]).wait()

        return carry

    lax.fori_loop(0, 2, turn, 0)
    for copy in mod_copies:
        copy.wait()
    mod_total = mod_in[0].astype(jnp.float32)
    for device in range(1, 8):
        mod_total += mod_in[device].astype(jnp.float32)
    every_mod[z] = mod_total.astype(every_mod.dtype)
    for copy in clip_copies:
        copy.start()
    lax.fori_loop(2, total + 6, turn, 0)
    for copy in clip_copies:
        copy.wait()


def reduce_grads(layers, mods, cid):
    tokens = layers[0][4].shape[0]
    rows, width = layers[0][0].shape[2], layers[0][5].shape[1]
    edge = width * 5 // 9 // 128 * 128
    low = jnp.bfloat16
    outs = []
    for ops in layers:
        for kind in range(4):
            tall = ops[kind].shape[2] if kind == 3 else 1
            outs.append(jax.ShapeDtypeStruct((tall * rows, ops[4 + kind].shape[1]), jnp.float32))
    outs.append(jax.ShapeDtypeStruct((4,) + mods.shape, mods.dtype))
    vm = pltpu.VMEM
    dma = pltpu.SemaphoreType.DMA
    flops = sum(2 * tokens * 8 * o.size for o in outs[:-1])
    got = pl.pallas_call(
        functools.partial(reduce_kernel, len(layers), rows, width, edge),
        out_shape=outs,
        in_specs=[pl.BlockSpec(memory_space=pl.ANY)] * (8 * len(layers))
        + [pl.BlockSpec(memory_space=vm)],
        out_specs=[pl.BlockSpec(memory_space=pl.ANY)] * (4 * len(layers))
        + [pl.BlockSpec(memory_space=vm)],
        scratch_shapes=[
            vm((2, 4, 2, rows, tokens), low),
            vm((2, tokens, width), low),
            vm((4, rows, width), low),
            vm((2, 4, rows, width), low),
            vm((SLOTS, 2, 2, rows, width), low),
            vm((SLOTS, 2, rows, edge), low),
            vm((SLOTS, 2, rows, width - edge), low),
            vm((2, 2, rows, edge), low),
            vm((2, 2, rows, width - edge), low),
            vm((SLOTS, rows, edge), low),
            vm((SLOTS, rows, width - edge), low),
            vm((2, rows, width), low),
            vm((SLOTS, rows, width), low),
            vm((2, rows, width), low),
            vm((SLOTS, rows, width), low),
            vm((2, rows, width), low),
            vm((BACK, rows, width), low),
            vm((2, rows, width), jnp.float32),
            vm((8,) + mods.shape, mods.dtype),
            dma((2, 2)),
            dma((2, 2)),
            dma((2, 4, SLOTS)),
            dma((2, 2, SLOTS)),
            dma((2, BACK)),
            dma((2,)),
            dma((2, 11)),
        ],
        compiler_params=pltpu.CompilerParams(
            collective_id=cid, has_side_effects=True, vmem_limit_bytes=48 << 20
        ),
        cost_estimate=pl.CostEstimate(flops=flops, bytes_accessed=4 * sum(o.size for o in outs), transcendentals=0),
        name="reduce_grads",
    )(*[op for ops in layers for op in ops], mods)
    return [tuple(got[4 * at : 4 * at + 4]) for at in range(len(layers))], got[-1]


def turned_rows(operand, tall):
    left = turned(operand)
    rows = left.shape[0] // 8 // tall
    shape = (4, 2, rows, left.shape[1]) if tall == 1 else (4, 2, tall, rows, left.shape[1])
    return left.reshape(shape)


def reduce_operands(grad_pairs):
    qkv_pair, out_pair, up_pair, down_pair = grad_pairs
    tall = down_pair[0].shape[-1] // down_pair[1].shape[-1]
    return (
        turned_rows(qkv_pair[0], 1),
        turned_rows(out_pair[0], 1),
        turned_rows(up_pair[0], 1),
        turned_rows(down_pair[0], tall),
    ) + tuple(flat(pair[1]) for pair in grad_pairs)


def per_device(
    frames_in,
    conditioning,
    mod_first,
    qkv_first,
    out_first,
    up_first,
    down_first,
    mod_second,
    qkv_second,
    out_second,
    up_second,
    down_second,
    cotangent,
):
    clip_count, _, frame_dev, half_places, features = frames_in.shape
    fused = lax.axis_size("seq") == 8 and lax.axis_size("rep") == 4 and clip_count == 1
    start_stream = frames_in.reshape(clip_count, frame_dev, half_places, features).astype(
        jnp.float32
    )
    row_count = mod_first.shape[0]
    row_start = lax.axis_index("seq") * row_count
    mod_width = mod_first.shape[1]
    rows_of = lambda whole: lax.dynamic_slice_in_dim(whole, row_start, row_count, 1)
    silu_local = rows_of(jax.nn.silu(conditioning)).astype(jnp.bfloat16)
    partial_mod = jnp.concatenate(
        [
            jnp.dot(silu_local, mod_first, preferred_element_type=jnp.float32),
            jnp.dot(silu_local, mod_second, preferred_element_type=jnp.float32),
        ],
        1,
    )
    shards = (
        qkv_first, out_first, up_first, down_first,
        qkv_second, out_second, up_second, down_second,
    )
    if fused:
        weights, partials, conditions = gather_weights(
            shards, partial_mod.reshape(-1, 128), conditioning.reshape(-1, 128), 0
        )
        modulation = jnp.sum(partials, 0).reshape(1, -1)
        every_silu = rows_of(jax.nn.silu(conditions.reshape(-1, features))).astype(jnp.bfloat16)
    else:
        weights = [lax.all_gather(shard, "seq", axis=0, tiled=True) for shard in shards]
        modulation = lax.psum(partial_mod, "seq")
        every_silu = lax.all_gather(silu_local, "rep", axis=0, tiled=True)
    mod_one, mod_two = modulation[:, :mod_width], modulation[:, mod_width:]
    weights_one, weights_two = weights[:4], weights[4:]
    spatial_out, state_one = forward_layer(start_stream, mod_one, weights_one, True)
    placed = to_places(spatial_out)
    temporal_out, state_two = forward_layer(placed, mod_two, weights_two, False)
    block_out = to_frames(temporal_out, frame_dev)
    cotangent_sites = to_places(cotangent.reshape(clip_count, frame_dev, half_places, features))
    placed_grad, mod_grad_two, pairs_two = backward_layer(
        cotangent_sites, placed, mod_two, weights_two, state_two, False
    )
    spatial_grad = to_frames(placed_grad, frame_dev)
    stream_grad, mod_grad_one, pairs_one = backward_layer(
        spatial_grad, start_stream, mod_one, weights_one, state_one, True
    )
    mod_grads = jnp.concatenate([mod_grad_one, mod_grad_two], 1).astype(jnp.bfloat16)
    if fused:
        (grads_two, grads_one), every_mod = reduce_grads(
            [reduce_operands(pairs_two), reduce_operands(pairs_one)],
            mod_grads.reshape(-1, 128),
            1,
        )
        every_mod = every_mod.reshape(-1, 2 * mod_width)
        mod_total = lax.dynamic_slice_in_dim(every_mod, lax.axis_index("rep"), 1, 0)
    else:
        grads_two, grads_one = layer_grads(pairs_two), layer_grads(pairs_one)
        mod_total = lax.psum(mod_grads, "seq").astype(jnp.bfloat16)
        every_mod = lax.all_gather(mod_total, "rep", axis=0, tiled=True)
    low_one, low_two = mod_total[:, :mod_width], mod_total[:, mod_width:]
    mod_weight_one = jnp.einsum(
        "cd,ce->de", every_silu, every_mod[:, :mod_width], preferred_element_type=jnp.float32
    )
    mod_weight_two = jnp.einsum(
        "cd,ce->de", every_silu, every_mod[:, mod_width:], preferred_element_type=jnp.float32
    )
    silu_grad = jnp.einsum("ce,de->cd", low_one, mod_first, preferred_element_type=jnp.float32)
    silu_grad = silu_grad + jnp.einsum(
        "ce,de->cd", low_two, mod_second, preferred_element_type=jnp.float32
    )
    condition_grad = jax.vjp(jax.nn.silu, rows_of(conditioning))[1](silu_grad)[0]
    out_shape = (clip_count, 1, frame_dev, half_places, features)
    return (
        block_out.reshape(out_shape),
        stream_grad.reshape(out_shape),
        condition_grad,
        mod_weight_one,
        *grads_one,
        mod_weight_two,
        *grads_two,
    )


def solution(mesh):
    return jax.shard_map(
        per_device,
        mesh=mesh,
        in_specs=(
            P("rep", "seq", None, None, None),
            P("rep", None),
            P("seq", None),
            P("seq", None),
            P("seq", None),
            P("seq", None),
            P("seq", None),
            P("seq", None),
            P("seq", None),
            P("seq", None),
            P("seq", None),
            P("seq", None),
            P("rep", "seq", None, None, None),
        ),
        out_specs=(
            P("rep", "seq", None, None, None),
            P("rep", "seq", None, None, None),
            P("rep", "seq"),
            P("seq", None),
            P("seq", None),
            P("seq", None),
            P("seq", None),
            P("seq", None),
            P("seq", None),
            P("seq", None),
            P("seq", None),
            P("seq", None),
            P("seq", None),
        ),
        check_vma=False,
    )
```

```python
import functools

import jax
import jax.numpy as jnp
from jax import lax
from jax.experimental import pallas as pl
from jax.experimental.pallas import tpu as pltpu
from jax.sharding import PartitionSpec as P

HEADS = 16
HEAD_WIDTH = 72


norm_epsilon = 1e-06


def from_partner(block, axis, apart):
    count = lax.axis_size(axis)
    route = []
    for low in range(count):
        high = low | 1 << apart
        if high != low and high < count:
            route += [(low, high), (high, low)]
    return lax.ppermute(block, axis, route)


def shortened(x):
    return jax.tree.map(lambda a: a.astype(jnp.bfloat16) if a.dtype == jnp.float32 else a, x)


def layer_mod(stream, shift_part, scale_part):
    row_mean = jnp.mean(stream, axis=-1, keepdims=True)
    centred = stream - row_mean
    row_var = jnp.mean(centred * centred, axis=-1, keepdims=True)
    return centred * lax.rsqrt(row_var + norm_epsilon) * (1.0 + scale_part) + shift_part


def gelu_tanh(pre_value):
    return jax.nn.gelu(pre_value, approximate=True)


def project(left_operand, right_operand):
    return jnp.einsum(
        "csld,de->csle", left_operand, right_operand, preferred_element_type=jnp.float32
    )


def project_back(incoming, right_operand):
    return jnp.einsum("csle,de->csld", incoming, right_operand, preferred_element_type=jnp.float32)


def mod_parts(modulation):
    return [segment[:, None, None, :] for segment in jnp.split(modulation, 6, axis=-1)]


def partner_values(stacked):
    return from_partner(stacked, "seq", 0)


def partner_grads(stacked):
    return from_partner(stacked.astype(jnp.bfloat16), "seq", 0).astype(stacked.dtype)


def to_places(stream):
    clip_count, frame_dev, half_places, features = stream.shape
    devices = lax.axis_size("seq")
    place_part = half_places // devices
    exchanged = lax.all_to_all(
        stream.reshape(1, clip_count, frame_dev, devices, place_part, features).astype(
            jnp.bfloat16
        ),
        "seq",
        split_axis=3,
        concat_axis=0,
        tiled=True,
    ).astype(jnp.float32)
    exchanged = exchanged.reshape(devices // 2, 2, clip_count, frame_dev, place_part, features)
    exchanged = jnp.transpose(exchanged, (2, 1, 4, 0, 3, 5))
    return exchanged.reshape(clip_count, 2 * place_part, devices // 2 * frame_dev, features)


def to_frames(stream, frame_dev):
    clip_count, place_count, frame_total, features = stream.shape
    devices = lax.axis_size("seq")
    place_part = place_count // 2
    arranged = stream.reshape(clip_count, 2, place_part, devices // 2, frame_dev, features)
    arranged = jnp.transpose(arranged, (3, 1, 0, 4, 2, 5)).reshape(
        devices, clip_count, frame_dev, 1, place_part, features
    )
    exchanged = lax.all_to_all(
        shortened(arranged), "seq", split_axis=0, concat_axis=3, tiled=True
    ).astype(arranged.dtype)
    return exchanged.reshape(clip_count, frame_dev, devices * place_part, features)


def forward_layer(stream, modulation, weights, spatial):
    qkv_w, out_w, up_w, down_w = weights
    shift_attn, scale_attn, gate_attn, shift_mlp, scale_mlp, gate_mlp = mod_parts(modulation)
    clip_count, seq_count, seq_len, features = stream.shape
    normed = layer_mod(stream, shift_attn, scale_attn).astype(jnp.bfloat16)
    projected = project(normed, qkv_w).astype(jnp.bfloat16)
    queries, keys_all, values_all = jnp.split(projected, 3, axis=-1)
    if spatial:
        remote = partner_values(jnp.stack([keys_all, values_all]))
        keys_all = jnp.concatenate([keys_all, remote[0]], axis=2)
        values_all = jnp.concatenate([values_all, remote[1]], axis=2)
    key_len = keys_all.shape[2]
    queries = queries.reshape(clip_count, seq_count, seq_len, HEADS, HEAD_WIDTH)
    keys_all = keys_all.reshape(clip_count, seq_count, key_len, HEADS, HEAD_WIDTH)
    values_all = values_all.reshape(clip_count, seq_count, key_len, HEADS, HEAD_WIDTH)
    scores = jnp.einsum(
        "cslhe,csmhe->cshlm", queries, keys_all, preferred_element_type=jnp.float32
    ) * HEAD_WIDTH ** (-0.5)
    peak_score = jnp.max(scores, axis=-1, keepdims=True)
    scaled_exp = jnp.exp(scores - peak_score)
    attention = scaled_exp / jnp.sum(scaled_exp, axis=-1, keepdims=True)
    attention_low = attention.astype(jnp.bfloat16)
    attended = jnp.einsum(
        "cshlm,csmhe->cslhe", attention_low, values_all, preferred_element_type=jnp.float32
    )
    attended = attended.astype(jnp.bfloat16).reshape(clip_count, seq_count, seq_len, features)
    branch = project(attended, out_w)
    middle = stream + gate_attn * branch
    normed_mid = layer_mod(middle, shift_mlp, scale_mlp).astype(jnp.bfloat16)
    hidden_pre = project(normed_mid, up_w)
    hidden = gelu_tanh(hidden_pre).astype(jnp.bfloat16)
    mlp_out = project(hidden, down_w)
    result = middle + gate_mlp * mlp_out
    kept_state = (
        normed,
        queries,
        keys_all,
        values_all,
        attention,
        attention_low,
        attended,
        branch,
        middle,
        normed_mid,
        hidden_pre,
        hidden,
        mlp_out,
    )
    return (result, kept_state)


def backward_layer(result_grad, stream, modulation, weights, kept_state, spatial):
    qkv_w, out_w, up_w, down_w = weights
    (
        normed,
        queries,
        keys_all,
        values_all,
        attention,
        attention_low,
        attended,
        branch,
        middle,
        normed_mid,
        hidden_pre,
        hidden,
        mlp_out,
    ) = kept_state
    shift_attn, scale_attn, gate_attn, shift_mlp, scale_mlp, gate_mlp = mod_parts(modulation)
    clip_count, seq_count, seq_len, features = stream.shape
    gate_mlp_grad = jnp.sum(result_grad * mlp_out, axis=(1, 2))
    mlp_grad = (gate_mlp * result_grad).astype(jnp.bfloat16)
    hidden_grad = project_back(mlp_grad, down_w)
    pre_grad = jax.vjp(gelu_tanh, hidden_pre)[1](hidden_grad)[0].astype(jnp.bfloat16)
    normed_mid_grad = project_back(pre_grad, up_w)
    middle_ln_grad, shift_mlp_grad, scale_mlp_grad = jax.vjp(
        layer_mod, middle, shift_mlp, scale_mlp
    )[1](normed_mid_grad)
    middle_grad = result_grad + middle_ln_grad
    gate_attn_grad = jnp.sum(middle_grad * branch, axis=(1, 2))
    branch_grad = (gate_attn * middle_grad).astype(jnp.bfloat16)
    attended_grad = project_back(branch_grad, out_w).astype(jnp.bfloat16)
    attended_grad = attended_grad.reshape(clip_count, seq_count, seq_len, HEADS, HEAD_WIDTH)
    attention_grad = jnp.einsum(
        "cslhe,csmhe->cshlm", attended_grad, values_all, preferred_element_type=jnp.float32
    )
    scores_grad = attention * (
        attention_grad - jnp.sum(attention_grad * attention, axis=-1, keepdims=True)
    )
    scores_grad = scores_grad.astype(jnp.bfloat16)
    inv_root = HEAD_WIDTH ** (-0.5)
    queries_grad = (
        jnp.einsum("cshlm,csmhe->cslhe", scores_grad, keys_all, preferred_element_type=jnp.float32)
        * inv_root
    )
    keys_grad = (
        jnp.einsum("cshlm,cslhe->csmhe", scores_grad, queries, preferred_element_type=jnp.float32)
        * inv_root
    )
    values_grad = jnp.einsum(
        "cshlm,cslhe->csmhe", attention_low, attended_grad, preferred_element_type=jnp.float32
    )
    if spatial:
        returned = partner_grads(
            jnp.stack([keys_grad[:, :, seq_len:], values_grad[:, :, seq_len:]])
        )
        keys_grad = keys_grad[:, :, :seq_len] + returned[0]
        values_grad = values_grad[:, :, :seq_len] + returned[1]
    qkv_grad = jnp.concatenate(
        [
            component.reshape(clip_count, seq_count, seq_len, features)
            for component in (queries_grad, keys_grad, values_grad)
        ],
        axis=-1,
    )
    qkv_grad = qkv_grad.astype(jnp.bfloat16)
    normed_grad = project_back(qkv_grad, qkv_w)
    stream_ln_grad, attention_shift_gradient, scale_attn_grad = jax.vjp(
        layer_mod, stream, shift_attn, scale_attn
    )[1](normed_grad)
    stream_grad = middle_grad + stream_ln_grad
    mod_grad = jnp.concatenate(
        [
            attention_shift_gradient.reshape(clip_count, features),
            scale_attn_grad.reshape(clip_count, features),
            gate_attn_grad,
            shift_mlp_grad.reshape(clip_count, features),
            scale_mlp_grad.reshape(clip_count, features),
            gate_mlp_grad,
        ],
        axis=-1,
    )
    grad_pairs = (
        (normed, qkv_grad),
        (attended, branch_grad),
        (normed_mid, pre_grad),
        (hidden, mlp_grad),
    )
    return (stream_grad, mod_grad, grad_pairs)


def bit_count(axis):
    return lax.axis_size(axis).bit_length() - 1


def swap(block, axis, bit):
    count = lax.axis_size(axis)
    return lax.ppermute(block, axis, [(at, at ^ (1 << bit)) for at in range(count)])


def bit_of(axis, bit):
    return (lax.axis_index(axis) >> bit) & 1


def pick(block, which, axis):
    return lax.dynamic_index_in_dim(block, which, axis, keepdims=False)


def spread_rows_out(left_turned, right_operand, flipped):
    bits = bit_count("seq")
    total_rows, tokens = left_turned.shape
    rows = total_rows >> bits
    halves = left_turned.reshape(1 << (bits - 1), 2, rows, tokens)
    core = bit_of("seq", 0)

    def product(which):
        left = pick(halves, which, 1).reshape(-1, tokens)
        return jnp.dot(left, right_operand, preferred_element_type=jnp.float32).astype(
            jnp.bfloat16
        )

    arrived = swap(product(1 - core), "seq", 0)
    held = product(core)
    left_bits = list(range(bits - 1, 0, -1))
    shape = [2] * (bits - 1) + [rows, right_operand.shape[1]]
    held = held.reshape(shape)
    arrived = arrived.reshape(shape)
    order = list(left_bits) if flipped else left_bits[::-1]
    for bit in order:
        at = left_bits.index(bit)
        mine = bit_of("seq", bit)
        away = pick(held, 1 - mine, at).astype(jnp.float32) + pick(arrived, 1 - mine, at)
        kept = pick(held, mine, at).astype(jnp.float32) + pick(arrived, mine, at)
        arrived = swap(away.astype(jnp.bfloat16), "seq", bit)
        held = kept.astype(jnp.bfloat16)
        left_bits.remove(bit)
    return held.astype(jnp.float32) + arrived


def rep_sum(block, axis):
    bits = bit_count("rep")
    held = block.astype(jnp.bfloat16)
    for bit in range(bits):
        mine = bit_of("rep", bit)
        low, high = jnp.split(held, 2, axis)
        away = jnp.where(mine == 0, high, low)
        kept = jnp.where(mine == 0, low, high)
        held = (kept.astype(jnp.float32) + swap(away, "rep", bit)).astype(jnp.bfloat16)
    for bit in reversed(range(bits)):
        mine = bit_of("rep", bit)
        other = swap(held, "rep", bit)
        low = jnp.where(mine == 0, held, other)
        high = jnp.where(mine == 0, other, held)
        held = jnp.concatenate([low, high], axis)
    return held.astype(jnp.float32)


def turned(operand):
    return operand.reshape(-1, operand.shape[-1]).T


def flat(operand):
    return operand.reshape(-1, operand.shape[-1])


def cut(width, parts, of):
    return width * parts // of // 128 * 128


def down_grad(pair):
    left, right = turned(pair[0]), flat(pair[1])
    edge = cut(right.shape[1], 5, 9)
    return jnp.concatenate(
        [
            rep_sum(spread_rows_out(left, right[:, :edge], False), 0),
            rep_sum(spread_rows_out(left, right[:, edge:], True), 0),
        ],
        1,
    )


def up_grad(pair):
    left, right = turned(pair[0]), flat(pair[1])
    edge = cut(right.shape[1], 4, 9)
    return jnp.concatenate(
        [
            rep_sum(spread_rows_out(left, right[:, :edge], False), 1),
            rep_sum(spread_rows_out(left, right[:, edge:], True), 1),
        ],
        1,
    )


def attention_grads(qkv_pair, out_pair):
    left, right = turned(qkv_pair[0]), flat(qkv_pair[1])
    width = right.shape[1]
    edge = cut(width, 16, 27)
    first = rep_sum(spread_rows_out(left, right[:, :edge], False), 1)
    second = spread_rows_out(left, right[:, edge:], True)
    third = spread_rows_out(turned(out_pair[0]), flat(out_pair[1]), True)
    joined = rep_sum(jnp.concatenate([second, third], 1), 1)
    return (
        jnp.concatenate([first, joined[:, : width - edge]], 1),
        joined[:, width - edge :],
    )


def layer_grads(grad_pairs):
    qkv_pair, out_pair, up_pair, down_pair = grad_pairs
    down = down_grad(down_pair)
    up = up_grad(up_pair)
    qkv, out = attention_grads(qkv_pair, out_pair)
    return (qkv, out, up, down)


LOW = jnp.bfloat16
WIDE = jnp.float32
LANES = 128
STRIP = 64
KEYS = 256


def whole_block(shape):
    return pl.BlockSpec(shape, lambda *at: (0,) * len(shape))


def strips(total, body):
    def step(j, carry):
        body(pl.ds(pl.multiple_of(j * STRIP, STRIP), STRIP))
        return carry

    lax.fori_loop(0, total // STRIP, step, 0)


def turn_into(target, source):
    for j in range(source.shape[1] // LANES):
        target[j * LANES : (j + 1) * LANES, :] = source[:, j * LANES : (j + 1) * LANES].T


def unit_rows(block):
    centred = block - jnp.mean(block, axis=-1, keepdims=True)
    spread = lax.rsqrt(jnp.mean(centred * centred, axis=-1, keepdims=True) + norm_epsilon)
    return centred * spread, spread


def into_norm(grad, scaled, unit, spread):
    inner = grad * scaled
    level = jnp.mean(inner, axis=-1, keepdims=True)
    slope = jnp.mean(inner * unit, axis=-1, keepdims=True)
    return spread * (inner - level - unit * slope)


def times(left, right):
    return jnp.dot(left, right, preferred_element_type=WIDE)


def times_turned(left, right):
    return lax.dot_general(left, right, (((1,), (1,)), ((), ())), preferred_element_type=WIDE)


def turned_times(left, right):
    return lax.dot_general(left, right, (((0,), (0,)), ((), ())), preferred_element_type=WIDE)


def params(size, cid=None):
    if cid is None:
        return pltpu.CompilerParams(vmem_limit_bytes=size << 20)
    return pltpu.CompilerParams(
        vmem_limit_bytes=size << 20, collective_id=cid, has_side_effects=True
    )


def cost(flops, size):
    return pl.CostEstimate(flops=flops, bytes_accessed=size, transcendentals=0)


def qkv_kernel(x_ref, mod_ref, w_ref, qkv_ref, turned_ref, held):
    @pl.when(pl.program_id(0) == 0)
    def _():
        scaled, shift = 1.0 + mod_ref[1:2], mod_ref[0:1]

        def norm(at):
            unit, _ = unit_rows(x_ref[at].astype(WIDE))
            held[at] = (unit * scaled + shift).astype(LOW)

        strips(held.shape[0], norm)
        turn_into(turned_ref, held)

    qkv_ref[...] = times(held[...], w_ref[...]).astype(LOW)


def qkv_forward(x, mod, weight):
    tokens, features = x.shape
    steps = weight.shape[1] // features
    return pl.pallas_call(
        qkv_kernel,
        grid=(steps,),
        in_specs=[
            whole_block(x.shape),
            whole_block(mod.shape),
            pl.BlockSpec((features, features), lambda j: (0, j)),
        ],
        out_specs=[
            pl.BlockSpec((tokens, features), lambda j: (0, j)),
            whole_block((features, tokens)),
        ],
        out_shape=[
            jax.ShapeDtypeStruct((tokens, weight.shape[1]), LOW),
            jax.ShapeDtypeStruct((features, tokens), LOW),
        ],
        scratch_shapes=[pltpu.VMEM((tokens, features), LOW)],
        compiler_params=params(40),
        cost_estimate=cost(2 * tokens * weight.size, 2 * weight.size),
        name="qkv_forward",
    )(x, mod, weight)


def window(head):
    low, high = head * HEAD_WIDTH, (head + 1) * HEAD_WIDTH
    start = low // LANES * LANES
    stop = -(-high // LANES) * LANES
    return start, stop - start, low - start


def head_mask(head):
    start, wide, offset = window(head)
    lane = lax.broadcasted_iota(jnp.int32, (1, wide), 1)
    return ((lane >= offset) & (lane < offset + HEAD_WIDTH)).astype(WIDE).astype(LOW)


def add_window(total, head, block):
    start, wide, _ = window(head)
    for j in range(wide // LANES):
        tile = start // LANES + j
        lanes = slice(tile * LANES, (tile + 1) * LANES)
        piece = block[:, j * LANES : (j + 1) * LANES]
        if head == tile * LANES // HEAD_WIDTH:
            total[:, lanes] = piece
        else:
            total[:, lanes] = total[:, lanes] + piece


def group_rows(ref, group, column, wide, spatial):
    lanes = slice(column, column + wide)
    if spatial:
        return ref[group, :, lanes]
    block = ref[:, group, :, lanes]
    return block.reshape(-1, wide)


def same_place():
    row = lax.broadcasted_iota(jnp.int32, (KEYS, KEYS), 0)
    column = lax.broadcasted_iota(jnp.int32, (KEYS, KEYS), 1)
    return (row & 15) == (column & 15)


def put_rows(ref, group, block, spatial):
    if spatial:
        ref[group] = block
    else:
        ref[:, group] = block.reshape(ref.shape[0], ref.shape[2], ref.shape[3])


def sibling_barrier(me):
    barrier = pltpu.get_barrier_semaphore()
    pl.semaphore_signal(barrier, inc=1, device_id={"seq": me ^ 1})
    pl.semaphore_wait(barrier, 1)


def attend_kernel(spatial, *refs):
    qkv_ref, x_ref, mod_ref, w_ref = refs[:4]
    prob_ref, turned_ref, x1_ref, branch_ref, h2_ref, h2_turned_ref = refs[4:10]
    if spatial:
        other_ref, held, total, branch, other, send_sem, arrive_sem, keep_sem = refs[10:]
    else:
        held, total, branch = refs[10:]
    group, groups = pl.program_id(0), pl.num_programs(0)
    features = x_ref.shape[1]

    if spatial:
        me = lax.axis_index("seq")

        def exchange(j):
            return pltpu.make_async_remote_copy(
                qkv_ref.at[j, :, pl.ds(features, 2 * features)], other.at[j],
                send_sem.at[j], arrive_sem.at[j], device_id={"seq": me ^ 1},
            )

        @pl.when(group == 0)
        def _():
            sibling_barrier(me)
            for j in range(other.shape[0]):
                exchange(j).start()

        exchange(group).wait_recv()
    else:
        allowed = same_place()

    for head in range(HEADS):
        start, wide, _ = window(head)
        mask = head_mask(head)
        queries = group_rows(qkv_ref, group, start, wide, spatial) * mask
        keys = group_rows(qkv_ref, group, features + start, wide, spatial)
        values = group_rows(qkv_ref, group, 2 * features + start, wide, spatial)
        if spatial:
            keys = jnp.concatenate([keys, other[group, :, start : start + wide]], 0)
            values = jnp.concatenate(
                [values, other[group, :, features + start : features + start + wide]], 0
            )
        scores = times_turned(queries, keys) * HEAD_WIDTH ** (-0.5)
        if not spatial:
            scores = jnp.where(allowed, scores, -3e38)
        grown = jnp.exp(scores - jnp.max(scores, axis=-1, keepdims=True))
        prob = (grown / jnp.sum(grown, axis=-1, keepdims=True)).astype(LOW)
        prob_ref[0, head] = prob
        add_window(total, head, times(prob, values * mask))
    put_rows(held, group, total[...].astype(LOW), spatial)

    @pl.when(group == groups - 1)
    def _():
        if spatial:
            keep = pltpu.make_async_copy(other, other_ref, keep_sem)
            keep.start()
        attended = held[...].reshape(-1, features)
        branch[...] = times(attended, w_ref[...])
        for j in range(features // LANES):
            lanes = slice(j * LANES, (j + 1) * LANES)
            turned_ref[lanes, :] = attended[:, lanes].T
        gate, shift, scaled = mod_ref[2:3], mod_ref[3:4], 1.0 + mod_ref[4:5]

        def finish(at):
            part = branch[at]
            branch_ref[at] = part.astype(LOW)
            middle = x_ref[at].astype(WIDE) + gate * part
            x1_ref[at] = middle
            unit, _ = unit_rows(middle)
            h2_ref[at] = (unit * scaled + shift).astype(LOW)

        strips(x_ref.shape[0], finish)
        turn_into(h2_turned_ref, h2_ref)
        if spatial:
            for j in range(other.shape[0]):
                exchange(j).wait_send()
            keep.wait()


def attention_forward(qkv, x, mod, weight, spatial, groups, cid=None):
    tokens, features = x.shape
    span = tokens // groups
    shape = (groups, span, 3 * features) if spatial else (4, groups, span // 4, 3 * features)
    rest = shape[:-1]
    out_shape = [
        jax.ShapeDtypeStruct((groups, HEADS, span, KEYS), LOW),
        jax.ShapeDtypeStruct((features, tokens), LOW),
        jax.ShapeDtypeStruct((tokens, features), WIDE),
        jax.ShapeDtypeStruct((tokens, features), LOW),
        jax.ShapeDtypeStruct((tokens, features), LOW),
        jax.ShapeDtypeStruct((features, tokens), LOW),
    ]
    out_specs = [pl.BlockSpec((1, HEADS, span, KEYS), lambda g: (g, 0, 0, 0))]
    out_specs += [whole_block(o.shape) for o in out_shape[1:]]
    scratch = [
        pltpu.VMEM(rest + (features,), LOW),
        pltpu.VMEM((span, features), WIDE),
        pltpu.VMEM((tokens, features), WIDE),
    ]
    if spatial:
        both = rest + (2 * features,)
        out_shape.append(jax.ShapeDtypeStruct(both, LOW))
        out_specs.append(pl.BlockSpec(memory_space=pl.ANY))
        scratch += [
            pltpu.VMEM(both, LOW),
            pltpu.SemaphoreType.DMA((groups,)),
            pltpu.SemaphoreType.DMA((groups,)),
            pltpu.SemaphoreType.DMA(()),
        ]
    return pl.pallas_call(
        functools.partial(attend_kernel, spatial),
        grid=(groups,),
        in_specs=[
            whole_block(shape), whole_block(x.shape), whole_block(mod.shape), whole_block(weight.shape),
        ],
        out_specs=out_specs,
        out_shape=out_shape,
        scratch_shapes=scratch,
        compiler_params=params(56, cid),
        cost_estimate=cost(2 * tokens * (weight.size + 2 * features * KEYS), 4 * qkv.size),
        name="attend_spatial" if spatial else "attend_temporal",
    )(qkv.reshape(shape), x, mod, weight)


def attend_back_kernel(spatial, *refs):
    if spatial:
        (
            da_ref, qkv_ref, prob_ref, w_ref, other_ref, dqkv_ref,
            dout, total_q, total_k, total_v, other, give, take, load_sem, send_sem, arrive_sem,
        ) = refs
    else:
        da_ref, qkv_ref, prob_ref, w_ref, dqkv_ref, dout, total_q, total_k, total_v = refs
    group, groups = pl.program_id(0), pl.num_programs(0)
    features = da_ref.shape[1]
    root = HEAD_WIDTH ** (-0.5)
    if spatial:
        me = lax.axis_index("seq")

        def exchange(j):
            return pltpu.make_async_remote_copy(
                give.at[j], take.at[j], send_sem.at[j], arrive_sem.at[j], device_id={"seq": me ^ 1},
            )

    @pl.when(group == 0)
    def _():
        if spatial:
            load = pltpu.make_async_copy(other_ref, other, load_sem)
            load.start()
            sibling_barrier(me)
        half = da_ref.shape[0] // 2
        for j in range(2):
            got = times_turned(da_ref[j * half : (j + 1) * half], w_ref[...]).astype(LOW)
            if spatial:
                dout[2 * j : 2 * j + 2] = got.reshape(2, half // 2, features)
            else:
                dout[2 * j : 2 * j + 2] = got.reshape(2, 2, half // 4, features)
        if spatial:
            load.wait()

    for head in range(HEADS):
        start, wide, _ = window(head)
        mask = head_mask(head)
        queries = group_rows(qkv_ref, group, start, wide, spatial) * mask
        keys = group_rows(qkv_ref, group, features + start, wide, spatial)
        values = group_rows(qkv_ref, group, 2 * features + start, wide, spatial)
        grads = group_rows(dout, group, start, wide, spatial) * mask
        if spatial:
            keys = jnp.concatenate([keys, other[group, :, start : start + wide]], 0)
            values = jnp.concatenate(
                [values, other[group, :, features + start : features + start + wide]], 0
            )
        prob = prob_ref[0, head]
        known = prob.astype(WIDE)
        dprob = times_turned(grads, values)
        level = jnp.sum(dprob * known, axis=-1, keepdims=True)
        dscores = (known * (dprob - level)).astype(LOW)
        add_window(total_q, head, times(dscores, keys * mask))
        add_window(total_k, head, turned_times(dscores, queries))
        add_window(total_v, head, turned_times(prob, grads))

    own = total_q.shape[0]
    pieces = (
        (total_q[...] * root).astype(LOW),
        (total_k[:own] * root).astype(LOW),
        total_v[:own].astype(LOW),
    )
    for j, piece in enumerate(pieces):
        lanes = slice(j * features, (j + 1) * features)
        if spatial:
            dqkv_ref[group, :, lanes] = piece
        else:
            dqkv_ref[:, group, :, lanes] = piece.reshape(4, -1, features)
    if spatial:
        give[group, :, :features] = (total_k[own:] * root).astype(LOW)
        give[group, :, features:] = total_v[own:].astype(LOW)
        exchange(group).start()

        @pl.when(group == groups - 1)
        def _():
            for j in range(take.shape[0]):
                exchange(j).wait()
                lanes = slice(features, 3 * features)
                dqkv_ref[j, :, lanes] = dqkv_ref[j, :, lanes] + take[j]


def attention_backward(da, qkv, prob, weight, other, spatial, cid=None):
    tokens, features = da.shape
    groups = prob.shape[0]
    span = tokens // groups
    shape = (groups, span, 3 * features) if spatial else (4, groups, span // 4, 3 * features)
    rest = shape[:-1]
    in_specs = [
        whole_block(da.shape),
        whole_block(shape),
        pl.BlockSpec((1, HEADS, span, KEYS), lambda g: (g, 0, 0, 0)),
        whole_block(weight.shape),
    ]
    scratch = [
        pltpu.VMEM(rest + (features,), LOW),
        pltpu.VMEM((span, features), WIDE),
        pltpu.VMEM((KEYS, features), WIDE),
        pltpu.VMEM((KEYS, features), WIDE),
    ]
    args = [da, qkv.reshape(shape), prob, weight]
    if spatial:
        in_specs.append(pl.BlockSpec(memory_space=pl.ANY))
        args.append(other)
        scratch += [pltpu.VMEM(other.shape, LOW)] * 3
        scratch += [
            pltpu.SemaphoreType.DMA(()),
            pltpu.SemaphoreType.DMA((groups,)),
            pltpu.SemaphoreType.DMA((groups,)),
        ]
    got = pl.pallas_call(
        functools.partial(attend_back_kernel, spatial),
        grid=(groups,),
        in_specs=in_specs,
        out_specs=whole_block(shape),
        out_shape=jax.ShapeDtypeStruct(shape, LOW),
        scratch_shapes=scratch,
        compiler_params=params(56, cid),
        cost_estimate=cost(2 * tokens * (weight.size + 5 * features * KEYS), 4 * qkv.size),
        name="attend_spatial_back" if spatial else "attend_temporal_back",
    )(*args)
    return got.reshape(tokens, 3 * features)


def seq_barrier(me):
    barrier = pltpu.get_barrier_semaphore()
    for mask in range(1, 8):
        pl.semaphore_signal(barrier, inc=1, device_id={"seq": me ^ mask})
    pl.semaphore_wait(barrier, 7)


def moves(source, target, sems, local_sem, me, to_places):
    part = source.shape[-2] // 8 if to_places else source.shape[-2]

    def ends(device):
        if to_places:
            return source.at[:, pl.ds(pl.multiple_of(device * part, part), part)], target.at[me]
        return source.at[device], target.at[:, pl.ds(pl.multiple_of(me * part, part), part)]

    copies = [pltpu.make_async_copy(*ends(me), local_sem)]
    for mask in (6, 7, 2, 3, 4, 5, 1):
        copies.append(
            pltpu.make_async_remote_copy(
                *ends(me ^ mask), sems.at[0, mask], sems.at[1, mask], device_id={"seq": me ^ mask}
            )
        )
    return copies


def move_scratch():
    return [pltpu.SemaphoreType.DMA((2, 8)), pltpu.SemaphoreType.DMA(())]


def gelu_and_slope(value):
    inner = 0.7978845608028654 * (value + 0.044715 * value * value * value)
    bent = jnp.tanh(inner)
    half = 0.5 * (1.0 + bent)
    slope = half + 0.5 * value * (1.0 - bent * bent) * (
        0.7978845608028654 * (1.0 + 3 * 0.044715 * value * value)
    )
    return value * half, slope


def mlp_kernel(send, *refs):
    x1_ref, h2_ref, mod_ref, up_ref, down_ref = refs[:5]
    turned_ref, slope_ref, out_ref, mlp_ref, total = refs[5:10]
    step, steps = pl.program_id(0), pl.num_programs(0)
    half = h2_ref.shape[0] // 2

    for j in range(2):
        rows = slice(j * half, (j + 1) * half)
        hidden, slope = gelu_and_slope(times(h2_ref[rows], up_ref[...]))
        slope_ref[rows] = slope.astype(LOW)
        hidden = hidden.astype(LOW)
        turned_ref[:, rows] = hidden.T
        part = times(hidden, down_ref[...])

        @pl.when(step == 0)
        def _():
            total[rows] = part

        @pl.when(step > 0)
        def _():
            total[rows] = total[rows] + part

    @pl.when(step == steps - 1)
    def _():
        gate = mod_ref[5:6]
        if send:
            ready, sems, local_sem = refs[10:]
            me = lax.axis_index("seq")
            seq_barrier(me)
            target = ready
        else:
            target = out_ref
        per = target.shape[1] if send else target.shape[0]

        def finish(at):
            mlp = total[at]
            mlp_ref[at] = mlp.astype(LOW)
            total[at] = x1_ref[at] + gate * mlp

        strips(total.shape[0], finish)
        if send:
            ready[...] = total[...].astype(LOW).reshape(ready.shape)
            copies = moves(ready, out_ref, sems, local_sem, me, True)
            for copy in copies:
                copy.start()
            for copy in copies:
                copy.wait()
        else:
            out_ref[...] = total[...].astype(LOW)


def mlp_forward(x1, h2, mod, up, down, frames=None, cid=None):
    tokens, features = x1.shape
    wide = up.shape[1]
    block = 768
    out_shape = [
        jax.ShapeDtypeStruct((wide, tokens), LOW),
        jax.ShapeDtypeStruct((tokens, wide), LOW),
        jax.ShapeDtypeStruct((tokens, features), LOW),
        jax.ShapeDtypeStruct((tokens, features), LOW),
    ]
    scratch = [pltpu.VMEM((tokens, features), WIDE)]
    send = frames is not None
    if send:
        places = tokens // frames
        out_shape[2] = jax.ShapeDtypeStruct((8, frames, places // 8, features), LOW)
        scratch += [pltpu.VMEM((frames, places, features), LOW)] + move_scratch()
    out_specs = [
        pl.BlockSpec((block, tokens), lambda j: (j, 0)),
        pl.BlockSpec((tokens, block), lambda j: (0, j)),
        pl.BlockSpec(memory_space=pl.ANY) if send else whole_block((tokens, features)),
        whole_block((tokens, features)),
    ]
    return pl.pallas_call(
        functools.partial(mlp_kernel, send),
        grid=(wide // block,),
        in_specs=[
            whole_block(x1.shape), whole_block(h2.shape), whole_block(mod.shape),
            pl.BlockSpec((features, block), lambda j: (0, j)),
            pl.BlockSpec((block, features), lambda j: (j, 0)),
        ],
        out_specs=out_specs,
        out_shape=out_shape,
        scratch_shapes=scratch,
        compiler_params=params(56, cid),
        cost_estimate=cost(4 * tokens * up.size, 4 * up.size),
        name="mlp_forward",
    )(x1, h2, mod, up, down)


def mlp_back_kernel(send, *refs):
    g_ref, x1_ref, branch_ref, mlp_ref, mod_ref, up_ref, down_ref, slope_ref = refs[:8]
    refs = refs[8:]
    if send:
        done_ref, refs = refs[0], refs[1:]
    du_ref, df_ref, dx1_ref, da_ref, sums_ref = refs[:5]
    refs = refs[5:]
    if send:
        moved_ref, refs = refs[0], refs[1:]
    df, total = refs[:2]
    step, steps = pl.program_id(0), pl.num_programs(0)
    if send:
        me = lax.axis_index("seq")
        copies = moves(done_ref, moved_ref, refs[2], refs[3], me, False)

    @pl.when(step == 0)
    def _():
        if send:
            seq_barrier(me)
            for copy in copies:
                copy.start()
        gate = mod_ref[5:6]
        sums_ref[...] = jnp.zeros_like(sums_ref)

        def begin(at):
            grad = g_ref[at].astype(WIDE)
            low = (gate * grad).astype(LOW)
            df[at] = low
            df_ref[at] = low
            sums_ref[3:4] += jnp.sum(grad * mlp_ref[at].astype(WIDE), axis=0, keepdims=True)

        strips(df.shape[0], begin)

    half = df.shape[0] // 2
    for j in range(2):
        rows = slice(j * half, (j + 1) * half)
        du = times_turned(df[rows], down_ref[...]) * slope_ref[rows].astype(WIDE)
        du = du.astype(LOW)
        du_ref[rows] = du
        part = times_turned(du, up_ref[...])

        @pl.when(step == 0)
        def _():
            total[rows] = part

        @pl.when(step > 0)
        def _():
            total[rows] = total[rows] + part

    @pl.when(step == steps - 1)
    def _():
        gate, scaled = mod_ref[2:3], 1.0 + mod_ref[4:5]

        def finish(at):
            grad = total[at]
            unit, spread = unit_rows(x1_ref[at])
            middle = g_ref[at].astype(WIDE) + into_norm(grad, scaled, unit, spread)
            dx1_ref[at] = middle
            da_ref[at] = (gate * middle).astype(LOW)
            sums_ref[0:1] += jnp.sum(
                middle * branch_ref[at].astype(WIDE), axis=0, keepdims=True
            )
            sums_ref[1:2] += jnp.sum(grad, axis=0, keepdims=True)
            sums_ref[2:3] += jnp.sum(grad * unit, axis=0, keepdims=True)

        strips(df.shape[0], finish)
        if send:
            for copy in copies:
                copy.wait()


def mlp_backward(g, x1, branch, mlp, mod, up, down, slope, done=None, cid=None):
    tokens, features = x1.shape
    wide = up.shape[1]
    block = 768
    send = done is not None
    in_specs = [
        whole_block(g.shape), whole_block(x1.shape), whole_block(branch.shape),
        whole_block(mlp.shape), whole_block(mod.shape),
        pl.BlockSpec((features, block), lambda j: (0, j)),
        pl.BlockSpec((block, features), lambda j: (j, 0)),
        pl.BlockSpec((tokens, block), lambda j: (0, j)),
    ]
    args = [g, x1, branch, mlp, mod, up, down, slope]
    out_shape = [
        jax.ShapeDtypeStruct((tokens, wide), LOW),
        jax.ShapeDtypeStruct((tokens, features), LOW),
        jax.ShapeDtypeStruct((tokens, features), WIDE),
        jax.ShapeDtypeStruct((tokens, features), LOW),
        jax.ShapeDtypeStruct((8, features), WIDE),
    ]
    out_specs = [pl.BlockSpec((tokens, block), lambda j: (0, j))]
    out_specs += [whole_block(o.shape) for o in out_shape[1:]]
    scratch = [pltpu.VMEM((tokens, features), LOW), pltpu.VMEM((tokens, features), WIDE)]
    if send:
        in_specs.append(pl.BlockSpec(memory_space=pl.ANY))
        args.append(done)
        out_shape.append(
            jax.ShapeDtypeStruct((done.shape[1], 8 * done.shape[2], features), LOW)
        )
        out_specs.append(pl.BlockSpec(memory_space=pl.ANY))
        scratch += move_scratch()
    return pl.pallas_call(
        functools.partial(mlp_back_kernel, send),
        grid=(wide // block,),
        in_specs=in_specs,
        out_specs=out_specs,
        out_shape=out_shape,
        scratch_shapes=scratch,
        compiler_params=params(56, cid),
        cost_estimate=cost(4 * tokens * up.size, 4 * up.size),
        name="mlp_backward",
    )(*args)


def qkv_back_kernel(send, *refs):
    dqkv_ref, w_ref, x_ref, dx1_ref, mod_ref, dx_ref, sums_ref, total = refs[:8]
    step, steps = pl.program_id(0), pl.num_programs(0)
    part = times_turned(dqkv_ref[...], w_ref[...])

    @pl.when(step == 0)
    def _():
        total[...] = part

    @pl.when(step > 0)
    def _():
        total[...] = total[...] + part

    @pl.when(step == steps - 1)
    def _():
        scaled = 1.0 + mod_ref[1:2]
        sums_ref[...] = jnp.zeros_like(sums_ref)
        if send:
            ready, sems, local_sem = refs[8:]
            me = lax.axis_index("seq")
            seq_barrier(me)

        def finish(at):
            grad = total[at]
            unit, spread = unit_rows(x_ref[at].astype(WIDE))
            sums_ref[0:1] += jnp.sum(grad, axis=0, keepdims=True)
            sums_ref[1:2] += jnp.sum(grad * unit, axis=0, keepdims=True)
            got = dx1_ref[at] + into_norm(grad, scaled, unit, spread)
            if send:
                total[at] = got
            else:
                dx_ref[at] = got

        strips(total.shape[0], finish)
        if send:
            ready[...] = total[...].astype(LOW).reshape(ready.shape)
            copies = moves(ready, dx_ref, sems, local_sem, me, False)
            for copy in copies:
                copy.start()
            for copy in copies:
                copy.wait()


def qkv_backward(dqkv, weight, x, dx1, mod, frames=None, cid=None):
    tokens, features = x.shape
    steps = weight.shape[1] // features
    send = frames is not None
    out_shape = [
        jax.ShapeDtypeStruct((tokens, features), WIDE),
        jax.ShapeDtypeStruct((8, features), WIDE),
    ]
    scratch = [pltpu.VMEM((tokens, features), WIDE)]
    if send:
        places = tokens // frames
        out_shape[0] = jax.ShapeDtypeStruct((frames, places, features), LOW)
        scratch += [pltpu.VMEM((8, frames, places // 8, features), LOW)] + move_scratch()
    return pl.pallas_call(
        functools.partial(qkv_back_kernel, send),
        grid=(steps,),
        in_specs=[
            pl.BlockSpec((tokens, features), lambda j: (0, j)),
            pl.BlockSpec((features, features), lambda j: (0, j)),
            whole_block(x.shape), whole_block(dx1.shape), whole_block(mod.shape),
        ],
        out_specs=[
            pl.BlockSpec(memory_space=pl.ANY) if send else whole_block((tokens, features)),
            whole_block((8, features)),
        ],
        out_shape=out_shape,
        scratch_shapes=scratch,
        compiler_params=params(48, cid),
        cost_estimate=cost(2 * tokens * weight.size, 2 * weight.size),
        name="qkv_backward",
    )(dqkv, weight, x, dx1, mod)


AHEAD = 2


def gather_pieces(shapes):
    pieces = []
    for at, (rows, columns) in enumerate(shapes):
        last = at == len(shapes) - 1
        if rows > columns // 3:
            parts = 4 if last else 2
            tall = rows // parts
            pieces += [(at, j * tall, tall, 0, columns) for j in range(parts)]
        elif columns % 256 == 0 and columns > 2048:
            wide = columns // 2
            pieces += [(at, 0, rows, j * wide, wide) for j in range(2)]
        else:
            pieces.append((at, 0, rows, 0, columns))
    return pieces


def gather_kernel(pieces, count, *refs):
    shards, partial, condition, tokens = refs[:count], *refs[count : count + 3]
    fulls = refs[count + 3 : 2 * count + 3]
    partials, conditions, moved = refs[2 * count + 3 : 2 * count + 6]
    held = refs[2 * count + 6 : 3 * count + 6]
    (
        first_sem, second_sem, rep_sem, pair_sem, local_sem, small_sem, move_sem, stay_sem,
    ) = refs[3 * count + 6 :]
    me, z = lax.axis_index("seq"), lax.axis_index("rep")
    odd = z & 1
    first, second = 2 + 2 * odd, 4 - 2 * odd

    barrier = pltpu.get_barrier_semaphore()
    for mask in range(1, 8):
        pl.semaphore_signal(barrier, inc=1, device_id={"seq": me ^ mask})
    for mask in range(1, 4):
        pl.semaphore_signal(barrier, inc=1, device_id={"rep": z ^ mask})
    pl.semaphore_wait(barrier, 10)

    small = []
    for mask in range(1, 8):
        small.append(pltpu.make_async_remote_copy(
            partial, partials.at[me], small_sem.at[0, mask], small_sem.at[1, mask],
            device_id={"seq": me ^ mask}))
    for mask in range(1, 4):
        small.append(pltpu.make_async_remote_copy(
            condition, conditions.at[z], small_sem.at[0, 7 + mask], small_sem.at[1, 7 + mask],
            device_id={"rep": z ^ mask}))
    small.append(pltpu.make_async_copy(partial, partials.at[me], small_sem.at[0, 0]))
    small.append(pltpu.make_async_copy(condition, conditions.at[z], small_sem.at[1, 0]))
    small += moves(tokens, moved, move_sem, stay_sem, me, True)
    for copy in small:
        copy.start()

    def place(owner, piece):
        at, row, rows, column, columns = piece
        return fulls[at].at[owner, pl.ds(row, rows), pl.ds(column, columns)]

    def own(piece):
        at, row, rows, column, columns = piece
        return shards[at].at[pl.ds(row, rows), pl.ds(column, columns)]

    def send(source, owner, piece, sems, at, target):
        return pltpu.make_async_remote_copy(
            source, place(owner, piece), sems.at[0, at], sems.at[1, at], device_id=target)

    firsts, pairs, others, stores = [], [], [], []
    fetches = [
        pltpu.make_async_copy(shard, hold, local_sem.at[0, at])
        for at, (shard, hold) in enumerate(zip(shards, held))
    ]
    for copy in fetches:
        copy.start()

    def begin(at):
        piece = pieces[at]
        copy = send(own(piece), me, piece, first_sem, at, {"seq": me ^ first})
        copy.start()
        firsts.append(copy)
        copy = send(own(piece), me, piece, pair_sem.at[0], at, {"seq": me ^ 1})
        copy.start()
        pairs.append(copy)

    for at in range(AHEAD):
        begin(at)
    for at, copy in enumerate(fetches):
        copy.wait()
        stores.append(pltpu.make_async_copy(held[at], fulls[at].at[me], local_sem.at[1, at]))
        stores[-1].start()

    def forward(at):
        others[at][0].wait_recv()
        others[at][1].wait_recv()
        piece = pieces[at]
        for which, mask in ((2, first ^ second), (3, second)):
            owner = me ^ mask
            copy = send(place(owner, piece), owner, piece, pair_sem.at[which], at, {"seq": me ^ 1})
            copy.start()
            pairs.append(copy)

    for at, piece in enumerate(pieces):
        firsts[at].wait_recv()
        if at + AHEAD < len(pieces):
            begin(at + AHEAD)
        owner = me ^ first
        two = [
            send(place(owner, piece), owner, piece, second_sem, at, {"seq": me ^ second}),
            send(place(owner, piece), owner, piece, rep_sem, at, {"rep": z ^ 1}),
        ]
        copy = send(place(owner, piece), owner, piece, pair_sem.at[1], at, {"seq": me ^ 1})
        for each in two + [copy]:
            each.start()
        others.append(two)
        pairs.append(copy)
        if at:
            forward(at - 1)
    forward(len(pieces) - 1)
    for copy in firsts:
        copy.wait_send()
    for two in others:
        for copy in two:
            copy.wait_send()
    for copy in pairs + stores + small:
        copy.wait()


def gather_weights(shards, partial, condition, tokens, cid):
    shapes = [shard.shape for shard in shards]
    pieces = gather_pieces(shapes)
    count = len(shards)
    dma = pltpu.SemaphoreType.DMA
    size = len(pieces)
    outs = [jax.ShapeDtypeStruct((8,) + shape, jnp.bfloat16) for shape in shapes]
    outs.append(jax.ShapeDtypeStruct((8,) + partial.shape, partial.dtype))
    outs.append(jax.ShapeDtypeStruct((4,) + condition.shape, condition.dtype))
    frames, places, features = tokens.shape
    outs.append(jax.ShapeDtypeStruct((8, frames, places // 8, features), tokens.dtype))
    got = pl.pallas_call(
        functools.partial(gather_kernel, pieces, count),
        out_shape=outs,
        in_specs=[pl.BlockSpec(memory_space=pl.ANY)] * (count + 3),
        out_specs=[pl.BlockSpec(memory_space=pl.ANY)] * len(outs),
        scratch_shapes=[pltpu.VMEM(shape, jnp.bfloat16) for shape in shapes]
        + [
            dma((2, size)), dma((2, size)), dma((2, size)), dma((4, 2, size)), dma((2, count)), dma((2, 11)),
        ]
        + move_scratch(),
        compiler_params=pltpu.CompilerParams(
            collective_id=cid, has_side_effects=True,
        ),
        name="gather_weights",
    )(*shards, partial, condition, tokens)
    fulls = [full.reshape(-1, full.shape[2]) for full in got[:count]]
    return fulls, got[count:]


SLOTS = 3
BACK = 4


def reduce_kernel(layers, rows, width, edge, *refs):
    ins, mods = refs[: 8 * layers], refs[8 * layers]
    outs, every_mod = refs[8 * layers + 1 : 12 * layers + 1], refs[12 * layers + 1]
    (
        left, right, away, pair_in, part,
        first_in_a, first_in_b, mid_a, mid_b, second_in_a, second_in_b,
        clip, rep_in, joined, inner_in, final, back_in, wide,
        mod_in, load_sem, pair_sem, link_sem, rep_sem, back_sem, store_sem, mod_sem,
    ) = refs[12 * layers + 2 :]
    me, z = lax.axis_index("seq"), lax.axis_index("rep")
    core, x, y = me & 1, (me >> 1) & 1, (me >> 2) & 1
    inner = (z == 1) | (z == 2)
    outer = (z == 0) | (z == 3)

    barrier = pltpu.get_barrier_semaphore()
    for mask in range(1, 8):
        pl.semaphore_signal(barrier, inc=1, device_id={"seq": me ^ mask})
    for mask in range(1, 4):
        pl.semaphore_signal(barrier, inc=1, device_id={"rep": z ^ mask})
    pl.semaphore_wait(barrier, 10)

    mod_copies = [
        pltpu.make_async_remote_copy(
            mods, mod_in.at[me], mod_sem.at[0, mask], mod_sem.at[1, mask],
            device_id={"seq": me ^ mask},
        )
        for mask in range(1, 8)
    ]
    clip_copies = [
        pltpu.make_async_remote_copy(
            every_mod.at[z], every_mod.at[z], mod_sem.at[0, 7 + mask], mod_sem.at[1, 7 + mask],
            device_id={"rep": z ^ mask},
        )
        for mask in range(1, 4)
    ]
    for copy in mod_copies:
        copy.start()
    mod_in[me] = mods[...]

    spans, start = [], 0
    for layer in range(layers):
        for kind in range(4):
            shape = outs[4 * layer + kind].shape
            count = shape[0] // rows * (shape[1] // width)
            spans.append((layer, kind, start, count))
            start += count
    total = start

    def loads(block, slot):
        for layer, kind, first, count in spans:
            @pl.when((block >= first) & (block < first + count))
            def _():
                source = ins[8 * layer + kind]
                if kind == 3:
                    source = source.at[:, :, block - first]
                pltpu.make_async_copy(source, left.at[slot], load_sem.at[0, slot]).start()
                source = ins[8 * layer + 4 + kind]
                if kind in (0, 2):
                    column = pl.multiple_of((block - first) * width, width)
                    source = source.at[:, pl.ds(column, width)]
                pltpu.make_async_copy(source, right.at[slot], load_sem.at[1, slot]).start()

    def wait_loads(slot):
        pltpu.make_async_copy(ins[0], left.at[slot], load_sem.at[0, slot]).wait()
        pltpu.make_async_copy(ins[5], right.at[slot], load_sem.at[1, slot]).wait()

    def store(block, slot):
        for layer, kind, first, count in spans:
            @pl.when((block >= first) & (block < first + count))
            def _():
                target = outs[4 * layer + kind]
                if kind == 3:
                    row = pl.multiple_of((block - first) * rows, rows)
                    target = target.at[pl.ds(row, rows)]
                elif kind in (0, 2):
                    column = pl.multiple_of((block - first) * width, width)
                    target = target.at[:, pl.ds(column, width)]
                pltpu.make_async_copy(wide.at[slot], target, store_sem.at[slot]).start()

    def to_seq(source, target, which, slot, mask):
        return pltpu.make_async_remote_copy(
            source, target, link_sem.at[0, which, slot], link_sem.at[1, which, slot],
            device_id={"seq": me ^ mask},
        )

    def pair_copy(t):
        slot = lax.rem(t, 2)
        return pltpu.make_async_remote_copy(
            away, pair_in.at[slot], pair_sem.at[0, slot], pair_sem.at[1, slot],
            device_id={"seq": me ^ 1},
        )

    def first_copies(t):
        slot, block = lax.rem(t, SLOTS), lax.rem(t - 1, SLOTS)
        return (
            to_seq(part.at[block, :, 1 - x, :, pl.ds(0, edge)], first_in_a.at[slot], 0, slot, 2),
            to_seq(
                part.at[block, 1 - y, :, :, pl.ds(edge, width - edge)],
                first_in_b.at[slot], 1, slot, 4,
            ),
        )

    def second_copies(t):
        slot, block = lax.rem(t, SLOTS), lax.rem(t, 2)
        return (
            to_seq(mid_a.at[block, 1 - y], second_in_a.at[slot], 2, slot, 4),
            to_seq(mid_b.at[block, 1 - x], second_in_b.at[slot], 3, slot, 2),
        )

    def rep_copy(t):
        slot = lax.rem(t, SLOTS)
        return pltpu.make_async_remote_copy(
            clip.at[lax.rem(t, 2)], rep_in.at[slot], rep_sem.at[0, 0, slot], rep_sem.at[1, 0, slot],
            device_id={"rep": z ^ 1},
        )

    def inner_copy(t):
        slot = lax.rem(t, SLOTS)
        return pltpu.make_async_remote_copy(
            joined.at[lax.rem(t, 2)], inner_in.at[slot],
            rep_sem.at[0, 1, slot], rep_sem.at[1, 1, slot],
            device_id={"rep": z ^ 3},
        )

    def back_copy(t):
        slot = lax.rem(t, BACK)
        return pltpu.make_async_remote_copy(
            final.at[lax.rem(t, 2)], back_in.at[slot], back_sem.at[0, slot], back_sem.at[1, slot],
            device_id={"rep": z ^ 1},
        )

    loads(0, 0)

    def turn(t, carry):
        def stage(back):
            return (t >= back) & (t < total + back)

        now2, was2 = lax.rem(t, 2), lax.rem(t + 1, 2)
        was3 = lax.rem(t + 2, SLOTS)

        @pl.when(t + 1 < total)
        def _():
            loads(t + 1, was2)

        @pl.when(stage(1))
        def _():
            for copy in first_copies(t):
                copy.start()

        @pl.when(stage(2))
        def _():
            block = lax.rem(t + 1, SLOTS)
            for at in range(2):
                mid_a[now2, at] = part[block, at, x, :, :edge] + first_in_a[was3, at]
                mid_b[now2, at] = part[block, y, at, :, edge:] + first_in_b[was3, at]
            for copy in second_copies(t):
                copy.start()

        @pl.when(stage(3))
        def _():
            clip[now2, :, :edge] = mid_a[was2, y] + second_in_a[was3]
            clip[now2, :, edge:] = mid_b[was2, x] + second_in_b[was3]

            @pl.when(outer)
            def _():
                rep_copy(t).start()

        @pl.when(stage(4) & inner)
        def _():
            joined[now2] = clip[was2] + rep_in[was3]
            inner_copy(t).start()

        @pl.when(stage(5) & inner)
        def _():
            final[now2] = joined[was2] + inner_in[was3]
            back_copy(t).start()

        @pl.when(stage(6))
        def _():
            @pl.when(inner)
            def _():
                wide[now2] = final[was2].astype(jnp.float32)

            @pl.when(outer)
            def _():
                wide[now2] = back_in[lax.rem(t + 3, BACK)].astype(jnp.float32)

            store(t - 6, now2)

        @pl.when(t < total)
        def _():
            wait_loads(now2)
            slot3 = lax.rem(t, SLOTS)

            def product(which):
                def columns(j, carry):
                    at = pl.ds(pl.multiple_of(j * (width // 3), width // 3), width // 3)
                    block = left[now2, :, which]
                    four, _, depth = block.shape
                    got = jnp.dot(
                        block.reshape(four * rows, depth), right[now2, :, at],
                        preferred_element_type=jnp.float32,
                    ).astype(jnp.bfloat16)
                    return at, got.reshape(four, rows, width // 3)
                return columns

            def away_columns(j, carry):
                at, got = product(1 - core)(j, carry)
                away[:, :, at] = got
                return carry

            lax.fori_loop(0, 3, away_columns, 0)
            pair_copy(t).start()

            def kept_columns(j, carry):
                at, got = product(core)(j, carry)
                part[slot3, 0, :, :, at] = got[:2]
                part[slot3, 1, :, :, at] = got[2:]
                return carry

            lax.fori_loop(0, 3, kept_columns, 0)
            pair_copy(t).wait()

            def add(j, carry):
                part[slot3, j // 2, j % 2] = part[slot3, j // 2, j % 2] + pair_in[now2, j]
                return carry

            lax.fori_loop(0, 4, add, 0)

        @pl.when(stage(1))
        def _():
            for copy in first_copies(t):
                copy.wait()

        @pl.when(stage(2))
        def _():
            for copy in second_copies(t):
                copy.wait()

        @pl.when(stage(3))
        def _():
            @pl.when(outer)
            def _():
                rep_copy(t).wait_send()

            @pl.when(inner)
            def _():
                rep_copy(t).wait_recv()

        @pl.when(stage(4) & inner)
        def _():
            inner_copy(t).wait()

        @pl.when(stage(5))
        def _():
            @pl.when(inner)
            def _():
                back_copy(t).wait_send()

            @pl.when(outer)
            def _():
                back_copy(t).wait_recv()

        @pl.when(stage(6))
        def _():
            pltpu.make_async_copy(wide.at[now2], outs[1], store_sem.at[now2]).wait()

        return carry

    lax.fori_loop(0, 2, turn, 0)
    for copy in mod_copies:
        copy.wait()
    mod_total = mod_in[0].astype(jnp.float32)
    for device in range(1, 8):
        mod_total += mod_in[device].astype(jnp.float32)
    every_mod[z] = mod_total.astype(every_mod.dtype)
    for copy in clip_copies:
        copy.start()
    lax.fori_loop(2, total + 6, turn, 0)
    for copy in clip_copies:
        copy.wait()


def reduce_grads(layers, mods, cid):
    tokens = layers[0][4].shape[0]
    rows, width = layers[0][0].shape[2], layers[0][5].shape[1]
    edge = width * 5 // 9 // 128 * 128
    low = jnp.bfloat16
    outs = []
    for ops in layers:
        for kind in range(4):
            tall = ops[kind].shape[2] if kind == 3 else 1
            outs.append(jax.ShapeDtypeStruct((tall * rows, ops[4 + kind].shape[1]), jnp.float32))
    outs.append(jax.ShapeDtypeStruct((4,) + mods.shape, mods.dtype))
    vm = pltpu.VMEM
    dma = pltpu.SemaphoreType.DMA
    flops = sum(2 * tokens * 8 * o.size for o in outs[:-1])
    got = pl.pallas_call(
        functools.partial(reduce_kernel, len(layers), rows, width, edge),
        out_shape=outs,
        in_specs=[pl.BlockSpec(memory_space=pl.ANY)] * (8 * len(layers))
        + [pl.BlockSpec(memory_space=vm)],
        out_specs=[pl.BlockSpec(memory_space=pl.ANY)] * (4 * len(layers))
        + [pl.BlockSpec(memory_space=vm)],
        scratch_shapes=[
            vm((2, 4, 2, rows, tokens), low),
            vm((2, tokens, width), low),
            vm((4, rows, width), low),
            vm((2, 4, rows, width), low),
            vm((SLOTS, 2, 2, rows, width), low),
            vm((SLOTS, 2, rows, edge), low),
            vm((SLOTS, 2, rows, width - edge), low),
            vm((2, 2, rows, edge), low),
            vm((2, 2, rows, width - edge), low),
            vm((SLOTS, rows, edge), low),
            vm((SLOTS, rows, width - edge), low),
            vm((2, rows, width), low),
            vm((SLOTS, rows, width), low),
            vm((2, rows, width), low),
            vm((SLOTS, rows, width), low),
            vm((2, rows, width), low),
            vm((BACK, rows, width), low),
            vm((2, rows, width), jnp.float32),
            vm((8,) + mods.shape, mods.dtype),
            dma((2, 2)),
            dma((2, 2)),
            dma((2, 4, SLOTS)),
            dma((2, 2, SLOTS)),
            dma((2, BACK)),
            dma((2,)),
            dma((2, 11)),
        ],
        compiler_params=pltpu.CompilerParams(
            collective_id=cid, has_side_effects=True, vmem_limit_bytes=48 << 20
        ),
        cost_estimate=pl.CostEstimate(flops=flops, bytes_accessed=4 * sum(o.size for o in outs), transcendentals=0),
        name="reduce_grads",
    )(*[op for ops in layers for op in ops], mods)
    return [tuple(got[4 * at : 4 * at + 4]) for at in range(len(layers))], got[-1]


def reduce_operands(lefts, rights):
    features = rights[1].shape[1]
    shaped = []
    for left in lefts:
        tall, tokens = left.shape[0] // features, left.shape[1]
        shape = (4, 2, features // 8, tokens) if tall == 1 else (4, 2, tall, features // 8, tokens)
        shaped.append(left.reshape(shape))
    return (*shaped, *rights)


def layer_forward(x, mod, weights, spatial, groups, frames=None, cids=(None, None)):
    qkv_w, out_w, up_w, down_w = weights
    qkv, h_turned = qkv_forward(x, mod, qkv_w)
    prob, o_turned, x1, branch, h2, h2_turned, *other = attention_forward(
        qkv, x, mod, out_w, spatial, groups, cids[0]
    )
    z_turned, slope, out, mlp = mlp_forward(x1, h2, mod, up_w, down_w, frames, cids[1])
    lefts = (h_turned, o_turned, h2_turned, z_turned)
    return out, (qkv, prob, other[0] if spatial else None, x1, branch, slope, mlp), lefts


def layer_backward(g, x, mod, weights, kept, lefts, spatial, done=None, frames=None, cids=(None,) * 3):
    qkv_w, out_w, up_w, down_w = weights
    qkv, prob, other, x1, branch, slope, mlp = kept
    du, df, dx1, da, sums, *moved = mlp_backward(
        g, x1, branch, mlp, mod, up_w, down_w, slope, done, cids[0]
    )
    dqkv = attention_backward(da, qkv, prob, out_w, other, spatial, cids[1])
    dx, last_sums = qkv_backward(dqkv, qkv_w, x, dx1, mod, frames, cids[2])
    mod_grad = jnp.concatenate([last_sums[:2], sums[:4]], 0).reshape(1, -1)
    return dx, moved, mod_grad, reduce_operands(lefts, (dqkv, da, du, df))


def fused_device(frames_in, conditioning, shards, partial_mod, cotangent):
    _, _, frames, places, features = frames_in.shape
    tokens = frames * places
    low_cotangent = cotangent.reshape(frames, places, features).astype(LOW)
    weights, (partials, conditions, g_two) = gather_weights(
        shards, partial_mod.reshape(-1, LANES), conditioning.reshape(-1, LANES), low_cotangent, 0
    )
    modulation = jnp.sum(partials, 0).reshape(2, 6, features)
    mod_one, mod_two = modulation[0], modulation[1]
    weights_one, weights_two = weights[:4], weights[4:]
    x_one = frames_in.reshape(tokens, features)
    x_two, kept_one, lefts_one = layer_forward(
        x_one, mod_one, weights_one, True, frames, frames, (2, 4)
    )
    x_two = x_two.reshape(tokens, features)
    y_two, kept_two, lefts_two = layer_forward(x_two, mod_two, weights_two, False, 2)
    g_one, (block_out,), mod_grad_two, operands_two = layer_backward(
        g_two.reshape(tokens, features), x_two, mod_two, weights_two, kept_two, lefts_two, False,
        y_two.reshape(g_two.shape), frames, (5, None, 6),
    )
    input_grad, _, mod_grad_one, operands_one = layer_backward(
        g_one.reshape(tokens, features), x_one, mod_one, weights_one, kept_one, lefts_one, True,
        cids=(None, 3, None),
    )
    mod_grads = jnp.concatenate([mod_grad_one, mod_grad_two], 1).astype(LOW)
    (grads_two, grads_one), every_mod = reduce_grads(
        [operands_two, operands_one], mod_grads.reshape(-1, LANES), 1
    )
    every_mod = every_mod.reshape(-1, mod_grads.shape[1])
    return (
        block_out.astype(WIDE), input_grad, grads_one, grads_two, every_mod,
        conditions.reshape(-1, features),
    )


def per_device(
    frames_in,
    conditioning,
    mod_first,
    qkv_first,
    out_first,
    up_first,
    down_first,
    mod_second,
    qkv_second,
    out_second,
    up_second,
    down_second,
    cotangent,
):
    clip_count, _, frame_dev, half_places, features = frames_in.shape
    fused = lax.axis_size("seq") == 8 and lax.axis_size("rep") == 4 and clip_count == 1
    row_count = mod_first.shape[0]
    row_start = lax.axis_index("seq") * row_count
    mod_width = mod_first.shape[1]
    rows_of = lambda whole: lax.dynamic_slice_in_dim(whole, row_start, row_count, 1)
    silu_local = rows_of(jax.nn.silu(conditioning)).astype(jnp.bfloat16)
    partial_mod = jnp.concatenate(
        [
            jnp.dot(silu_local, mod_first, preferred_element_type=jnp.float32),
            jnp.dot(silu_local, mod_second, preferred_element_type=jnp.float32),
        ],
        1,
    )
    shards = (
        qkv_first, out_first, up_first, down_first,
        qkv_second, out_second, up_second, down_second,
    )
    if fused:
        block_out, stream_grad, grads_one, grads_two, every_mod, conditions = fused_device(
            frames_in, conditioning, shards, partial_mod, cotangent
        )
        every_silu = rows_of(jax.nn.silu(conditions)).astype(jnp.bfloat16)
        mod_total = lax.dynamic_slice_in_dim(every_mod, lax.axis_index("rep"), 1, 0)
    else:
        weights = [lax.all_gather(shard, "seq", axis=0, tiled=True) for shard in shards]
        modulation = lax.psum(partial_mod, "seq")
        every_silu = lax.all_gather(silu_local, "rep", axis=0, tiled=True)
        mod_one, mod_two = modulation[:, :mod_width], modulation[:, mod_width:]
        weights_one, weights_two = weights[:4], weights[4:]
        start_stream = frames_in.reshape(clip_count, frame_dev, half_places, features).astype(
            jnp.float32
        )
        spatial_out, state_one = forward_layer(start_stream, mod_one, weights_one, True)
        placed = to_places(spatial_out)
        temporal_out, state_two = forward_layer(placed, mod_two, weights_two, False)
        block_out = to_frames(temporal_out, frame_dev)
        cotangent_sites = to_places(
            cotangent.reshape(clip_count, frame_dev, half_places, features)
        )
        placed_grad, mod_grad_two, pairs_two = backward_layer(
            cotangent_sites, placed, mod_two, weights_two, state_two, False
        )
        spatial_grad = to_frames(placed_grad, frame_dev)
        stream_grad, mod_grad_one, pairs_one = backward_layer(
            spatial_grad, start_stream, mod_one, weights_one, state_one, True
        )
        mod_grads = jnp.concatenate([mod_grad_one, mod_grad_two], 1).astype(jnp.bfloat16)
        grads_two, grads_one = layer_grads(pairs_two), layer_grads(pairs_one)
        mod_total = lax.psum(mod_grads, "seq").astype(jnp.bfloat16)
        every_mod = lax.all_gather(mod_total, "rep", axis=0, tiled=True)
    low_one, low_two = mod_total[:, :mod_width], mod_total[:, mod_width:]
    mod_weight_one = jnp.einsum(
        "cd,ce->de", every_silu, every_mod[:, :mod_width], preferred_element_type=jnp.float32
    )
    mod_weight_two = jnp.einsum(
        "cd,ce->de", every_silu, every_mod[:, mod_width:], preferred_element_type=jnp.float32
    )
    silu_grad = jnp.einsum("ce,de->cd", low_one, mod_first, preferred_element_type=jnp.float32)
    silu_grad = silu_grad + jnp.einsum(
        "ce,de->cd", low_two, mod_second, preferred_element_type=jnp.float32
    )
    condition_grad = jax.vjp(jax.nn.silu, rows_of(conditioning))[1](silu_grad)[0]
    out_shape = (clip_count, 1, frame_dev, half_places, features)
    return (
        block_out.reshape(out_shape),
        stream_grad.reshape(out_shape),
        condition_grad,
        mod_weight_one,
        *grads_one,
        mod_weight_two,
        *grads_two,
    )


def solution(mesh):
    return jax.shard_map(
        per_device,
        mesh=mesh,
        in_specs=(
            P("rep", "seq", None, None, None),
            P("rep", None),
            P("seq", None),
            P("seq", None),
            P("seq", None),
            P("seq", None),
            P("seq", None),
            P("seq", None),
            P("seq", None),
            P("seq", None),
            P("seq", None),
            P("seq", None),
            P("rep", "seq", None, None, None),
        ),
        out_specs=(
            P("rep", "seq", None, None, None),
            P("rep", "seq", None, None, None),
            P("rep", "seq"),
            P("seq", None),
            P("seq", None),
            P("seq", None),
            P("seq", None),
            P("seq", None),
            P("seq", None),
            P("seq", None),
            P("seq", None),
            P("seq", None),
            P("seq", None),
        ),
        check_vma=False,
    )
```

```python
import functools
import math

import jax
import jax.numpy as jnp
from jax import lax
from jax.experimental import pallas as pl
from jax.experimental.pallas import tpu as pltpu
from jax.sharding import PartitionSpec as P

HEADS = 16
HEAD_WIDTH = 72


norm_epsilon = 1e-06


def from_partner(block, axis, apart):
    count = lax.axis_size(axis)
    route = []
    for low in range(count):
        high = low | 1 << apart
        if high != low and high < count:
            route += [(low, high), (high, low)]
    return lax.ppermute(block, axis, route)


def shortened(x):
    return jax.tree.map(lambda a: a.astype(jnp.bfloat16) if a.dtype == jnp.float32 else a, x)


def layer_mod(stream, shift_part, scale_part):
    row_mean = jnp.mean(stream, axis=-1, keepdims=True)
    centred = stream - row_mean
    row_var = jnp.mean(centred * centred, axis=-1, keepdims=True)
    return centred * lax.rsqrt(row_var + norm_epsilon) * (1.0 + scale_part) + shift_part


def gelu_tanh(pre_value):
    return jax.nn.gelu(pre_value, approximate=True)


def project(left_operand, right_operand):
    return jnp.einsum(
        "csld,de->csle", left_operand, right_operand, preferred_element_type=jnp.float32
    )


def project_back(incoming, right_operand):
    return jnp.einsum("csle,de->csld", incoming, right_operand, preferred_element_type=jnp.float32)


def mod_parts(modulation):
    return [segment[:, None, None, :] for segment in jnp.split(modulation, 6, axis=-1)]


def partner_values(stacked):
    return from_partner(stacked, "seq", 0)


def partner_grads(stacked):
    return from_partner(stacked.astype(jnp.bfloat16), "seq", 0).astype(stacked.dtype)


def to_places(stream):
    clip_count, frame_dev, half_places, features = stream.shape
    devices = lax.axis_size("seq")
    place_part = half_places // devices
    exchanged = lax.all_to_all(
        stream.reshape(1, clip_count, frame_dev, devices, place_part, features).astype(
            jnp.bfloat16
        ),
        "seq",
        split_axis=3,
        concat_axis=0,
        tiled=True,
    ).astype(jnp.float32)
    exchanged = exchanged.reshape(devices // 2, 2, clip_count, frame_dev, place_part, features)
    exchanged = jnp.transpose(exchanged, (2, 1, 4, 0, 3, 5))
    return exchanged.reshape(clip_count, 2 * place_part, devices // 2 * frame_dev, features)


def to_frames(stream, frame_dev):
    clip_count, place_count, frame_total, features = stream.shape
    devices = lax.axis_size("seq")
    place_part = place_count // 2
    arranged = stream.reshape(clip_count, 2, place_part, devices // 2, frame_dev, features)
    arranged = jnp.transpose(arranged, (3, 1, 0, 4, 2, 5)).reshape(
        devices, clip_count, frame_dev, 1, place_part, features
    )
    exchanged = lax.all_to_all(
        shortened(arranged), "seq", split_axis=0, concat_axis=3, tiled=True
    ).astype(arranged.dtype)
    return exchanged.reshape(clip_count, frame_dev, devices * place_part, features)


def forward_layer(stream, modulation, weights, spatial):
    qkv_w, out_w, up_w, down_w = weights
    shift_attn, scale_attn, gate_attn, shift_mlp, scale_mlp, gate_mlp = mod_parts(modulation)
    clip_count, seq_count, seq_len, features = stream.shape
    normed = layer_mod(stream, shift_attn, scale_attn).astype(jnp.bfloat16)
    projected = project(normed, qkv_w).astype(jnp.bfloat16)
    queries, keys_all, values_all = jnp.split(projected, 3, axis=-1)
    if spatial:
        remote = partner_values(jnp.stack([keys_all, values_all]))
        keys_all = jnp.concatenate([keys_all, remote[0]], axis=2)
        values_all = jnp.concatenate([values_all, remote[1]], axis=2)
    key_len = keys_all.shape[2]
    queries = queries.reshape(clip_count, seq_count, seq_len, HEADS, HEAD_WIDTH)
    keys_all = keys_all.reshape(clip_count, seq_count, key_len, HEADS, HEAD_WIDTH)
    values_all = values_all.reshape(clip_count, seq_count, key_len, HEADS, HEAD_WIDTH)
    scores = jnp.einsum(
        "cslhe,csmhe->cshlm", queries, keys_all, preferred_element_type=jnp.float32
    ) * HEAD_WIDTH ** (-0.5)
    peak_score = jnp.max(scores, axis=-1, keepdims=True)
    scaled_exp = jnp.exp(scores - peak_score)
    attention = scaled_exp / jnp.sum(scaled_exp, axis=-1, keepdims=True)
    attention_low = attention.astype(jnp.bfloat16)
    attended = jnp.einsum(
        "cshlm,csmhe->cslhe", attention_low, values_all, preferred_element_type=jnp.float32
    )
    attended = attended.astype(jnp.bfloat16).reshape(clip_count, seq_count, seq_len, features)
    branch = project(attended, out_w)
    middle = stream + gate_attn * branch
    normed_mid = layer_mod(middle, shift_mlp, scale_mlp).astype(jnp.bfloat16)
    hidden_pre = project(normed_mid, up_w)
    hidden = gelu_tanh(hidden_pre).astype(jnp.bfloat16)
    mlp_out = project(hidden, down_w)
    result = middle + gate_mlp * mlp_out
    kept_state = (
        normed,
        queries,
        keys_all,
        values_all,
        attention,
        attention_low,
        attended,
        branch,
        middle,
        normed_mid,
        hidden_pre,
        hidden,
        mlp_out,
    )
    return (result, kept_state)


def backward_layer(result_grad, stream, modulation, weights, kept_state, spatial):
    qkv_w, out_w, up_w, down_w = weights
    (
        normed,
        queries,
        keys_all,
        values_all,
        attention,
        attention_low,
        attended,
        branch,
        middle,
        normed_mid,
        hidden_pre,
        hidden,
        mlp_out,
    ) = kept_state
    shift_attn, scale_attn, gate_attn, shift_mlp, scale_mlp, gate_mlp = mod_parts(modulation)
    clip_count, seq_count, seq_len, features = stream.shape
    gate_mlp_grad = jnp.sum(result_grad * mlp_out, axis=(1, 2))
    mlp_grad = (gate_mlp * result_grad).astype(jnp.bfloat16)
    hidden_grad = project_back(mlp_grad, down_w)
    pre_grad = jax.vjp(gelu_tanh, hidden_pre)[1](hidden_grad)[0].astype(jnp.bfloat16)
    normed_mid_grad = project_back(pre_grad, up_w)
    middle_ln_grad, shift_mlp_grad, scale_mlp_grad = jax.vjp(
        layer_mod, middle, shift_mlp, scale_mlp
    )[1](normed_mid_grad)
    middle_grad = result_grad + middle_ln_grad
    gate_attn_grad = jnp.sum(middle_grad * branch, axis=(1, 2))
    branch_grad = (gate_attn * middle_grad).astype(jnp.bfloat16)
    attended_grad = project_back(branch_grad, out_w).astype(jnp.bfloat16)
    attended_grad = attended_grad.reshape(clip_count, seq_count, seq_len, HEADS, HEAD_WIDTH)
    attention_grad = jnp.einsum(
        "cslhe,csmhe->cshlm", attended_grad, values_all, preferred_element_type=jnp.float32
    )
    scores_grad = attention * (
        attention_grad - jnp.sum(attention_grad * attention, axis=-1, keepdims=True)
    )
    scores_grad = scores_grad.astype(jnp.bfloat16)
    inv_root = HEAD_WIDTH ** (-0.5)
    queries_grad = (
        jnp.einsum("cshlm,csmhe->cslhe", scores_grad, keys_all, preferred_element_type=jnp.float32)
        * inv_root
    )
    keys_grad = (
        jnp.einsum("cshlm,cslhe->csmhe", scores_grad, queries, preferred_element_type=jnp.float32)
        * inv_root
    )
    values_grad = jnp.einsum(
        "cshlm,cslhe->csmhe", attention_low, attended_grad, preferred_element_type=jnp.float32
    )
    if spatial:
        returned = partner_grads(
            jnp.stack([keys_grad[:, :, seq_len:], values_grad[:, :, seq_len:]])
        )
        keys_grad = keys_grad[:, :, :seq_len] + returned[0]
        values_grad = values_grad[:, :, :seq_len] + returned[1]
    qkv_grad = jnp.concatenate(
        [
            component.reshape(clip_count, seq_count, seq_len, features)
            for component in (queries_grad, keys_grad, values_grad)
        ],
        axis=-1,
    )
    qkv_grad = qkv_grad.astype(jnp.bfloat16)
    normed_grad = project_back(qkv_grad, qkv_w)
    stream_ln_grad, attention_shift_gradient, scale_attn_grad = jax.vjp(
        layer_mod, stream, shift_attn, scale_attn
    )[1](normed_grad)
    stream_grad = middle_grad + stream_ln_grad
    mod_grad = jnp.concatenate(
        [
            attention_shift_gradient.reshape(clip_count, features),
            scale_attn_grad.reshape(clip_count, features),
            gate_attn_grad,
            shift_mlp_grad.reshape(clip_count, features),
            scale_mlp_grad.reshape(clip_count, features),
            gate_mlp_grad,
        ],
        axis=-1,
    )
    grad_pairs = (
        (normed, qkv_grad),
        (attended, branch_grad),
        (normed_mid, pre_grad),
        (hidden, mlp_grad),
    )
    return (stream_grad, mod_grad, grad_pairs)


def bit_count(axis):
    return lax.axis_size(axis).bit_length() - 1


def swap(block, axis, bit):
    count = lax.axis_size(axis)
    return lax.ppermute(block, axis, [(at, at ^ (1 << bit)) for at in range(count)])


def bit_of(axis, bit):
    return (lax.axis_index(axis) >> bit) & 1


def pick(block, which, axis):
    return lax.dynamic_index_in_dim(block, which, axis, keepdims=False)


def spread_rows_out(left_turned, right_operand, flipped):
    bits = bit_count("seq")
    total_rows, tokens = left_turned.shape
    rows = total_rows >> bits
    halves = left_turned.reshape(1 << (bits - 1), 2, rows, tokens)
    core = bit_of("seq", 0)

    def product(which):
        left = pick(halves, which, 1).reshape(-1, tokens)
        return jnp.dot(left, right_operand, preferred_element_type=jnp.float32).astype(
            jnp.bfloat16
        )

    arrived = swap(product(1 - core), "seq", 0)
    held = product(core)
    left_bits = list(range(bits - 1, 0, -1))
    shape = [2] * (bits - 1) + [rows, right_operand.shape[1]]
    held = held.reshape(shape)
    arrived = arrived.reshape(shape)
    order = list(left_bits) if flipped else left_bits[::-1]
    for bit in order:
        at = left_bits.index(bit)
        mine = bit_of("seq", bit)
        away = pick(held, 1 - mine, at).astype(jnp.float32) + pick(arrived, 1 - mine, at)
        kept = pick(held, mine, at).astype(jnp.float32) + pick(arrived, mine, at)
        arrived = swap(away.astype(jnp.bfloat16), "seq", bit)
        held = kept.astype(jnp.bfloat16)
        left_bits.remove(bit)
    return held.astype(jnp.float32) + arrived


def rep_sum(block, axis):
    bits = bit_count("rep")
    held = block.astype(jnp.bfloat16)
    for bit in range(bits):
        mine = bit_of("rep", bit)
        low, high = jnp.split(held, 2, axis)
        away = jnp.where(mine == 0, high, low)
        kept = jnp.where(mine == 0, low, high)
        held = (kept.astype(jnp.float32) + swap(away, "rep", bit)).astype(jnp.bfloat16)
    for bit in reversed(range(bits)):
        mine = bit_of("rep", bit)
        other = swap(held, "rep", bit)
        low = jnp.where(mine == 0, held, other)
        high = jnp.where(mine == 0, other, held)
        held = jnp.concatenate([low, high], axis)
    return held.astype(jnp.float32)


def turned(operand):
    return operand.reshape(-1, operand.shape[-1]).T


def flat(operand):
    return operand.reshape(-1, operand.shape[-1])


def cut(width, parts, of):
    return width * parts // of // 128 * 128


def down_grad(pair):
    left, right = turned(pair[0]), flat(pair[1])
    edge = cut(right.shape[1], 5, 9)
    return jnp.concatenate(
        [
            rep_sum(spread_rows_out(left, right[:, :edge], False), 0),
            rep_sum(spread_rows_out(left, right[:, edge:], True), 0),
        ],
        1,
    )


def up_grad(pair):
    left, right = turned(pair[0]), flat(pair[1])
    edge = cut(right.shape[1], 4, 9)
    return jnp.concatenate(
        [
            rep_sum(spread_rows_out(left, right[:, :edge], False), 1),
            rep_sum(spread_rows_out(left, right[:, edge:], True), 1),
        ],
        1,
    )


def attention_grads(qkv_pair, out_pair):
    left, right = turned(qkv_pair[0]), flat(qkv_pair[1])
    width = right.shape[1]
    edge = cut(width, 16, 27)
    first = rep_sum(spread_rows_out(left, right[:, :edge], False), 1)
    second = spread_rows_out(left, right[:, edge:], True)
    third = spread_rows_out(turned(out_pair[0]), flat(out_pair[1]), True)
    joined = rep_sum(jnp.concatenate([second, third], 1), 1)
    return (
        jnp.concatenate([first, joined[:, : width - edge]], 1),
        joined[:, width - edge :],
    )


def layer_grads(grad_pairs):
    qkv_pair, out_pair, up_pair, down_pair = grad_pairs
    down = down_grad(down_pair)
    up = up_grad(up_pair)
    qkv, out = attention_grads(qkv_pair, out_pair)
    return (qkv, out, up, down)


AHEAD = 2


def gather_pieces(shapes):
    features = math.gcd(*(columns for _, columns in shapes), 8 * shapes[0][0])
    rows_of = features // 8
    return rows_of, features, [
        (at, row, column)
        for at, (rows, columns) in enumerate(shapes)
        for row in range(0, rows, rows_of)
        for column in range(0, columns, features)
    ]


class Gather:
    def __init__(self, shapes, refs):
        count = len(shapes)
        self.count = count
        self.least, self.wide, self.pieces = gather_pieces(shapes)
        self.shards, self.fulls = refs[0], refs[1]
        self.held = refs[2][: count // 2]
        self.first_sem, self.second_sem, self.rep_sem, self.pair_sem, self.local_sem = refs[2][
            count // 2 :
        ]
        self.me, self.z = lax.axis_index("seq"), lax.axis_index("rep")
        odd = self.z & 1
        self.first, self.second = 2 + 2 * odd, 4 - 2 * odd

    @staticmethod
    def scratch(shapes):
        size = len(gather_pieces(shapes)[2])
        dma = pltpu.SemaphoreType.DMA
        half = shapes[: len(shapes) // 2]
        return [pltpu.VMEM(shape, jnp.bfloat16) for shape in half] + [
            dma((2, size)), dma((2, size)), dma((2, size)), dma((4, 2, size)), dma((2, len(shapes))),
        ]

    @staticmethod
    def outs(shapes):
        return [jax.ShapeDtypeStruct((8,) + shape, jnp.bfloat16) for shape in shapes]

    def place(self, owner, at):
        weight, row, column = self.pieces[at]
        return self.fulls[weight].at[owner, pl.ds(row, self.least), pl.ds(column, self.wide)]

    def own(self, at):
        weight, row, column = self.pieces[at]
        return self.shards[weight].at[pl.ds(row, self.least), pl.ds(column, self.wide)]

    def to_seq(self, source, owner, at, sems, mask):
        return pltpu.make_async_remote_copy(
            source, self.place(owner, at), sems.at[0, at], sems.at[1, at],
            device_id={"seq": self.me ^ mask},
        )

    def first_copy(self, at):
        return self.to_seq(self.own(at), self.me, at, self.first_sem, self.first)

    def second_copy(self, at):
        owner = self.me ^ self.first
        return self.to_seq(self.place(owner, at), owner, at, self.second_sem, self.second)

    def rep_copy(self, at):
        owner = self.me ^ self.first
        return pltpu.make_async_remote_copy(
            self.place(owner, at), self.place(owner, at), self.rep_sem.at[0, at], self.rep_sem.at[1, at],
            device_id={"rep": self.z ^ 1},
        )

    def pair_copy(self, which, at):
        if which == 0:
            return self.to_seq(self.own(at), self.me, at, self.pair_sem.at[0], 1)
        owner = self.me ^ (self.first, self.first ^ self.second, self.second)[which - 1]
        return self.to_seq(self.place(owner, at), owner, at, self.pair_sem.at[which], 1)

    def begin(self, at):
        self.first_copy(at).start()
        self.pair_copy(0, at).start()

    def fetch(self, weight):
        return pltpu.make_async_copy(
            self.shards[weight], self.held[weight % len(self.held)], self.local_sem.at[0, weight]
        )

    def keep(self, weight):
        return pltpu.make_async_copy(
            self.held[weight % len(self.held)], self.fulls[weight].at[self.me], self.local_sem.at[1, weight]
        )

    def start(self):
        for at in range(AHEAD):
            self.begin(at)
        self.local(0)

    def local(self, first):
        for weight in range(first, first + len(self.held)):
            self.fetch(weight).start()
        for weight in range(first, first + len(self.held)):
            self.fetch(weight).wait()
            self.keep(weight).start()

    def ready(self, weight):
        for at, piece in enumerate(self.pieces):
            if piece[0] == weight:
                for which in range(4):
                    self.pair_copy(which, at).wait_recv()
        self.keep(weight).wait()

    def advance(self, at):
        self.first_copy(at).wait_recv()
        if at + AHEAD < len(self.pieces):
            self.begin(at + AHEAD)
        self.second_copy(at).start()
        self.rep_copy(at).start()
        self.pair_copy(1, at).start()
        if at:
            self.share(at - 1)

    def share(self, at):
        self.second_copy(at).wait_recv()
        self.rep_copy(at).wait_recv()
        self.pair_copy(2, at).start()
        self.pair_copy(3, at).start()

    def finish(self):
        for at in range(len(self.pieces)):
            for copy in (self.first_copy(at), self.second_copy(at), self.rep_copy(at)):
                copy.wait_send()
            for which in range(4):
                self.pair_copy(which, at).wait_send()


def enter(seq_masks, rep_masks):
    me, z = lax.axis_index("seq"), lax.axis_index("rep")
    barrier = pltpu.get_barrier_semaphore()
    for mask in seq_masks:
        pl.semaphore_signal(barrier, inc=1, device_id={"seq": me ^ mask})
    for mask in rep_masks:
        pl.semaphore_signal(barrier, inc=1, device_id={"rep": z ^ mask})
    pl.semaphore_wait(barrier, len(seq_masks) + len(rep_masks))


def joined_rows(fulls):
    return [full.reshape(-1, full.shape[2]) for full in fulls]


LOW = jnp.bfloat16
WIDE = jnp.float32
LANES = 128
STRIP = 64
KEYS = 256


def whole_block(shape):
    return pl.BlockSpec(shape, lambda *at: (0,) * len(shape))


def strips(total, body):
    def step(j, carry):
        body(pl.ds(pl.multiple_of(j * STRIP, STRIP), STRIP))
        return carry

    lax.fori_loop(0, total // STRIP, step, 0)


def turn_into(target, source):
    for j in range(source.shape[1] // LANES):
        target[j * LANES : (j + 1) * LANES, :] = source[:, j * LANES : (j + 1) * LANES].T


def unit_rows(block):
    centred = block - jnp.mean(block, axis=-1, keepdims=True)
    spread = lax.rsqrt(jnp.mean(centred * centred, axis=-1, keepdims=True) + norm_epsilon)
    return centred * spread, spread


def into_norm(grad, scaled, unit, spread):
    inner = grad * scaled
    level = jnp.mean(inner, axis=-1, keepdims=True)
    slope = jnp.mean(inner * unit, axis=-1, keepdims=True)
    return spread * (inner - level - unit * slope)


def times(left, right):
    return jnp.dot(left, right, preferred_element_type=WIDE)


def times_turned(left, right):
    return lax.dot_general(left, right, (((1,), (1,)), ((), ())), preferred_element_type=WIDE)


def turned_times(left, right):
    return lax.dot_general(left, right, (((0,), (0,)), ((), ())), preferred_element_type=WIDE)


def params(size, cid=None):
    if cid is None:
        return pltpu.CompilerParams(vmem_limit_bytes=size << 20)
    return pltpu.CompilerParams(
        vmem_limit_bytes=size << 20, collective_id=cid, has_side_effects=True
    )


def cost(flops, size):
    return pl.CostEstimate(flops=flops, bytes_accessed=size, transcendentals=0)


def window(head):
    low, high = head * HEAD_WIDTH, (head + 1) * HEAD_WIDTH
    start = low // LANES * LANES
    stop = -(-high // LANES) * LANES
    return start, stop - start, low - start


def head_mask(head):
    start, wide, offset = window(head)
    lane = lax.broadcasted_iota(jnp.int32, (1, wide), 1)
    return ((lane >= offset) & (lane < offset + HEAD_WIDTH)).astype(WIDE).astype(LOW)


def add_window(total, head, block):
    start, wide, _ = window(head)
    for j in range(wide // LANES):
        tile = start // LANES + j
        lanes = slice(tile * LANES, (tile + 1) * LANES)
        piece = block[:, j * LANES : (j + 1) * LANES]
        if head == tile * LANES // HEAD_WIDTH:
            total[:, lanes] = piece
        else:
            total[:, lanes] = total[:, lanes] + piece


def group_rows(ref, group, column, wide, spatial):
    lanes = slice(column, column + wide)
    if spatial:
        return ref[group, :, lanes]
    block = ref[:, group, :, lanes]
    return block.reshape(-1, wide)


def same_place():
    row = lax.broadcasted_iota(jnp.int32, (KEYS, KEYS), 0)
    column = lax.broadcasted_iota(jnp.int32, (KEYS, KEYS), 1)
    return (row & 15) == (column & 15)


def put_rows(ref, group, block, spatial):
    if spatial:
        ref[group] = block
    else:
        ref[:, group] = block.reshape(ref.shape[0], ref.shape[2], ref.shape[3])


def sibling_barrier(me):
    barrier = pltpu.get_barrier_semaphore()
    pl.semaphore_signal(barrier, inc=1, device_id={"seq": me ^ 1})
    pl.semaphore_wait(barrier, 1)


def attend_back_kernel(spatial, *refs):
    if spatial:
        (
            da_ref, qkv_ref, prob_ref, w_ref, other_ref, dqkv_ref,
            dout, total_q, total_k, total_v, other, give, take, load_sem, send_sem, arrive_sem,
        ) = refs
    else:
        da_ref, qkv_ref, prob_ref, w_ref, dqkv_ref, dout, total_q, total_k, total_v = refs
    group, groups = pl.program_id(0), pl.num_programs(0)
    features = da_ref.shape[1]
    root = HEAD_WIDTH ** (-0.5)
    if spatial:
        me = lax.axis_index("seq")

        def exchange(j):
            return pltpu.make_async_remote_copy(
                give.at[j], take.at[j], send_sem.at[j], arrive_sem.at[j], device_id={"seq": me ^ 1},
            )

    @pl.when(group == 0)
    def _():
        if spatial:
            load = pltpu.make_async_copy(other_ref, other, load_sem)
            load.start()
            sibling_barrier(me)
        half = da_ref.shape[0] // 2
        for j in range(2):
            got = times_turned(da_ref[j * half : (j + 1) * half], w_ref[...]).astype(LOW)
            if spatial:
                dout[2 * j : 2 * j + 2] = got.reshape(2, half // 2, features)
            else:
                dout[2 * j : 2 * j + 2] = got.reshape(2, 2, half // 4, features)
        if spatial:
            load.wait()

    for head in range(HEADS):
        start, wide, _ = window(head)
        mask = head_mask(head)
        queries = group_rows(qkv_ref, group, start, wide, spatial) * mask
        keys = group_rows(qkv_ref, group, features + start, wide, spatial)
        values = group_rows(qkv_ref, group, 2 * features + start, wide, spatial)
        grads = group_rows(dout, group, start, wide, spatial) * mask
        if spatial:
            keys = jnp.concatenate([keys, other[group, :, start : start + wide]], 0)
            values = jnp.concatenate(
                [values, other[group, :, features + start : features + start + wide]], 0
            )
        prob = prob_ref[0, head]
        known = prob.astype(WIDE)
        dprob = times_turned(grads, values)
        level = jnp.sum(dprob * known, axis=-1, keepdims=True)
        dscores = (known * (dprob - level)).astype(LOW)
        add_window(total_q, head, times(dscores, keys * mask))
        add_window(total_k, head, turned_times(dscores, queries))
        add_window(total_v, head, turned_times(prob, grads))

    own = total_q.shape[0]
    pieces = (
        (total_q[...] * root).astype(LOW),
        (total_k[:own] * root).astype(LOW),
        total_v[:own].astype(LOW),
    )
    for j, piece in enumerate(pieces):
        lanes = slice(j * features, (j + 1) * features)
        if spatial:
            dqkv_ref[group, :, lanes] = piece
        else:
            dqkv_ref[:, group, :, lanes] = piece.reshape(4, -1, features)
    if spatial:
        give[group, :, :features] = (total_k[own:] * root).astype(LOW)
        give[group, :, features:] = total_v[own:].astype(LOW)
        exchange(group).start()

        @pl.when(group == groups - 1)
        def _():
            for j in range(take.shape[0]):
                exchange(j).wait()
                lanes = slice(features, 3 * features)
                dqkv_ref[j, :, lanes] = dqkv_ref[j, :, lanes] + take[j]


def attention_backward(da, qkv, prob, weight, other, spatial, cid=None):
    tokens, features = da.shape
    groups = prob.shape[0]
    span = tokens // groups
    shape = (groups, span, 3 * features) if spatial else (4, groups, span // 4, 3 * features)
    rest = shape[:-1]
    in_specs = [
        whole_block(da.shape),
        whole_block(shape),
        pl.BlockSpec((1, HEADS, span, KEYS), lambda g: (g, 0, 0, 0)),
        whole_block(weight.shape),
    ]
    scratch = [
        pltpu.VMEM(rest + (features,), LOW),
        pltpu.VMEM((span, features), WIDE),
        pltpu.VMEM((KEYS, features), WIDE),
        pltpu.VMEM((KEYS, features), WIDE),
    ]
    args = [da, qkv.reshape(shape), prob, weight]
    if spatial:
        in_specs.append(pl.BlockSpec(memory_space=pl.ANY))
        args.append(other)
        scratch += [pltpu.VMEM(other.shape, LOW)] * 3
        scratch += [
            pltpu.SemaphoreType.DMA(()),
            pltpu.SemaphoreType.DMA((groups,)),
            pltpu.SemaphoreType.DMA((groups,)),
        ]
    got = pl.pallas_call(
        functools.partial(attend_back_kernel, spatial),
        grid=(groups,),
        in_specs=in_specs,
        out_specs=whole_block(shape),
        out_shape=jax.ShapeDtypeStruct(shape, LOW),
        scratch_shapes=scratch,
        compiler_params=params(56, cid),
        cost_estimate=cost(2 * tokens * (weight.size + 5 * features * KEYS), 4 * qkv.size),
        name="attend_spatial_back" if spatial else "attend_temporal_back",
    )(*args)
    return got.reshape(tokens, 3 * features)


def seq_barrier(me):
    barrier = pltpu.get_barrier_semaphore()
    for mask in range(1, 8):
        pl.semaphore_signal(barrier, inc=1, device_id={"seq": me ^ mask})
    pl.semaphore_wait(barrier, 7)


def moves(source, target, sems, local_sem, me, to_places):
    part = source.shape[-2] // 8 if to_places else source.shape[-2]

    def ends(device):
        if to_places:
            return source.at[:, pl.ds(pl.multiple_of(device * part, part), part)], target.at[me]
        return source.at[device], target.at[:, pl.ds(pl.multiple_of(me * part, part), part)]

    copies = [pltpu.make_async_copy(*ends(me), local_sem)]
    for mask in (6, 7, 2, 3, 4, 5, 1):
        copies.append(
            pltpu.make_async_remote_copy(
                *ends(me ^ mask), sems.at[0, mask], sems.at[1, mask], device_id={"seq": me ^ mask}
            )
        )
    return copies


def move_scratch():
    return [pltpu.SemaphoreType.DMA((2, 8)), pltpu.SemaphoreType.DMA(())]


def gelu_and_slope(value):
    inner = 0.7978845608028654 * (value + 0.044715 * value * value * value)
    bent = jnp.tanh(inner)
    half = 0.5 * (1.0 + bent)
    slope = half + 0.5 * value * (1.0 - bent * bent) * (
        0.7978845608028654 * (1.0 + 3 * 0.044715 * value * value)
    )
    return value * half, slope


OUTS = ("qkv", "prob", "h", "o", "h2", "z", "slope", "x1", "branch", "mlp")
CHUNK = 768


def forward_kernel(shapes, *refs):
    count = len(shapes)
    shards, refs = refs[:count], refs[count:]
    partial, condition, tokens, x_ref = refs[:4]
    fulls, refs = refs[4 : 4 + count], refs[4 + count :]
    mod_ref, conditions, moved, other_ref, x2_ref, y_ref = refs[:6]
    outs = [dict(zip(OUTS, refs[6:16])), dict(zip(OUTS, refs[16:26]))]
    refs = refs[26:]
    (
        partials, x2, qkv, other, held, normed, total, middle, part, prob, turned, low, ready,
        tall, short, hidden, slope, small_sem, move_sem, stay_sem, next_move_sem, next_stay_sem, next_sem,
        pair_sem, weight_sem, out_sem, prob_sem, chunk_sem,
    ) = refs[:28]
    gather = Gather(shapes, (shards, fulls, refs[28:]))
    me, z = gather.me, gather.z
    features = x_ref.shape[1]
    steps = shapes[2][1] // CHUNK
    enter(range(1, 8), range(1, 4))

    small = []
    for mask in range(1, 8):
        small.append(pltpu.make_async_remote_copy(
            partial, partials.at[me], small_sem.at[0, mask], small_sem.at[1, mask],
            device_id={"seq": me ^ mask}))
    for mask in range(1, 4):
        small.append(pltpu.make_async_remote_copy(
            condition, conditions.at[z], small_sem.at[0, 7 + mask], small_sem.at[1, 7 + mask],
            device_id={"rep": z ^ mask}))
    small.append(pltpu.make_async_copy(partial, partials.at[me], small_sem.at[0, 0]))
    small.append(pltpu.make_async_copy(condition, conditions.at[z], small_sem.at[1, 0]))
    for copy in small:
        copy.start()
    gather.start()
    gather.advance(0)
    later = moves(tokens, moved, move_sem, stay_sem, me, True)
    for copy in later:
        copy.start()
    for copy in small:
        copy.wait()
    modulation = partials[0]
    for device in range(1, 8):
        modulation = modulation + partials[device]
    width = features // LANES
    for row in range(12):
        for j in range(width):
            at = row * width + j
            mod_ref[row // 6, row % 6 : row % 6 + 1, j * LANES : (j + 1) * LANES] = modulation[
                at : at + 1
            ]

    pending = {}
    names = ("turned", "qkv", "other", "low", "middle", "ready")

    def begin(name, source, target):
        settle(name)
        pending[name] = pltpu.make_async_copy(source, target, out_sem.at[names.index(name)])
        pending[name].start()

    def settle(name):
        copy = pending.pop(name, None)
        if copy is not None:
            copy.wait()

    def full(weight):
        return fulls[weight]

    def load(slot, source):
        return pltpu.make_async_copy(source, tall.at[slot], weight_sem.at[slot])

    def column_block(weight, column):
        return full(weight).at[:, :, pl.ds(column, features)]

    def exchange(j):
        return pltpu.make_async_remote_copy(
            qkv.at[pl.ds(2 * j, 2), :, pl.ds(features, 2 * features)], other.at[pl.ds(2 * j, 2)],
            pair_sem.at[0, j], pair_sem.at[1, j], device_id={"seq": me ^ 1},
        )

    def rows_of(ref, group, column, wide, spatial):
        lanes = slice(column, column + wide)
        if spatial:
            return ref[pl.ds(2 * group, 2), :, lanes].reshape(-1, wide)
        return jnp.concatenate([ref[2 * block + group, :, lanes] for block in range(4)], 0)

    def attend(layer, spatial, group, span, allowed):
        for head in range(HEADS):
            start, wide, _ = window(head)
            mask = head_mask(head)
            queries = rows_of(qkv, group, start, wide, spatial) * mask
            keys = rows_of(qkv, group, features + start, wide, spatial)
            values = rows_of(qkv, group, 2 * features + start, wide, spatial)
            if spatial:
                keys = jnp.concatenate([keys, rows_of(other, group, start, wide, True)], 0)
                values = jnp.concatenate(
                    [values, rows_of(other, group, features + start, wide, True)], 0
                )
            scores = times_turned(queries, keys) * HEAD_WIDTH ** (-0.5)
            if not spatial:
                scores = jnp.where(allowed, scores, -3e38)
            grown = jnp.exp(scores - jnp.max(scores, axis=-1, keepdims=True))
            chance = (grown / jnp.sum(grown, axis=-1, keepdims=True)).astype(LOW)
            prob[head, :span] = chance
            add_window(part.at[pl.ds(0, span)], head, times(chance, values * mask))
        got = part[:span].astype(LOW)
        if spatial:
            held[pl.ds(2 * group, 2)] = got.reshape(2, -1, features)
        else:
            for block in range(4):
                held[2 * block + group] = got[block * 64 : (block + 1) * 64]

    def flat_rows(ref):
        return ref[...].reshape(-1, features)

    def turn_out(source, target):
        settle("turned")
        for j in range(features // LANES):
            lanes = slice(j * LANES, (j + 1) * LANES)
            turned[lanes, :] = source[:, lanes].T
        begin("turned", turned, target)

    def layer(at_layer, spatial, x, plan):
        first = 4 * at_layer
        out = outs[at_layer]
        groups = 4 if spatial else 2
        span = x.shape[0] // groups
        mod = mod_ref.at[at_layer]

        def go(place):
            for at in plan.get(place, ()):
                if at is None:
                    gather.share(len(gather.pieces) - 1)
                else:
                    gather.advance(at)

        def go_when(place, index):
            for key, pieces in plan.items():
                if isinstance(key, tuple) and key[0] == place:
                    @pl.when(index == key[1])
                    def _():
                        for at in pieces:
                            gather.advance(at)

        scaled, shift = 1.0 + mod[1:2], mod[0:1]

        def norm(at):
            unit, _ = unit_rows(x[at].astype(WIDE))
            normed[at] = (unit * scaled + shift).astype(LOW)

        strips(x.shape[0], norm)
        turn_out(normed[...], out["h"])
        go("norm")
        gather.ready(first)
        load(0, column_block(first, 0)).start()
        settle("qkv")
        for j in range(3):
            load(j % 2, column_block(first, 0)).wait()
            if j < 2:
                load((j + 1) % 2, column_block(first, (j + 1) * features)).start()
            got = times(normed[...], tall[j % 2].reshape(features, features)).astype(LOW)
            qkv[:, :, j * features : (j + 1) * features] = got.reshape(8, -1, features)
            go(f"qkv{j}")
        begin("qkv", qkv, out["qkv"])
        if spatial:
            for j in range(groups):
                exchange(j).start()
        allowed = None if spatial else same_place()

        def prob_copy(group):
            return pltpu.make_async_copy(
                prob.at[:, pl.ds(0, span)], out["prob"].at[group], prob_sem
            )

        def one_group(group, carry):
            go_when("group", group)
            if spatial:
                exchange(group).wait_recv()

            @pl.when(group > 0)
            def _():
                prob_copy(group).wait()

            attend(at_layer, spatial, group, span, allowed)
            prob_copy(group).start()
            return carry

        lax.fori_loop(0, groups, one_group, 0)
        prob_copy(0).wait()
        if spatial:
            begin("other", other, other_ref)
            for j in range(groups):
                exchange(j).wait_send()
        go("attended")
        gather.ready(first + 1)
        load(0, full(first + 1)).start()
        attended = flat_rows(held)
        turn_out(attended, out["o"])
        load(0, full(first + 1)).wait()
        total[...] = times(attended, tall[0].reshape(features, features))
        gate, move, grow = mod[2:3], mod[3:4], 1.0 + mod[4:5]
        settle("low")
        settle("middle")

        def finish(at):
            branch = total[at]
            low[at] = branch.astype(LOW)
            got = x[at].astype(WIDE) + gate * branch
            middle[at] = got
            unit, _ = unit_rows(got)
            normed[at] = (unit * grow + move).astype(LOW)

        strips(x.shape[0], finish)
        begin("low", low, out["branch"])
        begin("middle", middle, out["x1"])
        turn_out(normed[...], out["h2"])
        go("middle")
        gather.ready(first + 2)
        gather.ready(first + 3)

        down = full(first + 3)
        per = down.shape[0] * down.shape[1] // steps

        def chunk_loads(step, slot):
            column = pl.multiple_of(step * CHUNK, CHUNK)
            owner = step * CHUNK // down.shape[1]
            copies = [
                pltpu.make_async_copy(
                    full(first + 2).at[:, :, pl.ds(column, CHUNK)],
                    tall.at[slot, :, :, pl.ds(0, CHUNK)], weight_sem.at[slot],
                )
            ]
            return copies, column, owner

        def start_loads(step, slot):
            copies, column, owner = chunk_loads(step, slot)
            for copy in copies:
                copy.start()
            pltpu.make_async_copy(
                down_rows(step), short.at[slot], weight_sem.at[2 + slot]
            ).start()

        def down_rows(step):
            return fulls_flat[at_layer].at[pl.ds(pl.multiple_of(step * 4, 4), 4)]

        fulls_flat = [fulls[3].reshape(*split_rows(fulls[3].shape)), fulls[7].reshape(*split_rows(fulls[7].shape))]

        def wait_loads(slot):
            for copy in chunk_loads(0, slot)[0]:
                copy.wait()
            pltpu.make_async_copy(down_rows(0), short.at[slot], weight_sem.at[2 + slot]).wait()

        def chunk_outs(step, slot):
            column = pl.multiple_of(step * CHUNK, CHUNK)
            return (
                pltpu.make_async_copy(
                    hidden.at[slot], out["z"].at[pl.ds(column, CHUNK)], chunk_sem.at[0, slot]
                ),
                pltpu.make_async_copy(
                    slope.at[slot], out["slope"].at[:, pl.ds(column, CHUNK)], chunk_sem.at[1, slot]
                ),
            )

        start_loads(0, 0)
        half = x.shape[0] // 2

        def chunk(step, carry):
            slot = lax.rem(step, 2)
            go_when("chunk", step)
            wait_loads(slot)

            @pl.when(step + 1 < steps)
            def _():
                start_loads(step + 1, 1 - slot)

            @pl.when(step >= 2)
            def _():
                for copy in chunk_outs(step, slot):
                    copy.wait()

            up = tall[slot, :, :, :CHUNK].reshape(features, CHUNK)
            for j in range(2):
                rows = slice(j * half, (j + 1) * half)
                value, bend = gelu_and_slope(times(normed[rows], up))
                slope[slot, rows] = bend.astype(LOW)
                value = value.astype(LOW)
                hidden[slot, :, rows] = value.T
                got = times(value, short[slot].reshape(CHUNK, features))

                @pl.when(step == 0)
                def _():
                    total[rows] = got

                @pl.when(step > 0)
                def _():
                    total[rows] = total[rows] + got

            for copy in chunk_outs(step, slot):
                copy.start()
            return carry

        lax.fori_loop(0, steps, chunk, 0)
        for slot in range(2):
            for copy in chunk_outs(0, slot):
                copy.wait()
        last = mod[5:6]
        settle("low")

        def close(at):
            mlp = total[at]
            low[at] = mlp.astype(LOW)
            total[at] = middle[at] + last * mlp

        strips(x.shape[0], close)
        begin("low", low, out["mlp"])
        ready[...] = total[...].astype(LOW).reshape(ready.shape)

    layer(0, True, x_ref, {
        "norm": (1, 2, 3), "qkv1": (4,), ("group", 0): (5,), ("group", 1): (6,), ("group", 2): (7,),
        ("group", 3): (8,), "attended": (9,), "middle": (10, 11, 12), ("chunk", 1): (13,),
        ("chunk", 3): (14,), ("chunk", 4): (15,),
    })
    copies = moves(ready, x2_ref, next_move_sem, next_stay_sem, me, True)
    for copy in later:
        copy.wait()
    for copy in copies:
        copy.start()
    gather.local(4)
    gather.advance(16)
    gather.advance(17)
    for copy in copies:
        copy.wait()
    fetch = pltpu.make_async_copy(x2_ref, x2, next_sem)
    fetch.start()
    fetch.wait()
    x2_rows = x2.reshape(x_ref.shape)
    layer(1, False, x2_rows, {
        "norm": (18,), "qkv0": (19,), "qkv2": (20,), ("group", 1): (21,), "attended": (22,),
        "middle": (23, None),
    })
    begin("ready", ready, y_ref)
    for name in names:
        settle(name)
    gather.finish()


def split_rows(shape):
    return (shape[0] * shape[1] // (CHUNK // 4), CHUNK // 4, shape[2])


def forward(shards, partial, condition, cotangent, x, cid):
    shapes = [shard.shape for shard in shards]
    count = len(shapes)
    tokens, features = x.shape
    frames, places, _ = cotangent.shape
    wide = shapes[2][1]
    any_ = pl.BlockSpec(memory_space=pl.ANY)
    struct = jax.ShapeDtypeStruct
    moved = struct((8, frames, places // 8, features), LOW)
    outs = Gather.outs(shapes) + [
        struct((2, 6, features), WIDE),
        struct((4,) + condition.shape, condition.dtype),
        moved,
        struct((8, tokens // 8, 2 * features), LOW),
        moved,
        struct((frames, places, features), LOW),
    ]
    for groups in (4, 2):
        outs += [
            struct((8, tokens // 8, 3 * features), LOW),
            struct((groups, HEADS, tokens // groups, KEYS), LOW),
            struct((features, tokens), LOW),
            struct((features, tokens), LOW),
            struct((features, tokens), LOW),
            struct((wide, tokens), LOW),
            struct((tokens, wide), LOW),
            struct((tokens, features), WIDE),
            struct((tokens, features), LOW),
            struct((tokens, features), LOW),
        ]
    dma = pltpu.SemaphoreType.DMA
    vm = pltpu.VMEM
    flops = 2 * tokens * 8 * sum(shape[0] * shape[1] for shape in shapes)
    got = pl.pallas_call(
        functools.partial(forward_kernel, shapes),
        out_shape=outs,
        in_specs=[any_] * (count + 3) + [pl.BlockSpec(memory_space=vm)],
        out_specs=[any_] * count + [pl.BlockSpec(memory_space=vm)] + [any_] * (len(outs) - count - 1),
        scratch_shapes=[
            vm((8,) + partial.shape, WIDE),
            vm(moved.shape, LOW),
            vm((8, tokens // 8, 3 * features), LOW),
            vm((8, tokens // 8, 2 * features), LOW),
            vm((8, tokens // 8, features), LOW),
            vm((tokens, features), LOW),
            vm((tokens, features), WIDE),
            vm((tokens, features), WIDE),
            vm((KEYS, features), WIDE),
            vm((HEADS, KEYS, KEYS), LOW),
            vm((features, tokens), LOW),
            vm((tokens, features), LOW),
            vm((frames, places, features), LOW),
            vm((2, 8, features // 8, features), LOW),
            vm((2, 4, CHUNK // 4, features), LOW),
            vm((2, CHUNK, tokens), LOW),
            vm((2, tokens, CHUNK), LOW),
            dma((2, 11)),
            *move_scratch(),
            *move_scratch(),
            dma(()),
            dma((2, 4)),
            dma((4,)),
            dma((8,)),
            dma(()),
            dma((2, 2)),
        ]
        + Gather.scratch(shapes),
        compiler_params=params(60, cid),
        cost_estimate=cost(flops, 4 * flops // tokens),
        name="forward",
    )(*shards, partial, condition, cotangent, x)
    weights = joined_rows(got[:count])
    named = [dict(zip(OUTS, got[count + 6 + 10 * at : count + 16 + 10 * at])) for at in range(2)]
    return weights, got[count : count + 6], named


def mlp_back_kernel(send, *refs):
    g_ref, x1_ref, branch_ref, mlp_ref, mod_ref, up_ref, down_ref, slope_ref = refs[:8]
    refs = refs[8:]
    if send:
        done_ref, refs = refs[0], refs[1:]
    du_ref, df_ref, dx1_ref, da_ref, sums_ref = refs[:5]
    refs = refs[5:]
    if send:
        moved_ref, refs = refs[0], refs[1:]
    df, total = refs[:2]
    step, steps = pl.program_id(0), pl.num_programs(0)
    if send:
        me = lax.axis_index("seq")
        copies = moves(done_ref, moved_ref, refs[2], refs[3], me, False)

    @pl.when(step == 0)
    def _():
        if send:
            seq_barrier(me)
            for copy in copies:
                copy.start()
        gate = mod_ref[5:6]
        sums_ref[...] = jnp.zeros_like(sums_ref)

        def begin(at):
            grad = g_ref[at].astype(WIDE)
            low = (gate * grad).astype(LOW)
            df[at] = low
            df_ref[at] = low
            sums_ref[3:4] += jnp.sum(grad * mlp_ref[at].astype(WIDE), axis=0, keepdims=True)

        strips(df.shape[0], begin)

    half = df.shape[0] // 2
    for j in range(2):
        rows = slice(j * half, (j + 1) * half)
        du = times_turned(df[rows], down_ref[...]) * slope_ref[rows].astype(WIDE)
        du = du.astype(LOW)
        du_ref[rows] = du
        part = times_turned(du, up_ref[...])

        @pl.when(step == 0)
        def _():
            total[rows] = part

        @pl.when(step > 0)
        def _():
            total[rows] = total[rows] + part

    @pl.when(step == steps - 1)
    def _():
        gate, scaled = mod_ref[2:3], 1.0 + mod_ref[4:5]

        def finish(at):
            grad = total[at]
            unit, spread = unit_rows(x1_ref[at])
            middle = g_ref[at].astype(WIDE) + into_norm(grad, scaled, unit, spread)
            dx1_ref[at] = middle
            da_ref[at] = (gate * middle).astype(LOW)
            sums_ref[0:1] += jnp.sum(
                middle * branch_ref[at].astype(WIDE), axis=0, keepdims=True
            )
            sums_ref[1:2] += jnp.sum(grad, axis=0, keepdims=True)
            sums_ref[2:3] += jnp.sum(grad * unit, axis=0, keepdims=True)

        strips(df.shape[0], finish)
        if send:
            for copy in copies:
                copy.wait()


def mlp_backward(g, x1, branch, mlp, mod, up, down, slope, done=None, cid=None):
    tokens, features = x1.shape
    wide = up.shape[1]
    block = 768
    send = done is not None
    in_specs = [
        whole_block(g.shape), whole_block(x1.shape), whole_block(branch.shape),
        whole_block(mlp.shape), whole_block(mod.shape),
        pl.BlockSpec((features, block), lambda j: (0, j)),
        pl.BlockSpec((block, features), lambda j: (j, 0)),
        pl.BlockSpec((tokens, block), lambda j: (0, j)),
    ]
    args = [g, x1, branch, mlp, mod, up, down, slope]
    out_shape = [
        jax.ShapeDtypeStruct((tokens, wide), LOW),
        jax.ShapeDtypeStruct((tokens, features), LOW),
        jax.ShapeDtypeStruct((tokens, features), WIDE),
        jax.ShapeDtypeStruct((tokens, features), LOW),
        jax.ShapeDtypeStruct((8, features), WIDE),
    ]
    out_specs = [pl.BlockSpec((tokens, block), lambda j: (0, j))]
    out_specs += [whole_block(o.shape) for o in out_shape[1:]]
    scratch = [pltpu.VMEM((tokens, features), LOW), pltpu.VMEM((tokens, features), WIDE)]
    if send:
        in_specs.append(pl.BlockSpec(memory_space=pl.ANY))
        args.append(done)
        out_shape.append(
            jax.ShapeDtypeStruct((done.shape[1], 8 * done.shape[2], features), LOW)
        )
        out_specs.append(pl.BlockSpec(memory_space=pl.ANY))
        scratch += move_scratch()
    return pl.pallas_call(
        functools.partial(mlp_back_kernel, send),
        grid=(wide // block,),
        in_specs=in_specs,
        out_specs=out_specs,
        out_shape=out_shape,
        scratch_shapes=scratch,
        compiler_params=params(56, cid),
        cost_estimate=cost(4 * tokens * up.size, 4 * up.size),
        name="mlp_backward",
    )(*args)


def qkv_back_kernel(send, *refs):
    dqkv_ref, w_ref, x_ref, dx1_ref, mod_ref, dx_ref, sums_ref, total = refs[:8]
    step, steps = pl.program_id(0), pl.num_programs(0)
    part = times_turned(dqkv_ref[...], w_ref[...])

    @pl.when(step == 0)
    def _():
        total[...] = part

    @pl.when(step > 0)
    def _():
        total[...] = total[...] + part

    @pl.when(step == steps - 1)
    def _():
        scaled = 1.0 + mod_ref[1:2]
        sums_ref[...] = jnp.zeros_like(sums_ref)
        if send:
            ready, sems, local_sem = refs[8:]
            me = lax.axis_index("seq")
            seq_barrier(me)

        def finish(at):
            grad = total[at]
            unit, spread = unit_rows(x_ref[at].astype(WIDE))
            sums_ref[0:1] += jnp.sum(grad, axis=0, keepdims=True)
            sums_ref[1:2] += jnp.sum(grad * unit, axis=0, keepdims=True)
            got = dx1_ref[at] + into_norm(grad, scaled, unit, spread)
            if send:
                total[at] = got
            else:
                dx_ref[at] = got

        strips(total.shape[0], finish)
        if send:
            ready[...] = total[...].astype(LOW).reshape(ready.shape)
            copies = moves(ready, dx_ref, sems, local_sem, me, False)
            for copy in copies:
                copy.start()
            for copy in copies:
                copy.wait()


def qkv_backward(dqkv, weight, x, dx1, mod, frames=None, cid=None):
    tokens, features = x.shape
    steps = weight.shape[1] // features
    send = frames is not None
    out_shape = [
        jax.ShapeDtypeStruct((tokens, features), WIDE),
        jax.ShapeDtypeStruct((8, features), WIDE),
    ]
    scratch = [pltpu.VMEM((tokens, features), WIDE)]
    if send:
        places = tokens // frames
        out_shape[0] = jax.ShapeDtypeStruct((frames, places, features), LOW)
        scratch += [pltpu.VMEM((8, frames, places // 8, features), LOW)] + move_scratch()
    return pl.pallas_call(
        functools.partial(qkv_back_kernel, send),
        grid=(steps,),
        in_specs=[
            pl.BlockSpec((tokens, features), lambda j: (0, j)),
            pl.BlockSpec((features, features), lambda j: (0, j)),
            whole_block(x.shape), whole_block(dx1.shape), whole_block(mod.shape),
        ],
        out_specs=[
            pl.BlockSpec(memory_space=pl.ANY) if send else whole_block((tokens, features)),
            whole_block((8, features)),
        ],
        out_shape=out_shape,
        scratch_shapes=scratch,
        compiler_params=params(48, cid),
        cost_estimate=cost(2 * tokens * weight.size, 2 * weight.size),
        name="qkv_backward",
    )(dqkv, weight, x, dx1, mod)


SLOTS = 3
BACK = 4


def reduce_kernel(layers, rows, width, edge, *refs):
    ins, mods = refs[: 8 * layers], refs[8 * layers]
    outs, every_mod = refs[8 * layers + 1 : 12 * layers + 1], refs[12 * layers + 1]
    (
        left, right, away, pair_in, part,
        first_in_a, first_in_b, mid_a, mid_b, second_in_a, second_in_b,
        clip, rep_in, joined, inner_in, final, back_in, wide,
        mod_in, load_sem, pair_sem, link_sem, rep_sem, back_sem, store_sem, mod_sem,
    ) = refs[12 * layers + 2 :]
    me, z = lax.axis_index("seq"), lax.axis_index("rep")
    core, x, y = me & 1, (me >> 1) & 1, (me >> 2) & 1
    inner = (z == 1) | (z == 2)
    outer = (z == 0) | (z == 3)

    barrier = pltpu.get_barrier_semaphore()
    for mask in range(1, 8):
        pl.semaphore_signal(barrier, inc=1, device_id={"seq": me ^ mask})
    for mask in range(1, 4):
        pl.semaphore_signal(barrier, inc=1, device_id={"rep": z ^ mask})
    pl.semaphore_wait(barrier, 10)

    mod_copies = [
        pltpu.make_async_remote_copy(
            mods, mod_in.at[me], mod_sem.at[0, mask], mod_sem.at[1, mask],
            device_id={"seq": me ^ mask},
        )
        for mask in range(1, 8)
    ]
    clip_copies = [
        pltpu.make_async_remote_copy(
            every_mod.at[z], every_mod.at[z], mod_sem.at[0, 7 + mask], mod_sem.at[1, 7 + mask],
            device_id={"rep": z ^ mask},
        )
        for mask in range(1, 4)
    ]
    for copy in mod_copies:
        copy.start()
    mod_in[me] = mods[...]

    spans, start = [], 0
    for layer in range(layers):
        for kind in range(4):
            shape = outs[4 * layer + kind].shape
            count = shape[0] // rows * (shape[1] // width)
            spans.append((layer, kind, start, count))
            start += count
    total = start

    def loads(block, slot):
        for layer, kind, first, count in spans:
            @pl.when((block >= first) & (block < first + count))
            def _():
                source = ins[8 * layer + kind]
                if kind == 3:
                    source = source.at[:, :, block - first]
                pltpu.make_async_copy(source, left.at[slot], load_sem.at[0, slot]).start()
                source = ins[8 * layer + 4 + kind]
                if kind in (0, 2):
                    column = pl.multiple_of((block - first) * width, width)
                    source = source.at[:, pl.ds(column, width)]
                pltpu.make_async_copy(source, right.at[slot], load_sem.at[1, slot]).start()

    def wait_loads(slot):
        pltpu.make_async_copy(ins[0], left.at[slot], load_sem.at[0, slot]).wait()
        pltpu.make_async_copy(ins[5], right.at[slot], load_sem.at[1, slot]).wait()

    def store(block, slot):
        for layer, kind, first, count in spans:
            @pl.when((block >= first) & (block < first + count))
            def _():
                target = outs[4 * layer + kind]
                if kind == 3:
                    row = pl.multiple_of((block - first) * rows, rows)
                    target = target.at[pl.ds(row, rows)]
                elif kind in (0, 2):
                    column = pl.multiple_of((block - first) * width, width)
                    target = target.at[:, pl.ds(column, width)]
                pltpu.make_async_copy(wide.at[slot], target, store_sem.at[slot]).start()

    def to_seq(source, target, which, slot, mask):
        return pltpu.make_async_remote_copy(
            source, target, link_sem.at[0, which, slot], link_sem.at[1, which, slot],
            device_id={"seq": me ^ mask},
        )

    def pair_copy(t):
        slot = lax.rem(t, 2)
        return pltpu.make_async_remote_copy(
            away, pair_in.at[slot], pair_sem.at[0, slot], pair_sem.at[1, slot],
            device_id={"seq": me ^ 1},
        )

    def first_copies(t):
        slot, block = lax.rem(t, SLOTS), lax.rem(t - 1, SLOTS)
        return (
            to_seq(part.at[block, :, 1 - x, :, pl.ds(0, edge)], first_in_a.at[slot], 0, slot, 2),
            to_seq(
                part.at[block, 1 - y, :, :, pl.ds(edge, width - edge)],
                first_in_b.at[slot], 1, slot, 4,
            ),
        )

    def second_copies(t):
        slot, block = lax.rem(t, SLOTS), lax.rem(t, 2)
        return (
            to_seq(mid_a.at[block, 1 - y], second_in_a.at[slot], 2, slot, 4),
            to_seq(mid_b.at[block, 1 - x], second_in_b.at[slot], 3, slot, 2),
        )

    def rep_copy(t):
        slot = lax.rem(t, SLOTS)
        return pltpu.make_async_remote_copy(
            clip.at[lax.rem(t, 2)], rep_in.at[slot], rep_sem.at[0, 0, slot], rep_sem.at[1, 0, slot],
            device_id={"rep": z ^ 1},
        )

    def inner_copy(t):
        slot = lax.rem(t, SLOTS)
        return pltpu.make_async_remote_copy(
            joined.at[lax.rem(t, 2)], inner_in.at[slot],
            rep_sem.at[0, 1, slot], rep_sem.at[1, 1, slot],
            device_id={"rep": z ^ 3},
        )

    def back_copy(t):
        slot = lax.rem(t, BACK)
        return pltpu.make_async_remote_copy(
            final.at[lax.rem(t, 2)], back_in.at[slot], back_sem.at[0, slot], back_sem.at[1, slot],
            device_id={"rep": z ^ 1},
        )

    loads(0, 0)

    def turn(t, carry):
        def stage(back):
            return (t >= back) & (t < total + back)

        now2, was2 = lax.rem(t, 2), lax.rem(t + 1, 2)
        was3 = lax.rem(t + 2, SLOTS)

        @pl.when(t + 1 < total)
        def _():
            loads(t + 1, was2)

        @pl.when(stage(1))
        def _():
            for copy in first_copies(t):
                copy.start()

        @pl.when(stage(2))
        def _():
            block = lax.rem(t + 1, SLOTS)
            for at in range(2):
                mid_a[now2, at] = part[block, at, x, :, :edge] + first_in_a[was3, at]
                mid_b[now2, at] = part[block, y, at, :, edge:] + first_in_b[was3, at]
            for copy in second_copies(t):
                copy.start()

        @pl.when(stage(3))
        def _():
            clip[now2, :, :edge] = mid_a[was2, y] + second_in_a[was3]
            clip[now2, :, edge:] = mid_b[was2, x] + second_in_b[was3]

            @pl.when(outer)
            def _():
                rep_copy(t).start()

        @pl.when(stage(4) & inner)
        def _():
            joined[now2] = clip[was2] + rep_in[was3]
            inner_copy(t).start()

        @pl.when(stage(5) & inner)
        def _():
            final[now2] = joined[was2] + inner_in[was3]
            back_copy(t).start()

        @pl.when(stage(6))
        def _():
            @pl.when(inner)
            def _():
                wide[now2] = final[was2].astype(jnp.float32)

            @pl.when(outer)
            def _():
                wide[now2] = back_in[lax.rem(t + 3, BACK)].astype(jnp.float32)

            store(t - 6, now2)

        @pl.when(t < total)
        def _():
            wait_loads(now2)
            slot3 = lax.rem(t, SLOTS)

            def product(which):
                def columns(j, carry):
                    at = pl.ds(pl.multiple_of(j * (width // 3), width // 3), width // 3)
                    block = left[now2, :, which]
                    four, _, depth = block.shape
                    got = jnp.dot(
                        block.reshape(four * rows, depth), right[now2, :, at],
                        preferred_element_type=jnp.float32,
                    ).astype(jnp.bfloat16)
                    return at, got.reshape(four, rows, width // 3)
                return columns

            def away_columns(j, carry):
                at, got = product(1 - core)(j, carry)
                away[:, :, at] = got
                return carry

            lax.fori_loop(0, 3, away_columns, 0)
            pair_copy(t).start()

            def kept_columns(j, carry):
                at, got = product(core)(j, carry)
                part[slot3, 0, :, :, at] = got[:2]
                part[slot3, 1, :, :, at] = got[2:]
                return carry

            lax.fori_loop(0, 3, kept_columns, 0)
            pair_copy(t).wait()

            def add(j, carry):
                part[slot3, j // 2, j % 2] = part[slot3, j // 2, j % 2] + pair_in[now2, j]
                return carry

            lax.fori_loop(0, 4, add, 0)

        @pl.when(stage(1))
        def _():
            for copy in first_copies(t):
                copy.wait()

        @pl.when(stage(2))
        def _():
            for copy in second_copies(t):
                copy.wait()

        @pl.when(stage(3))
        def _():
            @pl.when(outer)
            def _():
                rep_copy(t).wait_send()

            @pl.when(inner)
            def _():
                rep_copy(t).wait_recv()

        @pl.when(stage(4) & inner)
        def _():
            inner_copy(t).wait()

        @pl.when(stage(5))
        def _():
            @pl.when(inner)
            def _():
                back_copy(t).wait_send()

            @pl.when(outer)
            def _():
                back_copy(t).wait_recv()

        @pl.when(stage(6))
        def _():
            pltpu.make_async_copy(wide.at[now2], outs[1], store_sem.at[now2]).wait()

        return carry

    lax.fori_loop(0, 2, turn, 0)
    for copy in mod_copies:
        copy.wait()
    mod_total = mod_in[0].astype(jnp.float32)
    for device in range(1, 8):
        mod_total += mod_in[device].astype(jnp.float32)
    every_mod[z] = mod_total.astype(every_mod.dtype)
    for copy in clip_copies:
        copy.start()
    lax.fori_loop(2, total + 6, turn, 0)
    for copy in clip_copies:
        copy.wait()


def reduce_grads(layers, mods, cid):
    tokens = layers[0][4].shape[0]
    rows, width = layers[0][0].shape[2], layers[0][5].shape[1]
    edge = width * 5 // 9 // 128 * 128
    low = jnp.bfloat16
    outs = []
    for ops in layers:
        for kind in range(4):
            tall = ops[kind].shape[2] if kind == 3 else 1
            outs.append(jax.ShapeDtypeStruct((tall * rows, ops[4 + kind].shape[1]), jnp.float32))
    outs.append(jax.ShapeDtypeStruct((4,) + mods.shape, mods.dtype))
    vm = pltpu.VMEM
    dma = pltpu.SemaphoreType.DMA
    flops = sum(2 * tokens * 8 * o.size for o in outs[:-1])
    got = pl.pallas_call(
        functools.partial(reduce_kernel, len(layers), rows, width, edge),
        out_shape=outs,
        in_specs=[pl.BlockSpec(memory_space=pl.ANY)] * (8 * len(layers))
        + [pl.BlockSpec(memory_space=vm)],
        out_specs=[pl.BlockSpec(memory_space=pl.ANY)] * (4 * len(layers))
        + [pl.BlockSpec(memory_space=vm)],
        scratch_shapes=[
            vm((2, 4, 2, rows, tokens), low),
            vm((2, tokens, width), low),
            vm((4, rows, width), low),
            vm((2, 4, rows, width), low),
            vm((SLOTS, 2, 2, rows, width), low),
            vm((SLOTS, 2, rows, edge), low),
            vm((SLOTS, 2, rows, width - edge), low),
            vm((2, 2, rows, edge), low),
            vm((2, 2, rows, width - edge), low),
            vm((SLOTS, rows, edge), low),
            vm((SLOTS, rows, width - edge), low),
            vm((2, rows, width), low),
            vm((SLOTS, rows, width), low),
            vm((2, rows, width), low),
            vm((SLOTS, rows, width), low),
            vm((2, rows, width), low),
            vm((BACK, rows, width), low),
            vm((2, rows, width), jnp.float32),
            vm((8,) + mods.shape, mods.dtype),
            dma((2, 2)),
            dma((2, 2)),
            dma((2, 4, SLOTS)),
            dma((2, 2, SLOTS)),
            dma((2, BACK)),
            dma((2,)),
            dma((2, 11)),
        ],
        compiler_params=pltpu.CompilerParams(
            collective_id=cid, has_side_effects=True, vmem_limit_bytes=48 << 20
        ),
        cost_estimate=pl.CostEstimate(flops=flops, bytes_accessed=4 * sum(o.size for o in outs), transcendentals=0),
        name="reduce_grads",
    )(*[op for ops in layers for op in ops], mods)
    return [tuple(got[4 * at : 4 * at + 4]) for at in range(len(layers))], got[-1]


def reduce_operands(lefts, rights):
    features = rights[1].shape[1]
    shaped = []
    for left in lefts:
        tall, tokens = left.shape[0] // features, left.shape[1]
        shape = (4, 2, features // 8, tokens) if tall == 1 else (4, 2, tall, features // 8, tokens)
        shaped.append(left.reshape(shape))
    return (*shaped, *rights)


def layer_backward(g, x, mod, weights, kept, other, spatial, done=None, frames=None, cids=(None,) * 3):
    qkv_w, out_w, up_w, down_w = weights
    du, df, dx1, da, sums, *moved = mlp_backward(
        g, kept["x1"], kept["branch"], kept["mlp"], mod, up_w, down_w, kept["slope"], done, cids[0]
    )
    dqkv = attention_backward(da, kept["qkv"], kept["prob"], out_w, other, spatial, cids[1])
    dx, last_sums = qkv_backward(dqkv, qkv_w, x, dx1, mod, frames, cids[2])
    mod_grad = jnp.concatenate([last_sums[:2], sums[:4]], 0).reshape(1, -1)
    lefts = [kept[name] for name in ("h", "o", "h2", "z")]
    return dx, moved, mod_grad, reduce_operands(lefts, (dqkv, da, du, df))


def fused_device(frames_in, conditioning, shards, partial_mod, cotangent):
    _, _, frames, places, features = frames_in.shape
    tokens = frames * places
    low_cotangent = cotangent.reshape(frames, places, features).astype(LOW)
    x_one = frames_in.reshape(tokens, features)
    weights, (mods, conditions, g_two, other, x_two, y_two), (kept_one, kept_two) = forward(
        shards, partial_mod.reshape(-1, LANES), conditioning.reshape(-1, LANES), low_cotangent,
        x_one, 0,
    )
    g_one, (block_out,), mod_grad_two, operands_two = layer_backward(
        g_two.reshape(tokens, features), x_two.reshape(tokens, features), mods[1], weights[4:],
        kept_two, None, False, y_two.reshape(g_two.shape), frames, (5, None, 6),
    )
    input_grad, _, mod_grad_one, operands_one = layer_backward(
        g_one.reshape(tokens, features), x_one, mods[0], weights[:4], kept_one,
        other.reshape(frames, places, 2 * features), True, cids=(None, 3, None),
    )
    mod_grads = jnp.concatenate([mod_grad_one, mod_grad_two], 1).astype(LOW)
    (grads_two, grads_one), every_mod = reduce_grads(
        [operands_two, operands_one], mod_grads.reshape(-1, LANES), 1
    )
    every_mod = every_mod.reshape(-1, mod_grads.shape[1])
    return (
        block_out.astype(WIDE), input_grad, grads_one, grads_two, every_mod,
        conditions.reshape(-1, features),
    )


def per_device(
    frames_in,
    conditioning,
    mod_first,
    qkv_first,
    out_first,
    up_first,
    down_first,
    mod_second,
    qkv_second,
    out_second,
    up_second,
    down_second,
    cotangent,
):
    clip_count, _, frame_dev, half_places, features = frames_in.shape
    fused = lax.axis_size("seq") == 8 and lax.axis_size("rep") == 4 and clip_count == 1
    row_count = mod_first.shape[0]
    row_start = lax.axis_index("seq") * row_count
    mod_width = mod_first.shape[1]
    rows_of = lambda whole: lax.dynamic_slice_in_dim(whole, row_start, row_count, 1)
    silu_local = rows_of(jax.nn.silu(conditioning)).astype(jnp.bfloat16)
    partial_mod = jnp.concatenate(
        [
            jnp.dot(silu_local, mod_first, preferred_element_type=jnp.float32),
            jnp.dot(silu_local, mod_second, preferred_element_type=jnp.float32),
        ],
        1,
    )
    shards = (
        qkv_first, out_first, up_first, down_first,
        qkv_second, out_second, up_second, down_second,
    )
    if fused:
        block_out, stream_grad, grads_one, grads_two, every_mod, conditions = fused_device(
            frames_in, conditioning, shards, partial_mod, cotangent
        )
        every_silu = rows_of(jax.nn.silu(conditions)).astype(jnp.bfloat16)
        mod_total = lax.dynamic_slice_in_dim(every_mod, lax.axis_index("rep"), 1, 0)
    else:
        weights = [lax.all_gather(shard, "seq", axis=0, tiled=True) for shard in shards]
        modulation = lax.psum(partial_mod, "seq")
        every_silu = lax.all_gather(silu_local, "rep", axis=0, tiled=True)
        mod_one, mod_two = modulation[:, :mod_width], modulation[:, mod_width:]
        weights_one, weights_two = weights[:4], weights[4:]
        start_stream = frames_in.reshape(clip_count, frame_dev, half_places, features).astype(
            jnp.float32
        )
        spatial_out, state_one = forward_layer(start_stream, mod_one, weights_one, True)
        placed = to_places(spatial_out)
        temporal_out, state_two = forward_layer(placed, mod_two, weights_two, False)
        block_out = to_frames(temporal_out, frame_dev)
        cotangent_sites = to_places(
            cotangent.reshape(clip_count, frame_dev, half_places, features)
        )
        placed_grad, mod_grad_two, pairs_two = backward_layer(
            cotangent_sites, placed, mod_two, weights_two, state_two, False
        )
        spatial_grad = to_frames(placed_grad, frame_dev)
        stream_grad, mod_grad_one, pairs_one = backward_layer(
            spatial_grad, start_stream, mod_one, weights_one, state_one, True
        )
        mod_grads = jnp.concatenate([mod_grad_one, mod_grad_two], 1).astype(jnp.bfloat16)
        grads_two, grads_one = layer_grads(pairs_two), layer_grads(pairs_one)
        mod_total = lax.psum(mod_grads, "seq").astype(jnp.bfloat16)
        every_mod = lax.all_gather(mod_total, "rep", axis=0, tiled=True)
    low_one, low_two = mod_total[:, :mod_width], mod_total[:, mod_width:]
    mod_weight_one = jnp.einsum(
        "cd,ce->de", every_silu, every_mod[:, :mod_width], preferred_element_type=jnp.float32
    )
    mod_weight_two = jnp.einsum(
        "cd,ce->de", every_silu, every_mod[:, mod_width:], preferred_element_type=jnp.float32
    )
    silu_grad = jnp.einsum("ce,de->cd", low_one, mod_first, preferred_element_type=jnp.float32)
    silu_grad = silu_grad + jnp.einsum(
        "ce,de->cd", low_two, mod_second, preferred_element_type=jnp.float32
    )
    condition_grad = jax.vjp(jax.nn.silu, rows_of(conditioning))[1](silu_grad)[0]
    out_shape = (clip_count, 1, frame_dev, half_places, features)
    return (
        block_out.reshape(out_shape),
        stream_grad.reshape(out_shape),
        condition_grad,
        mod_weight_one,
        *grads_one,
        mod_weight_two,
        *grads_two,
    )


def solution(mesh):
    return jax.shard_map(
        per_device,
        mesh=mesh,
        in_specs=(
            P("rep", "seq", None, None, None),
            P("rep", None),
            P("seq", None),
            P("seq", None),
            P("seq", None),
            P("seq", None),
            P("seq", None),
            P("seq", None),
            P("seq", None),
            P("seq", None),
            P("seq", None),
            P("seq", None),
            P("rep", "seq", None, None, None),
        ),
        out_specs=(
            P("rep", "seq", None, None, None),
            P("rep", "seq", None, None, None),
            P("rep", "seq"),
            P("seq", None),
            P("seq", None),
            P("seq", None),
            P("seq", None),
            P("seq", None),
            P("seq", None),
            P("seq", None),
            P("seq", None),
            P("seq", None),
            P("seq", None),
        ),
        check_vma=False,
    )
```

```python
import functools
import math

import jax
import jax.numpy as jnp
from jax import lax
from jax.experimental import pallas as pl
from jax.experimental.pallas import tpu as pltpu
from jax.sharding import PartitionSpec as P

HEADS = 16
HEAD_WIDTH = 72


norm_epsilon = 1e-06


def from_partner(block, axis, apart):
    count = lax.axis_size(axis)
    route = []
    for low in range(count):
        high = low | 1 << apart
        if high != low and high < count:
            route += [(low, high), (high, low)]
    return lax.ppermute(block, axis, route)


def shortened(x):
    return jax.tree.map(lambda a: a.astype(jnp.bfloat16) if a.dtype == jnp.float32 else a, x)


def layer_mod(stream, shift_part, scale_part):
    row_mean = jnp.mean(stream, axis=-1, keepdims=True)
    centred = stream - row_mean
    row_var = jnp.mean(centred * centred, axis=-1, keepdims=True)
    return centred * lax.rsqrt(row_var + norm_epsilon) * (1.0 + scale_part) + shift_part


def gelu_tanh(pre_value):
    return jax.nn.gelu(pre_value, approximate=True)


def project(left_operand, right_operand):
    return jnp.einsum(
        "csld,de->csle", left_operand, right_operand, preferred_element_type=jnp.float32
    )


def project_back(incoming, right_operand):
    return jnp.einsum("csle,de->csld", incoming, right_operand, preferred_element_type=jnp.float32)


def mod_parts(modulation):
    return [segment[:, None, None, :] for segment in jnp.split(modulation, 6, axis=-1)]


def partner_values(stacked):
    return from_partner(stacked, "seq", 0)


def partner_grads(stacked):
    return from_partner(stacked.astype(jnp.bfloat16), "seq", 0).astype(stacked.dtype)


def to_places(stream):
    clip_count, frame_dev, half_places, features = stream.shape
    devices = lax.axis_size("seq")
    place_part = half_places // devices
    exchanged = lax.all_to_all(
        stream.reshape(1, clip_count, frame_dev, devices, place_part, features).astype(
            jnp.bfloat16
        ),
        "seq",
        split_axis=3,
        concat_axis=0,
        tiled=True,
    ).astype(jnp.float32)
    exchanged = exchanged.reshape(devices // 2, 2, clip_count, frame_dev, place_part, features)
    exchanged = jnp.transpose(exchanged, (2, 1, 4, 0, 3, 5))
    return exchanged.reshape(clip_count, 2 * place_part, devices // 2 * frame_dev, features)


def to_frames(stream, frame_dev):
    clip_count, place_count, frame_total, features = stream.shape
    devices = lax.axis_size("seq")
    place_part = place_count // 2
    arranged = stream.reshape(clip_count, 2, place_part, devices // 2, frame_dev, features)
    arranged = jnp.transpose(arranged, (3, 1, 0, 4, 2, 5)).reshape(
        devices, clip_count, frame_dev, 1, place_part, features
    )
    exchanged = lax.all_to_all(
        shortened(arranged), "seq", split_axis=0, concat_axis=3, tiled=True
    ).astype(arranged.dtype)
    return exchanged.reshape(clip_count, frame_dev, devices * place_part, features)


def forward_layer(stream, modulation, weights, spatial):
    qkv_w, out_w, up_w, down_w = weights
    shift_attn, scale_attn, gate_attn, shift_mlp, scale_mlp, gate_mlp = mod_parts(modulation)
    clip_count, seq_count, seq_len, features = stream.shape
    normed = layer_mod(stream, shift_attn, scale_attn).astype(jnp.bfloat16)
    projected = project(normed, qkv_w).astype(jnp.bfloat16)
    queries, keys_all, values_all = jnp.split(projected, 3, axis=-1)
    if spatial:
        remote = partner_values(jnp.stack([keys_all, values_all]))
        keys_all = jnp.concatenate([keys_all, remote[0]], axis=2)
        values_all = jnp.concatenate([values_all, remote[1]], axis=2)
    key_len = keys_all.shape[2]
    queries = queries.reshape(clip_count, seq_count, seq_len, HEADS, HEAD_WIDTH)
    keys_all = keys_all.reshape(clip_count, seq_count, key_len, HEADS, HEAD_WIDTH)
    values_all = values_all.reshape(clip_count, seq_count, key_len, HEADS, HEAD_WIDTH)
    scores = jnp.einsum(
        "cslhe,csmhe->cshlm", queries, keys_all, preferred_element_type=jnp.float32
    ) * HEAD_WIDTH ** (-0.5)
    peak_score = jnp.max(scores, axis=-1, keepdims=True)
    scaled_exp = jnp.exp(scores - peak_score)
    attention = scaled_exp / jnp.sum(scaled_exp, axis=-1, keepdims=True)
    attention_low = attention.astype(jnp.bfloat16)
    attended = jnp.einsum(
        "cshlm,csmhe->cslhe", attention_low, values_all, preferred_element_type=jnp.float32
    )
    attended = attended.astype(jnp.bfloat16).reshape(clip_count, seq_count, seq_len, features)
    branch = project(attended, out_w)
    middle = stream + gate_attn * branch
    normed_mid = layer_mod(middle, shift_mlp, scale_mlp).astype(jnp.bfloat16)
    hidden_pre = project(normed_mid, up_w)
    hidden = gelu_tanh(hidden_pre).astype(jnp.bfloat16)
    mlp_out = project(hidden, down_w)
    result = middle + gate_mlp * mlp_out
    kept_state = (
        normed,
        queries,
        keys_all,
        values_all,
        attention,
        attention_low,
        attended,
        branch,
        middle,
        normed_mid,
        hidden_pre,
        hidden,
        mlp_out,
    )
    return (result, kept_state)


def backward_layer(result_grad, stream, modulation, weights, kept_state, spatial):
    qkv_w, out_w, up_w, down_w = weights
    (
        normed,
        queries,
        keys_all,
        values_all,
        attention,
        attention_low,
        attended,
        branch,
        middle,
        normed_mid,
        hidden_pre,
        hidden,
        mlp_out,
    ) = kept_state
    shift_attn, scale_attn, gate_attn, shift_mlp, scale_mlp, gate_mlp = mod_parts(modulation)
    clip_count, seq_count, seq_len, features = stream.shape
    gate_mlp_grad = jnp.sum(result_grad * mlp_out, axis=(1, 2))
    mlp_grad = (gate_mlp * result_grad).astype(jnp.bfloat16)
    hidden_grad = project_back(mlp_grad, down_w)
    pre_grad = jax.vjp(gelu_tanh, hidden_pre)[1](hidden_grad)[0].astype(jnp.bfloat16)
    normed_mid_grad = project_back(pre_grad, up_w)
    middle_ln_grad, shift_mlp_grad, scale_mlp_grad = jax.vjp(
        layer_mod, middle, shift_mlp, scale_mlp
    )[1](normed_mid_grad)
    middle_grad = result_grad + middle_ln_grad
    gate_attn_grad = jnp.sum(middle_grad * branch, axis=(1, 2))
    branch_grad = (gate_attn * middle_grad).astype(jnp.bfloat16)
    attended_grad = project_back(branch_grad, out_w).astype(jnp.bfloat16)
    attended_grad = attended_grad.reshape(clip_count, seq_count, seq_len, HEADS, HEAD_WIDTH)
    attention_grad = jnp.einsum(
        "cslhe,csmhe->cshlm", attended_grad, values_all, preferred_element_type=jnp.float32
    )
    scores_grad = attention * (
        attention_grad - jnp.sum(attention_grad * attention, axis=-1, keepdims=True)
    )
    scores_grad = scores_grad.astype(jnp.bfloat16)
    inv_root = HEAD_WIDTH ** (-0.5)
    queries_grad = (
        jnp.einsum("cshlm,csmhe->cslhe", scores_grad, keys_all, preferred_element_type=jnp.float32)
        * inv_root
    )
    keys_grad = (
        jnp.einsum("cshlm,cslhe->csmhe", scores_grad, queries, preferred_element_type=jnp.float32)
        * inv_root
    )
    values_grad = jnp.einsum(
        "cshlm,cslhe->csmhe", attention_low, attended_grad, preferred_element_type=jnp.float32
    )
    if spatial:
        returned = partner_grads(
            jnp.stack([keys_grad[:, :, seq_len:], values_grad[:, :, seq_len:]])
        )
        keys_grad = keys_grad[:, :, :seq_len] + returned[0]
        values_grad = values_grad[:, :, :seq_len] + returned[1]
    qkv_grad = jnp.concatenate(
        [
            component.reshape(clip_count, seq_count, seq_len, features)
            for component in (queries_grad, keys_grad, values_grad)
        ],
        axis=-1,
    )
    qkv_grad = qkv_grad.astype(jnp.bfloat16)
    normed_grad = project_back(qkv_grad, qkv_w)
    stream_ln_grad, attention_shift_gradient, scale_attn_grad = jax.vjp(
        layer_mod, stream, shift_attn, scale_attn
    )[1](normed_grad)
    stream_grad = middle_grad + stream_ln_grad
    mod_grad = jnp.concatenate(
        [
            attention_shift_gradient.reshape(clip_count, features),
            scale_attn_grad.reshape(clip_count, features),
            gate_attn_grad,
            shift_mlp_grad.reshape(clip_count, features),
            scale_mlp_grad.reshape(clip_count, features),
            gate_mlp_grad,
        ],
        axis=-1,
    )
    grad_pairs = (
        (normed, qkv_grad),
        (attended, branch_grad),
        (normed_mid, pre_grad),
        (hidden, mlp_grad),
    )
    return (stream_grad, mod_grad, grad_pairs)


def bit_count(axis):
    return lax.axis_size(axis).bit_length() - 1


def swap(block, axis, bit):
    count = lax.axis_size(axis)
    return lax.ppermute(block, axis, [(at, at ^ (1 << bit)) for at in range(count)])


def bit_of(axis, bit):
    return (lax.axis_index(axis) >> bit) & 1


def pick(block, which, axis):
    return lax.dynamic_index_in_dim(block, which, axis, keepdims=False)


def spread_rows_out(left_turned, right_operand, flipped):
    bits = bit_count("seq")
    total_rows, tokens = left_turned.shape
    rows = total_rows >> bits
    halves = left_turned.reshape(1 << (bits - 1), 2, rows, tokens)
    core = bit_of("seq", 0)

    def product(which):
        left = pick(halves, which, 1).reshape(-1, tokens)
        return jnp.dot(left, right_operand, preferred_element_type=jnp.float32).astype(
            jnp.bfloat16
        )

    arrived = swap(product(1 - core), "seq", 0)
    held = product(core)
    left_bits = list(range(bits - 1, 0, -1))
    shape = [2] * (bits - 1) + [rows, right_operand.shape[1]]
    held = held.reshape(shape)
    arrived = arrived.reshape(shape)
    order = list(left_bits) if flipped else left_bits[::-1]
    for bit in order:
        at = left_bits.index(bit)
        mine = bit_of("seq", bit)
        away = pick(held, 1 - mine, at).astype(jnp.float32) + pick(arrived, 1 - mine, at)
        kept = pick(held, mine, at).astype(jnp.float32) + pick(arrived, mine, at)
        arrived = swap(away.astype(jnp.bfloat16), "seq", bit)
        held = kept.astype(jnp.bfloat16)
        left_bits.remove(bit)
    return held.astype(jnp.float32) + arrived


def rep_sum(block, axis):
    bits = bit_count("rep")
    held = block.astype(jnp.bfloat16)
    for bit in range(bits):
        mine = bit_of("rep", bit)
        low, high = jnp.split(held, 2, axis)
        away = jnp.where(mine == 0, high, low)
        kept = jnp.where(mine == 0, low, high)
        held = (kept.astype(jnp.float32) + swap(away, "rep", bit)).astype(jnp.bfloat16)
    for bit in reversed(range(bits)):
        mine = bit_of("rep", bit)
        other = swap(held, "rep", bit)
        low = jnp.where(mine == 0, held, other)
        high = jnp.where(mine == 0, other, held)
        held = jnp.concatenate([low, high], axis)
    return held.astype(jnp.float32)


def turned(operand):
    return operand.reshape(-1, operand.shape[-1]).T


def flat(operand):
    return operand.reshape(-1, operand.shape[-1])


def cut(width, parts, of):
    return width * parts // of // 128 * 128


def down_grad(pair):
    left, right = turned(pair[0]), flat(pair[1])
    edge = cut(right.shape[1], 5, 9)
    return jnp.concatenate(
        [
            rep_sum(spread_rows_out(left, right[:, :edge], False), 0),
            rep_sum(spread_rows_out(left, right[:, edge:], True), 0),
        ],
        1,
    )


def up_grad(pair):
    left, right = turned(pair[0]), flat(pair[1])
    edge = cut(right.shape[1], 4, 9)
    return jnp.concatenate(
        [
            rep_sum(spread_rows_out(left, right[:, :edge], False), 1),
            rep_sum(spread_rows_out(left, right[:, edge:], True), 1),
        ],
        1,
    )


def attention_grads(qkv_pair, out_pair):
    left, right = turned(qkv_pair[0]), flat(qkv_pair[1])
    width = right.shape[1]
    edge = cut(width, 16, 27)
    first = rep_sum(spread_rows_out(left, right[:, :edge], False), 1)
    second = spread_rows_out(left, right[:, edge:], True)
    third = spread_rows_out(turned(out_pair[0]), flat(out_pair[1]), True)
    joined = rep_sum(jnp.concatenate([second, third], 1), 1)
    return (
        jnp.concatenate([first, joined[:, : width - edge]], 1),
        joined[:, width - edge :],
    )


def layer_grads(grad_pairs):
    qkv_pair, out_pair, up_pair, down_pair = grad_pairs
    down = down_grad(down_pair)
    up = up_grad(up_pair)
    qkv, out = attention_grads(qkv_pair, out_pair)
    return (qkv, out, up, down)


AHEAD = 2


def gather_pieces(shapes):
    features = math.gcd(*(columns for _, columns in shapes), 8 * shapes[0][0])
    rows_of = features // 8
    return rows_of, features, [
        (at, row, column)
        for at, (rows, columns) in enumerate(shapes)
        for row in range(0, rows, rows_of)
        for column in range(0, columns, features)
    ]


class Gather:
    def __init__(self, shapes, refs):
        count = len(shapes)
        self.count = count
        self.least, self.wide, self.pieces = gather_pieces(shapes)
        self.shards, self.fulls = refs[0], refs[1]
        self.held = refs[2][: count // 2]
        self.first_sem, self.second_sem, self.rep_sem, self.pair_sem, self.local_sem = refs[2][
            count // 2 :
        ]
        self.me, self.z = lax.axis_index("seq"), lax.axis_index("rep")
        odd = self.z & 1
        self.first, self.second = 2 + 2 * odd, 4 - 2 * odd

    @staticmethod
    def scratch(shapes):
        size = len(gather_pieces(shapes)[2])
        dma = pltpu.SemaphoreType.DMA
        half = shapes[: len(shapes) // 2]
        return [pltpu.VMEM(shape, jnp.bfloat16) for shape in half] + [
            dma((2, size)), dma((2, size)), dma((2, size)), dma((4, 2, size)), dma((2, len(shapes))),
        ]

    @staticmethod
    def outs(shapes):
        return [jax.ShapeDtypeStruct((8,) + shape, jnp.bfloat16) for shape in shapes]

    def place(self, owner, at):
        weight, row, column = self.pieces[at]
        return self.fulls[weight].at[owner, pl.ds(row, self.least), pl.ds(column, self.wide)]

    def own(self, at):
        weight, row, column = self.pieces[at]
        return self.shards[weight].at[pl.ds(row, self.least), pl.ds(column, self.wide)]

    def to_seq(self, source, owner, at, sems, mask):
        return pltpu.make_async_remote_copy(
            source, self.place(owner, at), sems.at[0, at], sems.at[1, at],
            device_id={"seq": self.me ^ mask},
        )

    def first_copy(self, at):
        return self.to_seq(self.own(at), self.me, at, self.first_sem, self.first)

    def second_copy(self, at):
        owner = self.me ^ self.first
        return self.to_seq(self.place(owner, at), owner, at, self.second_sem, self.second)

    def rep_copy(self, at):
        owner = self.me ^ self.first
        return pltpu.make_async_remote_copy(
            self.place(owner, at), self.place(owner, at), self.rep_sem.at[0, at], self.rep_sem.at[1, at],
            device_id={"rep": self.z ^ 1},
        )

    def pair_copy(self, which, at):
        if which == 0:
            return self.to_seq(self.own(at), self.me, at, self.pair_sem.at[0], 1)
        owner = self.me ^ (self.first, self.first ^ self.second, self.second)[which - 1]
        return self.to_seq(self.place(owner, at), owner, at, self.pair_sem.at[which], 1)

    def begin(self, at):
        self.first_copy(at).start()
        self.pair_copy(0, at).start()

    def fetch(self, weight):
        return pltpu.make_async_copy(
            self.shards[weight], self.held[weight % len(self.held)], self.local_sem.at[0, weight]
        )

    def keep(self, weight):
        return pltpu.make_async_copy(
            self.held[weight % len(self.held)], self.fulls[weight].at[self.me], self.local_sem.at[1, weight]
        )

    def start(self):
        for at in range(AHEAD):
            self.begin(at)
        self.local(0)

    def local(self, first):
        for weight in range(first, first + len(self.held)):
            self.fetch(weight).start()
        for weight in range(first, first + len(self.held)):
            self.fetch(weight).wait()
            self.keep(weight).start()

    def ready(self, weight):
        for at, piece in enumerate(self.pieces):
            if piece[0] == weight:
                for which in range(4):
                    self.pair_copy(which, at).wait_recv()
        self.keep(weight).wait()

    def advance(self, at):
        self.first_copy(at).wait_recv()
        if at + AHEAD < len(self.pieces):
            self.begin(at + AHEAD)
        self.second_copy(at).start()
        self.rep_copy(at).start()
        self.pair_copy(1, at).start()
        if at:
            self.share(at - 1)

    def share(self, at):
        self.second_copy(at).wait_recv()
        self.rep_copy(at).wait_recv()
        self.pair_copy(2, at).start()
        self.pair_copy(3, at).start()

    def finish(self):
        for at in range(len(self.pieces)):
            for copy in (self.first_copy(at), self.second_copy(at), self.rep_copy(at)):
                copy.wait_send()
            for which in range(4):
                self.pair_copy(which, at).wait_send()


def enter(seq_masks, rep_masks):
    me, z = lax.axis_index("seq"), lax.axis_index("rep")
    barrier = pltpu.get_barrier_semaphore()
    for mask in seq_masks:
        pl.semaphore_signal(barrier, inc=1, device_id={"seq": me ^ mask})
    for mask in rep_masks:
        pl.semaphore_signal(barrier, inc=1, device_id={"rep": z ^ mask})
    pl.semaphore_wait(barrier, len(seq_masks) + len(rep_masks))


LOW = jnp.bfloat16
WIDE = jnp.float32
LANES = 128
STRIP = 64
KEYS = 256


def whole_block(shape):
    return pl.BlockSpec(shape, lambda *at: (0,) * len(shape))


def strips(total, body):
    def step(j, carry):
        body(pl.ds(pl.multiple_of(j * STRIP, STRIP), STRIP))
        return carry

    lax.fori_loop(0, total // STRIP, step, 0)


def turn_into(target, source):
    for j in range(source.shape[1] // LANES):
        target[j * LANES : (j + 1) * LANES, :] = source[:, j * LANES : (j + 1) * LANES].T


def unit_rows(block):
    centred = block - jnp.mean(block, axis=-1, keepdims=True)
    spread = lax.rsqrt(jnp.mean(centred * centred, axis=-1, keepdims=True) + norm_epsilon)
    return centred * spread, spread


def into_norm(grad, scaled, unit, spread):
    inner = grad * scaled
    level = jnp.mean(inner, axis=-1, keepdims=True)
    slope = jnp.mean(inner * unit, axis=-1, keepdims=True)
    return spread * (inner - level - unit * slope)


def times(left, right):
    return jnp.dot(left, right, preferred_element_type=WIDE)


def times_turned(left, right):
    return lax.dot_general(left, right, (((1,), (1,)), ((), ())), preferred_element_type=WIDE)


def turned_times(left, right):
    return lax.dot_general(left, right, (((0,), (0,)), ((), ())), preferred_element_type=WIDE)


def params(size, cid=None):
    if cid is None:
        return pltpu.CompilerParams(vmem_limit_bytes=size << 20)
    return pltpu.CompilerParams(
        vmem_limit_bytes=size << 20, collective_id=cid, has_side_effects=True
    )


def cost(flops, size):
    return pl.CostEstimate(flops=flops, bytes_accessed=size, transcendentals=0)


def window(head):
    low, high = head * HEAD_WIDTH, (head + 1) * HEAD_WIDTH
    start = low // LANES * LANES
    stop = -(-high // LANES) * LANES
    return start, stop - start, low - start


def head_mask(head):
    start, wide, offset = window(head)
    lane = lax.broadcasted_iota(jnp.int32, (1, wide), 1)
    return ((lane >= offset) & (lane < offset + HEAD_WIDTH)).astype(WIDE).astype(LOW)


def add_window(total, head, block):
    start, wide, _ = window(head)
    for j in range(wide // LANES):
        tile = start // LANES + j
        lanes = slice(tile * LANES, (tile + 1) * LANES)
        piece = block[:, j * LANES : (j + 1) * LANES]
        if head == tile * LANES // HEAD_WIDTH:
            total[:, lanes] = piece
        else:
            total[:, lanes] = total[:, lanes] + piece


def same_place():
    row = lax.broadcasted_iota(jnp.int32, (KEYS, KEYS), 0)
    column = lax.broadcasted_iota(jnp.int32, (KEYS, KEYS), 1)
    return (row & 15) == (column & 15)


def moves(source, target, sems, local_sem, me, to_places):
    part = source.shape[-2] // 8 if to_places else source.shape[-2]

    def ends(device):
        if to_places:
            return source.at[:, pl.ds(pl.multiple_of(device * part, part), part)], target.at[me]
        return source.at[device], target.at[:, pl.ds(pl.multiple_of(me * part, part), part)]

    copies = [pltpu.make_async_copy(*ends(me), local_sem)]
    for mask in (6, 7, 2, 3, 4, 5, 1):
        copies.append(
            pltpu.make_async_remote_copy(
                *ends(me ^ mask), sems.at[0, mask], sems.at[1, mask], device_id={"seq": me ^ mask}
            )
        )
    return copies


def move_scratch():
    return [pltpu.SemaphoreType.DMA((2, 8)), pltpu.SemaphoreType.DMA(())]


def gelu_and_slope(value):
    inner = 0.7978845608028654 * (value + 0.044715 * value * value * value)
    bent = jnp.tanh(inner)
    half = 0.5 * (1.0 + bent)
    slope = half + 0.5 * value * (1.0 - bent * bent) * (
        0.7978845608028654 * (1.0 + 3 * 0.044715 * value * value)
    )
    return value * half, slope


OUTS = ("qkv", "prob", "h", "o", "h2", "z", "slope", "x1", "branch", "mlp")
CHUNK = 768


def forward_kernel(shapes, *refs):
    count = len(shapes)
    shards, refs = refs[:count], refs[count:]
    partial, condition, tokens, x_ref = refs[:4]
    fulls, refs = refs[4 : 4 + count], refs[4 + count :]
    mod_ref, conditions, moved, other_ref, x2_ref, y_ref = refs[:6]
    outs = [dict(zip(OUTS, refs[6:16])), dict(zip(OUTS, refs[16:26]))]
    refs = refs[26:]
    (
        partials, x2, qkv, other, held, normed, total, middle, part, prob, turned, low, ready,
        tall, short, hidden, slope, small_sem, move_sem, stay_sem, next_move_sem, next_stay_sem, next_sem,
        pair_sem, weight_sem, out_sem, prob_sem, chunk_sem,
    ) = refs[:28]
    gather = Gather(shapes, (shards, fulls, refs[28:]))
    me, z = gather.me, gather.z
    features = x_ref.shape[1]
    steps = shapes[2][1] // CHUNK
    enter(range(1, 8), range(1, 4))

    small = []
    for mask in range(1, 8):
        small.append(pltpu.make_async_remote_copy(
            partial, partials.at[me], small_sem.at[0, mask], small_sem.at[1, mask],
            device_id={"seq": me ^ mask}))
    for mask in range(1, 4):
        small.append(pltpu.make_async_remote_copy(
            condition, conditions.at[z], small_sem.at[0, 7 + mask], small_sem.at[1, 7 + mask],
            device_id={"rep": z ^ mask}))
    small.append(pltpu.make_async_copy(partial, partials.at[me], small_sem.at[0, 0]))
    small.append(pltpu.make_async_copy(condition, conditions.at[z], small_sem.at[1, 0]))
    for copy in small:
        copy.start()
    gather.start()
    gather.advance(0)
    later = moves(tokens, moved, move_sem, stay_sem, me, True)
    for copy in later:
        copy.start()
    for copy in small:
        copy.wait()
    modulation = partials[0]
    for device in range(1, 8):
        modulation = modulation + partials[device]
    width = features // LANES
    for row in range(12):
        for j in range(width):
            at = row * width + j
            mod_ref[row // 6, row % 6 : row % 6 + 1, j * LANES : (j + 1) * LANES] = modulation[
                at : at + 1
            ]

    pending = {}
    names = ("turned", "qkv", "other", "low", "middle", "ready")

    def begin(name, source, target):
        settle(name)
        pending[name] = pltpu.make_async_copy(source, target, out_sem.at[names.index(name)])
        pending[name].start()

    def settle(name):
        copy = pending.pop(name, None)
        if copy is not None:
            copy.wait()

    def full(weight):
        return fulls[weight]

    def load(slot, source):
        return pltpu.make_async_copy(source, tall.at[slot], weight_sem.at[slot])

    def column_block(weight, column):
        return full(weight).at[:, :, pl.ds(column, features)]

    def exchange(j):
        return pltpu.make_async_remote_copy(
            qkv.at[pl.ds(2 * j, 2), :, pl.ds(features, 2 * features)], other.at[pl.ds(2 * j, 2)],
            pair_sem.at[0, j], pair_sem.at[1, j], device_id={"seq": me ^ 1},
        )

    def rows_of(ref, group, column, wide, spatial):
        lanes = slice(column, column + wide)
        if spatial:
            return ref[pl.ds(2 * group, 2), :, lanes].reshape(-1, wide)
        return jnp.concatenate([ref[2 * block + group, :, lanes] for block in range(4)], 0)

    def attend(layer, spatial, group, span, allowed):
        for head in range(HEADS):
            start, wide, _ = window(head)
            mask = head_mask(head)
            queries = rows_of(qkv, group, start, wide, spatial) * mask
            keys = rows_of(qkv, group, features + start, wide, spatial)
            values = rows_of(qkv, group, 2 * features + start, wide, spatial)
            if spatial:
                keys = jnp.concatenate([keys, rows_of(other, group, start, wide, True)], 0)
                values = jnp.concatenate(
                    [values, rows_of(other, group, features + start, wide, True)], 0
                )
            scores = times_turned(queries, keys) * HEAD_WIDTH ** (-0.5)
            if not spatial:
                scores = jnp.where(allowed, scores, -3e38)
            grown = jnp.exp(scores - jnp.max(scores, axis=-1, keepdims=True))
            chance = (grown / jnp.sum(grown, axis=-1, keepdims=True)).astype(LOW)
            prob[head, :span] = chance
            add_window(part.at[pl.ds(0, span)], head, times(chance, values * mask))
        got = part[:span].astype(LOW)
        if spatial:
            held[pl.ds(2 * group, 2)] = got.reshape(2, -1, features)
        else:
            for block in range(4):
                held[2 * block + group] = got[block * 64 : (block + 1) * 64]

    def flat_rows(ref):
        return ref[...].reshape(-1, features)

    def turn_out(source, target):
        settle("turned")
        for j in range(features // LANES):
            lanes = slice(j * LANES, (j + 1) * LANES)
            turned[lanes, :] = source[:, lanes].T
        begin("turned", turned, target)

    def layer(at_layer, spatial, x, plan):
        first = 4 * at_layer
        out = outs[at_layer]
        groups = 4 if spatial else 2
        span = x.shape[0] // groups
        mod = mod_ref.at[at_layer]

        def go(place):
            for at in plan.get(place, ()):
                if at is None:
                    gather.share(len(gather.pieces) - 1)
                else:
                    gather.advance(at)

        def go_when(place, index):
            for key, pieces in plan.items():
                if isinstance(key, tuple) and key[0] == place:
                    @pl.when(index == key[1])
                    def _():
                        for at in pieces:
                            gather.advance(at)

        scaled, shift = 1.0 + mod[1:2], mod[0:1]

        def norm(at):
            unit, _ = unit_rows(x[at].astype(WIDE))
            normed[at] = (unit * scaled + shift).astype(LOW)

        strips(x.shape[0], norm)
        turn_out(normed[...], out["h"])
        go("norm")
        gather.ready(first)
        load(0, column_block(first, 0)).start()
        settle("qkv")
        for j in range(3):
            load(j % 2, column_block(first, 0)).wait()
            if j < 2:
                load((j + 1) % 2, column_block(first, (j + 1) * features)).start()
            got = times(normed[...], tall[j % 2].reshape(features, features)).astype(LOW)
            qkv[:, :, j * features : (j + 1) * features] = got.reshape(8, -1, features)
            go(f"qkv{j}")
        begin("qkv", qkv, out["qkv"])
        if spatial:
            for j in range(groups):
                exchange(j).start()
        allowed = None if spatial else same_place()

        def prob_copy(group):
            return pltpu.make_async_copy(
                prob.at[:, pl.ds(0, span)], out["prob"].at[group], prob_sem
            )

        def one_group(group, carry):
            go_when("group", group)
            if spatial:
                exchange(group).wait_recv()

            @pl.when(group > 0)
            def _():
                prob_copy(group).wait()

            attend(at_layer, spatial, group, span, allowed)
            prob_copy(group).start()
            return carry

        lax.fori_loop(0, groups, one_group, 0)
        prob_copy(0).wait()
        if spatial:
            begin("other", other, other_ref)
            for j in range(groups):
                exchange(j).wait_send()
        go("attended")
        gather.ready(first + 1)
        load(0, full(first + 1)).start()
        attended = flat_rows(held)
        turn_out(attended, out["o"])
        load(0, full(first + 1)).wait()
        total[...] = times(attended, tall[0].reshape(features, features))
        gate, move, grow = mod[2:3], mod[3:4], 1.0 + mod[4:5]
        settle("low")
        settle("middle")

        def finish(at):
            branch = total[at]
            low[at] = branch.astype(LOW)
            got = x[at].astype(WIDE) + gate * branch
            middle[at] = got
            unit, _ = unit_rows(got)
            normed[at] = (unit * grow + move).astype(LOW)

        strips(x.shape[0], finish)
        begin("low", low, out["branch"])
        begin("middle", middle, out["x1"])
        turn_out(normed[...], out["h2"])
        go("middle")
        gather.ready(first + 2)
        gather.ready(first + 3)

        down = full(first + 3)
        per = down.shape[0] * down.shape[1] // steps

        def chunk_loads(step, slot):
            column = pl.multiple_of(step * CHUNK, CHUNK)
            owner = step * CHUNK // down.shape[1]
            copies = [
                pltpu.make_async_copy(
                    full(first + 2).at[:, :, pl.ds(column, CHUNK)],
                    tall.at[slot, :, :, pl.ds(0, CHUNK)], weight_sem.at[slot],
                )
            ]
            return copies, column, owner

        def start_loads(step, slot):
            copies, column, owner = chunk_loads(step, slot)
            for copy in copies:
                copy.start()
            pltpu.make_async_copy(
                down_rows(step), short.at[slot], weight_sem.at[2 + slot]
            ).start()

        def down_rows(step):
            return fulls_flat[at_layer].at[pl.ds(pl.multiple_of(step * 4, 4), 4)]

        fulls_flat = [fulls[3].reshape(*split_rows(fulls[3].shape)), fulls[7].reshape(*split_rows(fulls[7].shape))]

        def wait_loads(slot):
            for copy in chunk_loads(0, slot)[0]:
                copy.wait()
            pltpu.make_async_copy(down_rows(0), short.at[slot], weight_sem.at[2 + slot]).wait()

        def chunk_outs(step, slot):
            column = pl.multiple_of(step * CHUNK, CHUNK)
            return (
                pltpu.make_async_copy(
                    hidden.at[slot], out["z"].at[pl.ds(column, CHUNK)], chunk_sem.at[0, slot]
                ),
                pltpu.make_async_copy(
                    slope.at[slot], out["slope"].at[:, pl.ds(column, CHUNK)], chunk_sem.at[1, slot]
                ),
            )

        start_loads(0, 0)
        half = x.shape[0] // 2

        def chunk(step, carry):
            slot = lax.rem(step, 2)
            go_when("chunk", step)
            wait_loads(slot)

            @pl.when(step + 1 < steps)
            def _():
                start_loads(step + 1, 1 - slot)

            @pl.when(step >= 2)
            def _():
                for copy in chunk_outs(step, slot):
                    copy.wait()

            up = tall[slot, :, :, :CHUNK].reshape(features, CHUNK)
            for j in range(2):
                rows = slice(j * half, (j + 1) * half)
                value, bend = gelu_and_slope(times(normed[rows], up))
                slope[slot, rows] = bend.astype(LOW)
                value = value.astype(LOW)
                hidden[slot, :, rows] = value.T
                got = times(value, short[slot].reshape(CHUNK, features))

                @pl.when(step == 0)
                def _():
                    total[rows] = got

                @pl.when(step > 0)
                def _():
                    total[rows] = total[rows] + got

            for copy in chunk_outs(step, slot):
                copy.start()
            return carry

        lax.fori_loop(0, steps, chunk, 0)
        for slot in range(2):
            for copy in chunk_outs(0, slot):
                copy.wait()
        last = mod[5:6]
        settle("low")

        def close(at):
            mlp = total[at]
            low[at] = mlp.astype(LOW)
            total[at] = middle[at] + last * mlp

        strips(x.shape[0], close)
        begin("low", low, out["mlp"])
        ready[...] = total[...].astype(LOW).reshape(ready.shape)

    layer(0, True, x_ref, {
        "norm": (1, 2, 3), "qkv1": (4,), ("group", 0): (5,), ("group", 1): (6,), ("group", 2): (7,),
        ("group", 3): (8,), "attended": (9,), "middle": (10, 11, 12), ("chunk", 1): (13,),
        ("chunk", 3): (14,), ("chunk", 4): (15,),
    })
    copies = moves(ready, x2_ref, next_move_sem, next_stay_sem, me, True)
    for copy in later:
        copy.wait()
    for copy in copies:
        copy.start()
    gather.local(4)
    gather.advance(16)
    gather.advance(17)
    for copy in copies:
        copy.wait()
    fetch = pltpu.make_async_copy(x2_ref, x2, next_sem)
    fetch.start()
    fetch.wait()
    x2_rows = x2.reshape(x_ref.shape)
    layer(1, False, x2_rows, {
        "norm": (18,), "qkv0": (19,), "qkv2": (20,), ("group", 1): (21,), "attended": (22,),
        "middle": (23, None),
    })
    begin("ready", ready, y_ref)
    for name in names:
        settle(name)
    gather.finish()


def split_rows(shape):
    return (shape[0] * shape[1] // (CHUNK // 4), CHUNK // 4, shape[2])


def forward(shards, partial, condition, cotangent, x, cid):
    shapes = [shard.shape for shard in shards]
    count = len(shapes)
    tokens, features = x.shape
    frames, places, _ = cotangent.shape
    wide = shapes[2][1]
    any_ = pl.BlockSpec(memory_space=pl.ANY)
    struct = jax.ShapeDtypeStruct
    moved = struct((8, frames, places // 8, features), LOW)
    outs = Gather.outs(shapes) + [
        struct((2, 6, features), WIDE),
        struct((4,) + condition.shape, condition.dtype),
        moved,
        struct((8, tokens // 8, 2 * features), LOW),
        moved,
        struct((frames, places, features), LOW),
    ]
    for groups in (4, 2):
        outs += [
            struct((8, tokens // 8, 3 * features), LOW),
            struct((groups, HEADS, tokens // groups, KEYS), LOW),
            struct((features, tokens), LOW),
            struct((features, tokens), LOW),
            struct((features, tokens), LOW),
            struct((wide, tokens), LOW),
            struct((tokens, wide), LOW),
            struct((tokens, features), WIDE),
            struct((tokens, features), LOW),
            struct((tokens, features), LOW),
        ]
    dma = pltpu.SemaphoreType.DMA
    vm = pltpu.VMEM
    flops = 2 * tokens * 8 * sum(shape[0] * shape[1] for shape in shapes)
    got = pl.pallas_call(
        functools.partial(forward_kernel, shapes),
        out_shape=outs,
        in_specs=[any_] * (count + 3) + [pl.BlockSpec(memory_space=vm)],
        out_specs=[any_] * count + [pl.BlockSpec(memory_space=vm)] + [any_] * (len(outs) - count - 1),
        scratch_shapes=[
            vm((8,) + partial.shape, WIDE),
            vm(moved.shape, LOW),
            vm((8, tokens // 8, 3 * features), LOW),
            vm((8, tokens // 8, 2 * features), LOW),
            vm((8, tokens // 8, features), LOW),
            vm((tokens, features), LOW),
            vm((tokens, features), WIDE),
            vm((tokens, features), WIDE),
            vm((KEYS, features), WIDE),
            vm((HEADS, KEYS, KEYS), LOW),
            vm((features, tokens), LOW),
            vm((tokens, features), LOW),
            vm((frames, places, features), LOW),
            vm((2, 8, features // 8, features), LOW),
            vm((2, 4, CHUNK // 4, features), LOW),
            vm((2, CHUNK, tokens), LOW),
            vm((2, tokens, CHUNK), LOW),
            dma((2, 11)),
            *move_scratch(),
            *move_scratch(),
            dma(()),
            dma((2, 4)),
            dma((4,)),
            dma((8,)),
            dma(()),
            dma((2, 2)),
        ]
        + Gather.scratch(shapes),
        compiler_params=params(60, cid),
        cost_estimate=cost(flops, 4 * flops // tokens),
        name="forward",
    )(*shards, partial, condition, cotangent, x)
    weights = got[:count]
    named = [dict(zip(OUTS, got[count + 6 + 10 * at : count + 16 + 10 * at])) for at in range(2)]
    return weights, got[count : count + 6], named


SLOTS = 3
BACK = 4


KEPT = ("h", "o", "h2", "z", "qkv", "prob", "slope", "x1", "branch", "mlp")
RIGHTS = ("qkv", "da", "du", "df")
ORDER = (3, 2, 1, 0)


def backward_kernel(dims, *refs):
    rows, width, edge, tokens, total, spans = dims
    weights, refs = (refs[:4], refs[4:8]), refs[8:]
    kept = [dict(zip(KEPT, refs[10 * at : 10 * at + 10])) for at in range(2)]
    g_in, other_in, y_in, x_ins, mod_ref = refs[20], refs[21], refs[22], refs[23:25], refs[25]
    refs = refs[26:]
    grads, refs = (refs[:4], refs[4:8]), refs[8:]
    rights = [dict(zip(RIGHTS, refs[4 * at : 4 * at + 4])) for at in range(2)]
    every_mod, moved, input_grad, g_out = refs[8:12]
    (
        left, right, away, pair_in, part, first_in_a, first_in_b, mid_a, mid_b, second_in_a, second_in_b,
        clip, rep_in, joined, inner_in, final, back_in, wide,
        tall, short, acc, middle, grad_in, low, aux, slope, du, qkv, other, take, prob, dout,
        total_q, total_k, total_v, ready, sums, mod_low, mod_in,
        load_sem, pair_sem, link_sem, rep_sem, back_sem, store_sem, mod_sem, tall_sem, short_sem, slope_sem,
        in_sem, prob_sem, out_sem, swap_sem, move_sem, stay_sem, last_move_sem, last_stay_sem,
    ) = refs[12:]
    me, z = lax.axis_index("seq"), lax.axis_index("rep")
    core, x, y = me & 1, (me >> 1) & 1, (me >> 2) & 1
    inner = (z == 1) | (z == 2)
    outer = (z == 0) | (z == 3)
    features = width
    steps = weights[0][2].shape[2] // CHUNK
    root = HEAD_WIDTH ** (-0.5)


    def wait_out(source, target):
        copy = pltpu.make_async_copy(source, target, out_sem)
        copy.start()
        copy.wait()

    def flat_in(ref):
        return ref if len(ref.shape) == 2 else ref.reshape(tokens, features)

    def load_in(name, at):
        source, target = {
            "grad": (flat_in((g_out, g_in)[at]), grad_in),
            "mlp": (kept[at]["mlp"], aux),
            "branch": (kept[at]["branch"], aux),
            "x": (flat_in(x_ins[at]), aux),
            "x1": (kept[at]["x1"], middle),
            "qkv": (kept[at]["qkv"], qkv),
            "other": (other_in, other),
        }[name]
        order = ("grad", "mlp", "branch", "x", "x1", "qkv", "other")
        return pltpu.make_async_copy(source, target, in_sem.at[order.index(name)])

    def chunk_loads(at, step, slot):
        column = pl.multiple_of(step * CHUNK, CHUNK)
        down = weights[at][3].reshape(*split_rows(weights[at][3].shape))
        return (
            pltpu.make_async_copy(
                weights[at][2].at[:, :, pl.ds(column, CHUNK)],
                tall.at[slot, :, :, pl.ds(0, CHUNK)], tall_sem.at[slot],
            ),
            pltpu.make_async_copy(
                down.at[pl.ds(pl.multiple_of(step * 4, 4), 4)], short.at[slot], short_sem.at[slot]
            ),
            pltpu.make_async_copy(
                kept[at]["slope"].at[:, pl.ds(column, CHUNK)], slope.at[slot], slope_sem.at[slot]
            ),
        )

    def tall_load(source, slot):
        return pltpu.make_async_copy(source, tall.at[slot], tall_sem.at[slot])

    def qkv_block(at, j):
        return weights[at][0].at[:, :, pl.ds(j * features, features)]

    def mlp_begin(at):
        load_in("grad", at).start()
        load_in("mlp", at).start()
        load_in("x1", at).start()
        for slot in range(2):
            for copy in chunk_loads(at, slot, slot):
                copy.start()
        load_in("grad", at).wait()
        load_in("mlp", at).wait()
        gate = mod_ref[at, 5:6]
        sums[at] = jnp.zeros_like(sums[at])

        def begin(strip):
            grad = grad_in[strip].astype(WIDE)
            low[strip] = (gate * grad).astype(LOW)
            sums[at, 5:6] += jnp.sum(grad * aux[strip].astype(WIDE), axis=0, keepdims=True)

        strips(tokens, begin)
        load_in("branch", at).start()
        wait_out(low, rights[at]["df"])

    def mlp_chunk(at, step):
        slot = lax.rem(step, 2)
        for copy in chunk_loads(at, step, slot):
            copy.wait()
        half = tokens // 2
        up = tall[slot, :, :, :CHUNK].reshape(features, CHUNK)
        for j in range(2):
            strip = slice(j * half, (j + 1) * half)
            got = times_turned(low[strip], short[slot].reshape(CHUNK, features))
            got = (got * slope[slot, strip].astype(WIDE)).astype(LOW)
            du[strip] = got
            got = times_turned(got, up)

            @pl.when(step == 0)
            def _():
                acc[strip] = got

            @pl.when(step > 0)
            def _():
                acc[strip] = acc[strip] + got

        @pl.when(step + 2 < steps)
        def _():
            for copy in chunk_loads(at, step + 2, slot):
                copy.start()

        column = pl.multiple_of(step * CHUNK, CHUNK)
        wait_out(du, rights[at]["du"].at[:, pl.ds(column, CHUNK)])

    def prob_load(at, group):
        span = tokens // kept[at]["prob"].shape[0]
        return pltpu.make_async_copy(
            kept[at]["prob"].at[group], prob.at[:, pl.ds(0, span)], prob_sem
        )

    def mlp_finish(at):
        tall_load(weights[at][1], 0).start()
        tall_load(qkv_block(at, 0), 1).start()
        load_in("qkv", at).start()
        prob_load(at, 0).start()
        if at == 0:
            load_in("other", at).start()
        load_in("branch", at).wait()
        load_in("x1", at).wait()
        gate, scaled = mod_ref[at, 2:3], 1.0 + mod_ref[at, 4:5]

        def finish(strip):
            grad = acc[strip]
            unit, spread = unit_rows(middle[strip])
            got = grad_in[strip].astype(WIDE) + into_norm(grad, scaled, unit, spread)
            middle[strip] = got
            low[strip] = (gate * got).astype(LOW)
            sums[at, 2:3] += jnp.sum(got * aux[strip].astype(WIDE), axis=0, keepdims=True)
            sums[at, 3:4] += jnp.sum(grad, axis=0, keepdims=True)
            sums[at, 4:5] += jnp.sum(grad * unit, axis=0, keepdims=True)

        strips(tokens, finish)
        load_in("x", at).start()
        wait_out(low, rights[at]["da"])

    def project(at):
        tall_load(weights[at][1], 0).wait()
        half = tokens // 2
        for j in range(2):
            got = times_turned(
                low[j * half : (j + 1) * half], tall[0].reshape(features, features)
            ).astype(LOW)
            dout[4 * j : 4 * j + 4] = got.reshape(4, -1, features)
        tall_load(qkv_block(at, 1), 0).start()
        load_in("qkv", at).wait()
        if at == 0:
            load_in("other", at).wait()

    def rows_of(ref, group, column, lanes, spatial):
        lanes = slice(column, column + lanes)
        if spatial:
            block = ref[pl.ds(2 * group, 2), :, lanes]
            return block.reshape(-1, block.shape[2])
        return jnp.concatenate([ref[2 * block + group, :, lanes] for block in range(4)], 0)

    def swap_copy(j):
        return pltpu.make_async_remote_copy(
            other.at[pl.ds(2 * j, 2)], take.at[pl.ds(2 * j, 2)],
            swap_sem.at[0, j], swap_sem.at[1, j], device_id={"seq": me ^ 1},
        )

    def attend_group(at, group):
        spatial = at == 0
        groups = kept[at]["prob"].shape[0]
        span = tokens // groups
        prob_load(at, group).wait()
        for head in range(HEADS):
            start, lanes, _ = window(head)
            mask = head_mask(head)
            queries = rows_of(qkv, group, start, lanes, spatial) * mask
            keys = rows_of(qkv, group, features + start, lanes, spatial)
            values = rows_of(qkv, group, 2 * features + start, lanes, spatial)
            coming = rows_of(dout, group, start, lanes, spatial) * mask
            if spatial:
                keys = jnp.concatenate([keys, rows_of(other, group, start, lanes, True)], 0)
                values = jnp.concatenate(
                    [values, rows_of(other, group, features + start, lanes, True)], 0
                )
            chance = prob[head, :span]
            known = chance.astype(WIDE)
            dprob = times_turned(coming, values)
            level = jnp.sum(dprob * known, axis=-1, keepdims=True)
            dscores = (known * (dprob - level)).astype(LOW)
            add_window(total_q.at[pl.ds(0, span)], head, times(dscores, keys * mask))
            add_window(total_k, head, turned_times(dscores, queries))
            add_window(total_v, head, turned_times(chance, coming))

        @pl.when(group + 1 < groups)
        def _():
            prob_load(at, group + 1).start()

        pieces = (
            (total_q[:span] * root).astype(LOW),
            (total_k[:span] * root).astype(LOW),
            total_v[:span].astype(LOW),
        )
        for j, piece in enumerate(pieces):
            lanes = slice(j * features, (j + 1) * features)
            if spatial:
                qkv[pl.ds(2 * group, 2), :, lanes] = piece.reshape(2, -1, features)
            else:
                for block in range(4):
                    qkv[2 * block + group, :, lanes] = piece[block * 64 : (block + 1) * 64]
        if spatial:
            other[pl.ds(2 * group, 2), :, :features] = (
                (total_k[span:] * root).astype(LOW).reshape(2, -1, features)
            )
            other[pl.ds(2 * group, 2), :, features:] = (
                total_v[span:].astype(LOW).reshape(2, -1, features)
            )
            swap_copy(group).start()

    def attend_finish(at):
        if at == 0:
            for j in range(4):
                swap_copy(j).wait()
                pair = slice(2 * j, 2 * j + 2)
                lanes = slice(features, 3 * features)
                qkv[pair, :, lanes] = qkv[pair, :, lanes] + take[pair]
        wait_out(qkv, rights[at]["qkv"].reshape(*qkv.shape))

    def qkv_chunks(at):
        for j in range(3):
            slot = 1 - j % 2
            tall_load(qkv_block(at, j), slot).wait()
            got = times_turned(
                qkv[:, :, j * features : (j + 1) * features].reshape(tokens, features),
                tall[slot].reshape(features, features),
            )
            if j == 0:
                acc[...] = got
                tall_load(qkv_block(at, 2), slot).start()
            else:
                acc[...] = acc[...] + got

    def last_moves():
        return moves(y_in, moved, last_move_sem, last_stay_sem, me, False)

    def grad_moves():
        return moves(ready, g_out, move_sem, stay_sem, me, False)

    def qkv_finish(at):
        load_in("x", at).wait()
        scaled = 1.0 + mod_ref[at, 1:2]

        def finish(strip):
            grad = acc[strip]
            unit, spread = unit_rows(aux[strip].astype(WIDE))
            sums[at, 0:1] += jnp.sum(grad, axis=0, keepdims=True)
            sums[at, 1:2] += jnp.sum(grad * unit, axis=0, keepdims=True)
            acc[strip] = middle[strip] + into_norm(grad, scaled, unit, spread)

        strips(tokens, finish)
        if at == 0:
            wait_out(acc, input_grad)
        else:
            ready[...] = acc[...].astype(LOW).reshape(ready.shape)
            for copy in grad_moves():
                copy.start()

    def backward_step(t):
        def at_turn(turn):
            return pl.when(t == turn)

        @pl.when(t < steps - 1)
        def _():
            mlp_chunk(1, t + 1)

        @at_turn(4)
        def _():
            mlp_finish(1)
            project(1)

        @pl.when((t >= 5) & (t < 7))
        def _():
            attend_group(1, t - 5)

        @at_turn(6)
        def _():
            attend_finish(1)

        @at_turn(7)
        def _():
            qkv_chunks(1)

        @at_turn(8)
        def _():
            qkv_finish(1)

        @at_turn(10)
        def _():
            for copy in grad_moves():
                copy.wait()
            mlp_begin(0)

        @pl.when((t >= 10) & (t < 10 + steps))
        def _():
            mlp_chunk(0, t - 10)

        @at_turn(15)
        def _():
            mlp_finish(0)
            project(0)

        @pl.when((t >= 16) & (t < 20))
        def _():
            attend_group(0, t - 16)

        @at_turn(19)
        def _():
            attend_finish(0)

        @at_turn(20)
        def _():
            qkv_chunks(0)

        @at_turn(21)
        def _():
            qkv_finish(0)
            mod_low[...] = jnp.zeros_like(mod_low)
            for at in range(2):
                mod_low[8 * at : 8 * at + 8] = sums[at].astype(LOW)
            mod_in[me] = mod_low[...]
            for copy in mod_copies():
                copy.start()

        @at_turn(23)
        def _():
            for copy in mod_copies():
                copy.wait()
            summed = mod_in[0].astype(WIDE)
            for device in range(1, 8):
                summed += mod_in[device].astype(WIDE)
            every_mod[z] = summed.astype(LOW)
            for copy in clip_copies():
                copy.start()

        @at_turn(25)
        def _():
            for copy in last_moves():
                copy.start()

        @at_turn(total + 5)
        def _():
            for copy in clip_copies():
                copy.wait()
            for copy in last_moves():
                copy.wait()

    def mod_copies():
        return [
            pltpu.make_async_remote_copy(
                mod_low, mod_in.at[me], mod_sem.at[0, mask], mod_sem.at[1, mask],
                device_id={"seq": me ^ mask},
            )
            for mask in range(1, 8)
        ]

    def clip_copies():
        return [
            pltpu.make_async_remote_copy(
                every_mod.at[z], every_mod.at[z], mod_sem.at[0, 7 + mask], mod_sem.at[1, 7 + mask],
                device_id={"rep": z ^ mask},
            )
            for mask in range(1, 4)
        ]


    names = ("h", "o", "h2", "z")

    def loads(block, slot):
        for layer, kind, first, count in spans:
            @pl.when((block >= first) & (block < first + count))
            def _():
                source = kept[layer][names[kind]]
                if kind == 3:
                    source = source.at[:, :, block - first]
                pltpu.make_async_copy(source, left.at[slot], load_sem.at[0, slot]).start()
                source = rights[layer][RIGHTS[kind]]
                if kind in (0, 2):
                    column = pl.multiple_of((block - first) * width, width)
                    source = source.at[:, pl.ds(column, width)]
                pltpu.make_async_copy(source, right.at[slot], load_sem.at[1, slot]).start()

    def wait_loads(slot):
        pltpu.make_async_copy(kept[0]["h"], left.at[slot], load_sem.at[0, slot]).wait()
        pltpu.make_async_copy(rights[0]["da"], right.at[slot], load_sem.at[1, slot]).wait()

    def store(block):
        for layer, kind, first, count in spans:
            @pl.when((block >= first) & (block < first + count))
            def _():
                target = grads[layer][kind]
                if kind == 3:
                    row = pl.multiple_of((block - first) * rows, rows)
                    target = target.at[pl.ds(row, rows)]
                elif kind in (0, 2):
                    column = pl.multiple_of((block - first) * width, width)
                    target = target.at[:, pl.ds(column, width)]
                pltpu.make_async_copy(wide, target, store_sem).start()

    def to_seq(source, target, which, slot, mask):
        return pltpu.make_async_remote_copy(
            source, target, link_sem.at[0, which, slot], link_sem.at[1, which, slot],
            device_id={"seq": me ^ mask},
        )

    def pair_copy(t):
        slot = lax.rem(t, 2)
        return pltpu.make_async_remote_copy(
            away, pair_in.at[slot], pair_sem.at[0, slot], pair_sem.at[1, slot],
            device_id={"seq": me ^ 1},
        )

    def first_copies(t):
        slot, block = lax.rem(t, SLOTS), lax.rem(t - 1, SLOTS)
        return (
            to_seq(part.at[block, :, 1 - x, :, pl.ds(0, edge)], first_in_a.at[slot], 0, slot, 2),
            to_seq(
                part.at[block, 1 - y, :, :, pl.ds(edge, width - edge)],
                first_in_b.at[slot], 1, slot, 4,
            ),
        )

    def second_copies(t):
        slot, block = lax.rem(t, SLOTS), lax.rem(t, 2)
        return (
            to_seq(mid_a.at[block, 1 - y], second_in_a.at[slot], 2, slot, 4),
            to_seq(mid_b.at[block, 1 - x], second_in_b.at[slot], 3, slot, 2),
        )

    def rep_copy(t):
        slot = lax.rem(t, SLOTS)
        return pltpu.make_async_remote_copy(
            clip.at[lax.rem(t, 2)], rep_in.at[slot], rep_sem.at[0, 0, slot], rep_sem.at[1, 0, slot],
            device_id={"rep": z ^ 1},
        )

    def inner_copy(t):
        slot = lax.rem(t, SLOTS)
        return pltpu.make_async_remote_copy(
            joined.at[lax.rem(t, 2)], inner_in.at[slot],
            rep_sem.at[0, 1, slot], rep_sem.at[1, 1, slot],
            device_id={"rep": z ^ 3},
        )

    def back_copy(t):
        slot = lax.rem(t, BACK)
        return pltpu.make_async_remote_copy(
            final.at[lax.rem(t, 2)], back_in.at[slot], back_sem.at[0, slot], back_sem.at[1, slot],
            device_id={"rep": z ^ 1},
        )

    def turn(t, carry):
        def stage(back):
            return (t >= back) & (t < total + back)

        now2, was2 = lax.rem(t, 2), lax.rem(t + 1, 2)
        was3 = lax.rem(t + 2, SLOTS)

        @pl.when(t + 1 < total)
        def _():
            loads(t + 1, was2)

        @pl.when(stage(1))
        def _():
            for copy in first_copies(t):
                copy.start()

        @pl.when(stage(2))
        def _():
            block = lax.rem(t + 1, SLOTS)
            for at in range(2):
                mid_a[now2, at] = part[block, at, x, :, :edge] + first_in_a[was3, at]
                mid_b[now2, at] = part[block, y, at, :, edge:] + first_in_b[was3, at]
            for copy in second_copies(t):
                copy.start()

        @pl.when(stage(3))
        def _():
            clip[now2, :, :edge] = mid_a[was2, y] + second_in_a[was3]
            clip[now2, :, edge:] = mid_b[was2, x] + second_in_b[was3]

            @pl.when(outer)
            def _():
                rep_copy(t).start()

        @pl.when(stage(4) & inner)
        def _():
            joined[now2] = clip[was2] + rep_in[was3]
            inner_copy(t).start()

        @pl.when(stage(5) & inner)
        def _():
            final[now2] = joined[was2] + inner_in[was3]
            back_copy(t).start()

        @pl.when(stage(6))
        def _():
            @pl.when(inner)
            def _():
                wide[...] = final[was2].astype(WIDE)

            @pl.when(outer)
            def _():
                wide[...] = back_in[lax.rem(t + 3, BACK)].astype(WIDE)

            store(t - 6)

        @pl.when(t < total)
        def _():
            wait_loads(now2)
            slot3 = lax.rem(t, SLOTS)
            third = width // 3

            def product(which, j):
                at = pl.ds(pl.multiple_of(j * third, third), third)
                block = left[now2, :, which]
                four, _, depth = block.shape
                got = times(block.reshape(four * rows, depth), right[now2, :, at]).astype(LOW)
                return at, got.reshape(four, rows, third)

            def away_columns(j, carry):
                at, got = product(1 - core, j)
                away[:, :, at] = got
                return carry

            lax.fori_loop(0, 3, away_columns, 0)
            pair_copy(t).start()

            def kept_columns(j, carry):
                at, got = product(core, j)
                part[slot3, 0, :, :, at] = got[:2]
                part[slot3, 1, :, :, at] = got[2:]
                return carry

            lax.fori_loop(0, 3, kept_columns, 0)
            pair_copy(t).wait()

            def add(j, carry):
                part[slot3, j // 2, j % 2] = part[slot3, j // 2, j % 2] + pair_in[now2, j]
                return carry

            lax.fori_loop(0, 4, add, 0)

        backward_step(t)

        @pl.when(stage(1))
        def _():
            for copy in first_copies(t):
                copy.wait()

        @pl.when(stage(2))
        def _():
            for copy in second_copies(t):
                copy.wait()

        @pl.when(stage(3))
        def _():
            @pl.when(outer)
            def _():
                rep_copy(t).wait_send()

            @pl.when(inner)
            def _():
                rep_copy(t).wait_recv()

        @pl.when(stage(4) & inner)
        def _():
            inner_copy(t).wait()

        @pl.when(stage(5))
        def _():
            @pl.when(inner)
            def _():
                back_copy(t).wait_send()

            @pl.when(outer)
            def _():
                back_copy(t).wait_recv()

        @pl.when(stage(6))
        def _():
            pltpu.make_async_copy(wide, grads[0][1], store_sem).wait()

        return carry

    enter(range(1, 8), range(1, 4))
    mlp_begin(1)
    mlp_chunk(1, jnp.int32(0))
    loads(0, 0)
    lax.fori_loop(0, total + 6, turn, 0)


def backward(weights, kept, g, other, y, xs, mods, cid):
    struct = jax.ShapeDtypeStruct
    tokens, features = xs[0].shape
    rows = features // 8
    wide = weights[0][2].shape[2]
    edge = features * 5 // 9 // 128 * 128
    frames, places = g.shape[1], 8 * g.shape[2]
    out_shapes = [(rows, 3 * features), (rows, features), (rows, wide), (wide // 8, features)]
    spans, total = [], 0
    for layer in (1, 0):
        for kind in ORDER:
            count = out_shapes[kind][0] * out_shapes[kind][1] // (rows * features)
            spans.append((layer, kind, total, count))
            total += count
    dims = (rows, features, edge, tokens, total, spans)
    any_ = pl.BlockSpec(memory_space=pl.ANY)
    outs = [struct(shape, WIDE) for shape in out_shapes] * 2
    outs += [
        struct((tokens, 3 * features), LOW), struct((tokens, features), LOW),
        struct((tokens, wide), LOW), struct((tokens, features), LOW),
    ] * 2
    outs += [
        struct((4, 16, features), LOW),
        struct((frames, places, features), LOW),
        struct((tokens, features), WIDE),
        struct((frames, places, features), LOW),
    ]
    vm, dma = pltpu.VMEM, pltpu.SemaphoreType.DMA
    rest = features - edge
    scratch = [
        vm((2, 4, 2, rows, tokens), LOW),
        vm((2, tokens, features), LOW),
        vm((4, rows, features), LOW),
        vm((2, 4, rows, features), LOW),
        vm((SLOTS, 2, 2, rows, features), LOW),
        vm((SLOTS, 2, rows, edge), LOW),
        vm((SLOTS, 2, rows, rest), LOW),
        vm((2, 2, rows, edge), LOW),
        vm((2, 2, rows, rest), LOW),
        vm((SLOTS, rows, edge), LOW),
        vm((SLOTS, rows, rest), LOW),
        vm((2, rows, features), LOW),
        vm((SLOTS, rows, features), LOW),
        vm((2, rows, features), LOW),
        vm((SLOTS, rows, features), LOW),
        vm((2, rows, features), LOW),
        vm((BACK, rows, features), LOW),
        vm((rows, features), WIDE),
        vm((2, 8, rows, features), LOW),
        vm((2, 4, CHUNK // 4, features), LOW),
        vm((tokens, features), WIDE),
        vm((tokens, features), WIDE),
        vm((tokens, features), LOW),
        vm((tokens, features), LOW),
        vm((tokens, features), LOW),
        vm((2, tokens, CHUNK), LOW),
        vm((tokens, CHUNK), LOW),
        vm((8, tokens // 8, 3 * features), LOW),
        vm((8, tokens // 8, 2 * features), LOW),
        vm((8, tokens // 8, 2 * features), LOW),
        vm((HEADS, KEYS, KEYS), LOW),
        vm((8, tokens // 8, features), LOW),
        vm((KEYS, features), WIDE),
        vm((KEYS, features), WIDE),
        vm((KEYS, features), WIDE),
        vm((8, frames, places // 8, features), LOW),
        vm((2, 8, features), WIDE),
        vm((16, features), LOW),
        vm((8, 16, features), LOW),
        dma((2, 2)),
        dma((2, 2)),
        dma((2, 4, SLOTS)),
        dma((2, 2, SLOTS)),
        dma((2, BACK)),
        dma(()),
        dma((2, 11)),
        dma((2,)),
        dma((2,)),
        dma((2,)),
        dma((7,)),
        dma(()),
        dma(()),
        dma((2, 4)),
        *move_scratch(),
        *move_scratch(),
    ]
    flops = 4 * tokens * 8 * sum(a * b for a, b in out_shapes) * 2
    got = pl.pallas_call(
        functools.partial(backward_kernel, dims),
        out_shape=outs,
        in_specs=[any_] * (8 + 20 + 5) + [pl.BlockSpec(memory_space=vm)],
        out_specs=[any_] * 16 + [pl.BlockSpec(memory_space=vm)] + [any_] * 3,
        scratch_shapes=scratch,
        compiler_params=params(63, cid),
        cost_estimate=cost(flops, flops // tokens),
        name="backward",
    )(
        *weights[0], *weights[1], *[each[name] for each in kept for name in KEPT],
        g, other, y, *xs, mods,
    )
    return got[:4], got[4:8], got[16], got[17], got[18]


def by_device(left, features):
    tall, tokens = left.shape[0] // features, left.shape[1]
    rows = features // 8
    return left.reshape((4, 2, rows, tokens) if tall == 1 else (4, 2, tall, rows, tokens))


def fused_device(frames_in, conditioning, shards, partial_mod, cotangent):
    _, _, frames, places, features = frames_in.shape
    tokens = frames * places
    low_cotangent = cotangent.reshape(frames, places, features).astype(LOW)
    x_one = frames_in.reshape(tokens, features)
    weights, (mods, conditions, g_two, other, x_two, y_two), kept = forward(
        shards, partial_mod.reshape(-1, LANES), conditioning.reshape(-1, LANES), low_cotangent,
        x_one, 0,
    )
    for each in kept:
        for name in ("h", "o", "h2", "z"):
            each[name] = by_device(each[name], features)
    grads_one, grads_two, every_mod, block_out, input_grad = backward(
        (weights[:4], weights[4:]), kept, g_two, other, y_two.reshape(g_two.shape),
        (x_one, x_two.reshape(tokens, features)), mods, 1,
    )
    every_mod = every_mod.reshape(-1, 2, 8, features)[:, :, :6].reshape(-1, 12 * features)
    return (
        block_out.astype(WIDE), input_grad, grads_one, grads_two, every_mod,
        conditions.reshape(-1, features),
    )


def per_device(
    frames_in,
    conditioning,
    mod_first,
    qkv_first,
    out_first,
    up_first,
    down_first,
    mod_second,
    qkv_second,
    out_second,
    up_second,
    down_second,
    cotangent,
):
    clip_count, _, frame_dev, half_places, features = frames_in.shape
    fused = lax.axis_size("seq") == 8 and lax.axis_size("rep") == 4 and clip_count == 1
    row_count = mod_first.shape[0]
    row_start = lax.axis_index("seq") * row_count
    mod_width = mod_first.shape[1]
    rows_of = lambda whole: lax.dynamic_slice_in_dim(whole, row_start, row_count, 1)
    silu_local = rows_of(jax.nn.silu(conditioning)).astype(jnp.bfloat16)
    partial_mod = jnp.concatenate(
        [
            jnp.dot(silu_local, mod_first, preferred_element_type=jnp.float32),
            jnp.dot(silu_local, mod_second, preferred_element_type=jnp.float32),
        ],
        1,
    )
    shards = (
        qkv_first, out_first, up_first, down_first,
        qkv_second, out_second, up_second, down_second,
    )
    if fused:
        block_out, stream_grad, grads_one, grads_two, every_mod, conditions = fused_device(
            frames_in, conditioning, shards, partial_mod, cotangent
        )
        every_silu = rows_of(jax.nn.silu(conditions)).astype(jnp.bfloat16)
        mod_total = lax.dynamic_slice_in_dim(every_mod, lax.axis_index("rep"), 1, 0)
    else:
        weights = [lax.all_gather(shard, "seq", axis=0, tiled=True) for shard in shards]
        modulation = lax.psum(partial_mod, "seq")
        every_silu = lax.all_gather(silu_local, "rep", axis=0, tiled=True)
        mod_one, mod_two = modulation[:, :mod_width], modulation[:, mod_width:]
        weights_one, weights_two = weights[:4], weights[4:]
        start_stream = frames_in.reshape(clip_count, frame_dev, half_places, features).astype(
            jnp.float32
        )
        spatial_out, state_one = forward_layer(start_stream, mod_one, weights_one, True)
        placed = to_places(spatial_out)
        temporal_out, state_two = forward_layer(placed, mod_two, weights_two, False)
        block_out = to_frames(temporal_out, frame_dev)
        cotangent_sites = to_places(
            cotangent.reshape(clip_count, frame_dev, half_places, features)
        )
        placed_grad, mod_grad_two, pairs_two = backward_layer(
            cotangent_sites, placed, mod_two, weights_two, state_two, False
        )
        spatial_grad = to_frames(placed_grad, frame_dev)
        stream_grad, mod_grad_one, pairs_one = backward_layer(
            spatial_grad, start_stream, mod_one, weights_one, state_one, True
        )
        mod_grads = jnp.concatenate([mod_grad_one, mod_grad_two], 1).astype(jnp.bfloat16)
        grads_two, grads_one = layer_grads(pairs_two), layer_grads(pairs_one)
        mod_total = lax.psum(mod_grads, "seq").astype(jnp.bfloat16)
        every_mod = lax.all_gather(mod_total, "rep", axis=0, tiled=True)
    low_one, low_two = mod_total[:, :mod_width], mod_total[:, mod_width:]
    mod_weight_one = jnp.einsum(
        "cd,ce->de", every_silu, every_mod[:, :mod_width], preferred_element_type=jnp.float32
    )
    mod_weight_two = jnp.einsum(
        "cd,ce->de", every_silu, every_mod[:, mod_width:], preferred_element_type=jnp.float32
    )
    silu_grad = jnp.einsum("ce,de->cd", low_one, mod_first, preferred_element_type=jnp.float32)
    silu_grad = silu_grad + jnp.einsum(
        "ce,de->cd", low_two, mod_second, preferred_element_type=jnp.float32
    )
    condition_grad = jax.vjp(jax.nn.silu, rows_of(conditioning))[1](silu_grad)[0]
    out_shape = (clip_count, 1, frame_dev, half_places, features)
    return (
        block_out.reshape(out_shape),
        stream_grad.reshape(out_shape),
        condition_grad,
        mod_weight_one,
        *grads_one,
        mod_weight_two,
        *grads_two,
    )


def solution(mesh):
    return jax.shard_map(
        per_device,
        mesh=mesh,
        in_specs=(
            P("rep", "seq", None, None, None),
            P("rep", None),
            P("seq", None),
            P("seq", None),
            P("seq", None),
            P("seq", None),
            P("seq", None),
            P("seq", None),
            P("seq", None),
            P("seq", None),
            P("seq", None),
            P("seq", None),
            P("rep", "seq", None, None, None),
        ),
        out_specs=(
            P("rep", "seq", None, None, None),
            P("rep", "seq", None, None, None),
            P("rep", "seq"),
            P("seq", None),
            P("seq", None),
            P("seq", None),
            P("seq", None),
            P("seq", None),
            P("seq", None),
            P("seq", None),
            P("seq", None),
            P("seq", None),
            P("seq", None),
        ),
        check_vma=False,
    )
```

```python
import functools
import math

import jax
import jax.numpy as jnp
from jax import lax
from jax.experimental import pallas as pl
from jax.experimental.pallas import tpu as pltpu
from jax.sharding import PartitionSpec as P

HEADS = 16
HEAD_WIDTH = 72


norm_epsilon = 1e-06


def from_partner(block, axis, apart):
    count = lax.axis_size(axis)
    route = []
    for low in range(count):
        high = low | 1 << apart
        if high != low and high < count:
            route += [(low, high), (high, low)]
    return lax.ppermute(block, axis, route)


def shortened(x):
    return jax.tree.map(lambda a: a.astype(jnp.bfloat16) if a.dtype == jnp.float32 else a, x)


def layer_mod(stream, shift_part, scale_part):
    row_mean = jnp.mean(stream, axis=-1, keepdims=True)
    centred = stream - row_mean
    row_var = jnp.mean(centred * centred, axis=-1, keepdims=True)
    return centred * lax.rsqrt(row_var + norm_epsilon) * (1.0 + scale_part) + shift_part


def gelu_tanh(pre_value):
    return jax.nn.gelu(pre_value, approximate=True)


def project(left_operand, right_operand):
    return jnp.einsum(
        "csld,de->csle", left_operand, right_operand, preferred_element_type=jnp.float32
    )


def project_back(incoming, right_operand):
    return jnp.einsum("csle,de->csld", incoming, right_operand, preferred_element_type=jnp.float32)


def mod_parts(modulation):
    return [segment[:, None, None, :] for segment in jnp.split(modulation, 6, axis=-1)]


def partner_values(stacked):
    return from_partner(stacked, "seq", 0)


def partner_grads(stacked):
    return from_partner(stacked.astype(jnp.bfloat16), "seq", 0).astype(stacked.dtype)


def to_places(stream):
    clip_count, frame_dev, half_places, features = stream.shape
    devices = lax.axis_size("seq")
    place_part = half_places // devices
    exchanged = lax.all_to_all(
        stream.reshape(1, clip_count, frame_dev, devices, place_part, features).astype(
            jnp.bfloat16
        ),
        "seq",
        split_axis=3,
        concat_axis=0,
        tiled=True,
    ).astype(jnp.float32)
    exchanged = exchanged.reshape(devices // 2, 2, clip_count, frame_dev, place_part, features)
    exchanged = jnp.transpose(exchanged, (2, 1, 4, 0, 3, 5))
    return exchanged.reshape(clip_count, 2 * place_part, devices // 2 * frame_dev, features)


def to_frames(stream, frame_dev):
    clip_count, place_count, frame_total, features = stream.shape
    devices = lax.axis_size("seq")
    place_part = place_count // 2
    arranged = stream.reshape(clip_count, 2, place_part, devices // 2, frame_dev, features)
    arranged = jnp.transpose(arranged, (3, 1, 0, 4, 2, 5)).reshape(
        devices, clip_count, frame_dev, 1, place_part, features
    )
    exchanged = lax.all_to_all(
        shortened(arranged), "seq", split_axis=0, concat_axis=3, tiled=True
    ).astype(arranged.dtype)
    return exchanged.reshape(clip_count, frame_dev, devices * place_part, features)


def forward_layer(stream, modulation, weights, spatial):
    qkv_w, out_w, up_w, down_w = weights
    shift_attn, scale_attn, gate_attn, shift_mlp, scale_mlp, gate_mlp = mod_parts(modulation)
    clip_count, seq_count, seq_len, features = stream.shape
    normed = layer_mod(stream, shift_attn, scale_attn).astype(jnp.bfloat16)
    projected = project(normed, qkv_w).astype(jnp.bfloat16)
    queries, keys_all, values_all = jnp.split(projected, 3, axis=-1)
    if spatial:
        remote = partner_values(jnp.stack([keys_all, values_all]))
        keys_all = jnp.concatenate([keys_all, remote[0]], axis=2)
        values_all = jnp.concatenate([values_all, remote[1]], axis=2)
    key_len = keys_all.shape[2]
    queries = queries.reshape(clip_count, seq_count, seq_len, HEADS, HEAD_WIDTH)
    keys_all = keys_all.reshape(clip_count, seq_count, key_len, HEADS, HEAD_WIDTH)
    values_all = values_all.reshape(clip_count, seq_count, key_len, HEADS, HEAD_WIDTH)
    scores = jnp.einsum(
        "cslhe,csmhe->cshlm", queries, keys_all, preferred_element_type=jnp.float32
    ) * HEAD_WIDTH ** (-0.5)
    peak_score = jnp.max(scores, axis=-1, keepdims=True)
    scaled_exp = jnp.exp(scores - peak_score)
    attention = scaled_exp / jnp.sum(scaled_exp, axis=-1, keepdims=True)
    attention_low = attention.astype(jnp.bfloat16)
    attended = jnp.einsum(
        "cshlm,csmhe->cslhe", attention_low, values_all, preferred_element_type=jnp.float32
    )
    attended = attended.astype(jnp.bfloat16).reshape(clip_count, seq_count, seq_len, features)
    branch = project(attended, out_w)
    middle = stream + gate_attn * branch
    normed_mid = layer_mod(middle, shift_mlp, scale_mlp).astype(jnp.bfloat16)
    hidden_pre = project(normed_mid, up_w)
    hidden = gelu_tanh(hidden_pre).astype(jnp.bfloat16)
    mlp_out = project(hidden, down_w)
    result = middle + gate_mlp * mlp_out
    kept_state = (
        normed,
        queries,
        keys_all,
        values_all,
        attention,
        attention_low,
        attended,
        branch,
        middle,
        normed_mid,
        hidden_pre,
        hidden,
        mlp_out,
    )
    return (result, kept_state)


def backward_layer(result_grad, stream, modulation, weights, kept_state, spatial):
    qkv_w, out_w, up_w, down_w = weights
    (
        normed,
        queries,
        keys_all,
        values_all,
        attention,
        attention_low,
        attended,
        branch,
        middle,
        normed_mid,
        hidden_pre,
        hidden,
        mlp_out,
    ) = kept_state
    shift_attn, scale_attn, gate_attn, shift_mlp, scale_mlp, gate_mlp = mod_parts(modulation)
    clip_count, seq_count, seq_len, features = stream.shape
    gate_mlp_grad = jnp.sum(result_grad * mlp_out, axis=(1, 2))
    mlp_grad = (gate_mlp * result_grad).astype(jnp.bfloat16)
    hidden_grad = project_back(mlp_grad, down_w)
    pre_grad = jax.vjp(gelu_tanh, hidden_pre)[1](hidden_grad)[0].astype(jnp.bfloat16)
    normed_mid_grad = project_back(pre_grad, up_w)
    middle_ln_grad, shift_mlp_grad, scale_mlp_grad = jax.vjp(
        layer_mod, middle, shift_mlp, scale_mlp
    )[1](normed_mid_grad)
    middle_grad = result_grad + middle_ln_grad
    gate_attn_grad = jnp.sum(middle_grad * branch, axis=(1, 2))
    branch_grad = (gate_attn * middle_grad).astype(jnp.bfloat16)
    attended_grad = project_back(branch_grad, out_w).astype(jnp.bfloat16)
    attended_grad = attended_grad.reshape(clip_count, seq_count, seq_len, HEADS, HEAD_WIDTH)
    attention_grad = jnp.einsum(
        "cslhe,csmhe->cshlm", attended_grad, values_all, preferred_element_type=jnp.float32
    )
    scores_grad = attention * (
        attention_grad - jnp.sum(attention_grad * attention, axis=-1, keepdims=True)
    )
    scores_grad = scores_grad.astype(jnp.bfloat16)
    inv_root = HEAD_WIDTH ** (-0.5)
    queries_grad = (
        jnp.einsum("cshlm,csmhe->cslhe", scores_grad, keys_all, preferred_element_type=jnp.float32)
        * inv_root
    )
    keys_grad = (
        jnp.einsum("cshlm,cslhe->csmhe", scores_grad, queries, preferred_element_type=jnp.float32)
        * inv_root
    )
    values_grad = jnp.einsum(
        "cshlm,cslhe->csmhe", attention_low, attended_grad, preferred_element_type=jnp.float32
    )
    if spatial:
        returned = partner_grads(
            jnp.stack([keys_grad[:, :, seq_len:], values_grad[:, :, seq_len:]])
        )
        keys_grad = keys_grad[:, :, :seq_len] + returned[0]
        values_grad = values_grad[:, :, :seq_len] + returned[1]
    qkv_grad = jnp.concatenate(
        [
            component.reshape(clip_count, seq_count, seq_len, features)
            for component in (queries_grad, keys_grad, values_grad)
        ],
        axis=-1,
    )
    qkv_grad = qkv_grad.astype(jnp.bfloat16)
    normed_grad = project_back(qkv_grad, qkv_w)
    stream_ln_grad, attention_shift_gradient, scale_attn_grad = jax.vjp(
        layer_mod, stream, shift_attn, scale_attn
    )[1](normed_grad)
    stream_grad = middle_grad + stream_ln_grad
    mod_grad = jnp.concatenate(
        [
            attention_shift_gradient.reshape(clip_count, features),
            scale_attn_grad.reshape(clip_count, features),
            gate_attn_grad,
            shift_mlp_grad.reshape(clip_count, features),
            scale_mlp_grad.reshape(clip_count, features),
            gate_mlp_grad,
        ],
        axis=-1,
    )
    grad_pairs = (
        (normed, qkv_grad),
        (attended, branch_grad),
        (normed_mid, pre_grad),
        (hidden, mlp_grad),
    )
    return (stream_grad, mod_grad, grad_pairs)


def bit_count(axis):
    return lax.axis_size(axis).bit_length() - 1


def swap(block, axis, bit):
    count = lax.axis_size(axis)
    return lax.ppermute(block, axis, [(at, at ^ (1 << bit)) for at in range(count)])


def bit_of(axis, bit):
    return (lax.axis_index(axis) >> bit) & 1


def pick(block, which, axis):
    return lax.dynamic_index_in_dim(block, which, axis, keepdims=False)


def spread_rows_out(left_turned, right_operand, flipped):
    bits = bit_count("seq")
    total_rows, tokens = left_turned.shape
    rows = total_rows >> bits
    halves = left_turned.reshape(1 << (bits - 1), 2, rows, tokens)
    core = bit_of("seq", 0)

    def product(which):
        left = pick(halves, which, 1).reshape(-1, tokens)
        return jnp.dot(left, right_operand, preferred_element_type=jnp.float32).astype(
            jnp.bfloat16
        )

    arrived = swap(product(1 - core), "seq", 0)
    held = product(core)
    left_bits = list(range(bits - 1, 0, -1))
    shape = [2] * (bits - 1) + [rows, right_operand.shape[1]]
    held = held.reshape(shape)
    arrived = arrived.reshape(shape)
    order = list(left_bits) if flipped else left_bits[::-1]
    for bit in order:
        at = left_bits.index(bit)
        mine = bit_of("seq", bit)
        away = pick(held, 1 - mine, at).astype(jnp.float32) + pick(arrived, 1 - mine, at)
        kept = pick(held, mine, at).astype(jnp.float32) + pick(arrived, mine, at)
        arrived = swap(away.astype(jnp.bfloat16), "seq", bit)
        held = kept.astype(jnp.bfloat16)
        left_bits.remove(bit)
    return held.astype(jnp.float32) + arrived


def rep_sum(block, axis):
    bits = bit_count("rep")
    held = block.astype(jnp.bfloat16)
    for bit in range(bits):
        mine = bit_of("rep", bit)
        low, high = jnp.split(held, 2, axis)
        away = jnp.where(mine == 0, high, low)
        kept = jnp.where(mine == 0, low, high)
        held = (kept.astype(jnp.float32) + swap(away, "rep", bit)).astype(jnp.bfloat16)
    for bit in reversed(range(bits)):
        mine = bit_of("rep", bit)
        other = swap(held, "rep", bit)
        low = jnp.where(mine == 0, held, other)
        high = jnp.where(mine == 0, other, held)
        held = jnp.concatenate([low, high], axis)
    return held.astype(jnp.float32)


def turned(operand):
    return operand.reshape(-1, operand.shape[-1]).T


def flat(operand):
    return operand.reshape(-1, operand.shape[-1])


def cut(width, parts, of):
    return width * parts // of // 128 * 128


def down_grad(pair):
    left, right = turned(pair[0]), flat(pair[1])
    edge = cut(right.shape[1], 5, 9)
    return jnp.concatenate(
        [
            rep_sum(spread_rows_out(left, right[:, :edge], False), 0),
            rep_sum(spread_rows_out(left, right[:, edge:], True), 0),
        ],
        1,
    )


def up_grad(pair):
    left, right = turned(pair[0]), flat(pair[1])
    edge = cut(right.shape[1], 4, 9)
    return jnp.concatenate(
        [
            rep_sum(spread_rows_out(left, right[:, :edge], False), 1),
            rep_sum(spread_rows_out(left, right[:, edge:], True), 1),
        ],
        1,
    )


def attention_grads(qkv_pair, out_pair):
    left, right = turned(qkv_pair[0]), flat(qkv_pair[1])
    width = right.shape[1]
    edge = cut(width, 16, 27)
    first = rep_sum(spread_rows_out(left, right[:, :edge], False), 1)
    second = spread_rows_out(left, right[:, edge:], True)
    third = spread_rows_out(turned(out_pair[0]), flat(out_pair[1]), True)
    joined = rep_sum(jnp.concatenate([second, third], 1), 1)
    return (
        jnp.concatenate([first, joined[:, : width - edge]], 1),
        joined[:, width - edge :],
    )


def layer_grads(grad_pairs):
    qkv_pair, out_pair, up_pair, down_pair = grad_pairs
    down = down_grad(down_pair)
    up = up_grad(up_pair)
    qkv, out = attention_grads(qkv_pair, out_pair)
    return (qkv, out, up, down)


AHEAD = 2


def gather_pieces(shapes):
    features = math.gcd(*(columns for _, columns in shapes), 8 * shapes[0][0])
    rows_of = features // 8
    return rows_of, features, [
        (at, row, column)
        for at, (rows, columns) in enumerate(shapes)
        for row in range(0, rows, rows_of)
        for column in range(0, columns, features)
    ]


class Gather:
    def __init__(self, shapes, refs):
        count = len(shapes)
        self.count = count
        self.least, self.wide, self.pieces = gather_pieces(shapes)
        self.shards, self.fulls = refs[0], refs[1]
        self.held = refs[2][: count // 2]
        self.first_sem, self.second_sem, self.rep_sem, self.pair_sem, self.local_sem = refs[2][
            count // 2 :
        ]
        self.me, self.z = lax.axis_index("seq"), lax.axis_index("rep")
        odd = self.z & 1
        self.first, self.second = 2 + 2 * odd, 4 - 2 * odd

    @staticmethod
    def scratch(shapes):
        size = len(gather_pieces(shapes)[2])
        dma = pltpu.SemaphoreType.DMA
        half = shapes[: len(shapes) // 2]
        return [pltpu.VMEM(shape, jnp.bfloat16) for shape in half] + [
            dma((2, size)), dma((2, size)), dma((2, size)), dma((4, 2, size)), dma((2, len(shapes))),
        ]

    @staticmethod
    def outs(shapes):
        return [jax.ShapeDtypeStruct((8,) + shape, jnp.bfloat16) for shape in shapes]

    def place(self, owner, at):
        weight, row, column = self.pieces[at]
        return self.fulls[weight].at[owner, pl.ds(row, self.least), pl.ds(column, self.wide)]

    def own(self, at):
        weight, row, column = self.pieces[at]
        return self.shards[weight].at[pl.ds(row, self.least), pl.ds(column, self.wide)]

    def to_seq(self, source, owner, at, sems, mask):
        return pltpu.make_async_remote_copy(
            source, self.place(owner, at), sems.at[0, at], sems.at[1, at],
            device_id={"seq": self.me ^ mask},
        )

    def first_copy(self, at):
        return self.to_seq(self.own(at), self.me, at, self.first_sem, self.first)

    def second_copy(self, at):
        owner = self.me ^ self.first
        return self.to_seq(self.place(owner, at), owner, at, self.second_sem, self.second)

    def rep_copy(self, at):
        owner = self.me ^ self.first
        return pltpu.make_async_remote_copy(
            self.place(owner, at), self.place(owner, at), self.rep_sem.at[0, at], self.rep_sem.at[1, at],
            device_id={"rep": self.z ^ 1},
        )

    def pair_copy(self, which, at):
        if which == 0:
            return self.to_seq(self.own(at), self.me, at, self.pair_sem.at[0], 1)
        owner = self.me ^ (self.first, self.first ^ self.second, self.second)[which - 1]
        return self.to_seq(self.place(owner, at), owner, at, self.pair_sem.at[which], 1)

    def begin(self, at):
        self.first_copy(at).start()
        self.pair_copy(0, at).start()

    def fetch(self, weight):
        return pltpu.make_async_copy(
            self.shards[weight], self.held[weight % len(self.held)], self.local_sem.at[0, weight]
        )

    def keep(self, weight):
        return pltpu.make_async_copy(
            self.held[weight % len(self.held)], self.fulls[weight].at[self.me], self.local_sem.at[1, weight]
        )

    def start(self):
        for at in range(AHEAD):
            self.begin(at)
        self.local(0)

    def local(self, first):
        for weight in range(first, first + len(self.held)):
            self.fetch(weight).start()
        for weight in range(first, first + len(self.held)):
            self.fetch(weight).wait()
            self.keep(weight).start()

    def ready(self, weight):
        for at, piece in enumerate(self.pieces):
            if piece[0] == weight:
                for which in range(4):
                    self.pair_copy(which, at).wait_recv()
        self.keep(weight).wait()

    def advance(self, at):
        self.first_copy(at).wait_recv()
        if at + AHEAD < len(self.pieces):
            self.begin(at + AHEAD)
        self.second_copy(at).start()
        self.rep_copy(at).start()
        self.pair_copy(1, at).start()
        if at:
            self.share(at - 1)

    def share(self, at):
        self.second_copy(at).wait_recv()
        self.rep_copy(at).wait_recv()
        self.pair_copy(2, at).start()
        self.pair_copy(3, at).start()

    def finish(self):
        for at in range(len(self.pieces)):
            for copy in (self.first_copy(at), self.second_copy(at), self.rep_copy(at)):
                copy.wait_send()
            for which in range(4):
                self.pair_copy(which, at).wait_send()


def enter(seq_masks, rep_masks):
    me, z = lax.axis_index("seq"), lax.axis_index("rep")
    barrier = pltpu.get_barrier_semaphore()
    for mask in seq_masks:
        pl.semaphore_signal(barrier, inc=1, device_id={"seq": me ^ mask})
    for mask in rep_masks:
        pl.semaphore_signal(barrier, inc=1, device_id={"rep": z ^ mask})
    pl.semaphore_wait(barrier, len(seq_masks) + len(rep_masks))


LOW = jnp.bfloat16
WIDE = jnp.float32
LANES = 128
STRIP = 64
KEYS = 256


def whole_block(shape):
    return pl.BlockSpec(shape, lambda *at: (0,) * len(shape))


def strips(total, body):
    def step(j, carry):
        body(pl.ds(pl.multiple_of(j * STRIP, STRIP), STRIP))
        return carry

    lax.fori_loop(0, total // STRIP, step, 0)


def clear(ref, at):
    ref[at] = jnp.zeros_like(ref[at])


def turn_into(target, source):
    for j in range(source.shape[1] // LANES):
        target[j * LANES : (j + 1) * LANES, :] = source[:, j * LANES : (j + 1) * LANES].T


def unit_rows(block):
    centred = block - jnp.mean(block, axis=-1, keepdims=True)
    spread = lax.rsqrt(jnp.mean(centred * centred, axis=-1, keepdims=True) + norm_epsilon)
    return centred * spread, spread


def into_norm(grad, scaled, unit, spread):
    inner = grad * scaled
    level = jnp.mean(inner, axis=-1, keepdims=True)
    slope = jnp.mean(inner * unit, axis=-1, keepdims=True)
    return spread * (inner - level - unit * slope)


def times(left, right):
    return jnp.dot(left, right, preferred_element_type=WIDE)


def times_turned(left, right):
    return lax.dot_general(left, right, (((1,), (1,)), ((), ())), preferred_element_type=WIDE)


def turned_times(left, right):
    return lax.dot_general(left, right, (((0,), (0,)), ((), ())), preferred_element_type=WIDE)


def params(size, cid=None):
    if cid is None:
        return pltpu.CompilerParams(vmem_limit_bytes=size << 20)
    return pltpu.CompilerParams(
        vmem_limit_bytes=size << 20, collective_id=cid, has_side_effects=True
    )


def cost(flops, size):
    return pl.CostEstimate(flops=flops, bytes_accessed=size, transcendentals=0)


def window(head):
    low, high = head * HEAD_WIDTH, (head + 1) * HEAD_WIDTH
    start = low // LANES * LANES
    stop = -(-high // LANES) * LANES
    return start, stop - start, low - start


def head_mask(head):
    start, wide, offset = window(head)
    lane = lax.broadcasted_iota(jnp.int32, (1, wide), 1)
    return ((lane >= offset) & (lane < offset + HEAD_WIDTH)).astype(WIDE).astype(LOW)


def add_window(total, head, block):
    start, wide, _ = window(head)
    for j in range(wide // LANES):
        tile = start // LANES + j
        lanes = slice(tile * LANES, (tile + 1) * LANES)
        piece = block[:, j * LANES : (j + 1) * LANES]
        if head == tile * LANES // HEAD_WIDTH:
            total[:, lanes] = piece
        else:
            total[:, lanes] = total[:, lanes] + piece


def same_place():
    row = lax.broadcasted_iota(jnp.int32, (KEYS, KEYS), 0)
    column = lax.broadcasted_iota(jnp.int32, (KEYS, KEYS), 1)
    return (row & 15) == (column & 15)


def moves(source, target, sems, local_sem, me, to_places):
    part = source.shape[-2] // 8 if to_places else source.shape[-2]

    def ends(device):
        if to_places:
            return source.at[:, pl.ds(pl.multiple_of(device * part, part), part)], target.at[me]
        return source.at[device], target.at[:, pl.ds(pl.multiple_of(me * part, part), part)]

    copies = [pltpu.make_async_copy(*ends(me), local_sem)]
    for mask in (6, 7, 2, 3, 4, 5, 1):
        copies.append(
            pltpu.make_async_remote_copy(
                *ends(me ^ mask), sems.at[0, mask], sems.at[1, mask], device_id={"seq": me ^ mask}
            )
        )
    return copies


def move_scratch():
    return [pltpu.SemaphoreType.DMA((2, 8)), pltpu.SemaphoreType.DMA(())]


def gelu_and_slope(value):
    inner = 0.7978845608028654 * (value + 0.044715 * value * value * value)
    bent = jnp.tanh(inner)
    half = 0.5 * (1.0 + bent)
    slope = half + 0.5 * value * (1.0 - bent * bent) * (
        0.7978845608028654 * (1.0 + 3 * 0.044715 * value * value)
    )
    return value * half, slope


OUTS = ("qkv", "prob", "h", "o", "h2", "z", "slope", "x1", "branch", "mlp")
CHUNK = 768


def forward_kernel(shapes, *refs):
    count = len(shapes)
    shards, refs = refs[:count], refs[count:]
    partial, condition, tokens, x_ref = refs[:4]
    fulls, refs = refs[4 : 4 + count], refs[4 + count :]
    mod_ref, conditions, moved, other_ref, x2_ref, y_ref = refs[:6]
    outs = [dict(zip(OUTS, refs[6:16])), dict(zip(OUTS, refs[16:26]))]
    refs = refs[26:]
    (
        partials, x2, qkv, other, held, normed, total, middle, part, prob, turned, low, ready,
        tall, short, hidden, slope, small_sem, move_sem, stay_sem, next_move_sem, next_stay_sem, next_sem,
        pair_sem, weight_sem, out_sem, prob_sem, chunk_sem,
    ) = refs[:28]
    gather = Gather(shapes, (shards, fulls, refs[28:]))
    me, z = gather.me, gather.z
    features = x_ref.shape[1]
    steps = shapes[2][1] // CHUNK
    enter(range(1, 8), range(1, 4))

    small = []
    for mask in range(1, 8):
        small.append(pltpu.make_async_remote_copy(
            partial, partials.at[me], small_sem.at[0, mask], small_sem.at[1, mask],
            device_id={"seq": me ^ mask}))
    for mask in range(1, 4):
        small.append(pltpu.make_async_remote_copy(
            condition, conditions.at[z], small_sem.at[0, 7 + mask], small_sem.at[1, 7 + mask],
            device_id={"rep": z ^ mask}))
    small.append(pltpu.make_async_copy(partial, partials.at[me], small_sem.at[0, 0]))
    small.append(pltpu.make_async_copy(condition, conditions.at[z], small_sem.at[1, 0]))
    for copy in small:
        copy.start()
    gather.start()
    for copy in small:
        copy.wait()
    modulation = partials[0]
    for device in range(1, 8):
        modulation = modulation + partials[device]
    width = features // LANES
    for row in range(12):
        for j in range(width):
            at = row * width + j
            mod_ref[row // 6, row % 6 : row % 6 + 1, j * LANES : (j + 1) * LANES] = modulation[
                at : at + 1
            ]

    pending = {}
    names = ("turned", "qkv", "other", "low", "middle", "ready")

    def begin(name, source, target):
        settle(name)
        pending[name] = pltpu.make_async_copy(source, target, out_sem.at[names.index(name)])
        pending[name].start()

    def settle(name):
        copy = pending.pop(name, None)
        if copy is not None:
            copy.wait()

    def full(weight):
        return fulls[weight]

    def load(slot, source):
        return pltpu.make_async_copy(source, tall.at[slot], weight_sem.at[slot])

    def column_block(weight, column):
        return full(weight).at[:, :, pl.ds(column, features)]

    def exchange(j):
        return pltpu.make_async_remote_copy(
            qkv.at[pl.ds(2 * j, 2), :, pl.ds(features, 2 * features)], other.at[pl.ds(2 * j, 2)],
            pair_sem.at[0, j], pair_sem.at[1, j], device_id={"seq": me ^ 1},
        )

    def rows_of(ref, group, column, wide, spatial):
        lanes = slice(column, column + wide)
        if spatial:
            return ref[pl.ds(2 * group, 2), :, lanes].reshape(-1, wide)
        return jnp.concatenate([ref[2 * block + group, :, lanes] for block in range(4)], 0)

    def attend(layer, spatial, group, span, allowed):
        for head in range(HEADS):
            start, wide, _ = window(head)
            mask = head_mask(head)
            queries = rows_of(qkv, group, start, wide, spatial) * mask
            keys = rows_of(qkv, group, features + start, wide, spatial)
            values = rows_of(qkv, group, 2 * features + start, wide, spatial)
            if spatial:
                keys = jnp.concatenate([keys, rows_of(other, group, start, wide, True)], 0)
                values = jnp.concatenate(
                    [values, rows_of(other, group, features + start, wide, True)], 0
                )
            scores = times_turned(queries, keys)
            if not spatial:
                scores = jnp.where(allowed, scores, -3e38)
            grown = jnp.exp2(
                (scores - jnp.max(scores, axis=-1, keepdims=True)) * (HEAD_WIDTH ** (-0.5) * 1.4426950408889634)
            )
            chance = (grown * (1.0 / jnp.sum(grown, axis=-1, keepdims=True))).astype(LOW)
            prob[head, :span] = chance
            add_window(part.at[pl.ds(0, span)], head, times(chance, values * mask))
        got = part[:span].astype(LOW)
        if spatial:
            held[pl.ds(2 * group, 2)] = got.reshape(2, -1, features)
        else:
            for block in range(4):
                held[2 * block + group] = got[block * 64 : (block + 1) * 64]

    def flat_rows(ref):
        return ref[...].reshape(-1, features)

    def turn_out(source, target):
        settle("turned")
        for j in range(features // LANES):
            lanes = slice(j * LANES, (j + 1) * LANES)
            turned[lanes, :] = source[:, lanes].T
        begin("turned", turned, target)

    def layer(at_layer, spatial, x, plan):
        first = 4 * at_layer
        out = outs[at_layer]
        groups = 4 if spatial else 2
        span = x.shape[0] // groups
        mod = mod_ref.at[at_layer]

        def go(place):
            for at in plan.get(place, ()):
                if at is None:
                    gather.share(len(gather.pieces) - 1)
                elif isinstance(at, list):
                    for copy in at:
                        copy.start()
                else:
                    gather.advance(at)

        def go_when(place, index):
            for key, pieces in plan.items():
                if isinstance(key, tuple) and key[0] == place:
                    @pl.when(index == key[1])
                    def _():
                        for at in pieces:
                            gather.advance(at)

        scaled, shift = 1.0 + mod[1:2], mod[0:1]

        def norm(at):
            unit, _ = unit_rows(x[at].astype(WIDE))
            normed[at] = (unit * scaled + shift).astype(LOW)

        strips(x.shape[0], norm)
        turn_out(normed[...], out["h"])
        go("norm")
        gather.ready(first)
        load(0, column_block(first, 0)).start()
        settle("qkv")
        for j in range(3):
            load(j % 2, column_block(first, 0)).wait()
            if j < 2:
                load((j + 1) % 2, column_block(first, (j + 1) * features)).start()
            got = times(normed[...], tall[j % 2].reshape(features, features)).astype(LOW)
            qkv[:, :, j * features : (j + 1) * features] = got.reshape(8, -1, features)
            go(f"qkv{j}")
        begin("qkv", qkv, out["qkv"])
        if spatial:
            for j in range(groups):
                exchange(j).start()
        allowed = None if spatial else same_place()

        def prob_copy(group):
            return pltpu.make_async_copy(
                prob.at[:, pl.ds(0, span)], out["prob"].at[group], prob_sem
            )

        def one_group(group, carry):
            go_when("group", group)
            if spatial:
                exchange(group).wait_recv()

            @pl.when(group > 0)
            def _():
                prob_copy(group).wait()

            attend(at_layer, spatial, group, span, allowed)
            prob_copy(group).start()
            return carry

        lax.fori_loop(0, groups, one_group, 0)
        prob_copy(0).wait()
        if spatial:
            begin("other", other, other_ref)
            for j in range(groups):
                exchange(j).wait_send()
        go("attended")
        gather.ready(first + 1)
        load(0, full(first + 1)).start()
        attended = flat_rows(held)
        turn_out(attended, out["o"])
        load(0, full(first + 1)).wait()
        total[...] = times(attended, tall[0].reshape(features, features))
        gate, move, grow = mod[2:3], mod[3:4], 1.0 + mod[4:5]
        settle("low")
        settle("middle")

        def finish(at):
            branch = total[at]
            low[at] = branch.astype(LOW)
            got = x[at].astype(WIDE) + gate * branch
            middle[at] = got
            unit, _ = unit_rows(got)
            normed[at] = (unit * grow + move).astype(LOW)

        strips(x.shape[0], finish)
        begin("low", low, out["branch"])
        begin("middle", middle, out["x1"])
        turn_out(normed[...], out["h2"])
        go("middle")
        gather.ready(first + 2)
        gather.ready(first + 3)

        down = full(first + 3)
        per = down.shape[0] * down.shape[1] // steps

        def chunk_loads(step, slot):
            column = pl.multiple_of(step * CHUNK, CHUNK)
            owner = step * CHUNK // down.shape[1]
            copies = [
                pltpu.make_async_copy(
                    full(first + 2).at[:, :, pl.ds(column, CHUNK)],
                    tall.at[slot, :, :, pl.ds(0, CHUNK)], weight_sem.at[slot],
                )
            ]
            return copies, column, owner

        def start_loads(step, slot):
            copies, column, owner = chunk_loads(step, slot)
            for copy in copies:
                copy.start()
            pltpu.make_async_copy(
                down_rows(step), short.at[slot], weight_sem.at[2 + slot]
            ).start()

        def down_rows(step):
            return fulls_flat[at_layer].at[pl.ds(pl.multiple_of(step * 4, 4), 4)]

        fulls_flat = [fulls[3].reshape(*split_rows(fulls[3].shape)), fulls[7].reshape(*split_rows(fulls[7].shape))]

        def wait_loads(slot):
            for copy in chunk_loads(0, slot)[0]:
                copy.wait()
            pltpu.make_async_copy(down_rows(0), short.at[slot], weight_sem.at[2 + slot]).wait()

        def chunk_outs(step, slot):
            column = pl.multiple_of(step * CHUNK, CHUNK)
            return (
                pltpu.make_async_copy(
                    hidden.at[slot], out["z"].at[pl.ds(column, CHUNK)], chunk_sem.at[0, slot]
                ),
                pltpu.make_async_copy(
                    slope.at[slot], out["slope"].at[:, pl.ds(column, CHUNK)], chunk_sem.at[1, slot]
                ),
            )

        start_loads(0, 0)
        half = x.shape[0] // 2
        strips(x.shape[0], lambda at: clear(total, at))

        def chunk(step, carry):
            slot = lax.rem(step, 2)
            go_when("chunk", step)
            wait_loads(slot)

            @pl.when(step + 1 < steps)
            def _():
                start_loads(step + 1, 1 - slot)

            @pl.when(step >= 2)
            def _():
                for copy in chunk_outs(step, slot):
                    copy.wait()

            up = tall[slot, :, :, :CHUNK].reshape(features, CHUNK)
            for j in range(2):
                rows = slice(j * half, (j + 1) * half)
                value, bend = gelu_and_slope(times(normed[rows], up))
                slope[slot, rows] = bend.astype(LOW)
                value = value.astype(LOW)
                hidden[slot, :, rows] = value.T
                total[rows] += times(value, short[slot].reshape(CHUNK, features))

            for copy in chunk_outs(step, slot):
                copy.start()
            return carry

        lax.fori_loop(0, steps, chunk, 0)
        for slot in range(2):
            for copy in chunk_outs(0, slot):
                copy.wait()
        last = mod[5:6]
        settle("low")

        def close(at):
            mlp = total[at]
            low[at] = mlp.astype(LOW)
            total[at] = middle[at] + last * mlp

        strips(x.shape[0], close)
        begin("low", low, out["mlp"])
        ready[...] = total[...].astype(LOW).reshape(ready.shape)

    layer(0, True, x_ref, {
        "norm": (0, 1, 2, 3), "qkv1": (4,), ("group", 0): (5,), ("group", 1): (6,), ("group", 2): (7,),
        ("group", 3): (8,), "attended": (9,), "middle": (10, 11, 12), ("chunk", 1): (13,),
        ("chunk", 3): (14,), ("chunk", 4): (15,),
    })
    copies = moves(ready, x2_ref, next_move_sem, next_stay_sem, me, True)
    for copy in copies:
        copy.start()
    gather.local(4)
    gather.advance(16)
    gather.advance(17)
    for copy in copies:
        copy.wait()
    fetch = pltpu.make_async_copy(x2_ref, x2, next_sem)
    fetch.start()
    fetch.wait()
    x2_rows = x2.reshape(x_ref.shape)
    later = moves(tokens, moved, move_sem, stay_sem, me, True)
    layer(1, False, x2_rows, {
        "norm": (18,), "qkv0": (19,), "qkv2": (20,), ("group", 1): (21,), "attended": (22,),
        "middle": (23, None, later),
    })
    begin("ready", ready, y_ref)
    for name in names:
        settle(name)
    for copy in later:
        copy.wait()
    gather.finish()


def split_rows(shape):
    return (shape[0] * shape[1] // (CHUNK // 4), CHUNK // 4, shape[2])


def forward(shards, partial, condition, cotangent, x, cid):
    shapes = [shard.shape for shard in shards]
    count = len(shapes)
    tokens, features = x.shape
    frames, places, _ = cotangent.shape
    wide = shapes[2][1]
    any_ = pl.BlockSpec(memory_space=pl.ANY)
    struct = jax.ShapeDtypeStruct
    moved = struct((8, frames, places // 8, features), LOW)
    outs = Gather.outs(shapes) + [
        struct((2, 6, features), WIDE),
        struct((4,) + condition.shape, condition.dtype),
        moved,
        struct((8, tokens // 8, 2 * features), LOW),
        moved,
        struct((frames, places, features), LOW),
    ]
    for groups in (4, 2):
        outs += [
            struct((8, tokens // 8, 3 * features), LOW),
            struct((groups, HEADS, tokens // groups, KEYS), LOW),
            struct((features, tokens), LOW),
            struct((features, tokens), LOW),
            struct((features, tokens), LOW),
            struct((wide, tokens), LOW),
            struct((tokens, wide), LOW),
            struct((tokens, features), WIDE),
            struct((tokens, features), LOW),
            struct((tokens, features), LOW),
        ]
    dma = pltpu.SemaphoreType.DMA
    vm = pltpu.VMEM
    flops = 2 * tokens * 8 * sum(shape[0] * shape[1] for shape in shapes)
    got = pl.pallas_call(
        functools.partial(forward_kernel, shapes),
        out_shape=outs,
        in_specs=[any_] * (count + 3) + [pl.BlockSpec(memory_space=vm)],
        out_specs=[any_] * count + [pl.BlockSpec(memory_space=vm)] + [any_] * (len(outs) - count - 1),
        scratch_shapes=[
            vm((8,) + partial.shape, WIDE),
            vm(moved.shape, LOW),
            vm((8, tokens // 8, 3 * features), LOW),
            vm((8, tokens // 8, 2 * features), LOW),
            vm((8, tokens // 8, features), LOW),
            vm((tokens, features), LOW),
            vm((tokens, features), WIDE),
            vm((tokens, features), WIDE),
            vm((KEYS, features), WIDE),
            vm((HEADS, KEYS, KEYS), LOW),
            vm((features, tokens), LOW),
            vm((tokens, features), LOW),
            vm((frames, places, features), LOW),
            vm((2, 8, features // 8, features), LOW),
            vm((2, 4, CHUNK // 4, features), LOW),
            vm((2, CHUNK, tokens), LOW),
            vm((2, tokens, CHUNK), LOW),
            dma((2, 11)),
            *move_scratch(),
            *move_scratch(),
            dma(()),
            dma((2, 4)),
            dma((4,)),
            dma((8,)),
            dma(()),
            dma((2, 2)),
        ]
        + Gather.scratch(shapes),
        compiler_params=params(60, cid),
        cost_estimate=cost(flops, 4 * flops // tokens),
        name="forward",
    )(*shards, partial, condition, cotangent, x)
    weights = got[:count]
    named = [dict(zip(OUTS, got[count + 6 + 10 * at : count + 16 + 10 * at])) for at in range(2)]
    return weights, got[count : count + 6], named


SLOTS = 3
BACK = 4


KEPT = ("h", "o", "h2", "z", "qkv", "prob", "slope", "x1", "branch", "mlp")
RIGHTS = ("qkv", "da", "du", "df")
ORDER = (3, 2, 1, 0)


def backward_kernel(dims, *refs):
    rows, width, edge, tokens, total, spans = dims
    weights, refs = (refs[:4], refs[4:8]), refs[8:]
    kept = [dict(zip(KEPT, refs[10 * at : 10 * at + 10])) for at in range(2)]
    g_in, other_in, y_in, x_ins, mod_ref = refs[20], refs[21], refs[22], refs[23:25], refs[25]
    refs = refs[26:]
    grads, refs = (refs[:4], refs[4:8]), refs[8:]
    rights = [dict(zip(RIGHTS, refs[4 * at : 4 * at + 4])) for at in range(2)]
    every_mod, moved, input_grad, g_out = refs[8:12]
    (
        left, right, away, pair_in, part, first_in_a, first_in_b, mid_a, mid_b, second_in_a, second_in_b,
        clip, rep_in, joined, inner_in, final, back_in, wide,
        tall, short, acc, middle, grad_in, low, aux, slope, du, qkv, other, take, prob, dout,
        total_q, total_k, total_v, ready, sums, mod_low, mod_in,
        load_sem, pair_sem, link_sem, rep_sem, back_sem, store_sem, mod_sem, tall_sem, short_sem, slope_sem,
        in_sem, prob_sem, out_sem, du_sem, swap_sem, move_sem, stay_sem, last_move_sem, last_stay_sem,
    ) = refs[12:]
    me, z = lax.axis_index("seq"), lax.axis_index("rep")
    core, x, y = me & 1, (me >> 1) & 1, (me >> 2) & 1
    inner = (z == 1) | (z == 2)
    outer = (z == 0) | (z == 3)
    features = width
    steps = weights[0][2].shape[2] // CHUNK
    root = HEAD_WIDTH ** (-0.5)


    def wait_out(source, target):
        copy = pltpu.make_async_copy(source, target, out_sem)
        copy.start()
        copy.wait()

    def flat_in(ref):
        return ref if len(ref.shape) == 2 else ref.reshape(tokens, features)

    def load_in(name, at):
        source, target = {
            "grad": (flat_in((g_out, g_in)[at]), grad_in),
            "mlp": (kept[at]["mlp"], aux),
            "branch": (kept[at]["branch"], aux),
            "x": (flat_in(x_ins[at]), aux),
            "x1": (kept[at]["x1"], middle),
            "qkv": (kept[at]["qkv"], qkv),
            "other": (other_in, other),
        }[name]
        order = ("grad", "mlp", "branch", "x", "x1", "qkv", "other")
        return pltpu.make_async_copy(source, target, in_sem.at[order.index(name)])

    def chunk_loads(at, step, slot):
        column = pl.multiple_of(step * CHUNK, CHUNK)
        down = weights[at][3].reshape(*split_rows(weights[at][3].shape))
        return (
            pltpu.make_async_copy(
                weights[at][2].at[:, :, pl.ds(column, CHUNK)],
                tall.at[slot, :, :, pl.ds(0, CHUNK)], tall_sem.at[slot],
            ),
            pltpu.make_async_copy(
                down.at[pl.ds(pl.multiple_of(step * 4, 4), 4)], short.at[slot], short_sem.at[slot]
            ),
            pltpu.make_async_copy(
                kept[at]["slope"].at[:, pl.ds(column, CHUNK)], slope.at[slot], slope_sem.at[slot]
            ),
        )

    def tall_load(source, slot):
        return pltpu.make_async_copy(source, tall.at[slot], tall_sem.at[slot])

    def qkv_block(at, j):
        return weights[at][0].at[:, :, pl.ds(j * features, features)]

    def mlp_begin(at):
        load_in("grad", at).start()
        load_in("mlp", at).start()
        load_in("x1", at).start()
        for slot in range(2):
            for copy in chunk_loads(at, slot, slot):
                copy.start()
        load_in("grad", at).wait()
        load_in("mlp", at).wait()
        gate = mod_ref[at, 5:6]
        sums[at] = jnp.zeros_like(sums[at])

        def begin(strip):
            grad = grad_in[strip].astype(WIDE)
            low[strip] = (gate * grad).astype(LOW)
            clear(acc, strip)
            sums[at, 5:6] += jnp.sum(grad * aux[strip].astype(WIDE), axis=0, keepdims=True)

        strips(tokens, begin)
        load_in("branch", at).start()
        wait_out(low, rights[at]["df"])

    def du_copy(at, step):
        column = pl.multiple_of(step * CHUNK, CHUNK)
        return pltpu.make_async_copy(du, rights[at]["du"].at[:, pl.ds(column, CHUNK)], du_sem)

    def mlp_chunk(at, step):
        slot = lax.rem(step, 2)

        @pl.when(step > 0)
        def _():
            du_copy(at, step).wait()

        for copy in chunk_loads(at, step, slot):
            copy.wait()
        half = tokens // 2
        up = tall[slot, :, :, :CHUNK].reshape(features, CHUNK)
        for j in range(2):
            strip = slice(j * half, (j + 1) * half)
            got = times_turned(low[strip], short[slot].reshape(CHUNK, features))
            got = (got * slope[slot, strip].astype(WIDE)).astype(LOW)
            du[strip] = got
            acc[strip] += times_turned(got, up)

        @pl.when(step + 2 < steps)
        def _():
            for copy in chunk_loads(at, step + 2, slot):
                copy.start()

        du_copy(at, step).start()

    def prob_load(at, group):
        span = tokens // kept[at]["prob"].shape[0]
        return pltpu.make_async_copy(
            kept[at]["prob"].at[group], prob.at[:, pl.ds(0, span)], prob_sem
        )

    def mlp_finish(at):
        tall_load(weights[at][1], 0).start()
        tall_load(qkv_block(at, 0), 1).start()
        load_in("qkv", at).start()
        prob_load(at, 0).start()
        if at == 0:
            load_in("other", at).start()
        du_copy(at, 0).wait()
        load_in("branch", at).wait()
        load_in("x1", at).wait()
        gate, scaled = mod_ref[at, 2:3], 1.0 + mod_ref[at, 4:5]

        def finish(strip):
            grad = acc[strip]
            unit, spread = unit_rows(middle[strip])
            got = grad_in[strip].astype(WIDE) + into_norm(grad, scaled, unit, spread)
            middle[strip] = got
            low[strip] = (gate * got).astype(LOW)
            sums[at, 2:3] += jnp.sum(got * aux[strip].astype(WIDE), axis=0, keepdims=True)
            sums[at, 3:4] += jnp.sum(grad, axis=0, keepdims=True)
            sums[at, 4:5] += jnp.sum(grad * unit, axis=0, keepdims=True)

        strips(tokens, finish)
        load_in("x", at).start()
        wait_out(low, rights[at]["da"])

    def project(at):
        tall_load(weights[at][1], 0).wait()
        half = tokens // 2
        for j in range(2):
            got = times_turned(
                low[j * half : (j + 1) * half], tall[0].reshape(features, features)
            ).astype(LOW)
            dout[4 * j : 4 * j + 4] = got.reshape(4, -1, features)
        tall_load(qkv_block(at, 1), 0).start()
        load_in("qkv", at).wait()
        if at == 0:
            load_in("other", at).wait()

    def rows_of(ref, group, column, lanes, spatial):
        lanes = slice(column, column + lanes)
        if spatial:
            block = ref[pl.ds(2 * group, 2), :, lanes]
            return block.reshape(-1, block.shape[2])
        return jnp.concatenate([ref[2 * block + group, :, lanes] for block in range(4)], 0)

    def swap_copy(j):
        return pltpu.make_async_remote_copy(
            other.at[pl.ds(2 * j, 2)], take.at[pl.ds(2 * j, 2)],
            swap_sem.at[0, j], swap_sem.at[1, j], device_id={"seq": me ^ 1},
        )

    def attend_group(at, group):
        spatial = at == 0
        groups = kept[at]["prob"].shape[0]
        span = tokens // groups
        prob_load(at, group).wait()
        for head in range(HEADS):
            start, lanes, _ = window(head)
            mask = head_mask(head)
            queries = rows_of(qkv, group, start, lanes, spatial) * mask
            keys = rows_of(qkv, group, features + start, lanes, spatial)
            values = rows_of(qkv, group, 2 * features + start, lanes, spatial)
            coming = rows_of(dout, group, start, lanes, spatial) * mask
            if spatial:
                keys = jnp.concatenate([keys, rows_of(other, group, start, lanes, True)], 0)
                values = jnp.concatenate(
                    [values, rows_of(other, group, features + start, lanes, True)], 0
                )
            chance = prob[head, :span]
            known = chance.astype(WIDE)
            dprob = times_turned(coming, values)
            level = jnp.sum(dprob * known, axis=-1, keepdims=True)
            dscores = (known * (dprob - level)).astype(LOW)
            add_window(total_q.at[pl.ds(0, span)], head, times(dscores, keys * mask))
            add_window(total_k, head, turned_times(dscores, queries))
            add_window(total_v, head, turned_times(chance, coming))

        @pl.when(group + 1 < groups)
        def _():
            prob_load(at, group + 1).start()

        pieces = (
            (total_q[:span] * root).astype(LOW),
            (total_k[:span] * root).astype(LOW),
            total_v[:span].astype(LOW),
        )
        for j, piece in enumerate(pieces):
            lanes = slice(j * features, (j + 1) * features)
            if spatial:
                qkv[pl.ds(2 * group, 2), :, lanes] = piece.reshape(2, -1, features)
            else:
                for block in range(4):
                    qkv[2 * block + group, :, lanes] = piece[block * 64 : (block + 1) * 64]
        if spatial:
            other[pl.ds(2 * group, 2), :, :features] = (
                (total_k[span:] * root).astype(LOW).reshape(2, -1, features)
            )
            other[pl.ds(2 * group, 2), :, features:] = (
                total_v[span:].astype(LOW).reshape(2, -1, features)
            )
            swap_copy(group).start()

    def attend_finish(at):
        if at == 0:
            for j in range(4):
                swap_copy(j).wait()
                pair = slice(2 * j, 2 * j + 2)
                lanes = slice(features, 3 * features)
                qkv[pair, :, lanes] = qkv[pair, :, lanes] + take[pair]
        wait_out(qkv, rights[at]["qkv"].reshape(*qkv.shape))

    def qkv_chunks(at):
        for j in range(3):
            slot = 1 - j % 2
            tall_load(qkv_block(at, j), slot).wait()
            got = times_turned(
                qkv[:, :, j * features : (j + 1) * features].reshape(tokens, features),
                tall[slot].reshape(features, features),
            )
            if j == 0:
                acc[...] = got
                tall_load(qkv_block(at, 2), slot).start()
            else:
                acc[...] = acc[...] + got

    def last_moves():
        return moves(y_in, moved, last_move_sem, last_stay_sem, me, False)

    def grad_moves():
        return moves(ready, g_out, move_sem, stay_sem, me, False)

    def qkv_finish(at):
        load_in("x", at).wait()
        scaled = 1.0 + mod_ref[at, 1:2]

        def finish(strip):
            grad = acc[strip]
            unit, spread = unit_rows(aux[strip].astype(WIDE))
            sums[at, 0:1] += jnp.sum(grad, axis=0, keepdims=True)
            sums[at, 1:2] += jnp.sum(grad * unit, axis=0, keepdims=True)
            acc[strip] = middle[strip] + into_norm(grad, scaled, unit, spread)

        strips(tokens, finish)
        if at == 0:
            wait_out(acc, input_grad)
        else:
            ready[...] = acc[...].astype(LOW).reshape(ready.shape)
            for copy in grad_moves():
                copy.start()

    def backward_step(t):
        def at_turn(turn):
            return pl.when(t == turn)

        @pl.when(t < steps - 1)
        def _():
            mlp_chunk(1, t + 1)

        @at_turn(4)
        def _():
            mlp_finish(1)
            project(1)

        @pl.when((t >= 5) & (t < 7))
        def _():
            attend_group(1, t - 5)

        @at_turn(6)
        def _():
            attend_finish(1)

        @at_turn(7)
        def _():
            qkv_chunks(1)

        @at_turn(8)
        def _():
            qkv_finish(1)

        @at_turn(10)
        def _():
            for copy in grad_moves():
                copy.wait()
            mlp_begin(0)

        @pl.when((t >= 10) & (t < 10 + steps))
        def _():
            mlp_chunk(0, t - 10)

        @at_turn(15)
        def _():
            mlp_finish(0)
            project(0)

        @pl.when((t >= 16) & (t < 20))
        def _():
            attend_group(0, t - 16)

        @at_turn(19)
        def _():
            attend_finish(0)

        @at_turn(20)
        def _():
            qkv_chunks(0)

        @at_turn(21)
        def _():
            qkv_finish(0)
            mod_low[...] = jnp.zeros_like(mod_low)
            for at in range(2):
                mod_low[8 * at : 8 * at + 8] = sums[at].astype(LOW)
            mod_in[me] = mod_low[...]
            for copy in mod_copies():
                copy.start()

        @at_turn(23)
        def _():
            for copy in mod_copies():
                copy.wait()
            summed = mod_in[0].astype(WIDE)
            for device in range(1, 8):
                summed += mod_in[device].astype(WIDE)
            every_mod[z] = summed.astype(LOW)
            for copy in clip_copies():
                copy.start()

        @at_turn(25)
        def _():
            for copy in last_moves():
                copy.start()

        @at_turn(total + 5)
        def _():
            for copy in clip_copies():
                copy.wait()
            for copy in last_moves():
                copy.wait()

    def mod_copies():
        return [
            pltpu.make_async_remote_copy(
                mod_low, mod_in.at[me], mod_sem.at[0, mask], mod_sem.at[1, mask],
                device_id={"seq": me ^ mask},
            )
            for mask in range(1, 8)
        ]

    def clip_copies():
        return [
            pltpu.make_async_remote_copy(
                every_mod.at[z], every_mod.at[z], mod_sem.at[0, 7 + mask], mod_sem.at[1, 7 + mask],
                device_id={"rep": z ^ mask},
            )
            for mask in range(1, 4)
        ]


    names = ("h", "o", "h2", "z")

    def loads(block, slot):
        for layer, kind, first, count in spans:
            @pl.when((block >= first) & (block < first + count))
            def _():
                source = kept[layer][names[kind]]
                if kind == 3:
                    source = source.at[:, :, block - first]
                pltpu.make_async_copy(source, left.at[slot], load_sem.at[0, slot]).start()
                source = rights[layer][RIGHTS[kind]]
                if kind in (0, 2):
                    column = pl.multiple_of((block - first) * width, width)
                    source = source.at[:, pl.ds(column, width)]
                pltpu.make_async_copy(source, right.at[slot], load_sem.at[1, slot]).start()

    def wait_loads(slot):
        pltpu.make_async_copy(kept[0]["h"], left.at[slot], load_sem.at[0, slot]).wait()
        pltpu.make_async_copy(rights[0]["da"], right.at[slot], load_sem.at[1, slot]).wait()

    def store(block):
        for layer, kind, first, count in spans:
            @pl.when((block >= first) & (block < first + count))
            def _():
                target = grads[layer][kind]
                if kind == 3:
                    row = pl.multiple_of((block - first) * rows, rows)
                    target = target.at[pl.ds(row, rows)]
                elif kind in (0, 2):
                    column = pl.multiple_of((block - first) * width, width)
                    target = target.at[:, pl.ds(column, width)]
                pltpu.make_async_copy(wide, target, store_sem).start()

    def to_seq(source, target, which, slot, mask):
        return pltpu.make_async_remote_copy(
            source, target, link_sem.at[0, which, slot], link_sem.at[1, which, slot],
            device_id={"seq": me ^ mask},
        )

    def pair_copy(t):
        slot = lax.rem(t, 2)
        return pltpu.make_async_remote_copy(
            away, pair_in.at[slot], pair_sem.at[0, slot], pair_sem.at[1, slot],
            device_id={"seq": me ^ 1},
        )

    def first_copies(t):
        slot, block = lax.rem(t, SLOTS), lax.rem(t - 1, SLOTS)
        return (
            to_seq(part.at[block, :, 1 - x, :, pl.ds(0, edge)], first_in_a.at[slot], 0, slot, 2),
            to_seq(
                part.at[block, 1 - y, :, :, pl.ds(edge, width - edge)],
                first_in_b.at[slot], 1, slot, 4,
            ),
        )

    def second_copies(t):
        slot, block = lax.rem(t, SLOTS), lax.rem(t, 2)
        return (
            to_seq(mid_a.at[block, 1 - y], second_in_a.at[slot], 2, slot, 4),
            to_seq(mid_b.at[block, 1 - x], second_in_b.at[slot], 3, slot, 2),
        )

    def rep_copy(t):
        slot = lax.rem(t, SLOTS)
        return pltpu.make_async_remote_copy(
            clip.at[lax.rem(t, 2)], rep_in.at[slot], rep_sem.at[0, 0, slot], rep_sem.at[1, 0, slot],
            device_id={"rep": z ^ 1},
        )

    def inner_copy(t):
        slot = lax.rem(t, SLOTS)
        return pltpu.make_async_remote_copy(
            joined.at[lax.rem(t, 2)], inner_in.at[slot],
            rep_sem.at[0, 1, slot], rep_sem.at[1, 1, slot],
            device_id={"rep": z ^ 3},
        )

    def back_copy(t):
        slot = lax.rem(t, BACK)
        return pltpu.make_async_remote_copy(
            final.at[lax.rem(t, 2)], back_in.at[slot], back_sem.at[0, slot], back_sem.at[1, slot],
            device_id={"rep": z ^ 1},
        )

    def turn(t, carry):
        def stage(back):
            return (t >= back) & (t < total + back)

        now2, was2 = lax.rem(t, 2), lax.rem(t + 1, 2)
        was3 = lax.rem(t + 2, SLOTS)

        @pl.when(t + 1 < total)
        def _():
            loads(t + 1, was2)

        @pl.when(stage(1))
        def _():
            for copy in first_copies(t):
                copy.start()

        @pl.when(stage(2))
        def _():
            block = lax.rem(t + 1, SLOTS)
            for at in range(2):
                mid_a[now2, at] = part[block, at, x, :, :edge] + first_in_a[was3, at]
                mid_b[now2, at] = part[block, y, at, :, edge:] + first_in_b[was3, at]
            for copy in second_copies(t):
                copy.start()

        @pl.when(stage(3))
        def _():
            clip[now2, :, :edge] = mid_a[was2, y] + second_in_a[was3]
            clip[now2, :, edge:] = mid_b[was2, x] + second_in_b[was3]

            @pl.when(outer)
            def _():
                rep_copy(t).start()

        @pl.when(stage(4) & inner)
        def _():
            joined[now2] = clip[was2] + rep_in[was3]
            inner_copy(t).start()

        @pl.when(stage(5) & inner)
        def _():
            final[now2] = joined[was2] + inner_in[was3]
            back_copy(t).start()

        @pl.when(stage(6))
        def _():
            @pl.when(inner)
            def _():
                wide[...] = final[was2]

            @pl.when(outer)
            def _():
                wide[...] = back_in[lax.rem(t + 3, BACK)]

            store(t - 6)

        @pl.when(t < total)
        def _():
            wait_loads(now2)
            slot3 = lax.rem(t, SLOTS)
            parts = (slice(0, 512), slice(512, width))

            def product(which, at):
                block = left[now2, :, which]
                four, _, depth = block.shape
                got = times(block.reshape(four * rows, depth), right[now2, :, at]).astype(LOW)
                return got.reshape(four, rows, -1)

            for at in parts:
                away[:, :, at] = product(1 - core, at)
            pair_copy(t).start()
            for at in parts:
                got = product(core, at)
                part[slot3, 0, :, :, at] = got[:2]
                part[slot3, 1, :, :, at] = got[2:]

        backward_step(t)

        @pl.when(t < total)
        def _():
            pair_copy(t).wait()
            slot3 = lax.rem(t, SLOTS)

            def add(j, carry):
                part[slot3, j // 2, j % 2] = part[slot3, j // 2, j % 2] + pair_in[now2, j]
                return carry

            lax.fori_loop(0, 4, add, 0)

        @pl.when(stage(1))
        def _():
            for copy in first_copies(t):
                copy.wait()

        @pl.when(stage(2))
        def _():
            for copy in second_copies(t):
                copy.wait()

        @pl.when(stage(3))
        def _():
            @pl.when(outer)
            def _():
                rep_copy(t).wait_send()

            @pl.when(inner)
            def _():
                rep_copy(t).wait_recv()

        @pl.when(stage(4) & inner)
        def _():
            inner_copy(t).wait()

        @pl.when(stage(5))
        def _():
            @pl.when(inner)
            def _():
                back_copy(t).wait_send()

            @pl.when(outer)
            def _():
                back_copy(t).wait_recv()

        @pl.when(stage(6))
        def _():
            pltpu.make_async_copy(wide, grads[0][1], store_sem).wait()

        return carry

    enter(range(1, 8), range(1, 4))
    mlp_begin(1)
    mlp_chunk(1, jnp.int32(0))
    loads(0, 0)
    lax.fori_loop(0, total + 6, turn, 0)


def backward(weights, kept, g, other, y, xs, mods, cid):
    struct = jax.ShapeDtypeStruct
    tokens, features = xs[0].shape
    rows = features // 8
    wide = weights[0][2].shape[2]
    edge = features * 5 // 9 // 128 * 128
    frames, places = g.shape[1], 8 * g.shape[2]
    out_shapes = [(rows, 3 * features), (rows, features), (rows, wide), (wide // 8, features)]
    spans, total = [], 0
    for layer in (1, 0):
        for kind in ORDER:
            count = out_shapes[kind][0] * out_shapes[kind][1] // (rows * features)
            spans.append((layer, kind, total, count))
            total += count
    dims = (rows, features, edge, tokens, total, spans)
    any_ = pl.BlockSpec(memory_space=pl.ANY)
    outs = [struct(shape, LOW) for shape in out_shapes] * 2
    outs += [
        struct((tokens, 3 * features), LOW), struct((tokens, features), LOW),
        struct((tokens, wide), LOW), struct((tokens, features), LOW),
    ] * 2
    outs += [
        struct((4, 16, features), LOW),
        struct((frames, places, features), LOW),
        struct((tokens, features), WIDE),
        struct((frames, places, features), LOW),
    ]
    vm, dma = pltpu.VMEM, pltpu.SemaphoreType.DMA
    rest = features - edge
    scratch = [
        vm((2, 4, 2, rows, tokens), LOW),
        vm((2, tokens, features), LOW),
        vm((4, rows, features), LOW),
        vm((2, 4, rows, features), LOW),
        vm((SLOTS, 2, 2, rows, features), LOW),
        vm((SLOTS, 2, rows, edge), LOW),
        vm((SLOTS, 2, rows, rest), LOW),
        vm((2, 2, rows, edge), LOW),
        vm((2, 2, rows, rest), LOW),
        vm((SLOTS, rows, edge), LOW),
        vm((SLOTS, rows, rest), LOW),
        vm((2, rows, features), LOW),
        vm((SLOTS, rows, features), LOW),
        vm((2, rows, features), LOW),
        vm((SLOTS, rows, features), LOW),
        vm((2, rows, features), LOW),
        vm((BACK, rows, features), LOW),
        vm((rows, features), LOW),
        vm((2, 8, rows, features), LOW),
        vm((2, 4, CHUNK // 4, features), LOW),
        vm((tokens, features), WIDE),
        vm((tokens, features), WIDE),
        vm((tokens, features), LOW),
        vm((tokens, features), LOW),
        vm((tokens, features), LOW),
        vm((2, tokens, CHUNK), LOW),
        vm((tokens, CHUNK), LOW),
        vm((8, tokens // 8, 3 * features), LOW),
        vm((8, tokens // 8, 2 * features), LOW),
        vm((8, tokens // 8, 2 * features), LOW),
        vm((HEADS, KEYS, KEYS), LOW),
        vm((8, tokens // 8, features), LOW),
        vm((KEYS, features), WIDE),
        vm((KEYS, features), WIDE),
        vm((KEYS, features), WIDE),
        vm((8, frames, places // 8, features), LOW),
        vm((2, 8, features), WIDE),
        vm((16, features), LOW),
        vm((8, 16, features), LOW),
        dma((2, 2)),
        dma((2, 2)),
        dma((2, 4, SLOTS)),
        dma((2, 2, SLOTS)),
        dma((2, BACK)),
        dma(()),
        dma((2, 11)),
        dma((2,)),
        dma((2,)),
        dma((2,)),
        dma((7,)),
        dma(()),
        dma(()),
        dma(()),
        dma((2, 4)),
        *move_scratch(),
        *move_scratch(),
    ]
    flops = 4 * tokens * 8 * sum(a * b for a, b in out_shapes) * 2
    got = pl.pallas_call(
        functools.partial(backward_kernel, dims),
        out_shape=outs,
        in_specs=[any_] * (8 + 20 + 5) + [pl.BlockSpec(memory_space=vm)],
        out_specs=[any_] * 16 + [pl.BlockSpec(memory_space=vm)] + [any_] * 3,
        scratch_shapes=scratch,
        compiler_params=params(63, cid),
        cost_estimate=cost(flops, flops // tokens),
        name="backward",
    )(
        *weights[0], *weights[1], *[each[name] for each in kept for name in KEPT],
        g, other, y, *xs, mods,
    )
    grads = [grad.astype(WIDE) for grad in got[:8]]
    return grads[:4], grads[4:], got[16], got[17], got[18]


def by_device(left, features):
    tall, tokens = left.shape[0] // features, left.shape[1]
    rows = features // 8
    return left.reshape((4, 2, rows, tokens) if tall == 1 else (4, 2, tall, rows, tokens))


def fused_device(frames_in, conditioning, shards, partial_mod, cotangent):
    _, _, frames, places, features = frames_in.shape
    tokens = frames * places
    low_cotangent = cotangent.reshape(frames, places, features).astype(LOW)
    x_one = frames_in.reshape(tokens, features)
    weights, (mods, conditions, g_two, other, x_two, y_two), kept = forward(
        shards, partial_mod.reshape(-1, LANES), conditioning.reshape(-1, LANES), low_cotangent,
        x_one, 0,
    )
    for each in kept:
        for name in ("h", "o", "h2", "z"):
            each[name] = by_device(each[name], features)
    grads_one, grads_two, every_mod, block_out, input_grad = backward(
        (weights[:4], weights[4:]), kept, g_two, other, y_two.reshape(g_two.shape),
        (x_one, x_two.reshape(tokens, features)), mods, 1,
    )
    every_mod = every_mod.reshape(-1, 2, 8, features)[:, :, :6].reshape(-1, 12 * features)
    return (
        block_out.astype(WIDE), input_grad, grads_one, grads_two, every_mod,
        conditions.reshape(-1, features),
    )


def per_device(
    frames_in,
    conditioning,
    mod_first,
    qkv_first,
    out_first,
    up_first,
    down_first,
    mod_second,
    qkv_second,
    out_second,
    up_second,
    down_second,
    cotangent,
):
    clip_count, _, frame_dev, half_places, features = frames_in.shape
    fused = lax.axis_size("seq") == 8 and lax.axis_size("rep") == 4 and clip_count == 1
    row_count = mod_first.shape[0]
    row_start = lax.axis_index("seq") * row_count
    mod_width = mod_first.shape[1]
    rows_of = lambda whole: lax.dynamic_slice_in_dim(whole, row_start, row_count, 1)
    silu_local = rows_of(jax.nn.silu(conditioning)).astype(jnp.bfloat16)
    partial_mod = jnp.concatenate(
        [
            jnp.dot(silu_local, mod_first, preferred_element_type=jnp.float32),
            jnp.dot(silu_local, mod_second, preferred_element_type=jnp.float32),
        ],
        1,
    )
    shards = (
        qkv_first, out_first, up_first, down_first,
        qkv_second, out_second, up_second, down_second,
    )
    if fused:
        block_out, stream_grad, grads_one, grads_two, every_mod, conditions = fused_device(
            frames_in, conditioning, shards, partial_mod, cotangent
        )
        every_silu = rows_of(jax.nn.silu(conditions)).astype(jnp.bfloat16)
        mod_total = lax.dynamic_slice_in_dim(every_mod, lax.axis_index("rep"), 1, 0)
    else:
        weights = [lax.all_gather(shard, "seq", axis=0, tiled=True) for shard in shards]
        modulation = lax.psum(partial_mod, "seq")
        every_silu = lax.all_gather(silu_local, "rep", axis=0, tiled=True)
        mod_one, mod_two = modulation[:, :mod_width], modulation[:, mod_width:]
        weights_one, weights_two = weights[:4], weights[4:]
        start_stream = frames_in.reshape(clip_count, frame_dev, half_places, features).astype(
            jnp.float32
        )
        spatial_out, state_one = forward_layer(start_stream, mod_one, weights_one, True)
        placed = to_places(spatial_out)
        temporal_out, state_two = forward_layer(placed, mod_two, weights_two, False)
        block_out = to_frames(temporal_out, frame_dev)
        cotangent_sites = to_places(
            cotangent.reshape(clip_count, frame_dev, half_places, features)
        )
        placed_grad, mod_grad_two, pairs_two = backward_layer(
            cotangent_sites, placed, mod_two, weights_two, state_two, False
        )
        spatial_grad = to_frames(placed_grad, frame_dev)
        stream_grad, mod_grad_one, pairs_one = backward_layer(
            spatial_grad, start_stream, mod_one, weights_one, state_one, True
        )
        mod_grads = jnp.concatenate([mod_grad_one, mod_grad_two], 1).astype(jnp.bfloat16)
        grads_two, grads_one = layer_grads(pairs_two), layer_grads(pairs_one)
        mod_total = lax.psum(mod_grads, "seq").astype(jnp.bfloat16)
        every_mod = lax.all_gather(mod_total, "rep", axis=0, tiled=True)
    low_one, low_two = mod_total[:, :mod_width], mod_total[:, mod_width:]
    mod_weight_one = jnp.einsum(
        "cd,ce->de", every_silu, every_mod[:, :mod_width], preferred_element_type=jnp.float32
    )
    mod_weight_two = jnp.einsum(
        "cd,ce->de", every_silu, every_mod[:, mod_width:], preferred_element_type=jnp.float32
    )
    silu_grad = jnp.einsum("ce,de->cd", low_one, mod_first, preferred_element_type=jnp.float32)
    silu_grad = silu_grad + jnp.einsum(
        "ce,de->cd", low_two, mod_second, preferred_element_type=jnp.float32
    )
    condition_grad = jax.vjp(jax.nn.silu, rows_of(conditioning))[1](silu_grad)[0]
    out_shape = (clip_count, 1, frame_dev, half_places, features)
    return (
        block_out.reshape(out_shape),
        stream_grad.reshape(out_shape),
        condition_grad,
        mod_weight_one,
        *grads_one,
        mod_weight_two,
        *grads_two,
    )


def solution(mesh):
    return jax.shard_map(
        per_device,
        mesh=mesh,
        in_specs=(
            P("rep", "seq", None, None, None),
            P("rep", None),
            P("seq", None),
            P("seq", None),
            P("seq", None),
            P("seq", None),
            P("seq", None),
            P("seq", None),
            P("seq", None),
            P("seq", None),
            P("seq", None),
            P("seq", None),
            P("rep", "seq", None, None, None),
        ),
        out_specs=(
            P("rep", "seq", None, None, None),
            P("rep", "seq", None, None, None),
            P("rep", "seq"),
            P("seq", None),
            P("seq", None),
            P("seq", None),
            P("seq", None),
            P("seq", None),
            P("seq", None),
            P("seq", None),
            P("seq", None),
            P("seq", None),
            P("seq", None),
        ),
        check_vma=False,
    )
```

```python
import functools
import math

import jax
import jax.numpy as jnp
from jax import lax
from jax.experimental import pallas as pl
from jax.experimental.pallas import tpu as pltpu
from jax.sharding import PartitionSpec as P

HEADS = 16
HEAD_WIDTH = 72


norm_epsilon = 1e-06


def from_partner(block, axis, apart):
    count = lax.axis_size(axis)
    route = []
    for low in range(count):
        high = low | 1 << apart
        if high != low and high < count:
            route += [(low, high), (high, low)]
    return lax.ppermute(block, axis, route)


def shortened(x):
    return jax.tree.map(lambda a: a.astype(jnp.bfloat16) if a.dtype == jnp.float32 else a, x)


def layer_mod(stream, shift_part, scale_part):
    row_mean = jnp.mean(stream, axis=-1, keepdims=True)
    centred = stream - row_mean
    row_var = jnp.mean(centred * centred, axis=-1, keepdims=True)
    return centred * lax.rsqrt(row_var + norm_epsilon) * (1.0 + scale_part) + shift_part


def gelu_tanh(pre_value):
    return jax.nn.gelu(pre_value, approximate=True)


def project(left_operand, right_operand):
    return jnp.einsum(
        "csld,de->csle", left_operand, right_operand, preferred_element_type=jnp.float32
    )


def project_back(incoming, right_operand):
    return jnp.einsum("csle,de->csld", incoming, right_operand, preferred_element_type=jnp.float32)


def mod_parts(modulation):
    return [segment[:, None, None, :] for segment in jnp.split(modulation, 6, axis=-1)]


def partner_values(stacked):
    return from_partner(stacked, "seq", 0)


def partner_grads(stacked):
    return from_partner(stacked.astype(jnp.bfloat16), "seq", 0).astype(stacked.dtype)


def to_places(stream):
    clip_count, frame_dev, half_places, features = stream.shape
    devices = lax.axis_size("seq")
    place_part = half_places // devices
    exchanged = lax.all_to_all(
        stream.reshape(1, clip_count, frame_dev, devices, place_part, features).astype(
            jnp.bfloat16
        ),
        "seq",
        split_axis=3,
        concat_axis=0,
        tiled=True,
    ).astype(jnp.float32)
    exchanged = exchanged.reshape(devices // 2, 2, clip_count, frame_dev, place_part, features)
    exchanged = jnp.transpose(exchanged, (2, 1, 4, 0, 3, 5))
    return exchanged.reshape(clip_count, 2 * place_part, devices // 2 * frame_dev, features)


def to_frames(stream, frame_dev):
    clip_count, place_count, frame_total, features = stream.shape
    devices = lax.axis_size("seq")
    place_part = place_count // 2
    arranged = stream.reshape(clip_count, 2, place_part, devices // 2, frame_dev, features)
    arranged = jnp.transpose(arranged, (3, 1, 0, 4, 2, 5)).reshape(
        devices, clip_count, frame_dev, 1, place_part, features
    )
    exchanged = lax.all_to_all(
        shortened(arranged), "seq", split_axis=0, concat_axis=3, tiled=True
    ).astype(arranged.dtype)
    return exchanged.reshape(clip_count, frame_dev, devices * place_part, features)


def forward_layer(stream, modulation, weights, spatial):
    qkv_w, out_w, up_w, down_w = weights
    shift_attn, scale_attn, gate_attn, shift_mlp, scale_mlp, gate_mlp = mod_parts(modulation)
    clip_count, seq_count, seq_len, features = stream.shape
    normed = layer_mod(stream, shift_attn, scale_attn).astype(jnp.bfloat16)
    projected = project(normed, qkv_w).astype(jnp.bfloat16)
    queries, keys_all, values_all = jnp.split(projected, 3, axis=-1)
    if spatial:
        remote = partner_values(jnp.stack([keys_all, values_all]))
        keys_all = jnp.concatenate([keys_all, remote[0]], axis=2)
        values_all = jnp.concatenate([values_all, remote[1]], axis=2)
    key_len = keys_all.shape[2]
    queries = queries.reshape(clip_count, seq_count, seq_len, HEADS, HEAD_WIDTH)
    keys_all = keys_all.reshape(clip_count, seq_count, key_len, HEADS, HEAD_WIDTH)
    values_all = values_all.reshape(clip_count, seq_count, key_len, HEADS, HEAD_WIDTH)
    scores = jnp.einsum(
        "cslhe,csmhe->cshlm", queries, keys_all, preferred_element_type=jnp.float32
    ) * HEAD_WIDTH ** (-0.5)
    peak_score = jnp.max(scores, axis=-1, keepdims=True)
    scaled_exp = jnp.exp(scores - peak_score)
    attention = scaled_exp / jnp.sum(scaled_exp, axis=-1, keepdims=True)
    attention_low = attention.astype(jnp.bfloat16)
    attended = jnp.einsum(
        "cshlm,csmhe->cslhe", attention_low, values_all, preferred_element_type=jnp.float32
    )
    attended = attended.astype(jnp.bfloat16).reshape(clip_count, seq_count, seq_len, features)
    branch = project(attended, out_w)
    middle = stream + gate_attn * branch
    normed_mid = layer_mod(middle, shift_mlp, scale_mlp).astype(jnp.bfloat16)
    hidden_pre = project(normed_mid, up_w)
    hidden = gelu_tanh(hidden_pre).astype(jnp.bfloat16)
    mlp_out = project(hidden, down_w)
    result = middle + gate_mlp * mlp_out
    kept_state = (
        normed,
        queries,
        keys_all,
        values_all,
        attention,
        attention_low,
        attended,
        branch,
        middle,
        normed_mid,
        hidden_pre,
        hidden,
        mlp_out,
    )
    return (result, kept_state)


def backward_layer(result_grad, stream, modulation, weights, kept_state, spatial):
    qkv_w, out_w, up_w, down_w = weights
    (
        normed,
        queries,
        keys_all,
        values_all,
        attention,
        attention_low,
        attended,
        branch,
        middle,
        normed_mid,
        hidden_pre,
        hidden,
        mlp_out,
    ) = kept_state
    shift_attn, scale_attn, gate_attn, shift_mlp, scale_mlp, gate_mlp = mod_parts(modulation)
    clip_count, seq_count, seq_len, features = stream.shape
    gate_mlp_grad = jnp.sum(result_grad * mlp_out, axis=(1, 2))
    mlp_grad = (gate_mlp * result_grad).astype(jnp.bfloat16)
    hidden_grad = project_back(mlp_grad, down_w)
    pre_grad = jax.vjp(gelu_tanh, hidden_pre)[1](hidden_grad)[0].astype(jnp.bfloat16)
    normed_mid_grad = project_back(pre_grad, up_w)
    middle_ln_grad, shift_mlp_grad, scale_mlp_grad = jax.vjp(
        layer_mod, middle, shift_mlp, scale_mlp
    )[1](normed_mid_grad)
    middle_grad = result_grad + middle_ln_grad
    gate_attn_grad = jnp.sum(middle_grad * branch, axis=(1, 2))
    branch_grad = (gate_attn * middle_grad).astype(jnp.bfloat16)
    attended_grad = project_back(branch_grad, out_w).astype(jnp.bfloat16)
    attended_grad = attended_grad.reshape(clip_count, seq_count, seq_len, HEADS, HEAD_WIDTH)
    attention_grad = jnp.einsum(
        "cslhe,csmhe->cshlm", attended_grad, values_all, preferred_element_type=jnp.float32
    )
    scores_grad = attention * (
        attention_grad - jnp.sum(attention_grad * attention, axis=-1, keepdims=True)
    )
    scores_grad = scores_grad.astype(jnp.bfloat16)
    inv_root = HEAD_WIDTH ** (-0.5)
    queries_grad = (
        jnp.einsum("cshlm,csmhe->cslhe", scores_grad, keys_all, preferred_element_type=jnp.float32)
        * inv_root
    )
    keys_grad = (
        jnp.einsum("cshlm,cslhe->csmhe", scores_grad, queries, preferred_element_type=jnp.float32)
        * inv_root
    )
    values_grad = jnp.einsum(
        "cshlm,cslhe->csmhe", attention_low, attended_grad, preferred_element_type=jnp.float32
    )
    if spatial:
        returned = partner_grads(
            jnp.stack([keys_grad[:, :, seq_len:], values_grad[:, :, seq_len:]])
        )
        keys_grad = keys_grad[:, :, :seq_len] + returned[0]
        values_grad = values_grad[:, :, :seq_len] + returned[1]
    qkv_grad = jnp.concatenate(
        [
            component.reshape(clip_count, seq_count, seq_len, features)
            for component in (queries_grad, keys_grad, values_grad)
        ],
        axis=-1,
    )
    qkv_grad = qkv_grad.astype(jnp.bfloat16)
    normed_grad = project_back(qkv_grad, qkv_w)
    stream_ln_grad, attention_shift_gradient, scale_attn_grad = jax.vjp(
        layer_mod, stream, shift_attn, scale_attn
    )[1](normed_grad)
    stream_grad = middle_grad + stream_ln_grad
    mod_grad = jnp.concatenate(
        [
            attention_shift_gradient.reshape(clip_count, features),
            scale_attn_grad.reshape(clip_count, features),
            gate_attn_grad,
            shift_mlp_grad.reshape(clip_count, features),
            scale_mlp_grad.reshape(clip_count, features),
            gate_mlp_grad,
        ],
        axis=-1,
    )
    grad_pairs = (
        (normed, qkv_grad),
        (attended, branch_grad),
        (normed_mid, pre_grad),
        (hidden, mlp_grad),
    )
    return (stream_grad, mod_grad, grad_pairs)


def bit_count(axis):
    return lax.axis_size(axis).bit_length() - 1


def swap(block, axis, bit):
    count = lax.axis_size(axis)
    return lax.ppermute(block, axis, [(at, at ^ (1 << bit)) for at in range(count)])


def bit_of(axis, bit):
    return (lax.axis_index(axis) >> bit) & 1


def pick(block, which, axis):
    return lax.dynamic_index_in_dim(block, which, axis, keepdims=False)


def spread_rows_out(left_turned, right_operand, flipped):
    bits = bit_count("seq")
    total_rows, tokens = left_turned.shape
    rows = total_rows >> bits
    halves = left_turned.reshape(1 << (bits - 1), 2, rows, tokens)
    core = bit_of("seq", 0)

    def product(which):
        left = pick(halves, which, 1).reshape(-1, tokens)
        return jnp.dot(left, right_operand, preferred_element_type=jnp.float32).astype(
            jnp.bfloat16
        )

    arrived = swap(product(1 - core), "seq", 0)
    held = product(core)
    left_bits = list(range(bits - 1, 0, -1))
    shape = [2] * (bits - 1) + [rows, right_operand.shape[1]]
    held = held.reshape(shape)
    arrived = arrived.reshape(shape)
    order = list(left_bits) if flipped else left_bits[::-1]
    for bit in order:
        at = left_bits.index(bit)
        mine = bit_of("seq", bit)
        away = pick(held, 1 - mine, at).astype(jnp.float32) + pick(arrived, 1 - mine, at)
        kept = pick(held, mine, at).astype(jnp.float32) + pick(arrived, mine, at)
        arrived = swap(away.astype(jnp.bfloat16), "seq", bit)
        held = kept.astype(jnp.bfloat16)
        left_bits.remove(bit)
    return held.astype(jnp.float32) + arrived


def rep_sum(block, axis):
    bits = bit_count("rep")
    held = block.astype(jnp.bfloat16)
    for bit in range(bits):
        mine = bit_of("rep", bit)
        low, high = jnp.split(held, 2, axis)
        away = jnp.where(mine == 0, high, low)
        kept = jnp.where(mine == 0, low, high)
        held = (kept.astype(jnp.float32) + swap(away, "rep", bit)).astype(jnp.bfloat16)
    for bit in reversed(range(bits)):
        mine = bit_of("rep", bit)
        other = swap(held, "rep", bit)
        low = jnp.where(mine == 0, held, other)
        high = jnp.where(mine == 0, other, held)
        held = jnp.concatenate([low, high], axis)
    return held.astype(jnp.float32)


def turned(operand):
    return operand.reshape(-1, operand.shape[-1]).T


def flat(operand):
    return operand.reshape(-1, operand.shape[-1])


def cut(width, parts, of):
    return width * parts // of // 128 * 128


def down_grad(pair):
    left, right = turned(pair[0]), flat(pair[1])
    edge = cut(right.shape[1], 5, 9)
    return jnp.concatenate(
        [
            rep_sum(spread_rows_out(left, right[:, :edge], False), 0),
            rep_sum(spread_rows_out(left, right[:, edge:], True), 0),
        ],
        1,
    )


def up_grad(pair):
    left, right = turned(pair[0]), flat(pair[1])
    edge = cut(right.shape[1], 4, 9)
    return jnp.concatenate(
        [
            rep_sum(spread_rows_out(left, right[:, :edge], False), 1),
            rep_sum(spread_rows_out(left, right[:, edge:], True), 1),
        ],
        1,
    )


def attention_grads(qkv_pair, out_pair):
    left, right = turned(qkv_pair[0]), flat(qkv_pair[1])
    width = right.shape[1]
    edge = cut(width, 16, 27)
    first = rep_sum(spread_rows_out(left, right[:, :edge], False), 1)
    second = spread_rows_out(left, right[:, edge:], True)
    third = spread_rows_out(turned(out_pair[0]), flat(out_pair[1]), True)
    joined = rep_sum(jnp.concatenate([second, third], 1), 1)
    return (
        jnp.concatenate([first, joined[:, : width - edge]], 1),
        joined[:, width - edge :],
    )


def layer_grads(grad_pairs):
    qkv_pair, out_pair, up_pair, down_pair = grad_pairs
    down = down_grad(down_pair)
    up = up_grad(up_pair)
    qkv, out = attention_grads(qkv_pair, out_pair)
    return (qkv, out, up, down)


AHEAD = 2


def gather_pieces(shapes):
    features = math.gcd(*(columns for _, columns in shapes), 8 * shapes[0][0])
    rows_of = features // 8
    return rows_of, features, [
        (at, row, column)
        for at, (rows, columns) in enumerate(shapes)
        for row in range(0, rows, rows_of)
        for column in range(0, columns, features)
    ]


class Gather:
    def __init__(self, shapes, refs):
        count = len(shapes)
        self.count = count
        self.least, self.wide, self.pieces = gather_pieces(shapes)
        self.shards, self.fulls = refs[0], refs[1]
        self.held = refs[2][: count // 2]
        self.first_sem, self.second_sem, self.rep_sem, self.pair_sem, self.local_sem = refs[2][
            count // 2 :
        ]
        self.me, self.z = lax.axis_index("seq"), lax.axis_index("rep")
        odd = self.z & 1
        self.first, self.second = 2 + 2 * odd, 4 - 2 * odd

    @staticmethod
    def scratch(shapes):
        size = len(gather_pieces(shapes)[2])
        dma = pltpu.SemaphoreType.DMA
        half = shapes[: len(shapes) // 2]
        return [pltpu.VMEM(shape, jnp.bfloat16) for shape in half] + [
            dma((2, size)), dma((2, size)), dma((2, size)), dma((4, 2, size)), dma((2, len(shapes))),
        ]

    @staticmethod
    def outs(shapes):
        return [jax.ShapeDtypeStruct((8,) + shape, jnp.bfloat16) for shape in shapes]

    def place(self, owner, at):
        weight, row, column = self.pieces[at]
        return self.fulls[weight].at[owner, pl.ds(row, self.least), pl.ds(column, self.wide)]

    def own(self, at):
        weight, row, column = self.pieces[at]
        return self.shards[weight].at[pl.ds(row, self.least), pl.ds(column, self.wide)]

    def to_seq(self, source, owner, at, sems, mask):
        return pltpu.make_async_remote_copy(
            source, self.place(owner, at), sems.at[0, at], sems.at[1, at],
            device_id={"seq": self.me ^ mask},
        )

    def first_copy(self, at):
        return self.to_seq(self.own(at), self.me, at, self.first_sem, self.first)

    def second_copy(self, at):
        owner = self.me ^ self.first
        return self.to_seq(self.place(owner, at), owner, at, self.second_sem, self.second)

    def rep_copy(self, at):
        owner = self.me ^ self.first
        return pltpu.make_async_remote_copy(
            self.place(owner, at), self.place(owner, at), self.rep_sem.at[0, at], self.rep_sem.at[1, at],
            device_id={"rep": self.z ^ 1},
        )

    def pair_copy(self, which, at):
        if which == 0:
            return self.to_seq(self.own(at), self.me, at, self.pair_sem.at[0], 1)
        owner = self.me ^ (self.first, self.first ^ self.second, self.second)[which - 1]
        return self.to_seq(self.place(owner, at), owner, at, self.pair_sem.at[which], 1)

    def begin(self, at):
        self.first_copy(at).start()
        self.pair_copy(0, at).start()

    def fetch(self, weight):
        return pltpu.make_async_copy(
            self.shards[weight], self.held[weight % len(self.held)], self.local_sem.at[0, weight]
        )

    def keep(self, weight):
        return pltpu.make_async_copy(
            self.held[weight % len(self.held)], self.fulls[weight].at[self.me], self.local_sem.at[1, weight]
        )

    def start(self):
        for at in range(AHEAD):
            self.begin(at)
        self.local(0)

    def local(self, first):
        for weight in range(first, first + len(self.held)):
            self.fetch(weight).start()
        for weight in range(first, first + len(self.held)):
            self.fetch(weight).wait()
            self.keep(weight).start()

    def ready(self, weight):
        for at, piece in enumerate(self.pieces):
            if piece[0] == weight:
                for which in range(4):
                    self.pair_copy(which, at).wait_recv()
        self.keep(weight).wait()

    def advance(self, at):
        self.first_copy(at).wait_recv()
        if at + AHEAD < len(self.pieces):
            self.begin(at + AHEAD)
        self.second_copy(at).start()
        self.rep_copy(at).start()
        self.pair_copy(1, at).start()
        if at:
            self.share(at - 1)

    def share(self, at):
        self.second_copy(at).wait_recv()
        self.rep_copy(at).wait_recv()
        self.pair_copy(2, at).start()
        self.pair_copy(3, at).start()

    def finish(self):
        for at in range(len(self.pieces)):
            for copy in (self.first_copy(at), self.second_copy(at), self.rep_copy(at)):
                copy.wait_send()
            for which in range(4):
                self.pair_copy(which, at).wait_send()


def enter(seq_masks, rep_masks):
    me, z = lax.axis_index("seq"), lax.axis_index("rep")
    barrier = pltpu.get_barrier_semaphore()
    for mask in seq_masks:
        pl.semaphore_signal(barrier, inc=1, device_id={"seq": me ^ mask})
    for mask in rep_masks:
        pl.semaphore_signal(barrier, inc=1, device_id={"rep": z ^ mask})
    pl.semaphore_wait(barrier, len(seq_masks) + len(rep_masks))


LOW = jnp.bfloat16
WIDE = jnp.float32
LANES = 128
STRIP = 64
KEYS = 256


def whole_block(shape):
    return pl.BlockSpec(shape, lambda *at: (0,) * len(shape))


def strips(total, body):
    def step(j, carry):
        body(pl.ds(pl.multiple_of(j * STRIP, STRIP), STRIP))
        return carry

    lax.fori_loop(0, total // STRIP, step, 0)


def clear(ref, at):
    ref[at] = jnp.zeros_like(ref[at])


def turn_into(target, source):
    for j in range(source.shape[1] // LANES):
        target[j * LANES : (j + 1) * LANES, :] = source[:, j * LANES : (j + 1) * LANES].T


def unit_rows(block):
    centred = block - jnp.mean(block, axis=-1, keepdims=True)
    spread = lax.rsqrt(jnp.mean(centred * centred, axis=-1, keepdims=True) + norm_epsilon)
    return centred * spread, spread


def into_norm(grad, scaled, unit, spread):
    inner = grad * scaled
    level = jnp.mean(inner, axis=-1, keepdims=True)
    slope = jnp.mean(inner * unit, axis=-1, keepdims=True)
    return spread * (inner - level - unit * slope)


def times(left, right):
    return jnp.dot(left, right, preferred_element_type=WIDE)


def times_turned(left, right):
    return lax.dot_general(left, right, (((1,), (1,)), ((), ())), preferred_element_type=WIDE)


def turned_times(left, right):
    return lax.dot_general(left, right, (((0,), (0,)), ((), ())), preferred_element_type=WIDE)


def params(size, cid=None):
    if cid is None:
        return pltpu.CompilerParams(vmem_limit_bytes=size << 20)
    return pltpu.CompilerParams(
        vmem_limit_bytes=size << 20, collective_id=cid, has_side_effects=True
    )


def cost(flops, size):
    return pl.CostEstimate(flops=flops, bytes_accessed=size, transcendentals=0)


def window(head):
    low, high = head * HEAD_WIDTH, (head + 1) * HEAD_WIDTH
    start = low // LANES * LANES
    stop = -(-high // LANES) * LANES
    return start, stop - start, low - start


def head_mask(head):
    start, wide, offset = window(head)
    lane = lax.broadcasted_iota(jnp.int32, (1, wide), 1)
    return ((lane >= offset) & (lane < offset + HEAD_WIDTH)).astype(WIDE).astype(LOW)


def add_window(total, head, block):
    start, wide, _ = window(head)
    for j in range(wide // LANES):
        tile = start // LANES + j
        lanes = slice(tile * LANES, (tile + 1) * LANES)
        piece = block[:, j * LANES : (j + 1) * LANES]
        if head == tile * LANES // HEAD_WIDTH:
            total[:, lanes] = piece
        else:
            total[:, lanes] = total[:, lanes] + piece


def same_place():
    row = lax.broadcasted_iota(jnp.int32, (KEYS, KEYS), 0)
    column = lax.broadcasted_iota(jnp.int32, (KEYS, KEYS), 1)
    return (row & 15) == (column & 15)


def moves(source, target, sems, local_sem, me, to_places):
    part = source.shape[-2] // 8 if to_places else source.shape[-2]

    def ends(device):
        if to_places:
            return source.at[:, pl.ds(pl.multiple_of(device * part, part), part)], target.at[me]
        return source.at[device], target.at[:, pl.ds(pl.multiple_of(me * part, part), part)]

    copies = [pltpu.make_async_copy(*ends(me), local_sem)]
    for mask in (6, 7, 2, 3, 4, 5, 1):
        copies.append(
            pltpu.make_async_remote_copy(
                *ends(me ^ mask), sems.at[0, mask], sems.at[1, mask], device_id={"seq": me ^ mask}
            )
        )
    return copies


def move_scratch():
    return [pltpu.SemaphoreType.DMA((2, 8)), pltpu.SemaphoreType.DMA(())]


def gelu_and_slope(value):
    inner = 0.7978845608028654 * (value + 0.044715 * value * value * value)
    bent = jnp.tanh(inner)
    half = 0.5 * (1.0 + bent)
    slope = half + 0.5 * value * (1.0 - bent * bent) * (
        0.7978845608028654 * (1.0 + 3 * 0.044715 * value * value)
    )
    return value * half, slope


OUTS = ("qkv", "prob", "h", "o", "h2", "z", "slope", "x1", "branch", "mlp")
CHUNK = 768


def forward_kernel(shapes, *refs):
    count = len(shapes)
    shards, refs = refs[:count], refs[count:]
    partial, condition, tokens, x_ref = refs[:4]
    fulls, refs = refs[4 : 4 + count], refs[4 + count :]
    mod_ref, conditions, moved, other_ref, x2_ref, y_ref = refs[:6]
    outs = [dict(zip(OUTS, refs[6:16])), dict(zip(OUTS, refs[16:26]))]
    refs = refs[26:]
    (
        partials, x2, qkv, other, held, normed, total, middle, part, prob, turned, low, ready,
        tall, short, hidden, slope, small_sem, move_sem, stay_sem, next_move_sem, next_stay_sem, next_sem,
        pair_sem, weight_sem, out_sem, prob_sem, chunk_sem,
    ) = refs[:28]
    gather = Gather(shapes, (shards, fulls, refs[28:]))
    me, z = gather.me, gather.z
    features = x_ref.shape[1]
    steps = shapes[2][1] // CHUNK
    enter(range(1, 8), range(1, 4))

    small = []
    for mask in range(1, 8):
        small.append(pltpu.make_async_remote_copy(
            partial, partials.at[me], small_sem.at[0, mask], small_sem.at[1, mask],
            device_id={"seq": me ^ mask}))
    for mask in range(1, 4):
        small.append(pltpu.make_async_remote_copy(
            condition, conditions.at[z], small_sem.at[0, 7 + mask], small_sem.at[1, 7 + mask],
            device_id={"rep": z ^ mask}))
    small.append(pltpu.make_async_copy(partial, partials.at[me], small_sem.at[0, 0]))
    small.append(pltpu.make_async_copy(condition, conditions.at[z], small_sem.at[1, 0]))
    for copy in small:
        copy.start()
    gather.start()
    for copy in small:
        copy.wait()
    modulation = partials[0]
    for device in range(1, 8):
        modulation = modulation + partials[device]
    width = features // LANES
    for row in range(12):
        for j in range(width):
            at = row * width + j
            mod_ref[row // 6, row % 6 : row % 6 + 1, j * LANES : (j + 1) * LANES] = modulation[
                at : at + 1
            ]

    pending = {}
    names = ("turned", "qkv", "other", "low", "middle", "ready")

    def begin(name, source, target):
        settle(name)
        pending[name] = pltpu.make_async_copy(source, target, out_sem.at[names.index(name)])
        pending[name].start()

    def settle(name):
        copy = pending.pop(name, None)
        if copy is not None:
            copy.wait()

    def full(weight):
        return fulls[weight]

    def load(slot, source):
        return pltpu.make_async_copy(source, tall.at[slot], weight_sem.at[slot])

    def column_block(weight, column):
        return full(weight).at[:, :, pl.ds(column, features)]

    def exchange(j):
        return pltpu.make_async_remote_copy(
            qkv.at[pl.ds(2 * j, 2), :, pl.ds(features, 2 * features)], other.at[pl.ds(2 * j, 2)],
            pair_sem.at[0, j], pair_sem.at[1, j], device_id={"seq": me ^ 1},
        )

    def rows_of(ref, group, column, wide, spatial):
        lanes = slice(column, column + wide)
        if spatial:
            return ref[pl.ds(2 * group, 2), :, lanes].reshape(-1, wide)
        return jnp.concatenate([ref[2 * block + group, :, lanes] for block in range(4)], 0)

    def attend(layer, spatial, group, span, allowed):
        for head in range(HEADS):
            start, wide, _ = window(head)
            mask = head_mask(head)
            queries = rows_of(qkv, group, start, wide, spatial) * mask
            keys = rows_of(qkv, group, features + start, wide, spatial)
            values = rows_of(qkv, group, 2 * features + start, wide, spatial)
            if spatial:
                keys = jnp.concatenate([keys, rows_of(other, group, start, wide, True)], 0)
                values = jnp.concatenate(
                    [values, rows_of(other, group, features + start, wide, True)], 0
                )
            scores = times_turned(queries, keys)
            if not spatial:
                scores = jnp.where(allowed, scores, -3e38)
            grown = jnp.exp2(
                (scores - jnp.max(scores, axis=-1, keepdims=True)) * (HEAD_WIDTH ** (-0.5) * 1.4426950408889634)
            )
            chance = (grown * (1.0 / jnp.sum(grown, axis=-1, keepdims=True))).astype(LOW)
            prob[head, :span] = chance
            add_window(part.at[pl.ds(0, span)], head, times(chance, values * mask))
        got = part[:span].astype(LOW)
        if spatial:
            held[pl.ds(2 * group, 2)] = got.reshape(2, -1, features)
        else:
            for block in range(4):
                held[2 * block + group] = got[block * 64 : (block + 1) * 64]

    def flat_rows(ref):
        return ref[...].reshape(-1, features)

    def turn_out(source, target):
        settle("turned")
        for j in range(features // LANES):
            lanes = slice(j * LANES, (j + 1) * LANES)
            turned[lanes, :] = source[:, lanes].T
        begin("turned", turned, target)

    def layer(at_layer, spatial, x, plan):
        first = 4 * at_layer
        out = outs[at_layer]
        groups = 4 if spatial else 2
        span = x.shape[0] // groups
        mod = mod_ref.at[at_layer]

        def go(place):
            for at in plan.get(place, ()):
                if at is None:
                    gather.share(len(gather.pieces) - 1)
                elif isinstance(at, list):
                    for copy in at:
                        copy.start()
                else:
                    gather.advance(at)

        def go_when(place, index):
            for key, pieces in plan.items():
                if isinstance(key, tuple) and key[0] == place:
                    @pl.when(index == key[1])
                    def _():
                        for at in pieces:
                            gather.advance(at)

        scaled, shift = 1.0 + mod[1:2], mod[0:1]

        def norm(at):
            unit, _ = unit_rows(x[at].astype(WIDE))
            normed[at] = (unit * scaled + shift).astype(LOW)

        strips(x.shape[0], norm)
        turn_out(normed[...], out["h"])
        go("norm")
        gather.ready(first)
        load(0, column_block(first, 0)).start()
        settle("qkv")
        for j in range(3):
            load(j % 2, column_block(first, 0)).wait()
            if j < 2:
                load((j + 1) % 2, column_block(first, (j + 1) * features)).start()
            got = times(normed[...], tall[j % 2].reshape(features, features)).astype(LOW)
            qkv[:, :, j * features : (j + 1) * features] = got.reshape(8, -1, features)
            go(f"qkv{j}")
        begin("qkv", qkv, out["qkv"])
        if spatial:
            for j in range(groups):
                exchange(j).start()
        allowed = None if spatial else same_place()

        def prob_copy(group):
            return pltpu.make_async_copy(
                prob.at[:, pl.ds(0, span)], out["prob"].at[group], prob_sem
            )

        def one_group(group, carry):
            go_when("group", group)
            if spatial:
                exchange(group).wait_recv()

            @pl.when(group > 0)
            def _():
                prob_copy(group).wait()

            attend(at_layer, spatial, group, span, allowed)
            prob_copy(group).start()
            return carry

        lax.fori_loop(0, groups, one_group, 0)
        prob_copy(0).wait()
        if spatial:
            begin("other", other, other_ref)
            for j in range(groups):
                exchange(j).wait_send()
        go("attended")
        gather.ready(first + 1)
        load(0, full(first + 1)).start()
        attended = flat_rows(held)
        turn_out(attended, out["o"])
        load(0, full(first + 1)).wait()
        total[...] = times(attended, tall[0].reshape(features, features))
        gate, move, grow = mod[2:3], mod[3:4], 1.0 + mod[4:5]
        settle("low")
        settle("middle")

        def finish(at):
            branch = total[at]
            low[at] = branch.astype(LOW)
            got = x[at].astype(WIDE) + gate * branch
            middle[at] = got
            unit, _ = unit_rows(got)
            normed[at] = (unit * grow + move).astype(LOW)

        strips(x.shape[0], finish)
        begin("low", low, out["branch"])
        begin("middle", middle, out["x1"])
        turn_out(normed[...], out["h2"])
        go("middle")
        gather.ready(first + 2)
        gather.ready(first + 3)

        down = full(first + 3)
        per = down.shape[0] * down.shape[1] // steps

        def chunk_loads(step, slot):
            column = pl.multiple_of(step * CHUNK, CHUNK)
            owner = step * CHUNK // down.shape[1]
            copies = [
                pltpu.make_async_copy(
                    full(first + 2).at[:, :, pl.ds(column, CHUNK)],
                    tall.at[slot, :, :, pl.ds(0, CHUNK)], weight_sem.at[slot],
                )
            ]
            return copies, column, owner

        def start_loads(step, slot):
            copies, column, owner = chunk_loads(step, slot)
            for copy in copies:
                copy.start()
            pltpu.make_async_copy(
                down_rows(step), short.at[slot], weight_sem.at[2 + slot]
            ).start()

        def down_rows(step):
            return fulls_flat[at_layer].at[pl.ds(pl.multiple_of(step * 4, 4), 4)]

        fulls_flat = [fulls[3].reshape(*split_rows(fulls[3].shape)), fulls[7].reshape(*split_rows(fulls[7].shape))]

        def wait_loads(slot):
            for copy in chunk_loads(0, slot)[0]:
                copy.wait()
            pltpu.make_async_copy(down_rows(0), short.at[slot], weight_sem.at[2 + slot]).wait()

        def chunk_outs(step, slot):
            column = pl.multiple_of(step * CHUNK, CHUNK)
            return (
                pltpu.make_async_copy(
                    hidden.at[slot], out["z"].at[pl.ds(column, CHUNK)], chunk_sem.at[0, slot]
                ),
                pltpu.make_async_copy(
                    slope.at[slot], out["slope"].at[:, pl.ds(column, CHUNK)], chunk_sem.at[1, slot]
                ),
            )

        start_loads(0, 0)
        half = x.shape[0] // 2
        strips(x.shape[0], lambda at: clear(total, at))

        def chunk(step, carry):
            slot = lax.rem(step, 2)
            go_when("chunk", step)
            wait_loads(slot)

            @pl.when(step + 1 < steps)
            def _():
                start_loads(step + 1, 1 - slot)

            @pl.when(step >= 2)
            def _():
                for copy in chunk_outs(step, slot):
                    copy.wait()

            up = tall[slot, :, :, :CHUNK].reshape(features, CHUNK)
            for j in range(2):
                rows = slice(j * half, (j + 1) * half)
                value, bend = gelu_and_slope(times(normed[rows], up))
                slope[slot, rows] = bend.astype(LOW)
                value = value.astype(LOW)
                hidden[slot, :, rows] = value.T
                total[rows] += times(value, short[slot].reshape(CHUNK, features))

            for copy in chunk_outs(step, slot):
                copy.start()
            return carry

        lax.fori_loop(0, steps, chunk, 0)
        for slot in range(2):
            for copy in chunk_outs(0, slot):
                copy.wait()
        last = mod[5:6]
        settle("low")

        def close(at):
            mlp = total[at]
            low[at] = mlp.astype(LOW)
            total[at] = middle[at] + last * mlp

        strips(x.shape[0], close)
        begin("low", low, out["mlp"])
        ready[...] = total[...].astype(LOW).reshape(ready.shape)

    layer(0, True, x_ref, {
        "norm": (0, 1, 2, 3), "qkv1": (4,), ("group", 0): (5,), ("group", 1): (6,), ("group", 2): (7,),
        ("group", 3): (8,), "attended": (9,), "middle": (10, 11, 12), ("chunk", 1): (13,),
        ("chunk", 3): (14,), ("chunk", 4): (15,),
    })
    copies = moves(ready, x2_ref, next_move_sem, next_stay_sem, me, True)
    for copy in copies:
        copy.start()
    gather.local(4)
    gather.advance(16)
    gather.advance(17)
    for copy in copies:
        copy.wait()
    fetch = pltpu.make_async_copy(x2_ref, x2, next_sem)
    fetch.start()
    fetch.wait()
    x2_rows = x2.reshape(x_ref.shape)
    later = moves(tokens, moved, move_sem, stay_sem, me, True)
    layer(1, False, x2_rows, {
        "norm": (18,), "qkv0": (19,), "qkv2": (20,), ("group", 1): (21,), "attended": (22,),
        "middle": (23, None, later),
    })
    begin("ready", ready, y_ref)
    for name in names:
        settle(name)
    for copy in later:
        copy.wait()
    gather.finish()


def split_rows(shape):
    return (shape[0] * shape[1] // (CHUNK // 4), CHUNK // 4, shape[2])


def forward(shards, partial, condition, cotangent, x, cid):
    shapes = [shard.shape for shard in shards]
    count = len(shapes)
    tokens, features = x.shape
    frames, places, _ = cotangent.shape
    wide = shapes[2][1]
    any_ = pl.BlockSpec(memory_space=pl.ANY)
    struct = jax.ShapeDtypeStruct
    moved = struct((8, frames, places // 8, features), LOW)
    outs = Gather.outs(shapes) + [
        struct((2, 6, features), WIDE),
        struct((4,) + condition.shape, condition.dtype),
        moved,
        struct((8, tokens // 8, 2 * features), LOW),
        moved,
        struct((frames, places, features), LOW),
    ]
    for groups in (4, 2):
        outs += [
            struct((8, tokens // 8, 3 * features), LOW),
            struct((groups, HEADS, tokens // groups, KEYS), LOW),
            struct((features, tokens), LOW),
            struct((features, tokens), LOW),
            struct((features, tokens), LOW),
            struct((wide, tokens), LOW),
            struct((tokens, wide), LOW),
            struct((tokens, features), WIDE),
            struct((tokens, features), LOW),
            struct((tokens, features), LOW),
        ]
    dma = pltpu.SemaphoreType.DMA
    vm = pltpu.VMEM
    flops = 2 * tokens * 8 * sum(shape[0] * shape[1] for shape in shapes)
    got = pl.pallas_call(
        functools.partial(forward_kernel, shapes),
        out_shape=outs,
        in_specs=[any_] * (count + 3) + [pl.BlockSpec(memory_space=vm)],
        out_specs=[any_] * count + [pl.BlockSpec(memory_space=vm)] + [any_] * (len(outs) - count - 1),
        scratch_shapes=[
            vm((8,) + partial.shape, WIDE),
            vm(moved.shape, LOW),
            vm((8, tokens // 8, 3 * features), LOW),
            vm((8, tokens // 8, 2 * features), LOW),
            vm((8, tokens // 8, features), LOW),
            vm((tokens, features), LOW),
            vm((tokens, features), WIDE),
            vm((tokens, features), WIDE),
            vm((KEYS, features), WIDE),
            vm((HEADS, KEYS, KEYS), LOW),
            vm((features, tokens), LOW),
            vm((tokens, features), LOW),
            vm((frames, places, features), LOW),
            vm((2, 8, features // 8, features), LOW),
            vm((2, 4, CHUNK // 4, features), LOW),
            vm((2, CHUNK, tokens), LOW),
            vm((2, tokens, CHUNK), LOW),
            dma((2, 11)),
            *move_scratch(),
            *move_scratch(),
            dma(()),
            dma((2, 4)),
            dma((4,)),
            dma((8,)),
            dma(()),
            dma((2, 2)),
        ]
        + Gather.scratch(shapes),
        compiler_params=params(60, cid),
        cost_estimate=cost(flops, 4 * flops // tokens),
        name="forward",
    )(*shards, partial, condition, cotangent, x)
    weights = got[:count]
    named = [dict(zip(OUTS, got[count + 6 + 10 * at : count + 16 + 10 * at])) for at in range(2)]
    return weights, got[count : count + 6], named


SLOTS = 3
BACK = 4


KEPT = ("h", "o", "h2", "z", "qkv", "prob", "slope", "x1", "branch", "mlp")
RIGHTS = ("qkv", "da", "du", "df")
ORDER = (3, 2, 1, 0)


def backward_kernel(dims, *refs):
    rows, width, edge, tokens, total, spans = dims
    weights, refs = (refs[:4], refs[4:8]), refs[8:]
    kept = [dict(zip(KEPT, refs[10 * at : 10 * at + 10])) for at in range(2)]
    g_in, other_in, y_in, x_ins, mod_ref = refs[20], refs[21], refs[22], refs[23:25], refs[25]
    refs = refs[26:]
    grads, refs = (refs[:4], refs[4:8]), refs[8:]
    rights = [dict(zip(RIGHTS, refs[4 * at : 4 * at + 4])) for at in range(2)]
    every_mod, moved, input_grad, g_out = refs[8:12]
    (
        left, right, away, pair_in, part, first_in_a, first_in_b, mid_a, mid_b, second_in_a, second_in_b,
        clip, rep_in, joined, inner_in, final, back_in, wide,
        tall, short, acc, middle, grad_in, low, aux, slope, du, qkv, other, take, prob, dout,
        total_q, total_k, total_v, ready, sums, mod_low, mod_in,
        load_sem, pair_sem, link_sem, rep_sem, back_sem, store_sem, mod_sem, tall_sem, short_sem, slope_sem,
        in_sem, prob_sem, out_sem, du_sem, swap_sem, move_sem, stay_sem, last_move_sem, last_stay_sem,
    ) = refs[12:]
    me, z = lax.axis_index("seq"), lax.axis_index("rep")
    core, x, y = me & 1, (me >> 1) & 1, (me >> 2) & 1
    inner = (z == 1) | (z == 2)
    outer = (z == 0) | (z == 3)
    features = width
    steps = weights[0][2].shape[2] // CHUNK
    root = HEAD_WIDTH ** (-0.5)


    def wait_out(source, target):
        copy = pltpu.make_async_copy(source, target, out_sem)
        copy.start()
        copy.wait()

    def flat_in(ref):
        return ref if len(ref.shape) == 2 else ref.reshape(tokens, features)

    def load_in(name, at):
        source, target = {
            "grad": (flat_in((g_out, g_in)[at]), grad_in),
            "mlp": (kept[at]["mlp"], aux),
            "branch": (kept[at]["branch"], aux),
            "x": (flat_in(x_ins[at]), aux),
            "x1": (kept[at]["x1"], middle),
            "qkv": (kept[at]["qkv"], qkv),
            "other": (other_in, other),
        }[name]
        order = ("grad", "mlp", "branch", "x", "x1", "qkv", "other")
        return pltpu.make_async_copy(source, target, in_sem.at[order.index(name)])

    def chunk_loads(at, step, slot):
        column = pl.multiple_of(step * CHUNK, CHUNK)
        down = weights[at][3].reshape(*split_rows(weights[at][3].shape))
        return (
            pltpu.make_async_copy(
                weights[at][2].at[:, :, pl.ds(column, CHUNK)],
                tall.at[slot, :, :, pl.ds(0, CHUNK)], tall_sem.at[slot],
            ),
            pltpu.make_async_copy(
                down.at[pl.ds(pl.multiple_of(step * 4, 4), 4)], short.at[slot], short_sem.at[slot]
            ),
            pltpu.make_async_copy(
                kept[at]["slope"].at[:, pl.ds(column, CHUNK)], slope.at[slot], slope_sem.at[slot]
            ),
        )

    def tall_load(source, slot):
        return pltpu.make_async_copy(source, tall.at[slot], tall_sem.at[slot])

    def qkv_block(at, j):
        return weights[at][0].at[:, :, pl.ds(j * features, features)]

    def mlp_begin(at):
        load_in("grad", at).start()
        load_in("mlp", at).start()
        load_in("x1", at).start()
        for slot in range(2):
            for copy in chunk_loads(at, slot, slot):
                copy.start()
        load_in("grad", at).wait()
        load_in("mlp", at).wait()
        gate = mod_ref[at, 5:6]
        sums[at] = jnp.zeros_like(sums[at])

        def begin(strip):
            grad = grad_in[strip].astype(WIDE)
            low[strip] = (gate * grad).astype(LOW)
            clear(acc, strip)
            sums[at, 5:6] += jnp.sum(grad * aux[strip].astype(WIDE), axis=0, keepdims=True)

        strips(tokens, begin)
        load_in("branch", at).start()
        wait_out(low, rights[at]["df"])

    def du_copy(at, step):
        column = pl.multiple_of(step * CHUNK, CHUNK)
        return pltpu.make_async_copy(du, rights[at]["du"].at[:, pl.ds(column, CHUNK)], du_sem)

    def mlp_chunk(at, step):
        slot = lax.rem(step, 2)

        @pl.when(step > 0)
        def _():
            du_copy(at, step).wait()

        for copy in chunk_loads(at, step, slot):
            copy.wait()
        half = tokens // 2
        up = tall[slot, :, :, :CHUNK].reshape(features, CHUNK)
        for j in range(2):
            strip = slice(j * half, (j + 1) * half)
            got = times_turned(low[strip], short[slot].reshape(CHUNK, features))
            got = (got * slope[slot, strip].astype(WIDE)).astype(LOW)
            du[strip] = got
            acc[strip] += times_turned(got, up)

        @pl.when(step + 2 < steps)
        def _():
            for copy in chunk_loads(at, step + 2, slot):
                copy.start()

        du_copy(at, step).start()

    def prob_load(at, group):
        span = tokens // kept[at]["prob"].shape[0]
        return pltpu.make_async_copy(
            kept[at]["prob"].at[group], prob.at[:, pl.ds(0, span)], prob_sem
        )

    def mlp_finish(at):
        tall_load(weights[at][1], 0).start()
        tall_load(qkv_block(at, 0), 1).start()
        load_in("qkv", at).start()
        prob_load(at, 0).start()
        if at == 0:
            load_in("other", at).start()
        du_copy(at, 0).wait()
        load_in("branch", at).wait()
        load_in("x1", at).wait()
        gate, scaled = mod_ref[at, 2:3], 1.0 + mod_ref[at, 4:5]

        def finish(strip):
            grad = acc[strip]
            unit, spread = unit_rows(middle[strip])
            got = grad_in[strip].astype(WIDE) + into_norm(grad, scaled, unit, spread)
            middle[strip] = got
            low[strip] = (gate * got).astype(LOW)
            sums[at, 2:3] += jnp.sum(got * aux[strip].astype(WIDE), axis=0, keepdims=True)
            sums[at, 3:4] += jnp.sum(grad, axis=0, keepdims=True)
            sums[at, 4:5] += jnp.sum(grad * unit, axis=0, keepdims=True)

        strips(tokens, finish)
        load_in("x", at).start()
        wait_out(low, rights[at]["da"])

    def project(at):
        tall_load(weights[at][1], 0).wait()
        half = tokens // 2
        for j in range(2):
            got = times_turned(
                low[j * half : (j + 1) * half], tall[0].reshape(features, features)
            ).astype(LOW)
            dout[4 * j : 4 * j + 4] = got.reshape(4, -1, features)
        tall_load(qkv_block(at, 1), 0).start()
        load_in("qkv", at).wait()
        if at == 0:
            load_in("other", at).wait()

    def rows_of(ref, group, column, lanes, spatial):
        lanes = slice(column, column + lanes)
        if spatial:
            block = ref[pl.ds(2 * group, 2), :, lanes]
            return block.reshape(-1, block.shape[2])
        return jnp.concatenate([ref[2 * block + group, :, lanes] for block in range(4)], 0)

    def swap_copy(j):
        return pltpu.make_async_remote_copy(
            other.at[pl.ds(2 * j, 2)], take.at[pl.ds(2 * j, 2)],
            swap_sem.at[0, j], swap_sem.at[1, j], device_id={"seq": me ^ 1},
        )

    def attend_group(at, group):
        spatial = at == 0
        groups = kept[at]["prob"].shape[0]
        span = tokens // groups
        prob_load(at, group).wait()
        for head in range(HEADS):
            start, lanes, _ = window(head)
            mask = head_mask(head)
            queries = rows_of(qkv, group, start, lanes, spatial) * mask
            keys = rows_of(qkv, group, features + start, lanes, spatial)
            values = rows_of(qkv, group, 2 * features + start, lanes, spatial)
            coming = rows_of(dout, group, start, lanes, spatial) * mask
            if spatial:
                keys = jnp.concatenate([keys, rows_of(other, group, start, lanes, True)], 0)
                values = jnp.concatenate(
                    [values, rows_of(other, group, features + start, lanes, True)], 0
                )
            chance = prob[head, :span]
            known = chance.astype(WIDE)
            dprob = times_turned(coming, values)
            level = jnp.sum(dprob * known, axis=-1, keepdims=True)
            dscores = (known * (dprob - level)).astype(LOW)
            add_window(total_q.at[pl.ds(0, span)], head, times(dscores, keys * mask))
            add_window(total_k, head, turned_times(dscores, queries))
            add_window(total_v, head, turned_times(chance, coming))

        @pl.when(group + 1 < groups)
        def _():
            prob_load(at, group + 1).start()

        pieces = (
            (total_q[:span] * root).astype(LOW),
            (total_k[:span] * root).astype(LOW),
            total_v[:span].astype(LOW),
        )
        for j, piece in enumerate(pieces):
            lanes = slice(j * features, (j + 1) * features)
            if spatial:
                qkv[pl.ds(2 * group, 2), :, lanes] = piece.reshape(2, -1, features)
            else:
                for block in range(4):
                    qkv[2 * block + group, :, lanes] = piece[block * 64 : (block + 1) * 64]
        if spatial:
            other[pl.ds(2 * group, 2), :, :features] = (
                (total_k[span:] * root).astype(LOW).reshape(2, -1, features)
            )
            other[pl.ds(2 * group, 2), :, features:] = (
                total_v[span:].astype(LOW).reshape(2, -1, features)
            )
            swap_copy(group).start()

    def attend_finish(at):
        if at == 0:
            for j in range(4):
                swap_copy(j).wait()
                pair = slice(2 * j, 2 * j + 2)
                lanes = slice(features, 3 * features)
                qkv[pair, :, lanes] = qkv[pair, :, lanes] + take[pair]
        wait_out(qkv, rights[at]["qkv"].reshape(*qkv.shape))

    def qkv_chunks(at):
        for j in range(3):
            slot = 1 - j % 2
            tall_load(qkv_block(at, j), slot).wait()
            got = times_turned(
                qkv[:, :, j * features : (j + 1) * features].reshape(tokens, features),
                tall[slot].reshape(features, features),
            )
            if j == 0:
                acc[...] = got
                tall_load(qkv_block(at, 2), slot).start()
            else:
                acc[...] = acc[...] + got

    def last_moves():
        return moves(y_in, moved, last_move_sem, last_stay_sem, me, False)

    def grad_moves():
        return moves(ready, g_out, move_sem, stay_sem, me, False)

    def qkv_finish(at):
        load_in("x", at).wait()
        scaled = 1.0 + mod_ref[at, 1:2]

        def finish(strip):
            grad = acc[strip]
            unit, spread = unit_rows(aux[strip].astype(WIDE))
            sums[at, 0:1] += jnp.sum(grad, axis=0, keepdims=True)
            sums[at, 1:2] += jnp.sum(grad * unit, axis=0, keepdims=True)
            acc[strip] = middle[strip] + into_norm(grad, scaled, unit, spread)

        strips(tokens, finish)
        if at == 0:
            wait_out(acc, input_grad)
        else:
            ready[...] = acc[...].astype(LOW).reshape(ready.shape)
            for copy in grad_moves():
                copy.start()

    def backward_step(t):
        def at_turn(turn):
            return pl.when(t == turn)

        @pl.when(t < steps - 1)
        def _():
            mlp_chunk(1, t + 1)

        @at_turn(4)
        def _():
            mlp_finish(1)
            project(1)

        @pl.when((t >= 5) & (t < 7))
        def _():
            attend_group(1, t - 5)

        @at_turn(6)
        def _():
            attend_finish(1)

        @at_turn(7)
        def _():
            qkv_chunks(1)

        @at_turn(8)
        def _():
            qkv_finish(1)

        @at_turn(10)
        def _():
            for copy in grad_moves():
                copy.wait()
            mlp_begin(0)

        @pl.when((t >= 10) & (t < 10 + steps))
        def _():
            mlp_chunk(0, t - 10)

        @at_turn(15)
        def _():
            mlp_finish(0)
            project(0)

        @pl.when((t >= 16) & (t < 20))
        def _():
            attend_group(0, t - 16)

        @at_turn(19)
        def _():
            attend_finish(0)

        @at_turn(20)
        def _():
            qkv_chunks(0)

        @at_turn(21)
        def _():
            qkv_finish(0)
            mod_low[...] = jnp.zeros_like(mod_low)
            for at in range(2):
                mod_low[8 * at : 8 * at + 8] = sums[at].astype(LOW)
            mod_in[me] = mod_low[...]
            for copy in mod_copies():
                copy.start()

        @at_turn(23)
        def _():
            for copy in mod_copies():
                copy.wait()
            summed = mod_in[0].astype(WIDE)
            for device in range(1, 8):
                summed += mod_in[device].astype(WIDE)
            every_mod[z] = summed.astype(LOW)
            for copy in clip_copies():
                copy.start()

        @at_turn(25)
        def _():
            for copy in last_moves():
                copy.start()

        @at_turn(total + 5)
        def _():
            for copy in clip_copies():
                copy.wait()
            for copy in last_moves():
                copy.wait()

    def mod_copies():
        return [
            pltpu.make_async_remote_copy(
                mod_low, mod_in.at[me], mod_sem.at[0, mask], mod_sem.at[1, mask],
                device_id={"seq": me ^ mask},
            )
            for mask in range(1, 8)
        ]

    def clip_copies():
        return [
            pltpu.make_async_remote_copy(
                every_mod.at[z], every_mod.at[z], mod_sem.at[0, 7 + mask], mod_sem.at[1, 7 + mask],
                device_id={"rep": z ^ mask},
            )
            for mask in range(1, 4)
        ]


    names = ("h", "o", "h2", "z")

    def loads(block, slot):
        for layer, kind, first, count in spans:
            @pl.when((block >= first) & (block < first + count))
            def _():
                source = kept[layer][names[kind]]
                if kind == 3:
                    source = source.at[:, :, block - first]
                pltpu.make_async_copy(source, left.at[slot], load_sem.at[0, slot]).start()
                source = rights[layer][RIGHTS[kind]]
                if kind in (0, 2):
                    column = pl.multiple_of((block - first) * width, width)
                    source = source.at[:, pl.ds(column, width)]
                pltpu.make_async_copy(source, right.at[slot], load_sem.at[1, slot]).start()

    def wait_loads(slot):
        pltpu.make_async_copy(kept[0]["h"], left.at[slot], load_sem.at[0, slot]).wait()
        pltpu.make_async_copy(rights[0]["da"], right.at[slot], load_sem.at[1, slot]).wait()

    def store(block):
        for layer, kind, first, count in spans:
            @pl.when((block >= first) & (block < first + count))
            def _():
                target = grads[layer][kind]
                if kind == 3:
                    row = pl.multiple_of((block - first) * rows, rows)
                    target = target.at[pl.ds(row, rows)]
                elif kind in (0, 2):
                    column = pl.multiple_of((block - first) * width, width)
                    target = target.at[:, pl.ds(column, width)]
                pltpu.make_async_copy(wide, target, store_sem).start()

    def to_seq(source, target, which, slot, mask):
        return pltpu.make_async_remote_copy(
            source, target, link_sem.at[0, which, slot], link_sem.at[1, which, slot],
            device_id={"seq": me ^ mask},
        )

    def pair_copy(t):
        slot = lax.rem(t, 2)
        return pltpu.make_async_remote_copy(
            away, pair_in.at[slot], pair_sem.at[0, slot], pair_sem.at[1, slot],
            device_id={"seq": me ^ 1},
        )

    def first_copies(t):
        slot, block = lax.rem(t, BACK), lax.rem(t - 1, SLOTS)
        return (
            to_seq(part.at[block, :, 1 - x, :, pl.ds(0, edge)], first_in_a.at[slot], 0, slot, 2),
            to_seq(
                part.at[block, 1 - y, :, :, pl.ds(edge, width - edge)],
                first_in_b.at[slot], 1, slot, 4,
            ),
        )

    def second_copies(t):
        slot, block = lax.rem(t, SLOTS), lax.rem(t, 2)
        return (
            to_seq(mid_a.at[block, 1 - y], second_in_a.at[slot], 2, slot, 4),
            to_seq(mid_b.at[block, 1 - x], second_in_b.at[slot], 3, slot, 2),
        )

    def rep_copy(t):
        slot = lax.rem(t, SLOTS)
        return pltpu.make_async_remote_copy(
            clip.at[lax.rem(t, 2)], rep_in.at[slot], rep_sem.at[0, 0, slot], rep_sem.at[1, 0, slot],
            device_id={"rep": z ^ 1},
        )

    def inner_copy(t):
        slot = lax.rem(t, SLOTS)
        return pltpu.make_async_remote_copy(
            joined.at[lax.rem(t, 2)], inner_in.at[slot],
            rep_sem.at[0, 1, slot], rep_sem.at[1, 1, slot],
            device_id={"rep": z ^ 3},
        )

    def back_copy(t):
        slot = lax.rem(t, BACK)
        return pltpu.make_async_remote_copy(
            final.at[lax.rem(t, 2)], back_in.at[slot], back_sem.at[0, slot], back_sem.at[1, slot],
            device_id={"rep": z ^ 1},
        )

    def turn(t, carry):
        def stage(back):
            return (t >= back) & (t < total + back)

        now2, was2 = lax.rem(t, 2), lax.rem(t + 1, 2)
        was3 = lax.rem(t + 2, SLOTS)
        was4 = lax.rem(t + 3, BACK)

        @pl.when(t + 1 < total)
        def _():
            loads(t + 1, was2)

        @pl.when(stage(2))
        def _():
            block = lax.rem(t + 1, SLOTS)
            for at in range(2):
                mid_a[now2, at] = part[block, at, x, :, :edge] + first_in_a[was4, at]
                mid_b[now2, at] = part[block, y, at, :, edge:] + first_in_b[was4, at]
            for copy in second_copies(t):
                copy.start()

        @pl.when(stage(3))
        def _():
            clip[now2, :, :edge] = mid_a[was2, y] + second_in_a[was3]
            clip[now2, :, edge:] = mid_b[was2, x] + second_in_b[was3]

            @pl.when(outer)
            def _():
                rep_copy(t).start()

        @pl.when(stage(4) & inner)
        def _():
            joined[now2] = clip[was2] + rep_in[was3]
            inner_copy(t).start()

        @pl.when(stage(5) & inner)
        def _():
            final[now2] = joined[was2] + inner_in[was3]
            back_copy(t).start()

        @pl.when(stage(6))
        def _():
            @pl.when(inner)
            def _():
                wide[...] = final[was2]

            @pl.when(outer)
            def _():
                wide[...] = back_in[lax.rem(t + 3, BACK)]

            store(t - 6)

        @pl.when(t < total)
        def _():
            wait_loads(now2)
            slot3 = lax.rem(t, SLOTS)
            parts = (slice(0, 512), slice(512, width))

            def product(which, at):
                block = left[now2, :, which]
                four, _, depth = block.shape
                got = times(block.reshape(four * rows, depth), right[now2, :, at]).astype(LOW)
                return got.reshape(four, rows, -1)

            for at in parts:
                away[:, :, at] = product(1 - core, at)
            pair_copy(t).start()
            for at in parts:
                got = product(core, at)
                part[slot3, 0, :, :, at] = got[:2]
                part[slot3, 1, :, :, at] = got[2:]

        backward_step(t)

        @pl.when(t < total)
        def _():
            pair_copy(t).wait()
            slot3 = lax.rem(t, SLOTS)

            def add(j, carry):
                part[slot3, j // 2, j % 2] = part[slot3, j // 2, j % 2] + pair_in[now2, j]
                return carry

            lax.fori_loop(0, 4, add, 0)
            for copy in first_copies(t + 1):
                copy.start()

        @pl.when(stage(1))
        def _():
            for copy in first_copies(t):
                copy.wait()

        @pl.when(stage(2))
        def _():
            for copy in second_copies(t):
                copy.wait()

        @pl.when(stage(3))
        def _():
            @pl.when(outer)
            def _():
                rep_copy(t).wait_send()

            @pl.when(inner)
            def _():
                rep_copy(t).wait_recv()

        @pl.when(stage(4) & inner)
        def _():
            inner_copy(t).wait()

        @pl.when(stage(5))
        def _():
            @pl.when(inner)
            def _():
                back_copy(t).wait_send()

            @pl.when(outer)
            def _():
                back_copy(t).wait_recv()

        @pl.when(stage(6))
        def _():
            pltpu.make_async_copy(wide, grads[0][1], store_sem).wait()

        return carry

    enter(range(1, 8), range(1, 4))
    mlp_begin(1)
    mlp_chunk(1, jnp.int32(0))
    loads(0, 0)
    lax.fori_loop(0, total + 6, turn, 0)


def backward(weights, kept, g, other, y, xs, mods, cid):
    struct = jax.ShapeDtypeStruct
    tokens, features = xs[0].shape
    rows = features // 8
    wide = weights[0][2].shape[2]
    edge = features * 5 // 9 // 128 * 128
    frames, places = g.shape[1], 8 * g.shape[2]
    out_shapes = [(rows, 3 * features), (rows, features), (rows, wide), (wide // 8, features)]
    spans, total = [], 0
    for layer in (1, 0):
        for kind in ORDER:
            count = out_shapes[kind][0] * out_shapes[kind][1] // (rows * features)
            spans.append((layer, kind, total, count))
            total += count
    dims = (rows, features, edge, tokens, total, spans)
    any_ = pl.BlockSpec(memory_space=pl.ANY)
    outs = [struct(shape, LOW) for shape in out_shapes] * 2
    outs += [
        struct((tokens, 3 * features), LOW), struct((tokens, features), LOW),
        struct((tokens, wide), LOW), struct((tokens, features), LOW),
    ] * 2
    outs += [
        struct((4, 16, features), LOW),
        struct((frames, places, features), LOW),
        struct((tokens, features), WIDE),
        struct((frames, places, features), LOW),
    ]
    vm, dma = pltpu.VMEM, pltpu.SemaphoreType.DMA
    rest = features - edge
    scratch = [
        vm((2, 4, 2, rows, tokens), LOW),
        vm((2, tokens, features), LOW),
        vm((4, rows, features), LOW),
        vm((2, 4, rows, features), LOW),
        vm((SLOTS, 2, 2, rows, features), LOW),
        vm((BACK, 2, rows, edge), LOW),
        vm((BACK, 2, rows, rest), LOW),
        vm((2, 2, rows, edge), LOW),
        vm((2, 2, rows, rest), LOW),
        vm((SLOTS, rows, edge), LOW),
        vm((SLOTS, rows, rest), LOW),
        vm((2, rows, features), LOW),
        vm((SLOTS, rows, features), LOW),
        vm((2, rows, features), LOW),
        vm((SLOTS, rows, features), LOW),
        vm((2, rows, features), LOW),
        vm((BACK, rows, features), LOW),
        vm((rows, features), LOW),
        vm((2, 8, rows, features), LOW),
        vm((2, 4, CHUNK // 4, features), LOW),
        vm((tokens, features), WIDE),
        vm((tokens, features), WIDE),
        vm((tokens, features), LOW),
        vm((tokens, features), LOW),
        vm((tokens, features), LOW),
        vm((2, tokens, CHUNK), LOW),
        vm((tokens, CHUNK), LOW),
        vm((8, tokens // 8, 3 * features), LOW),
        vm((8, tokens // 8, 2 * features), LOW),
        vm((8, tokens // 8, 2 * features), LOW),
        vm((HEADS, KEYS, KEYS), LOW),
        vm((8, tokens // 8, features), LOW),
        vm((KEYS, features), WIDE),
        vm((KEYS, features), WIDE),
        vm((KEYS, features), WIDE),
        vm((8, frames, places // 8, features), LOW),
        vm((2, 8, features), WIDE),
        vm((16, features), LOW),
        vm((8, 16, features), LOW),
        dma((2, 2)),
        dma((2, 2)),
        dma((2, 4, BACK)),
        dma((2, 2, SLOTS)),
        dma((2, BACK)),
        dma(()),
        dma((2, 11)),
        dma((2,)),
        dma((2,)),
        dma((2,)),
        dma((7,)),
        dma(()),
        dma(()),
        dma(()),
        dma((2, 4)),
        *move_scratch(),
        *move_scratch(),
    ]
    flops = 4 * tokens * 8 * sum(a * b for a, b in out_shapes) * 2
    got = pl.pallas_call(
        functools.partial(backward_kernel, dims),
        out_shape=outs,
        in_specs=[any_] * (8 + 20 + 5) + [pl.BlockSpec(memory_space=vm)],
        out_specs=[any_] * 16 + [pl.BlockSpec(memory_space=vm)] + [any_] * 3,
        scratch_shapes=scratch,
        compiler_params=params(63, cid),
        cost_estimate=cost(flops, flops // tokens),
        name="backward",
    )(
        *weights[0], *weights[1], *[each[name] for each in kept for name in KEPT],
        g, other, y, *xs, mods,
    )
    grads = [grad.astype(WIDE) for grad in got[:8]]
    return grads[:4], grads[4:], got[16], got[17], got[18]


def by_device(left, features):
    tall, tokens = left.shape[0] // features, left.shape[1]
    rows = features // 8
    return left.reshape((4, 2, rows, tokens) if tall == 1 else (4, 2, tall, rows, tokens))


def fused_device(frames_in, conditioning, shards, partial_mod, cotangent):
    _, _, frames, places, features = frames_in.shape
    tokens = frames * places
    low_cotangent = cotangent.reshape(frames, places, features).astype(LOW)
    x_one = frames_in.reshape(tokens, features)
    weights, (mods, conditions, g_two, other, x_two, y_two), kept = forward(
        shards, partial_mod.reshape(-1, LANES), conditioning.reshape(-1, LANES), low_cotangent,
        x_one, 0,
    )
    for each in kept:
        for name in ("h", "o", "h2", "z"):
            each[name] = by_device(each[name], features)
    grads_one, grads_two, every_mod, block_out, input_grad = backward(
        (weights[:4], weights[4:]), kept, g_two, other, y_two.reshape(g_two.shape),
        (x_one, x_two.reshape(tokens, features)), mods, 1,
    )
    every_mod = every_mod.reshape(-1, 2, 8, features)[:, :, :6].reshape(-1, 12 * features)
    return (
        block_out.astype(WIDE), input_grad, grads_one, grads_two, every_mod,
        conditions.reshape(-1, features),
    )


def outer_sum(left, right):
    total = 0.0
    for row in range(left.shape[0]):
        total = total + left[row, :, None].astype(jnp.float32) * right[row].astype(jnp.float32)
    return total


def per_device(
    frames_in,
    conditioning,
    mod_first,
    qkv_first,
    out_first,
    up_first,
    down_first,
    mod_second,
    qkv_second,
    out_second,
    up_second,
    down_second,
    cotangent,
):
    clip_count, _, frame_dev, half_places, features = frames_in.shape
    fused = lax.axis_size("seq") == 8 and lax.axis_size("rep") == 4 and clip_count == 1
    row_count = mod_first.shape[0]
    row_start = lax.axis_index("seq") * row_count
    mod_width = mod_first.shape[1]
    rows_of = lambda whole: lax.dynamic_slice_in_dim(whole, row_start, row_count, 1)
    silu_local = rows_of(jax.nn.silu(conditioning)).astype(jnp.bfloat16)
    partial_mod = jnp.concatenate(
        [
            jnp.dot(silu_local, mod_first, preferred_element_type=jnp.float32),
            jnp.dot(silu_local, mod_second, preferred_element_type=jnp.float32),
        ],
        1,
    )
    shards = (
        qkv_first, out_first, up_first, down_first,
        qkv_second, out_second, up_second, down_second,
    )
    if fused:
        block_out, stream_grad, grads_one, grads_two, every_mod, conditions = fused_device(
            frames_in, conditioning, shards, partial_mod, cotangent
        )
        every_silu = rows_of(jax.nn.silu(conditions)).astype(jnp.bfloat16)
        mod_total = lax.dynamic_slice_in_dim(every_mod, lax.axis_index("rep"), 1, 0)
    else:
        weights = [lax.all_gather(shard, "seq", axis=0, tiled=True) for shard in shards]
        modulation = lax.psum(partial_mod, "seq")
        every_silu = lax.all_gather(silu_local, "rep", axis=0, tiled=True)
        mod_one, mod_two = modulation[:, :mod_width], modulation[:, mod_width:]
        weights_one, weights_two = weights[:4], weights[4:]
        start_stream = frames_in.reshape(clip_count, frame_dev, half_places, features).astype(
            jnp.float32
        )
        spatial_out, state_one = forward_layer(start_stream, mod_one, weights_one, True)
        placed = to_places(spatial_out)
        temporal_out, state_two = forward_layer(placed, mod_two, weights_two, False)
        block_out = to_frames(temporal_out, frame_dev)
        cotangent_sites = to_places(
            cotangent.reshape(clip_count, frame_dev, half_places, features)
        )
        placed_grad, mod_grad_two, pairs_two = backward_layer(
            cotangent_sites, placed, mod_two, weights_two, state_two, False
        )
        spatial_grad = to_frames(placed_grad, frame_dev)
        stream_grad, mod_grad_one, pairs_one = backward_layer(
            spatial_grad, start_stream, mod_one, weights_one, state_one, True
        )
        mod_grads = jnp.concatenate([mod_grad_one, mod_grad_two], 1).astype(jnp.bfloat16)
        grads_two, grads_one = layer_grads(pairs_two), layer_grads(pairs_one)
        mod_total = lax.psum(mod_grads, "seq").astype(jnp.bfloat16)
        every_mod = lax.all_gather(mod_total, "rep", axis=0, tiled=True)
    low_one, low_two = mod_total[:, :mod_width], mod_total[:, mod_width:]
    mod_weight_one = outer_sum(every_silu, every_mod[:, :mod_width])
    mod_weight_two = outer_sum(every_silu, every_mod[:, mod_width:])
    silu_grad = jnp.einsum("ce,de->cd", low_one, mod_first, preferred_element_type=jnp.float32)
    silu_grad = silu_grad + jnp.einsum(
        "ce,de->cd", low_two, mod_second, preferred_element_type=jnp.float32
    )
    condition_grad = jax.vjp(jax.nn.silu, rows_of(conditioning))[1](silu_grad)[0]
    out_shape = (clip_count, 1, frame_dev, half_places, features)
    return (
        block_out.reshape(out_shape),
        stream_grad.reshape(out_shape),
        condition_grad,
        mod_weight_one,
        *grads_one,
        mod_weight_two,
        *grads_two,
    )


def solution(mesh):
    return jax.shard_map(
        per_device,
        mesh=mesh,
        in_specs=(
            P("rep", "seq", None, None, None),
            P("rep", None),
            P("seq", None),
            P("seq", None),
            P("seq", None),
            P("seq", None),
            P("seq", None),
            P("seq", None),
            P("seq", None),
            P("seq", None),
            P("seq", None),
            P("seq", None),
            P("rep", "seq", None, None, None),
        ),
        out_specs=(
            P("rep", "seq", None, None, None),
            P("rep", "seq", None, None, None),
            P("rep", "seq"),
            P("seq", None),
            P("seq", None),
            P("seq", None),
            P("seq", None),
            P("seq", None),
            P("seq", None),
            P("seq", None),
            P("seq", None),
            P("seq", None),
            P("seq", None),
        ),
        check_vma=False,
    )
```

```python
import functools
import math

import jax
import jax.numpy as jnp
from jax import lax
from jax.experimental import pallas as pl
from jax.experimental.pallas import tpu as pltpu
from jax.sharding import PartitionSpec as P

HEADS = 16
HEAD_WIDTH = 72


norm_epsilon = 1e-06


def from_partner(block, axis, apart):
    count = lax.axis_size(axis)
    route = []
    for low in range(count):
        high = low | 1 << apart
        if high != low and high < count:
            route += [(low, high), (high, low)]
    return lax.ppermute(block, axis, route)


def shortened(x):
    return jax.tree.map(lambda a: a.astype(jnp.bfloat16) if a.dtype == jnp.float32 else a, x)


def layer_mod(stream, shift_part, scale_part):
    row_mean = jnp.mean(stream, axis=-1, keepdims=True)
    centred = stream - row_mean
    row_var = jnp.mean(centred * centred, axis=-1, keepdims=True)
    return centred * lax.rsqrt(row_var + norm_epsilon) * (1.0 + scale_part) + shift_part


def gelu_tanh(pre_value):
    return jax.nn.gelu(pre_value, approximate=True)


def project(left_operand, right_operand):
    return jnp.einsum(
        "csld,de->csle", left_operand, right_operand, preferred_element_type=jnp.float32
    )


def project_back(incoming, right_operand):
    return jnp.einsum("csle,de->csld", incoming, right_operand, preferred_element_type=jnp.float32)


def mod_parts(modulation):
    return [segment[:, None, None, :] for segment in jnp.split(modulation, 6, axis=-1)]


def partner_values(stacked):
    return from_partner(stacked, "seq", 0)


def partner_grads(stacked):
    return from_partner(stacked.astype(jnp.bfloat16), "seq", 0).astype(stacked.dtype)


def to_places(stream):
    clip_count, frame_dev, half_places, features = stream.shape
    devices = lax.axis_size("seq")
    place_part = half_places // devices
    exchanged = lax.all_to_all(
        stream.reshape(1, clip_count, frame_dev, devices, place_part, features).astype(
            jnp.bfloat16
        ),
        "seq",
        split_axis=3,
        concat_axis=0,
        tiled=True,
    ).astype(jnp.float32)
    exchanged = exchanged.reshape(devices // 2, 2, clip_count, frame_dev, place_part, features)
    exchanged = jnp.transpose(exchanged, (2, 1, 4, 0, 3, 5))
    return exchanged.reshape(clip_count, 2 * place_part, devices // 2 * frame_dev, features)


def to_frames(stream, frame_dev):
    clip_count, place_count, frame_total, features = stream.shape
    devices = lax.axis_size("seq")
    place_part = place_count // 2
    arranged = stream.reshape(clip_count, 2, place_part, devices // 2, frame_dev, features)
    arranged = jnp.transpose(arranged, (3, 1, 0, 4, 2, 5)).reshape(
        devices, clip_count, frame_dev, 1, place_part, features
    )
    exchanged = lax.all_to_all(
        shortened(arranged), "seq", split_axis=0, concat_axis=3, tiled=True
    ).astype(arranged.dtype)
    return exchanged.reshape(clip_count, frame_dev, devices * place_part, features)


def forward_layer(stream, modulation, weights, spatial):
    qkv_w, out_w, up_w, down_w = weights
    shift_attn, scale_attn, gate_attn, shift_mlp, scale_mlp, gate_mlp = mod_parts(modulation)
    clip_count, seq_count, seq_len, features = stream.shape
    normed = layer_mod(stream, shift_attn, scale_attn).astype(jnp.bfloat16)
    projected = project(normed, qkv_w).astype(jnp.bfloat16)
    queries, keys_all, values_all = jnp.split(projected, 3, axis=-1)
    if spatial:
        remote = partner_values(jnp.stack([keys_all, values_all]))
        keys_all = jnp.concatenate([keys_all, remote[0]], axis=2)
        values_all = jnp.concatenate([values_all, remote[1]], axis=2)
    key_len = keys_all.shape[2]
    queries = queries.reshape(clip_count, seq_count, seq_len, HEADS, HEAD_WIDTH)
    keys_all = keys_all.reshape(clip_count, seq_count, key_len, HEADS, HEAD_WIDTH)
    values_all = values_all.reshape(clip_count, seq_count, key_len, HEADS, HEAD_WIDTH)
    scores = jnp.einsum(
        "cslhe,csmhe->cshlm", queries, keys_all, preferred_element_type=jnp.float32
    ) * HEAD_WIDTH ** (-0.5)
    peak_score = jnp.max(scores, axis=-1, keepdims=True)
    scaled_exp = jnp.exp(scores - peak_score)
    attention = scaled_exp / jnp.sum(scaled_exp, axis=-1, keepdims=True)
    attention_low = attention.astype(jnp.bfloat16)
    attended = jnp.einsum(
        "cshlm,csmhe->cslhe", attention_low, values_all, preferred_element_type=jnp.float32
    )
    attended = attended.astype(jnp.bfloat16).reshape(clip_count, seq_count, seq_len, features)
    branch = project(attended, out_w)
    middle = stream + gate_attn * branch
    normed_mid = layer_mod(middle, shift_mlp, scale_mlp).astype(jnp.bfloat16)
    hidden_pre = project(normed_mid, up_w)
    hidden = gelu_tanh(hidden_pre).astype(jnp.bfloat16)
    mlp_out = project(hidden, down_w)
    result = middle + gate_mlp * mlp_out
    kept_state = (
        normed,
        queries,
        keys_all,
        values_all,
        attention,
        attention_low,
        attended,
        branch,
        middle,
        normed_mid,
        hidden_pre,
        hidden,
        mlp_out,
    )
    return (result, kept_state)


def backward_layer(result_grad, stream, modulation, weights, kept_state, spatial):
    qkv_w, out_w, up_w, down_w = weights
    (
        normed,
        queries,
        keys_all,
        values_all,
        attention,
        attention_low,
        attended,
        branch,
        middle,
        normed_mid,
        hidden_pre,
        hidden,
        mlp_out,
    ) = kept_state
    shift_attn, scale_attn, gate_attn, shift_mlp, scale_mlp, gate_mlp = mod_parts(modulation)
    clip_count, seq_count, seq_len, features = stream.shape
    gate_mlp_grad = jnp.sum(result_grad * mlp_out, axis=(1, 2))
    mlp_grad = (gate_mlp * result_grad).astype(jnp.bfloat16)
    hidden_grad = project_back(mlp_grad, down_w)
    pre_grad = jax.vjp(gelu_tanh, hidden_pre)[1](hidden_grad)[0].astype(jnp.bfloat16)
    normed_mid_grad = project_back(pre_grad, up_w)
    middle_ln_grad, shift_mlp_grad, scale_mlp_grad = jax.vjp(
        layer_mod, middle, shift_mlp, scale_mlp
    )[1](normed_mid_grad)
    middle_grad = result_grad + middle_ln_grad
    gate_attn_grad = jnp.sum(middle_grad * branch, axis=(1, 2))
    branch_grad = (gate_attn * middle_grad).astype(jnp.bfloat16)
    attended_grad = project_back(branch_grad, out_w).astype(jnp.bfloat16)
    attended_grad = attended_grad.reshape(clip_count, seq_count, seq_len, HEADS, HEAD_WIDTH)
    attention_grad = jnp.einsum(
        "cslhe,csmhe->cshlm", attended_grad, values_all, preferred_element_type=jnp.float32
    )
    scores_grad = attention * (
        attention_grad - jnp.sum(attention_grad * attention, axis=-1, keepdims=True)
    )
    scores_grad = scores_grad.astype(jnp.bfloat16)
    inv_root = HEAD_WIDTH ** (-0.5)
    queries_grad = (
        jnp.einsum("cshlm,csmhe->cslhe", scores_grad, keys_all, preferred_element_type=jnp.float32)
        * inv_root
    )
    keys_grad = (
        jnp.einsum("cshlm,cslhe->csmhe", scores_grad, queries, preferred_element_type=jnp.float32)
        * inv_root
    )
    values_grad = jnp.einsum(
        "cshlm,cslhe->csmhe", attention_low, attended_grad, preferred_element_type=jnp.float32
    )
    if spatial:
        returned = partner_grads(
            jnp.stack([keys_grad[:, :, seq_len:], values_grad[:, :, seq_len:]])
        )
        keys_grad = keys_grad[:, :, :seq_len] + returned[0]
        values_grad = values_grad[:, :, :seq_len] + returned[1]
    qkv_grad = jnp.concatenate(
        [
            component.reshape(clip_count, seq_count, seq_len, features)
            for component in (queries_grad, keys_grad, values_grad)
        ],
        axis=-1,
    )
    qkv_grad = qkv_grad.astype(jnp.bfloat16)
    normed_grad = project_back(qkv_grad, qkv_w)
    stream_ln_grad, attention_shift_gradient, scale_attn_grad = jax.vjp(
        layer_mod, stream, shift_attn, scale_attn
    )[1](normed_grad)
    stream_grad = middle_grad + stream_ln_grad
    mod_grad = jnp.concatenate(
        [
            attention_shift_gradient.reshape(clip_count, features),
            scale_attn_grad.reshape(clip_count, features),
            gate_attn_grad,
            shift_mlp_grad.reshape(clip_count, features),
            scale_mlp_grad.reshape(clip_count, features),
            gate_mlp_grad,
        ],
        axis=-1,
    )
    grad_pairs = (
        (normed, qkv_grad),
        (attended, branch_grad),
        (normed_mid, pre_grad),
        (hidden, mlp_grad),
    )
    return (stream_grad, mod_grad, grad_pairs)


def bit_count(axis):
    return lax.axis_size(axis).bit_length() - 1


def swap(block, axis, bit):
    count = lax.axis_size(axis)
    return lax.ppermute(block, axis, [(at, at ^ (1 << bit)) for at in range(count)])


def bit_of(axis, bit):
    return (lax.axis_index(axis) >> bit) & 1


def pick(block, which, axis):
    return lax.dynamic_index_in_dim(block, which, axis, keepdims=False)


def spread_rows_out(left_turned, right_operand, flipped):
    bits = bit_count("seq")
    total_rows, tokens = left_turned.shape
    rows = total_rows >> bits
    halves = left_turned.reshape(1 << (bits - 1), 2, rows, tokens)
    core = bit_of("seq", 0)

    def product(which):
        left = pick(halves, which, 1).reshape(-1, tokens)
        return jnp.dot(left, right_operand, preferred_element_type=jnp.float32).astype(
            jnp.bfloat16
        )

    arrived = swap(product(1 - core), "seq", 0)
    held = product(core)
    left_bits = list(range(bits - 1, 0, -1))
    shape = [2] * (bits - 1) + [rows, right_operand.shape[1]]
    held = held.reshape(shape)
    arrived = arrived.reshape(shape)
    order = list(left_bits) if flipped else left_bits[::-1]
    for bit in order:
        at = left_bits.index(bit)
        mine = bit_of("seq", bit)
        away = pick(held, 1 - mine, at).astype(jnp.float32) + pick(arrived, 1 - mine, at)
        kept = pick(held, mine, at).astype(jnp.float32) + pick(arrived, mine, at)
        arrived = swap(away.astype(jnp.bfloat16), "seq", bit)
        held = kept.astype(jnp.bfloat16)
        left_bits.remove(bit)
    return held.astype(jnp.float32) + arrived


def rep_sum(block, axis):
    bits = bit_count("rep")
    held = block.astype(jnp.bfloat16)
    for bit in range(bits):
        mine = bit_of("rep", bit)
        low, high = jnp.split(held, 2, axis)
        away = jnp.where(mine == 0, high, low)
        kept = jnp.where(mine == 0, low, high)
        held = (kept.astype(jnp.float32) + swap(away, "rep", bit)).astype(jnp.bfloat16)
    for bit in reversed(range(bits)):
        mine = bit_of("rep", bit)
        other = swap(held, "rep", bit)
        low = jnp.where(mine == 0, held, other)
        high = jnp.where(mine == 0, other, held)
        held = jnp.concatenate([low, high], axis)
    return held.astype(jnp.float32)


def turned(operand):
    return operand.reshape(-1, operand.shape[-1]).T


def flat(operand):
    return operand.reshape(-1, operand.shape[-1])


def cut(width, parts, of):
    return width * parts // of // 128 * 128


def down_grad(pair):
    left, right = turned(pair[0]), flat(pair[1])
    edge = cut(right.shape[1], 5, 9)
    return jnp.concatenate(
        [
            rep_sum(spread_rows_out(left, right[:, :edge], False), 0),
            rep_sum(spread_rows_out(left, right[:, edge:], True), 0),
        ],
        1,
    )


def up_grad(pair):
    left, right = turned(pair[0]), flat(pair[1])
    edge = cut(right.shape[1], 4, 9)
    return jnp.concatenate(
        [
            rep_sum(spread_rows_out(left, right[:, :edge], False), 1),
            rep_sum(spread_rows_out(left, right[:, edge:], True), 1),
        ],
        1,
    )


def attention_grads(qkv_pair, out_pair):
    left, right = turned(qkv_pair[0]), flat(qkv_pair[1])
    width = right.shape[1]
    edge = cut(width, 16, 27)
    first = rep_sum(spread_rows_out(left, right[:, :edge], False), 1)
    second = spread_rows_out(left, right[:, edge:], True)
    third = spread_rows_out(turned(out_pair[0]), flat(out_pair[1]), True)
    joined = rep_sum(jnp.concatenate([second, third], 1), 1)
    return (
        jnp.concatenate([first, joined[:, : width - edge]], 1),
        joined[:, width - edge :],
    )


def layer_grads(grad_pairs):
    qkv_pair, out_pair, up_pair, down_pair = grad_pairs
    down = down_grad(down_pair)
    up = up_grad(up_pair)
    qkv, out = attention_grads(qkv_pair, out_pair)
    return (qkv, out, up, down)


AHEAD = 2


def gather_pieces(shapes):
    features = math.gcd(*(columns for _, columns in shapes), 8 * shapes[0][0])
    rows_of = features // 8
    return rows_of, features, [
        (at, row, column)
        for at, (rows, columns) in enumerate(shapes)
        for row in range(0, rows, rows_of)
        for column in range(0, columns, features)
    ]


class Gather:
    def __init__(self, shapes, refs):
        count = len(shapes)
        self.count = count
        self.least, self.wide, self.pieces = gather_pieces(shapes)
        self.shards, self.fulls = refs[0], refs[1]
        self.held = refs[2][: count // 2]
        self.first_sem, self.second_sem, self.rep_sem, self.pair_sem, self.local_sem = refs[2][
            count // 2 :
        ]
        self.me, self.z = lax.axis_index("seq"), lax.axis_index("rep")
        odd = self.z & 1
        self.first, self.second = 2 + 2 * odd, 4 - 2 * odd

    @staticmethod
    def scratch(shapes):
        size = len(gather_pieces(shapes)[2])
        dma = pltpu.SemaphoreType.DMA
        half = shapes[: len(shapes) // 2]
        return [pltpu.VMEM(shape, jnp.bfloat16) for shape in half] + [
            dma((2, size)), dma((2, size)), dma((2, size)), dma((4, 2, size)), dma((2, len(shapes))),
        ]

    @staticmethod
    def outs(shapes):
        return [jax.ShapeDtypeStruct((8,) + shape, jnp.bfloat16) for shape in shapes]

    def place(self, owner, at):
        weight, row, column = self.pieces[at]
        return self.fulls[weight].at[owner, pl.ds(row, self.least), pl.ds(column, self.wide)]

    def own(self, at):
        weight, row, column = self.pieces[at]
        return self.shards[weight].at[pl.ds(row, self.least), pl.ds(column, self.wide)]

    def to_seq(self, source, owner, at, sems, mask):
        return pltpu.make_async_remote_copy(
            source, self.place(owner, at), sems.at[0, at], sems.at[1, at],
            device_id={"seq": self.me ^ mask},
        )

    def first_copy(self, at):
        return self.to_seq(self.own(at), self.me, at, self.first_sem, self.first)

    def second_copy(self, at):
        owner = self.me ^ self.first
        return self.to_seq(self.place(owner, at), owner, at, self.second_sem, self.second)

    def rep_copy(self, at):
        owner = self.me ^ self.first
        return pltpu.make_async_remote_copy(
            self.place(owner, at), self.place(owner, at), self.rep_sem.at[0, at], self.rep_sem.at[1, at],
            device_id={"rep": self.z ^ 1},
        )

    def pair_copy(self, which, at):
        if which == 0:
            return self.to_seq(self.own(at), self.me, at, self.pair_sem.at[0], 1)
        owner = self.me ^ (self.first, self.first ^ self.second, self.second)[which - 1]
        return self.to_seq(self.place(owner, at), owner, at, self.pair_sem.at[which], 1)

    def begin(self, at):
        self.first_copy(at).start()
        self.pair_copy(0, at).start()

    def fetch(self, weight):
        return pltpu.make_async_copy(
            self.shards[weight], self.held[weight % len(self.held)], self.local_sem.at[0, weight]
        )

    def keep(self, weight):
        return pltpu.make_async_copy(
            self.held[weight % len(self.held)], self.fulls[weight].at[self.me], self.local_sem.at[1, weight]
        )

    def start(self):
        for at in range(AHEAD):
            self.begin(at)
        self.local(0)

    def local(self, first):
        for weight in range(first, first + len(self.held)):
            self.fetch(weight).start()
        for weight in range(first, first + len(self.held)):
            self.fetch(weight).wait()
            self.keep(weight).start()

    def ready(self, weight):
        for at, piece in enumerate(self.pieces):
            if piece[0] == weight:
                for which in range(4):
                    self.pair_copy(which, at).wait_recv()
        self.keep(weight).wait()

    def advance(self, at):
        self.first_copy(at).wait_recv()
        if at + AHEAD < len(self.pieces):
            self.begin(at + AHEAD)
        self.second_copy(at).start()
        self.rep_copy(at).start()
        self.pair_copy(1, at).start()
        if at:
            self.share(at - 1)

    def share(self, at):
        self.second_copy(at).wait_recv()
        self.rep_copy(at).wait_recv()
        self.pair_copy(2, at).start()
        self.pair_copy(3, at).start()

    def finish(self):
        for at in range(len(self.pieces)):
            for copy in (self.first_copy(at), self.second_copy(at), self.rep_copy(at)):
                copy.wait_send()
            for which in range(4):
                self.pair_copy(which, at).wait_send()


def enter(seq_masks, rep_masks):
    me, z = lax.axis_index("seq"), lax.axis_index("rep")
    barrier = pltpu.get_barrier_semaphore()
    for mask in seq_masks:
        pl.semaphore_signal(barrier, inc=1, device_id={"seq": me ^ mask})
    for mask in rep_masks:
        pl.semaphore_signal(barrier, inc=1, device_id={"rep": z ^ mask})
    pl.semaphore_wait(barrier, len(seq_masks) + len(rep_masks))


LOW = jnp.bfloat16
WIDE = jnp.float32
LANES = 128
STRIP = 64
KEYS = 256


def whole_block(shape):
    return pl.BlockSpec(shape, lambda *at: (0,) * len(shape))


def strips(total, body):
    def step(j, carry):
        body(pl.ds(pl.multiple_of(j * STRIP, STRIP), STRIP))
        return carry

    lax.fori_loop(0, total // STRIP, step, 0)


def clear(ref, at):
    ref[at] = jnp.zeros_like(ref[at])


def turn_into(target, source):
    for j in range(source.shape[1] // LANES):
        target[j * LANES : (j + 1) * LANES, :] = source[:, j * LANES : (j + 1) * LANES].T


def unit_rows(block):
    centred = block - jnp.mean(block, axis=-1, keepdims=True)
    spread = lax.rsqrt(jnp.mean(centred * centred, axis=-1, keepdims=True) + norm_epsilon)
    return centred * spread, spread


def into_norm(grad, scaled, unit, spread):
    inner = grad * scaled
    level = jnp.mean(inner, axis=-1, keepdims=True)
    slope = jnp.mean(inner * unit, axis=-1, keepdims=True)
    return spread * (inner - level - unit * slope)


def times(left, right):
    return jnp.dot(left, right, preferred_element_type=WIDE)


def times_turned(left, right):
    return lax.dot_general(left, right, (((1,), (1,)), ((), ())), preferred_element_type=WIDE)


def turned_times(left, right):
    return lax.dot_general(left, right, (((0,), (0,)), ((), ())), preferred_element_type=WIDE)


def params(size, cid=None):
    if cid is None:
        return pltpu.CompilerParams(vmem_limit_bytes=size << 20)
    return pltpu.CompilerParams(
        vmem_limit_bytes=size << 20, collective_id=cid, has_side_effects=True
    )


def cost(flops, size):
    return pl.CostEstimate(flops=flops, bytes_accessed=size, transcendentals=0)


def window(head):
    low, high = head * HEAD_WIDTH, (head + 1) * HEAD_WIDTH
    start = low // LANES * LANES
    stop = -(-high // LANES) * LANES
    return start, stop - start, low - start


def head_mask(head):
    start, wide, offset = window(head)
    lane = lax.broadcasted_iota(jnp.int32, (1, wide), 1)
    return ((lane >= offset) & (lane < offset + HEAD_WIDTH)).astype(WIDE).astype(LOW)


def add_window(total, head, block):
    start, wide, _ = window(head)
    for j in range(wide // LANES):
        tile = start // LANES + j
        lanes = slice(tile * LANES, (tile + 1) * LANES)
        piece = block[:, j * LANES : (j + 1) * LANES]
        if head == tile * LANES // HEAD_WIDTH:
            total[:, lanes] = piece
        else:
            total[:, lanes] = total[:, lanes] + piece


def same_place():
    row = lax.broadcasted_iota(jnp.int32, (KEYS, KEYS), 0)
    column = lax.broadcasted_iota(jnp.int32, (KEYS, KEYS), 1)
    return (row & 15) == (column & 15)


def moves(source, target, sems, local_sem, me, to_places):
    part = source.shape[-2] // 8 if to_places else source.shape[-2]

    def ends(device):
        if to_places:
            return source.at[:, pl.ds(pl.multiple_of(device * part, part), part)], target.at[me]
        return source.at[device], target.at[:, pl.ds(pl.multiple_of(me * part, part), part)]

    copies = [pltpu.make_async_copy(*ends(me), local_sem)]
    for mask in (6, 7, 2, 3, 4, 5, 1):
        copies.append(
            pltpu.make_async_remote_copy(
                *ends(me ^ mask), sems.at[0, mask], sems.at[1, mask], device_id={"seq": me ^ mask}
            )
        )
    return copies


def move_scratch():
    return [pltpu.SemaphoreType.DMA((2, 8)), pltpu.SemaphoreType.DMA(())]


def gelu_and_slope(value):
    inner = 0.7978845608028654 * (value + 0.044715 * value * value * value)
    bent = jnp.tanh(inner)
    half = 0.5 * (1.0 + bent)
    slope = half + 0.5 * value * (1.0 - bent * bent) * (
        0.7978845608028654 * (1.0 + 3 * 0.044715 * value * value)
    )
    return value * half, slope


OUTS = ("qkv", "prob", "h", "o", "h2", "z", "slope", "x1", "branch", "mlp")
CHUNK = 768


def forward_kernel(shapes, *refs):
    count = len(shapes)
    shards, refs = refs[:count], refs[count:]
    partial, condition, tokens, x_ref = refs[:4]
    fulls, refs = refs[4 : 4 + count], refs[4 + count :]
    mod_ref, conditions, moved, other_ref, x2_ref, y_ref = refs[:6]
    outs = [dict(zip(OUTS, refs[6:16])), dict(zip(OUTS, refs[16:26]))]
    refs = refs[26:]
    (
        partials, x2, qkv, other, held, normed, total, middle, part, prob, turned, low, ready,
        tall, short, hidden, slope, small_sem, move_sem, stay_sem, next_move_sem, next_stay_sem, next_sem,
        pair_sem, weight_sem, out_sem, prob_sem, chunk_sem,
    ) = refs[:28]
    gather = Gather(shapes, (shards, fulls, refs[28:]))
    me, z = gather.me, gather.z
    features = x_ref.shape[1]
    steps = shapes[2][1] // CHUNK
    enter(range(1, 8), range(1, 4))

    small = []
    for mask in range(1, 8):
        small.append(pltpu.make_async_remote_copy(
            partial, partials.at[me], small_sem.at[0, mask], small_sem.at[1, mask],
            device_id={"seq": me ^ mask}))
    for mask in range(1, 4):
        small.append(pltpu.make_async_remote_copy(
            condition, conditions.at[z], small_sem.at[0, 7 + mask], small_sem.at[1, 7 + mask],
            device_id={"rep": z ^ mask}))
    small.append(pltpu.make_async_copy(partial, partials.at[me], small_sem.at[0, 0]))
    small.append(pltpu.make_async_copy(condition, conditions.at[z], small_sem.at[1, 0]))
    for copy in small:
        copy.start()
    gather.start()
    for copy in small:
        copy.wait()
    modulation = partials[0]
    for device in range(1, 8):
        modulation = modulation + partials[device]
    width = features // LANES
    for row in range(12):
        for j in range(width):
            at = row * width + j
            mod_ref[row // 6, row % 6 : row % 6 + 1, j * LANES : (j + 1) * LANES] = modulation[
                at : at + 1
            ]

    pending = {}
    names = ("turned", "qkv", "other", "low", "middle", "ready")

    def begin(name, source, target):
        settle(name)
        pending[name] = pltpu.make_async_copy(source, target, out_sem.at[names.index(name)])
        pending[name].start()

    def settle(name):
        copy = pending.pop(name, None)
        if copy is not None:
            copy.wait()

    def full(weight):
        return fulls[weight]

    def load(slot, source):
        return pltpu.make_async_copy(source, tall.at[slot], weight_sem.at[slot])

    def column_block(weight, column):
        return full(weight).at[:, :, pl.ds(column, features)]

    def exchange(j):
        return pltpu.make_async_remote_copy(
            qkv.at[pl.ds(2 * j, 2), :, pl.ds(features, 2 * features)], other.at[pl.ds(2 * j, 2)],
            pair_sem.at[0, j], pair_sem.at[1, j], device_id={"seq": me ^ 1},
        )

    def rows_of(ref, group, column, wide, spatial):
        lanes = slice(column, column + wide)
        if spatial:
            return ref[pl.ds(2 * group, 2), :, lanes].reshape(-1, wide)
        return jnp.concatenate([ref[2 * block + group, :, lanes] for block in range(4)], 0)

    def attend(layer, spatial, group, span, allowed):
        for head in range(HEADS):
            start, wide, _ = window(head)
            mask = head_mask(head)
            queries = rows_of(qkv, group, start, wide, spatial) * mask
            keys = rows_of(qkv, group, features + start, wide, spatial)
            values = rows_of(qkv, group, 2 * features + start, wide, spatial)
            if spatial:
                keys = jnp.concatenate([keys, rows_of(other, group, start, wide, True)], 0)
                values = jnp.concatenate(
                    [values, rows_of(other, group, features + start, wide, True)], 0
                )
            scores = times_turned(queries, keys)
            if not spatial:
                scores = jnp.where(allowed, scores, -3e38)
            grown = jnp.exp2(
                (scores - jnp.max(scores, axis=-1, keepdims=True)) * (HEAD_WIDTH ** (-0.5) * 1.4426950408889634)
            )
            chance = (grown * (1.0 / jnp.sum(grown, axis=-1, keepdims=True))).astype(LOW)
            prob[head, :span] = chance
            add_window(part.at[pl.ds(0, span)], head, times(chance, values * mask))
        got = part[:span].astype(LOW)
        if spatial:
            held[pl.ds(2 * group, 2)] = got.reshape(2, -1, features)
        else:
            for block in range(4):
                held[2 * block + group] = got[block * 64 : (block + 1) * 64]

    def flat_rows(ref):
        return ref[...].reshape(-1, features)

    def turn_out(source, target):
        settle("turned")
        for j in range(features // LANES):
            lanes = slice(j * LANES, (j + 1) * LANES)
            turned[lanes, :] = source[:, lanes].T
        begin("turned", turned, target)

    def layer(at_layer, spatial, x, plan):
        first = 4 * at_layer
        out = outs[at_layer]
        groups = 4 if spatial else 2
        span = x.shape[0] // groups
        mod = mod_ref.at[at_layer]

        def go(place):
            for at in plan.get(place, ()):
                if at is None:
                    gather.share(len(gather.pieces) - 1)
                elif isinstance(at, list):
                    for copy in at:
                        copy.start()
                else:
                    gather.advance(at)

        def go_when(place, index):
            for key, pieces in plan.items():
                if isinstance(key, tuple) and key[0] == place:
                    @pl.when(index == key[1])
                    def _():
                        for at in pieces:
                            gather.advance(at)

        scaled, shift = 1.0 + mod[1:2], mod[0:1]

        def norm(at):
            unit, _ = unit_rows(x[at].astype(WIDE))
            normed[at] = (unit * scaled + shift).astype(LOW)

        strips(x.shape[0], norm)
        turn_out(normed[...], out["h"])
        go("norm")
        gather.ready(first)
        load(0, column_block(first, 0)).start()
        settle("qkv")
        for j in range(3):
            load(j % 2, column_block(first, 0)).wait()
            if j < 2:
                load((j + 1) % 2, column_block(first, (j + 1) * features)).start()
            got = times(normed[...], tall[j % 2].reshape(features, features)).astype(LOW)
            qkv[:, :, j * features : (j + 1) * features] = got.reshape(8, -1, features)
            go(f"qkv{j}")
        begin("qkv", qkv, out["qkv"])
        if spatial:
            for j in range(groups):
                exchange(j).start()
        allowed = None if spatial else same_place()

        def prob_copy(group):
            return pltpu.make_async_copy(
                prob.at[:, pl.ds(0, span)], out["prob"].at[group], prob_sem
            )

        def one_group(group, carry):
            go_when("group", group)
            if spatial:
                exchange(group).wait_recv()

            @pl.when(group > 0)
            def _():
                prob_copy(group).wait()

            attend(at_layer, spatial, group, span, allowed)
            prob_copy(group).start()
            return carry

        lax.fori_loop(0, groups, one_group, 0)
        prob_copy(0).wait()
        if spatial:
            begin("other", other, other_ref)
            for j in range(groups):
                exchange(j).wait_send()
        go("attended")
        gather.ready(first + 1)
        load(0, full(first + 1)).start()
        attended = flat_rows(held)
        turn_out(attended, out["o"])
        load(0, full(first + 1)).wait()
        total[...] = times(attended, tall[0].reshape(features, features))
        gate, move, grow = mod[2:3], mod[3:4], 1.0 + mod[4:5]
        settle("low")
        settle("middle")

        def finish(at):
            branch = total[at]
            low[at] = branch.astype(LOW)
            got = x[at].astype(WIDE) + gate * branch
            middle[at] = got
            unit, _ = unit_rows(got)
            normed[at] = (unit * grow + move).astype(LOW)

        strips(x.shape[0], finish)
        begin("low", low, out["branch"])
        begin("middle", middle, out["x1"])
        turn_out(normed[...], out["h2"])
        go("middle")
        gather.ready(first + 2)
        gather.ready(first + 3)

        down = full(first + 3)
        per = down.shape[0] * down.shape[1] // steps

        def chunk_loads(step, slot):
            column = pl.multiple_of(step * CHUNK, CHUNK)
            owner = step * CHUNK // down.shape[1]
            copies = [
                pltpu.make_async_copy(
                    full(first + 2).at[:, :, pl.ds(column, CHUNK)],
                    tall.at[slot, :, :, pl.ds(0, CHUNK)], weight_sem.at[slot],
                )
            ]
            return copies, column, owner

        def start_loads(step, slot):
            copies, column, owner = chunk_loads(step, slot)
            for copy in copies:
                copy.start()
            pltpu.make_async_copy(
                down_rows(step), short.at[slot], weight_sem.at[2 + slot]
            ).start()

        def down_rows(step):
            return fulls_flat[at_layer].at[pl.ds(pl.multiple_of(step * 4, 4), 4)]

        fulls_flat = [fulls[3].reshape(*split_rows(fulls[3].shape)), fulls[7].reshape(*split_rows(fulls[7].shape))]

        def wait_loads(slot):
            for copy in chunk_loads(0, slot)[0]:
                copy.wait()
            pltpu.make_async_copy(down_rows(0), short.at[slot], weight_sem.at[2 + slot]).wait()

        def chunk_outs(step, slot):
            column = pl.multiple_of(step * CHUNK, CHUNK)
            return (
                pltpu.make_async_copy(
                    hidden.at[slot], out["z"].at[pl.ds(column, CHUNK)], chunk_sem.at[0, slot]
                ),
                pltpu.make_async_copy(
                    slope.at[slot], out["slope"].at[:, pl.ds(column, CHUNK)], chunk_sem.at[1, slot]
                ),
            )

        start_loads(0, 0)
        half = x.shape[0] // 2
        strips(x.shape[0], lambda at: clear(total, at))

        def chunk(step, carry):
            slot = lax.rem(step, 2)
            go_when("chunk", step)
            wait_loads(slot)

            @pl.when(step + 1 < steps)
            def _():
                start_loads(step + 1, 1 - slot)

            @pl.when(step >= 2)
            def _():
                for copy in chunk_outs(step, slot):
                    copy.wait()

            up = tall[slot, :, :, :CHUNK].reshape(features, CHUNK)
            for j in range(2):
                rows = slice(j * half, (j + 1) * half)
                value, bend = gelu_and_slope(times(normed[rows], up))
                slope[slot, rows] = bend.astype(LOW)
                value = value.astype(LOW)
                hidden[slot, :, rows] = value.T
                total[rows] += times(value, short[slot].reshape(CHUNK, features))

            for copy in chunk_outs(step, slot):
                copy.start()
            return carry

        lax.fori_loop(0, steps, chunk, 0)
        for slot in range(2):
            for copy in chunk_outs(0, slot):
                copy.wait()
        last = mod[5:6]
        settle("low")

        def close(at):
            mlp = total[at]
            low[at] = mlp.astype(LOW)
            total[at] = middle[at] + last * mlp

        strips(x.shape[0], close)
        begin("low", low, out["mlp"])
        ready[...] = total[...].astype(LOW).reshape(ready.shape)

    layer(0, True, x_ref, {
        "norm": (0, 1, 2, 3), "qkv1": (4,), ("group", 0): (5,), ("group", 1): (6,), ("group", 2): (7,),
        ("group", 3): (8,), "attended": (9,), "middle": (10, 11, 12), ("chunk", 1): (13,),
        ("chunk", 3): (14,), ("chunk", 4): (15,),
    })
    copies = moves(ready, x2_ref, next_move_sem, next_stay_sem, me, True)
    for copy in copies:
        copy.start()
    gather.local(4)
    gather.advance(16)
    gather.advance(17)
    for copy in copies:
        copy.wait()
    fetch = pltpu.make_async_copy(x2_ref, x2, next_sem)
    fetch.start()
    fetch.wait()
    x2_rows = x2.reshape(x_ref.shape)
    later = moves(tokens, moved, move_sem, stay_sem, me, True)
    layer(1, False, x2_rows, {
        "norm": (18,), "qkv0": (19,), "qkv2": (20,), ("group", 1): (21,), "attended": (22,),
        "middle": (23, None, later),
    })
    begin("ready", ready, y_ref)
    for name in names:
        settle(name)
    for copy in later:
        copy.wait()
    gather.finish()


def split_rows(shape):
    return (shape[0] * shape[1] // (CHUNK // 4), CHUNK // 4, shape[2])


def forward(shards, partial, condition, cotangent, x, cid):
    shapes = [shard.shape for shard in shards]
    count = len(shapes)
    tokens, features = x.shape
    frames, places, _ = cotangent.shape
    wide = shapes[2][1]
    any_ = pl.BlockSpec(memory_space=pl.ANY)
    struct = jax.ShapeDtypeStruct
    moved = struct((8, frames, places // 8, features), LOW)
    outs = Gather.outs(shapes) + [
        struct((2, 6, features), WIDE),
        struct((4,) + condition.shape, condition.dtype),
        moved,
        struct((8, tokens // 8, 2 * features), LOW),
        moved,
        struct((frames, places, features), LOW),
    ]
    for groups in (4, 2):
        outs += [
            struct((8, tokens // 8, 3 * features), LOW),
            struct((groups, HEADS, tokens // groups, KEYS), LOW),
            struct((features, tokens), LOW),
            struct((features, tokens), LOW),
            struct((features, tokens), LOW),
            struct((wide, tokens), LOW),
            struct((tokens, wide), LOW),
            struct((tokens, features), WIDE),
            struct((tokens, features), LOW),
            struct((tokens, features), LOW),
        ]
    dma = pltpu.SemaphoreType.DMA
    vm = pltpu.VMEM
    flops = 2 * tokens * 8 * sum(shape[0] * shape[1] for shape in shapes)
    got = pl.pallas_call(
        functools.partial(forward_kernel, shapes),
        out_shape=outs,
        in_specs=[any_] * (count + 3) + [pl.BlockSpec(memory_space=vm)],
        out_specs=[any_] * count + [pl.BlockSpec(memory_space=vm)] + [any_] * (len(outs) - count - 1),
        scratch_shapes=[
            vm((8,) + partial.shape, WIDE),
            vm(moved.shape, LOW),
            vm((8, tokens // 8, 3 * features), LOW),
            vm((8, tokens // 8, 2 * features), LOW),
            vm((8, tokens // 8, features), LOW),
            vm((tokens, features), LOW),
            vm((tokens, features), WIDE),
            vm((tokens, features), WIDE),
            vm((KEYS, features), WIDE),
            vm((HEADS, KEYS, KEYS), LOW),
            vm((features, tokens), LOW),
            vm((tokens, features), LOW),
            vm((frames, places, features), LOW),
            vm((2, 8, features // 8, features), LOW),
            vm((2, 4, CHUNK // 4, features), LOW),
            vm((2, CHUNK, tokens), LOW),
            vm((2, tokens, CHUNK), LOW),
            dma((2, 11)),
            *move_scratch(),
            *move_scratch(),
            dma(()),
            dma((2, 4)),
            dma((4,)),
            dma((8,)),
            dma(()),
            dma((2, 2)),
        ]
        + Gather.scratch(shapes),
        compiler_params=params(60, cid),
        cost_estimate=cost(flops, 4 * flops // tokens),
        name="forward",
    )(*shards, partial, condition, cotangent, x)
    weights = got[:count]
    named = [dict(zip(OUTS, got[count + 6 + 10 * at : count + 16 + 10 * at])) for at in range(2)]
    return weights, got[count : count + 6], named


SLOTS = 3
BACK = 4


KEPT = ("h", "o", "h2", "z", "qkv", "prob", "slope", "x1", "branch", "mlp")
RIGHTS = ("qkv", "da", "du", "df")
ORDER = (3, 2, 1, 0)


def backward_kernel(dims, *refs):
    rows, width, edge, tokens, total, spans = dims
    weights, refs = (refs[:4], refs[4:8]), refs[8:]
    kept = [dict(zip(KEPT, refs[10 * at : 10 * at + 10])) for at in range(2)]
    g_in, other_in, y_in, x_ins, mod_ref = refs[20], refs[21], refs[22], refs[23:25], refs[25]
    refs = refs[26:]
    grads, refs = (refs[:4], refs[4:8]), refs[8:]
    rights = [dict(zip(RIGHTS, refs[4 * at : 4 * at + 4])) for at in range(2)]
    every_mod, moved, input_grad, g_out = refs[8:12]
    (
        left, right, away, pair_in, part, first_in_a, first_in_b, mid_a, mid_b, second_in_a, second_in_b,
        clip, rep_in, joined, inner_in, final, back_in, wide,
        tall, short, acc, middle, grad_in, low, aux, slope, du, qkv, other, take, prob, dout,
        total_q, total_k, total_v, ready, sums, mod_low, mod_in,
        load_sem, pair_sem, link_sem, rep_sem, back_sem, store_sem, mod_sem, tall_sem, short_sem, slope_sem,
        in_sem, prob_sem, out_sem, du_sem, swap_sem, move_sem, stay_sem, last_move_sem, last_stay_sem,
    ) = refs[12:]
    me, z = lax.axis_index("seq"), lax.axis_index("rep")
    core, x, y = me & 1, (me >> 1) & 1, (me >> 2) & 1
    inner = (z == 1) | (z == 2)
    outer = (z == 0) | (z == 3)
    features = width
    steps = weights[0][2].shape[2] // CHUNK
    root = HEAD_WIDTH ** (-0.5)


    def wait_out(source, target):
        copy = pltpu.make_async_copy(source, target, out_sem)
        copy.start()
        copy.wait()

    def flat_in(ref):
        return ref if len(ref.shape) == 2 else ref.reshape(tokens, features)

    def load_in(name, at):
        source, target = {
            "grad": (flat_in((g_out, g_in)[at]), grad_in),
            "mlp": (kept[at]["mlp"], aux),
            "branch": (kept[at]["branch"], aux),
            "x": (flat_in(x_ins[at]), aux),
            "x1": (kept[at]["x1"], middle),
            "qkv": (kept[at]["qkv"], qkv),
            "other": (other_in, other),
        }[name]
        order = ("grad", "mlp", "branch", "x", "x1", "qkv", "other")
        return pltpu.make_async_copy(source, target, in_sem.at[order.index(name)])

    def chunk_loads(at, step, slot):
        column = pl.multiple_of(step * CHUNK, CHUNK)
        down = weights[at][3].reshape(*split_rows(weights[at][3].shape))
        return (
            pltpu.make_async_copy(
                weights[at][2].at[:, :, pl.ds(column, CHUNK)],
                tall.at[slot, :, :, pl.ds(0, CHUNK)], tall_sem.at[slot],
            ),
            pltpu.make_async_copy(
                down.at[pl.ds(pl.multiple_of(step * 4, 4), 4)], short.at[slot], short_sem.at[slot]
            ),
            pltpu.make_async_copy(
                kept[at]["slope"].at[:, pl.ds(column, CHUNK)], slope.at[slot], slope_sem.at[slot]
            ),
        )

    def tall_load(source, slot):
        return pltpu.make_async_copy(source, tall.at[slot], tall_sem.at[slot])

    def qkv_block(at, j):
        return weights[at][0].at[:, :, pl.ds(j * features, features)]

    def mlp_begin(at):
        load_in("grad", at).start()
        load_in("mlp", at).start()
        load_in("x1", at).start()
        for slot in range(2):
            for copy in chunk_loads(at, slot, slot):
                copy.start()
        load_in("grad", at).wait()
        load_in("mlp", at).wait()
        gate = mod_ref[at, 5:6]
        sums[at] = jnp.zeros_like(sums[at])

        def begin(strip):
            grad = grad_in[strip].astype(WIDE)
            low[strip] = (gate * grad).astype(LOW)
            clear(acc, strip)
            sums[at, 5:6] += jnp.sum(grad * aux[strip].astype(WIDE), axis=0, keepdims=True)

        strips(tokens, begin)
        load_in("branch", at).start()
        wait_out(low, rights[at]["df"])

    def du_copy(at, step):
        column = pl.multiple_of(step * CHUNK, CHUNK)
        return pltpu.make_async_copy(du, rights[at]["du"].at[:, pl.ds(column, CHUNK)], du_sem)

    def mlp_chunk(at, step):
        slot = lax.rem(step, 2)

        @pl.when(step > 0)
        def _():
            du_copy(at, step).wait()

        for copy in chunk_loads(at, step, slot):
            copy.wait()
        half = tokens // 2
        up = tall[slot, :, :, :CHUNK].reshape(features, CHUNK)
        for j in range(2):
            strip = slice(j * half, (j + 1) * half)
            got = times_turned(low[strip], short[slot].reshape(CHUNK, features))
            got = (got * slope[slot, strip].astype(WIDE)).astype(LOW)
            du[strip] = got
            acc[strip] += times_turned(got, up)

        @pl.when(step + 2 < steps)
        def _():
            for copy in chunk_loads(at, step + 2, slot):
                copy.start()

        du_copy(at, step).start()

    def prob_load(at, group):
        span = tokens // kept[at]["prob"].shape[0]
        return pltpu.make_async_copy(
            kept[at]["prob"].at[group], prob.at[:, pl.ds(0, span)], prob_sem
        )

    def mlp_finish(at):
        tall_load(weights[at][1], 0).start()
        tall_load(qkv_block(at, 0), 1).start()
        load_in("qkv", at).start()
        prob_load(at, 0).start()
        if at == 0:
            load_in("other", at).start()
        du_copy(at, 0).wait()
        load_in("branch", at).wait()
        load_in("x1", at).wait()
        gate, scaled = mod_ref[at, 2:3], 1.0 + mod_ref[at, 4:5]

        def finish(strip):
            grad = acc[strip]
            unit, spread = unit_rows(middle[strip])
            got = grad_in[strip].astype(WIDE) + into_norm(grad, scaled, unit, spread)
            middle[strip] = got
            low[strip] = (gate * got).astype(LOW)
            sums[at, 2:3] += jnp.sum(got * aux[strip].astype(WIDE), axis=0, keepdims=True)
            sums[at, 3:4] += jnp.sum(grad, axis=0, keepdims=True)
            sums[at, 4:5] += jnp.sum(grad * unit, axis=0, keepdims=True)

        strips(tokens, finish)
        load_in("x", at).start()
        wait_out(low, rights[at]["da"])

    def project(at):
        tall_load(weights[at][1], 0).wait()
        half = tokens // 2
        for j in range(2):
            got = times_turned(
                low[j * half : (j + 1) * half], tall[0].reshape(features, features)
            ).astype(LOW)
            dout[4 * j : 4 * j + 4] = got.reshape(4, -1, features)
        tall_load(qkv_block(at, 1), 0).start()
        load_in("qkv", at).wait()
        if at == 0:
            load_in("other", at).wait()

    def rows_of(ref, group, column, lanes, spatial):
        lanes = slice(column, column + lanes)
        if spatial:
            block = ref[pl.ds(2 * group, 2), :, lanes]
            return block.reshape(-1, block.shape[2])
        return jnp.concatenate([ref[2 * block + group, :, lanes] for block in range(4)], 0)

    def swap_copy(j):
        return pltpu.make_async_remote_copy(
            other.at[pl.ds(2 * j, 2)], take.at[pl.ds(2 * j, 2)],
            swap_sem.at[0, j], swap_sem.at[1, j], device_id={"seq": me ^ 1},
        )

    def attend_group(at, group):
        spatial = at == 0
        groups = kept[at]["prob"].shape[0]
        span = tokens // groups
        prob_load(at, group).wait()
        for head in range(HEADS):
            start, lanes, _ = window(head)
            mask = head_mask(head)
            queries = rows_of(qkv, group, start, lanes, spatial) * mask
            keys = rows_of(qkv, group, features + start, lanes, spatial)
            values = rows_of(qkv, group, 2 * features + start, lanes, spatial)
            coming = rows_of(dout, group, start, lanes, spatial) * mask
            if spatial:
                keys = jnp.concatenate([keys, rows_of(other, group, start, lanes, True)], 0)
                values = jnp.concatenate(
                    [values, rows_of(other, group, features + start, lanes, True)], 0
                )
            chance = prob[head, :span]
            known = chance.astype(WIDE)
            dprob = times_turned(coming, values)
            level = jnp.sum(dprob * known, axis=-1, keepdims=True)
            dscores = (known * (dprob - level)).astype(LOW)
            add_window(total_q.at[pl.ds(0, span)], head, times(dscores, keys * mask))
            add_window(total_k, head, turned_times(dscores, queries))
            add_window(total_v, head, turned_times(chance, coming))

        @pl.when(group + 1 < groups)
        def _():
            prob_load(at, group + 1).start()

        pieces = (
            (total_q[:span] * root).astype(LOW),
            (total_k[:span] * root).astype(LOW),
            total_v[:span].astype(LOW),
        )
        for j, piece in enumerate(pieces):
            lanes = slice(j * features, (j + 1) * features)
            if spatial:
                qkv[pl.ds(2 * group, 2), :, lanes] = piece.reshape(2, -1, features)
            else:
                for block in range(4):
                    qkv[2 * block + group, :, lanes] = piece[block * 64 : (block + 1) * 64]
        if spatial:
            other[pl.ds(2 * group, 2), :, :features] = (
                (total_k[span:] * root).astype(LOW).reshape(2, -1, features)
            )
            other[pl.ds(2 * group, 2), :, features:] = (
                total_v[span:].astype(LOW).reshape(2, -1, features)
            )
            swap_copy(group).start()

    def attend_finish(at):
        if at == 0:
            for j in range(4):
                swap_copy(j).wait()
                pair = slice(2 * j, 2 * j + 2)
                lanes = slice(features, 3 * features)
                qkv[pair, :, lanes] = qkv[pair, :, lanes] + take[pair]
        wait_out(qkv, rights[at]["qkv"].reshape(*qkv.shape))

    def qkv_chunks(at, blocks):
        for j in blocks:
            slot = 1 - j % 2
            tall_load(qkv_block(at, j), slot).wait()
            got = times_turned(
                qkv[:, :, j * features : (j + 1) * features].reshape(tokens, features),
                tall[slot].reshape(features, features),
            )
            if j == 0:
                acc[...] = got
                tall_load(qkv_block(at, 2), slot).start()
            else:
                acc[...] = acc[...] + got

    def last_moves():
        return moves(y_in, moved, last_move_sem, last_stay_sem, me, False)

    def grad_moves():
        return moves(ready, g_out, move_sem, stay_sem, me, False)

    def qkv_finish(at):
        load_in("x", at).wait()
        scaled = 1.0 + mod_ref[at, 1:2]

        def finish(strip):
            grad = acc[strip]
            unit, spread = unit_rows(aux[strip].astype(WIDE))
            sums[at, 0:1] += jnp.sum(grad, axis=0, keepdims=True)
            sums[at, 1:2] += jnp.sum(grad * unit, axis=0, keepdims=True)
            acc[strip] = middle[strip] + into_norm(grad, scaled, unit, spread)

        strips(tokens, finish)
        if at == 0:
            wait_out(acc, input_grad)
        else:
            ready[...] = acc[...].astype(LOW).reshape(ready.shape)
            for copy in grad_moves():
                copy.start()

    def backward_step(t):
        def at_turn(turn):
            return pl.when(t == turn)

        @pl.when(t < steps - 1)
        def _():
            mlp_chunk(1, t + 1)

        @at_turn(4)
        def _():
            mlp_finish(1)
            project(1)

        @pl.when((t >= 5) & (t < 7))
        def _():
            attend_group(1, t - 5)

        @at_turn(7)
        def _():
            attend_finish(1)
            qkv_chunks(1, (0, 1))

        @at_turn(8)
        def _():
            qkv_chunks(1, (2,))
            qkv_finish(1)

        @at_turn(10)
        def _():
            for copy in grad_moves():
                copy.wait()
            mlp_begin(0)

        @pl.when((t >= 10) & (t < 10 + steps))
        def _():
            mlp_chunk(0, t - 10)

        @at_turn(15)
        def _():
            mlp_finish(0)
            project(0)

        @pl.when((t >= 16) & (t < 20))
        def _():
            attend_group(0, t - 16)

        @at_turn(19)
        def _():
            attend_finish(0)

        @at_turn(20)
        def _():
            qkv_chunks(0, (0, 1))

        @at_turn(21)
        def _():
            qkv_chunks(0, (2,))
            qkv_finish(0)
            mod_low[...] = jnp.zeros_like(mod_low)
            for at in range(2):
                mod_low[8 * at : 8 * at + 8] = sums[at].astype(LOW)
            mod_in[me] = mod_low[...]
            for copy in mod_copies():
                copy.start()

        @at_turn(23)
        def _():
            for copy in mod_copies():
                copy.wait()
            summed = mod_in[0].astype(WIDE)
            for device in range(1, 8):
                summed += mod_in[device].astype(WIDE)
            every_mod[z] = summed.astype(LOW)
            for copy in clip_copies():
                copy.start()

        @at_turn(25)
        def _():
            for copy in last_moves():
                copy.start()

        @at_turn(total + 5)
        def _():
            for copy in clip_copies():
                copy.wait()
            for copy in last_moves():
                copy.wait()

    def mod_copies():
        return [
            pltpu.make_async_remote_copy(
                mod_low, mod_in.at[me], mod_sem.at[0, mask], mod_sem.at[1, mask],
                device_id={"seq": me ^ mask},
            )
            for mask in range(1, 8)
        ]

    def clip_copies():
        return [
            pltpu.make_async_remote_copy(
                every_mod.at[z], every_mod.at[z], mod_sem.at[0, 7 + mask], mod_sem.at[1, 7 + mask],
                device_id={"rep": z ^ mask},
            )
            for mask in range(1, 4)
        ]


    names = ("h", "o", "h2", "z")

    def loads(block, slot):
        for layer, kind, first, count in spans:
            @pl.when((block >= first) & (block < first + count))
            def _():
                source = kept[layer][names[kind]]
                if kind == 3:
                    source = source.at[:, :, block - first]
                pltpu.make_async_copy(source, left.at[slot], load_sem.at[0, slot]).start()
                source = rights[layer][RIGHTS[kind]]
                if kind in (0, 2):
                    column = pl.multiple_of((block - first) * width, width)
                    source = source.at[:, pl.ds(column, width)]
                pltpu.make_async_copy(source, right.at[slot], load_sem.at[1, slot]).start()

    def wait_loads(slot):
        pltpu.make_async_copy(kept[0]["h"], left.at[slot], load_sem.at[0, slot]).wait()
        pltpu.make_async_copy(rights[0]["da"], right.at[slot], load_sem.at[1, slot]).wait()

    def store(block):
        for layer, kind, first, count in spans:
            @pl.when((block >= first) & (block < first + count))
            def _():
                target = grads[layer][kind]
                if kind == 3:
                    row = pl.multiple_of((block - first) * rows, rows)
                    target = target.at[pl.ds(row, rows)]
                elif kind in (0, 2):
                    column = pl.multiple_of((block - first) * width, width)
                    target = target.at[:, pl.ds(column, width)]
                pltpu.make_async_copy(wide, target, store_sem).start()

    def to_seq(source, target, which, slot, mask):
        return pltpu.make_async_remote_copy(
            source, target, link_sem.at[0, which, slot], link_sem.at[1, which, slot],
            device_id={"seq": me ^ mask},
        )

    def pair_copy(t):
        slot = lax.rem(t, 2)
        return pltpu.make_async_remote_copy(
            away, pair_in.at[slot], pair_sem.at[0, slot], pair_sem.at[1, slot],
            device_id={"seq": me ^ 1},
        )

    def first_copies(t):
        slot, block = lax.rem(t, BACK), lax.rem(t - 1, SLOTS)
        return (
            to_seq(part.at[block, :, 1 - x, :, pl.ds(0, edge)], first_in_a.at[slot], 0, slot, 2),
            to_seq(
                part.at[block, 1 - y, :, :, pl.ds(edge, width - edge)],
                first_in_b.at[slot], 1, slot, 4,
            ),
        )

    def second_copies(t):
        slot, block = lax.rem(t, SLOTS), lax.rem(t, 2)
        return (
            to_seq(mid_a.at[block, 1 - y], second_in_a.at[slot], 2, slot, 4),
            to_seq(mid_b.at[block, 1 - x], second_in_b.at[slot], 3, slot, 2),
        )

    def rep_copy(t):
        slot = lax.rem(t, SLOTS)
        return pltpu.make_async_remote_copy(
            clip.at[lax.rem(t, 2)], rep_in.at[slot], rep_sem.at[0, 0, slot], rep_sem.at[1, 0, slot],
            device_id={"rep": z ^ 1},
        )

    def inner_copy(t):
        slot = lax.rem(t, SLOTS)
        return pltpu.make_async_remote_copy(
            joined.at[lax.rem(t, 2)], inner_in.at[slot],
            rep_sem.at[0, 1, slot], rep_sem.at[1, 1, slot],
            device_id={"rep": z ^ 3},
        )

    def back_copy(t):
        slot = lax.rem(t, BACK)
        return pltpu.make_async_remote_copy(
            final.at[lax.rem(t, 2)], back_in.at[slot], back_sem.at[0, slot], back_sem.at[1, slot],
            device_id={"rep": z ^ 1},
        )

    def turn(t, carry):
        def stage(back):
            return (t >= back) & (t < total + back)

        now2, was2 = lax.rem(t, 2), lax.rem(t + 1, 2)
        was3 = lax.rem(t + 2, SLOTS)
        was4 = lax.rem(t + 3, BACK)

        @pl.when(t + 1 < total)
        def _():
            loads(t + 1, was2)

        @pl.when(stage(2))
        def _():
            block = lax.rem(t + 1, SLOTS)
            for at in range(2):
                mid_a[now2, at] = part[block, at, x, :, :edge] + first_in_a[was4, at]
                mid_b[now2, at] = part[block, y, at, :, edge:] + first_in_b[was4, at]
            for copy in second_copies(t):
                copy.start()

        @pl.when(stage(3))
        def _():
            clip[now2, :, :edge] = mid_a[was2, y] + second_in_a[was3]
            clip[now2, :, edge:] = mid_b[was2, x] + second_in_b[was3]

            @pl.when(outer)
            def _():
                rep_copy(t).start()

        @pl.when(stage(4) & inner)
        def _():
            joined[now2] = clip[was2] + rep_in[was3]
            inner_copy(t).start()

        @pl.when(stage(5) & inner)
        def _():
            final[now2] = joined[was2] + inner_in[was3]
            back_copy(t).start()

        @pl.when(stage(6))
        def _():
            @pl.when(inner)
            def _():
                wide[...] = final[was2]

            @pl.when(outer)
            def _():
                wide[...] = back_in[lax.rem(t + 3, BACK)]

            store(t - 6)

        @pl.when(t < total)
        def _():
            wait_loads(now2)
            slot3 = lax.rem(t, SLOTS)
            parts = (slice(0, 512), slice(512, width))

            def product(which, at):
                block = left[now2, :, which]
                four, _, depth = block.shape
                got = times(block.reshape(four * rows, depth), right[now2, :, at]).astype(LOW)
                return got.reshape(four, rows, -1)

            for at in parts:
                away[:, :, at] = product(1 - core, at)
            pair_copy(t).start()
            for at in parts:
                got = product(core, at)
                part[slot3, 0, :, :, at] = got[:2]
                part[slot3, 1, :, :, at] = got[2:]

        backward_step(t)

        @pl.when(t < total)
        def _():
            pair_copy(t).wait()
            slot3 = lax.rem(t, SLOTS)

            def add(j, carry):
                part[slot3, j // 2, j % 2] = part[slot3, j // 2, j % 2] + pair_in[now2, j]
                return carry

            lax.fori_loop(0, 4, add, 0)
            for copy in first_copies(t + 1):
                copy.start()

        @pl.when(stage(1))
        def _():
            for copy in first_copies(t):
                copy.wait()

        @pl.when(stage(2))
        def _():
            for copy in second_copies(t):
                copy.wait()

        @pl.when(stage(3))
        def _():
            @pl.when(outer)
            def _():
                rep_copy(t).wait_send()

            @pl.when(inner)
            def _():
                rep_copy(t).wait_recv()

        @pl.when(stage(4) & inner)
        def _():
            inner_copy(t).wait()

        @pl.when(stage(5))
        def _():
            @pl.when(inner)
            def _():
                back_copy(t).wait_send()

            @pl.when(outer)
            def _():
                back_copy(t).wait_recv()

        @pl.when(stage(6))
        def _():
            pltpu.make_async_copy(wide, grads[0][1], store_sem).wait()

        return carry

    enter(range(1, 8), range(1, 4))
    mlp_begin(1)
    mlp_chunk(1, jnp.int32(0))
    loads(0, 0)
    lax.fori_loop(0, total + 6, turn, 0)


def backward(weights, kept, g, other, y, xs, mods, cid):
    struct = jax.ShapeDtypeStruct
    tokens, features = xs[0].shape
    rows = features // 8
    wide = weights[0][2].shape[2]
    edge = features * 5 // 9 // 128 * 128
    frames, places = g.shape[1], 8 * g.shape[2]
    out_shapes = [(rows, 3 * features), (rows, features), (rows, wide), (wide // 8, features)]
    spans, total = [], 0
    for layer in (1, 0):
        for kind in ORDER:
            count = out_shapes[kind][0] * out_shapes[kind][1] // (rows * features)
            spans.append((layer, kind, total, count))
            total += count
    dims = (rows, features, edge, tokens, total, spans)
    any_ = pl.BlockSpec(memory_space=pl.ANY)
    outs = [struct(shape, LOW) for shape in out_shapes] * 2
    outs += [
        struct((tokens, 3 * features), LOW), struct((tokens, features), LOW),
        struct((tokens, wide), LOW), struct((tokens, features), LOW),
    ] * 2
    outs += [
        struct((4, 16, features), LOW),
        struct((frames, places, features), LOW),
        struct((tokens, features), WIDE),
        struct((frames, places, features), LOW),
    ]
    vm, dma = pltpu.VMEM, pltpu.SemaphoreType.DMA
    rest = features - edge
    scratch = [
        vm((2, 4, 2, rows, tokens), LOW),
        vm((2, tokens, features), LOW),
        vm((4, rows, features), LOW),
        vm((2, 4, rows, features), LOW),
        vm((SLOTS, 2, 2, rows, features), LOW),
        vm((BACK, 2, rows, edge), LOW),
        vm((BACK, 2, rows, rest), LOW),
        vm((2, 2, rows, edge), LOW),
        vm((2, 2, rows, rest), LOW),
        vm((SLOTS, rows, edge), LOW),
        vm((SLOTS, rows, rest), LOW),
        vm((2, rows, features), LOW),
        vm((SLOTS, rows, features), LOW),
        vm((2, rows, features), LOW),
        vm((SLOTS, rows, features), LOW),
        vm((2, rows, features), LOW),
        vm((BACK, rows, features), LOW),
        vm((rows, features), LOW),
        vm((2, 8, rows, features), LOW),
        vm((2, 4, CHUNK // 4, features), LOW),
        vm((tokens, features), WIDE),
        vm((tokens, features), WIDE),
        vm((tokens, features), LOW),
        vm((tokens, features), LOW),
        vm((tokens, features), LOW),
        vm((2, tokens, CHUNK), LOW),
        vm((tokens, CHUNK), LOW),
        vm((8, tokens // 8, 3 * features), LOW),
        vm((8, tokens // 8, 2 * features), LOW),
        vm((8, tokens // 8, 2 * features), LOW),
        vm((HEADS, KEYS, KEYS), LOW),
        vm((8, tokens // 8, features), LOW),
        vm((KEYS, features), WIDE),
        vm((KEYS, features), WIDE),
        vm((KEYS, features), WIDE),
        vm((8, frames, places // 8, features), LOW),
        vm((2, 8, features), WIDE),
        vm((16, features), LOW),
        vm((8, 16, features), LOW),
        dma((2, 2)),
        dma((2, 2)),
        dma((2, 4, BACK)),
        dma((2, 2, SLOTS)),
        dma((2, BACK)),
        dma(()),
        dma((2, 11)),
        dma((2,)),
        dma((2,)),
        dma((2,)),
        dma((7,)),
        dma(()),
        dma(()),
        dma(()),
        dma((2, 4)),
        *move_scratch(),
        *move_scratch(),
    ]
    flops = 4 * tokens * 8 * sum(a * b for a, b in out_shapes) * 2
    got = pl.pallas_call(
        functools.partial(backward_kernel, dims),
        out_shape=outs,
        in_specs=[any_] * (8 + 20 + 5) + [pl.BlockSpec(memory_space=vm)],
        out_specs=[any_] * 16 + [pl.BlockSpec(memory_space=vm)] + [any_] * 3,
        scratch_shapes=scratch,
        compiler_params=params(63, cid),
        cost_estimate=cost(flops, flops // tokens),
        name="backward",
    )(
        *weights[0], *weights[1], *[each[name] for each in kept for name in KEPT],
        g, other, y, *xs, mods,
    )
    grads = [grad.astype(WIDE) for grad in got[:8]]
    return grads[:4], grads[4:], got[16], got[17], got[18]


def by_device(left, features):
    tall, tokens = left.shape[0] // features, left.shape[1]
    rows = features // 8
    return left.reshape((4, 2, rows, tokens) if tall == 1 else (4, 2, tall, rows, tokens))


def fused_device(frames_in, conditioning, shards, partial_mod, cotangent):
    _, _, frames, places, features = frames_in.shape
    tokens = frames * places
    low_cotangent = cotangent.reshape(frames, places, features).astype(LOW)
    x_one = frames_in.reshape(tokens, features)
    weights, (mods, conditions, g_two, other, x_two, y_two), kept = forward(
        shards, partial_mod.reshape(-1, LANES), conditioning.reshape(-1, LANES), low_cotangent,
        x_one, 0,
    )
    for each in kept:
        for name in ("h", "o", "h2", "z"):
            each[name] = by_device(each[name], features)
    grads_one, grads_two, every_mod, block_out, input_grad = backward(
        (weights[:4], weights[4:]), kept, g_two, other, y_two.reshape(g_two.shape),
        (x_one, x_two.reshape(tokens, features)), mods, 1,
    )
    every_mod = every_mod.reshape(-1, 2, 8, features)[:, :, :6].reshape(-1, 12 * features)
    return (
        block_out.astype(WIDE), input_grad, grads_one, grads_two, every_mod,
        conditions.reshape(-1, features),
    )


def outer_sum(left, right):
    total = 0.0
    for row in range(left.shape[0]):
        total = total + left[row, :, None].astype(jnp.float32) * right[row].astype(jnp.float32)
    return total


def per_device(
    frames_in,
    conditioning,
    mod_first,
    qkv_first,
    out_first,
    up_first,
    down_first,
    mod_second,
    qkv_second,
    out_second,
    up_second,
    down_second,
    cotangent,
):
    clip_count, _, frame_dev, half_places, features = frames_in.shape
    fused = lax.axis_size("seq") == 8 and lax.axis_size("rep") == 4 and clip_count == 1
    row_count = mod_first.shape[0]
    row_start = lax.axis_index("seq") * row_count
    mod_width = mod_first.shape[1]
    rows_of = lambda whole: lax.dynamic_slice_in_dim(whole, row_start, row_count, 1)
    silu_local = rows_of(jax.nn.silu(conditioning)).astype(jnp.bfloat16)
    partial_mod = jnp.concatenate(
        [
            jnp.dot(silu_local, mod_first, preferred_element_type=jnp.float32),
            jnp.dot(silu_local, mod_second, preferred_element_type=jnp.float32),
        ],
        1,
    )
    shards = (
        qkv_first, out_first, up_first, down_first,
        qkv_second, out_second, up_second, down_second,
    )
    if fused:
        block_out, stream_grad, grads_one, grads_two, every_mod, conditions = fused_device(
            frames_in, conditioning, shards, partial_mod, cotangent
        )
        every_silu = rows_of(jax.nn.silu(conditions)).astype(jnp.bfloat16)
        mod_total = lax.dynamic_slice_in_dim(every_mod, lax.axis_index("rep"), 1, 0)
    else:
        weights = [lax.all_gather(shard, "seq", axis=0, tiled=True) for shard in shards]
        modulation = lax.psum(partial_mod, "seq")
        every_silu = lax.all_gather(silu_local, "rep", axis=0, tiled=True)
        mod_one, mod_two = modulation[:, :mod_width], modulation[:, mod_width:]
        weights_one, weights_two = weights[:4], weights[4:]
        start_stream = frames_in.reshape(clip_count, frame_dev, half_places, features).astype(
            jnp.float32
        )
        spatial_out, state_one = forward_layer(start_stream, mod_one, weights_one, True)
        placed = to_places(spatial_out)
        temporal_out, state_two = forward_layer(placed, mod_two, weights_two, False)
        block_out = to_frames(temporal_out, frame_dev)
        cotangent_sites = to_places(
            cotangent.reshape(clip_count, frame_dev, half_places, features)
        )
        placed_grad, mod_grad_two, pairs_two = backward_layer(
            cotangent_sites, placed, mod_two, weights_two, state_two, False
        )
        spatial_grad = to_frames(placed_grad, frame_dev)
        stream_grad, mod_grad_one, pairs_one = backward_layer(
            spatial_grad, start_stream, mod_one, weights_one, state_one, True
        )
        mod_grads = jnp.concatenate([mod_grad_one, mod_grad_two], 1).astype(jnp.bfloat16)
        grads_two, grads_one = layer_grads(pairs_two), layer_grads(pairs_one)
        mod_total = lax.psum(mod_grads, "seq").astype(jnp.bfloat16)
        every_mod = lax.all_gather(mod_total, "rep", axis=0, tiled=True)
    low_one, low_two = mod_total[:, :mod_width], mod_total[:, mod_width:]
    mod_weight_one = outer_sum(every_silu, every_mod[:, :mod_width])
    mod_weight_two = outer_sum(every_silu, every_mod[:, mod_width:])
    silu_grad = jnp.einsum("ce,de->cd", low_one, mod_first, preferred_element_type=jnp.float32)
    silu_grad = silu_grad + jnp.einsum(
        "ce,de->cd", low_two, mod_second, preferred_element_type=jnp.float32
    )
    condition_grad = jax.vjp(jax.nn.silu, rows_of(conditioning))[1](silu_grad)[0]
    out_shape = (clip_count, 1, frame_dev, half_places, features)
    return (
        block_out.reshape(out_shape),
        stream_grad.reshape(out_shape),
        condition_grad,
        mod_weight_one,
        *grads_one,
        mod_weight_two,
        *grads_two,
    )


def solution(mesh):
    return jax.shard_map(
        per_device,
        mesh=mesh,
        in_specs=(
            P("rep", "seq", None, None, None),
            P("rep", None),
            P("seq", None),
            P("seq", None),
            P("seq", None),
            P("seq", None),
            P("seq", None),
            P("seq", None),
            P("seq", None),
            P("seq", None),
            P("seq", None),
            P("seq", None),
            P("rep", "seq", None, None, None),
        ),
        out_specs=(
            P("rep", "seq", None, None, None),
            P("rep", "seq", None, None, None),
            P("rep", "seq"),
            P("seq", None),
            P("seq", None),
            P("seq", None),
            P("seq", None),
            P("seq", None),
            P("seq", None),
            P("seq", None),
            P("seq", None),
            P("seq", None),
            P("seq", None),
        ),
        check_vma=False,
    )
```
